32 devices in a mesh: ctx: 8 (over z, y), tp: 4 (over x, core).
Axes of the slice: x: 2, y: 2, z: 4, core: 2. Of those that a mesh axis runs over, the one named last changes fastest.
Arguments:
- stream_in: float32 [3072, 2048], P('ctx'), may hold values from -6 to 6
- cotangent: float32 [3072, 2048], P('ctx'), may hold values from -6 to 6
- ln_gain: float32 [2, 2048], replicated, may hold values from 0.5 to 1.5
- ln_bias: float32 [2, 2048], replicated, may hold values from -3 to 3
- w_qkv: bfloat16 [2048, 6144], P(None, 'tp'), may hold values from -0.46403883 to 0.46403883
- b_qkv: float32 [6144], P('tp'), may hold values from -1 to 1
- w_out: bfloat16 [2048, 2048], P('tp'), may hold values from -0.5 to 0.5
- out_bias: float32 [2048], replicated, may hold values from -3 to 3
- w_up: bfloat16 [2048, 8192], P(None, 'tp'), may hold values from -0.125 to 0.125
- b_up: float32 [8192], P('tp'), may hold values from -3 to 3
- w_down: bfloat16 [8192, 2048], P('tp'), may hold values from -0.0625 to 0.0625
- block_order: int32 [16], replicated, may hold values from 0 to 15, as said below
Outputs:
- stream_out: float32 [3072, 2048], P('ctx')
- grad_in: float32 [3072, 2048], P('ctx')
- grad_w_qkv: float32 [2048, 6144], P('ctx', 'tp')
- grad_b_qkv: float32 [6144], P('tp')
- grad_w_out: float32 [2048, 2048], P('tp', 'ctx')
- grad_out_bias: float32 [2048], replicated
- grad_w_up: float32 [2048, 8192], P('ctx', 'tp')
- grad_b_up: float32 [8192], P('tp')
- grad_w_down: float32 [8192, 2048], P('tp', 'ctx')
- grad_ln_gain: float32 [2, 2048], replicated
- grad_ln_bias: float32 [2, 2048], replicated
The draws below stay inside these ranges and needn't reach their ends.
Inputs may be any that keep to these rules, and one draw needn't show every extreme that they name: `block_order`: entries 2 d and 2 d + 1 are b and 15 - b for some b; each value appears once.
All inputs are finite; a program needn't handle non-finite values.
Results may differ from the reference program's by a relative error of at most 0.04.
Values may be sent and summed in bfloat16 or wider, within the bound.
A program may use at most 384 MiB of HBM per device.

```python
import math
import jax
import jax.numpy as jnp
from jax import lax

D = 2048
H = 8
HD = 256
ROT = 64
FF = 8192
BLK = 192
SEQ = 3072
N_CTX = 8


def draw_block_order(key, part):
    perm_order = jax.random.permutation(key, N_CTX).astype(jnp.int32)
    mirror = (2 * N_CTX - 1 - perm_order).astype(jnp.int32)
    return jnp.stack([perm_order, mirror], axis=1).reshape(2 * N_CTX)


def draw_w_qkv(key, part):
    drawn = jnp.clip(jax.random.normal(key, (D, 3 * D), jnp.float32), -6.0, 6.0) * D ** (-0.5)
    return drawn.astype(jnp.bfloat16)


def steps_of(stream_key, shape, cuts, smallest, high):
    level, own = 1.0, jax.random.fold_in(stream_key, 6)
    for axis_at, parts in cuts:
        draws = jnp.exp(jax.random.uniform(jax.random.fold_in(own, axis_at), (parts,), jnp.float32, smallest / len(cuts), high / len(cuts)))
        level = level * jnp.repeat(draws, shape[axis_at] // parts).reshape([-1 if axis == axis_at else 1 for axis in range(len(shape))])
    return level


def gaussian(own_key, shape, scale, bound, pieces=(), held_as=jnp.bfloat16):
    values = jax.random.normal(own_key, shape, jnp.float32) * scale
    if len(pieces) > 0:
        values = steps_of(own_key, shape, pieces, -0.22, 0.18) * values
    return jnp.clip(values, min=-bound, max=bound).astype(held_as)


def setup_inputs(seed: int = 0) -> dict:
    arg_keys = jax.random.split(jax.random.key(seed), 13)
    return {
        "stream_in": gaussian(arg_keys[0], (SEQ, D), 1.0, 6.0, ((0, 8),), jnp.float32),
        "cotangent": gaussian(arg_keys[1], (SEQ, D), 1.0, 6.0, ((0, 8),), jnp.float32),
        "ln_gain": jnp.clip(1.0 + 0.1 * jax.random.normal(arg_keys[2], (2, D), jnp.float32), 0.5, 1.5),
        "ln_bias": gaussian(arg_keys[3], (2, D), 0.5, 3.0, (), jnp.float32),
        "w_qkv": draw_w_qkv(jax.random.fold_in(arg_keys[12], 71), 0),
        "b_qkv": gaussian(arg_keys[5], (3 * D,), 0.2, 1.0, ((0, 4),), jnp.float32),
        "w_out": gaussian(arg_keys[6], (D, D), (D // 16) ** -0.5, 0.5, ((0, 4),)),
        "out_bias": gaussian(arg_keys[7], (D,), 0.5, 3.0, (), jnp.float32),
        "w_up": gaussian(arg_keys[8], (D, FF), D ** -0.5, 0.125, ((1, 4),)),
        "b_up": gaussian(arg_keys[9], (FF,), 0.5, 3.0, ((0, 4),), jnp.float32),
        "w_down": gaussian(arg_keys[10], (FF, D), FF ** -0.5, 0.0625, ((0, 4),)),
        "block_order": draw_block_order(jax.random.fold_in(arg_keys[12], 71), 0),
    }


masked_value = -1e+30
norm_epsilon = 1e-05
root_half = 0.7071067811865476
inverse_root_two_pi = 0.3989422804014327

def rounded(tensor):
    return lax.optimization_barrier(tensor.astype(jnp.bfloat16)).astype(jnp.float32)

def rope_tables(positions, rotary_dims):
    half_rot = rotary_dims // 2
    frequency = jnp.exp(jnp.arange(half_rot, dtype=jnp.float32) * (-2.0 * math.log(10000.0) / rotary_dims))
    angles = positions.astype(jnp.float32)[:, None] * frequency[None, :]
    angles = jnp.concatenate([angles, angles], axis=1)
    return (jnp.cos(angles), jnp.sin(angles))

def rotate(tensor, cosine, sine_table, rotary_dims):
    half_rot = rotary_dims // 2
    rotary_part = tensor[..., :rotary_dims]
    turned = jnp.concatenate([-rotary_part[..., half_rot:], rotary_part[..., :half_rot]], axis=-1)
    moved = rotary_part * cosine[:, None, :] + turned * sine_table[:, None, :]
    return jnp.concatenate([moved, tensor[..., rotary_dims:]], axis=-1)

def unrotate(incoming, cosine, sine_table, rotary_dims):
    half_rot = rotary_dims // 2
    rotary_part = incoming[..., :rotary_dims]
    scaled = rotary_part * sine_table[:, None, :]
    swapped = jnp.concatenate([scaled[..., half_rot:], -scaled[..., :half_rot]], axis=-1)
    moved = rotary_part * cosine[:, None, :] + swapped
    return jnp.concatenate([moved, incoming[..., rotary_dims:]], axis=-1)

def normalize(tensor, gain_row, shift_row):
    row_mean = lax.optimization_barrier(jnp.mean(tensor, axis=-1, keepdims=True))
    centred = tensor - row_mean
    variance = lax.optimization_barrier(jnp.mean(centred * centred, axis=-1, keepdims=True))
    inv_scale = lax.rsqrt(variance + norm_epsilon)
    unit_field = centred * inv_scale
    return (unit_field * gain_row + shift_row, unit_field, inv_scale)

def normalize_back(incoming, unit_field, inv_scale, gain_row):
    unit_grad = incoming * gain_row
    return inv_scale * (unit_grad - lax.optimization_barrier(jnp.mean(unit_grad, axis=-1, keepdims=True)) - unit_field * lax.optimization_barrier(jnp.mean(unit_grad * unit_field, axis=-1, keepdims=True)))

def gelu_exact(argument):
    return 0.5 * argument * (1.0 + jax.scipy.special.erf(argument * root_half))

def gelu_slope(argument):
    return 0.5 * (1.0 + jax.scipy.special.erf(argument * root_half)) + argument * jnp.exp(-0.5 * argument * argument) * inverse_root_two_pi

def reference(stream_in, cotangent, ln_gain, ln_bias, w_qkv, b_qkv, w_out, out_bias, w_up, b_up, w_down, block_order):
    row_index = jnp.arange(SEQ, dtype=jnp.int32)
    positions = (block_order[row_index // BLK] * BLK + row_index % BLK).astype(jnp.int32)
    cosine, sine_table = rope_tables(positions, ROT)
    score_scale = HD ** (-0.5)
    normed_a, unit_a, scale_a = normalize(stream_in, ln_gain[0], ln_bias[0])
    normed_m, unit_m, scale_m = normalize(stream_in, ln_gain[1], ln_bias[1])
    attn_in = normed_a.astype(jnp.bfloat16)
    mlp_in = normed_m.astype(jnp.bfloat16)
    joined = (jnp.dot(attn_in, w_qkv, preferred_element_type=jnp.float32) + b_qkv).reshape(SEQ, H, 3, HD)
    query_f = rounded(rotate(joined[:, :, 0], cosine, sine_table, ROT))
    key_f = rounded(rotate(joined[:, :, 1], cosine, sine_table, ROT))
    value_f = rounded(joined[:, :, 2])
    query_block = min(512, SEQ)
    block_count = SEQ // query_block

    def attend(inputs):
        queries, query_pos = inputs
        scores = jnp.einsum('qhd,khd->hqk', queries, key_f) * score_scale
        allowed = (positions[None, :] <= query_pos[:, None])[None]
        row_max = lax.optimization_barrier(jnp.max(jnp.where(allowed, scores, masked_value), axis=2))
        row_sum = lax.optimization_barrier(jnp.sum(jnp.exp(jnp.where(allowed, scores - row_max[:, :, None], masked_value)), axis=2))
        log_total = row_max + jnp.log(row_sum)
        probability = jnp.exp(jnp.where(allowed, scores - log_total[:, :, None], masked_value))
        attended = jnp.einsum('hqk,khd->qhd', rounded(probability), value_f)
        return (attended, log_total)
    attended, log_blocks = lax.map(attend, (query_f.reshape(block_count, query_block, H, HD), positions.reshape(block_count, query_block)))
    attn_out = attended.reshape(SEQ, D).astype(jnp.bfloat16)
    hidden = jnp.dot(mlp_in, w_up, preferred_element_type=jnp.float32) + b_up
    gelu_out = gelu_exact(hidden).astype(jnp.bfloat16)
    stream_out = stream_in + out_bias + (jnp.dot(attn_out, w_out, preferred_element_type=jnp.float32) + jnp.dot(gelu_out, w_down, preferred_element_type=jnp.float32))
    cot_b = cotangent.astype(jnp.bfloat16)
    grad_w_down = jnp.dot(gelu_out.T, cot_b, preferred_element_type=jnp.float32)
    grad_w_out = jnp.dot(attn_out.T, cot_b, preferred_element_type=jnp.float32)
    hidden_grad = jnp.dot(cot_b, w_down.T, preferred_element_type=jnp.float32) * gelu_slope(hidden)
    grad_b_up = lax.optimization_barrier(jnp.sum(hidden_grad, axis=0))
    hidden_b = hidden_grad.astype(jnp.bfloat16)
    grad_w_up = jnp.dot(mlp_in.T, hidden_b, preferred_element_type=jnp.float32)
    mlp_back = jnp.dot(hidden_b, w_up.T, preferred_element_type=jnp.float32)
    out_grad = jnp.dot(cot_b, w_out.T, preferred_element_type=jnp.float32).astype(jnp.bfloat16)
    out_grad_f = out_grad.astype(jnp.float32).reshape(SEQ, H, HD)
    row_dot = lax.optimization_barrier(jnp.sum(out_grad_f * attn_out.astype(jnp.float32).reshape(SEQ, H, HD), axis=2))
    row_dot_blocks = row_dot.reshape(block_count, query_block, H).transpose(0, 2, 1)

    def back_block(running, inputs):
        key_acc, value_acc = running
        queries, grads_here, query_pos, log_total, dots_here = inputs
        scores = jnp.einsum('qhd,khd->hqk', queries, key_f) * score_scale
        allowed = (positions[None, :] <= query_pos[:, None])[None]
        probability = jnp.exp(jnp.where(allowed, scores - log_total[:, :, None], masked_value))
        prob_grad = jnp.einsum('qhd,khd->hqk', grads_here, value_f)
        score_grad = rounded(probability * (prob_grad - dots_here[:, :, None]) * score_scale)
        query_grad = jnp.einsum('hqk,khd->qhd', score_grad, key_f)
        key_acc = key_acc + jnp.einsum('hqk,qhd->khd', score_grad, queries)
        value_acc = value_acc + jnp.einsum('hqk,qhd->khd', rounded(probability), grads_here)
        return ((key_acc, value_acc), query_grad)
    zero_keys = jnp.zeros((SEQ, H, HD), jnp.float32)
    (key_grad, value_grad), query_grads = lax.scan(back_block, (zero_keys, zero_keys), (query_f.reshape(block_count, query_block, H, HD), out_grad_f.reshape(block_count, query_block, H, HD), positions.reshape(block_count, query_block), log_blocks, row_dot_blocks))
    query_grad = query_grads.reshape(SEQ, H, HD)
    joined_grad = jnp.stack([unrotate(query_grad, cosine, sine_table, ROT), unrotate(key_grad, cosine, sine_table, ROT), value_grad], axis=2).reshape(SEQ, 3 * D)
    grad_b_qkv = lax.optimization_barrier(jnp.sum(joined_grad, axis=0))
    joined_b = joined_grad.astype(jnp.bfloat16)
    grad_w_qkv = jnp.dot(attn_in.T, joined_b, preferred_element_type=jnp.float32)
    attn_back = jnp.dot(joined_b, w_qkv.T, preferred_element_type=jnp.float32)
    grad_in = cotangent + normalize_back(attn_back, unit_a, scale_a, ln_gain[0]) + normalize_back(mlp_back, unit_m, scale_m, ln_gain[1])
    grad_ln_gain = jnp.stack([lax.optimization_barrier(jnp.sum(attn_back * unit_a, axis=0)), lax.optimization_barrier(jnp.sum(mlp_back * unit_m, axis=0))])
    grad_ln_bias = jnp.stack([lax.optimization_barrier(jnp.sum(attn_back, axis=0)), lax.optimization_barrier(jnp.sum(mlp_back, axis=0))])
    grad_out_bias = lax.optimization_barrier(jnp.sum(cotangent, axis=0))
    return (stream_out, grad_in, grad_w_qkv, grad_b_qkv, grad_w_out, grad_out_bias, grad_w_up, grad_b_up, grad_w_down, grad_ln_gain, grad_ln_bias)
```

```python
import functools
import math

import jax
import jax.numpy as jnp
from jax import lax
from jax.experimental import pallas as pl
from jax.experimental.pallas import tpu as pltpu
from jax.sharding import PartitionSpec as P

HD = 256
ROT = 64

masked_value = -1e30
norm_epsilon = 1e-05
root_half = 0.7071067811865476
inverse_root_two_pi = 0.3989422804014327

F32 = jnp.float32
BF16 = jnp.bfloat16


def rope_tables(block_numbers, block_rows, rotary_dims):
    positions = (
        block_numbers[:, None] * block_rows + jnp.arange(block_rows, dtype=jnp.int32)[None, :]
    ).reshape(-1)
    half_rot = rotary_dims // 2
    frequency = jnp.exp(
        jnp.arange(half_rot, dtype=F32) * (-2.0 * math.log(10000.0) / rotary_dims)
    )
    angles = positions.astype(F32)[:, None] * frequency[None, :]
    angles = jnp.concatenate([angles, angles], axis=1)
    return (jnp.cos(angles), jnp.sin(angles))


def rotate(tensor, cosine, sine_table):
    half_rot = ROT // 2
    rotary_part = tensor[:, :ROT]
    turned = jnp.concatenate([-rotary_part[:, half_rot:], rotary_part[:, :half_rot]], axis=-1)
    moved = rotary_part * cosine + turned * sine_table
    return jnp.concatenate([moved, tensor[:, ROT:]], axis=-1)


def unrotate(incoming, cosine, sine_table):
    half_rot = ROT // 2
    rotary_part = incoming[:, :ROT]
    scaled = rotary_part * sine_table
    swapped = jnp.concatenate([scaled[:, half_rot:], -scaled[:, :half_rot]], axis=-1)
    moved = rotary_part * cosine + swapped
    return jnp.concatenate([moved, incoming[:, ROT:]], axis=-1)


def normalize_back(incoming, unit_field, inv_scale, gain_row):
    unit_grad = incoming * gain_row
    return inv_scale * (
        unit_grad
        - jnp.mean(unit_grad, axis=-1, keepdims=True)
        - unit_field * jnp.mean(unit_grad * unit_field, axis=-1, keepdims=True)
    )


class Fabric:
    def __init__(self, n_ctx, n_tp):
        self.n, self.tp = n_ctx, n_tp
        self.line = n_ctx // 2
        self.pair_perm = [(i, i ^ 1) for i in range(n_ctx)]

    def swap(self, value):
        return lax.ppermute(value, "ctx", self.pair_perm)

    def hop(self, value, senders, step):
        perm = [
            (2 * p + s, 2 * (p + step) + s)
            for p in senders
            for s in range(2)
        ]
        return lax.ppermute(value, "ctx", perm)

    def line_gather(self, value):
        line = self.line
        right, left = [value], [value]
        for t in range(1, line):
            right.append(self.hop(right[-1], range(t - 1, line - 1), 1))
            left.append(self.hop(left[-1], range(1, line - t + 1), -1))
        return [value] + [left[j] + right[line - j] for j in range(1, line)]

    def line_shift(self, value):
        line = self.line
        out = [value]
        for j in range(1, line):
            perm = [
                (2 * ((p + j) % line) + s, 2 * p + s) for p in range(line) for s in range(2)
            ]
            out.append(lax.ppermute(value, "ctx", perm))
        return out

    def line_scatter(self, part):
        line = self.line
        right = left = None
        for t in range(1, line):
            r, l = part(line - t), part(t)
            if t > 1:
                r, l = r + right.astype(F32), l + left.astype(F32)
            right = self.hop(r.astype(BF16), range(0, t), 1)
            left = self.hop(l.astype(BF16), range(line - t, line), -1)
        return part(0) + right.astype(F32) + left.astype(F32)

    def ctx_sum(self, value):
        step = 1
        while step < self.n:
            value = value + lax.ppermute(value, "ctx", [(i, i ^ step) for i in range(self.n)])
            step *= 2
        return value

    def tp_sum(self, value):
        core = lax.axis_index("tp") % 2
        half = value.shape[0] // 2
        sibling = [(i, i ^ 1) for i in range(self.tp)]
        away = lax.dynamic_slice_in_dim(value, (1 - core) * half, half, 0).astype(BF16)
        mine = lax.dynamic_slice_in_dim(value, core * half, half, 0)
        mine = (mine + lax.ppermute(away, "tp", sibling).astype(F32)).astype(BF16)
        step = 2
        while step < self.tp:
            other = lax.ppermute(mine, "tp", [(i, i ^ step) for i in range(self.tp)])
            mine = (mine.astype(F32) + other.astype(F32)).astype(BF16)
            step *= 2
        theirs = lax.ppermute(mine, "tp", sibling)
        return both_ways(core, mine, theirs, 0)


def both_ways(which, mine, theirs, axis):
    return jnp.where(
        which == 0,
        jnp.concatenate([mine, theirs], axis=axis),
        jnp.concatenate([theirs, mine], axis=axis),
    )


def nt(a, b):
    return lax.dot_general(a, b, (((1,), (1,)), ((), ())), preferred_element_type=F32)


def nn(a, b):
    return lax.dot_general(a, b, (((1,), (0,)), ((), ())), preferred_element_type=F32)


def forward_kernel(
    rows, heads, q_num, k_num, q_ref, g_ref, kv_ref, o_ref, stat_ref, s_ref, m_ref, l_ref, acc_ref
):
    scale = HD ** (-0.5)
    q_blocks, k_blocks = q_ref.shape[0] // rows, kv_ref.shape[0] // rows
    width = heads * HD
    row_id = lax.broadcasted_iota(jnp.int32, (rows, rows), 0)
    col_id = lax.broadcasted_iota(jnp.int32, (rows, rows), 1)
    causal = col_id <= row_id
    same = col_id == row_id

    for head in range(heads):
        at_k = slice(head * HD, (head + 1) * HD)
        at_v = slice(width + head * HD, width + (head + 1) * HD)

        def one_query_block(qi, _):
            q_rows = pl.ds(pl.multiple_of(qi * rows, rows), rows)
            q = q_ref[q_rows, at_k]
            number = q_num[qi]
            m_ref[...] = jnp.full((rows, rows), masked_value, F32)
            l_ref[...] = jnp.zeros((rows, rows), F32)
            acc_ref[...] = jnp.zeros((rows, HD), F32)

            def score(kj, _):
                @pl.when(k_num[kj] <= number)
                def _():
                    k_rows = pl.ds(pl.multiple_of(kj * rows, rows), rows)
                    s = nt(q, kv_ref[k_rows, at_k]) * scale
                    s = jnp.where(jnp.logical_or(causal, k_num[kj] < number), s, masked_value)
                    s_ref[kj] = s
                    m_ref[...] = jnp.maximum(m_ref[...], s)

                return 0

            lax.fori_loop(0, k_blocks, score, 0)
            top = jnp.max(m_ref[...], axis=1, keepdims=True)

            def weigh(kj, _):
                @pl.when(k_num[kj] <= number)
                def _():
                    k_rows = pl.ds(pl.multiple_of(kj * rows, rows), rows)
                    p = jnp.exp(s_ref[kj] - top)
                    l_ref[...] += p
                    acc_ref[...] += nn(p.astype(BF16), kv_ref[k_rows, at_v])

                return 0

            lax.fori_loop(0, k_blocks, weigh, 0)
            total = jnp.sum(l_ref[...], axis=1, keepdims=True)
            out = (acc_ref[...] / total).astype(BF16)
            o_ref[q_rows, at_k] = out
            log_total = top + jnp.log(total)
            dots = jnp.sum(
                g_ref[q_rows, at_k].astype(F32) * out.astype(F32), axis=1, keepdims=True
            )
            place = 2 * (head * q_blocks + qi)
            stat_ref[pl.ds(place, 1), :] = jnp.sum(
                jnp.where(same, log_total, 0.0), axis=0, keepdims=True
            )
            stat_ref[pl.ds(place + 1, 1), :] = jnp.sum(
                jnp.where(same, dots, 0.0), axis=0, keepdims=True
            )
            return 0

        lax.fori_loop(0, q_blocks, one_query_block, 0)


def query_kernel(rows, heads, q_num, k_num, q_ref, g_ref, kv_ref, stat_ref, dq_ref, acc_ref):
    scale = HD ** (-0.5)
    q_blocks, k_blocks = q_ref.shape[0] // rows, kv_ref.shape[0] // rows
    width = heads * HD
    row_id = lax.broadcasted_iota(jnp.int32, (rows, rows), 0)
    col_id = lax.broadcasted_iota(jnp.int32, (rows, rows), 1)
    causal = col_id <= row_id
    same = col_id == row_id
    for head in range(heads):
        at_k = slice(head * HD, (head + 1) * HD)
        at_v = slice(width + head * HD, width + (head + 1) * HD)

        def one_query_block(qi, _):
            q_rows = pl.ds(pl.multiple_of(qi * rows, rows), rows)
            q = q_ref[q_rows, at_k]
            g = g_ref[q_rows, at_k]
            number = q_num[qi]
            place = 2 * (head * q_blocks + qi)
            log_total = jnp.sum(
                jnp.where(same, stat_ref[pl.ds(place, 1), :], 0.0), axis=1, keepdims=True
            )
            dots = jnp.sum(
                jnp.where(same, stat_ref[pl.ds(place + 1, 1), :], 0.0), axis=1, keepdims=True
            )
            acc_ref[...] = jnp.zeros((rows, HD), F32)

            def step(kj, _):
                @pl.when(k_num[kj] <= number)
                def _():
                    k_rows = pl.ds(pl.multiple_of(kj * rows, rows), rows)
                    k = kv_ref[k_rows, at_k]
                    s = nt(q, k) * scale
                    s = jnp.where(jnp.logical_or(causal, k_num[kj] < number), s, masked_value)
                    p = jnp.exp(s - log_total)
                    dp = nt(g, kv_ref[k_rows, at_v])
                    ds = (p * (dp - dots) * scale).astype(BF16)
                    acc_ref[...] += nn(ds, k)

                return 0

            lax.fori_loop(0, k_blocks, step, 0)
            dq_ref[q_rows, at_k] = acc_ref[...]
            return 0

        lax.fori_loop(0, q_blocks, one_query_block, 0)


def key_kernel(
    rows, heads, k_num, q_num, kv_ref, qg_ref, stat_ref, dk_ref, dv_ref, dk_acc, dv_acc
):
    scale = HD ** (-0.5)
    k_blocks, q_blocks = kv_ref.shape[0] // rows, qg_ref.shape[0] // rows
    per_pair = stat_ref.shape[0] // (2 * heads * q_blocks)
    width = heads * HD
    row_id = lax.broadcasted_iota(jnp.int32, (rows, rows), 0)
    col_id = lax.broadcasted_iota(jnp.int32, (rows, rows), 1)
    causal = row_id <= col_id
    for head in range(heads):
        at_k = slice(head * HD, (head + 1) * HD)
        at_v = slice(width + head * HD, width + (head + 1) * HD)

        def one_key_block(ki, _):
            k_rows = pl.ds(pl.multiple_of(ki * rows, rows), rows)
            k = kv_ref[k_rows, at_k]
            v = kv_ref[k_rows, at_v]
            number = k_num[ki]
            dk_acc[...] = jnp.zeros((rows, HD), F32)
            dv_acc[...] = jnp.zeros((rows, HD), F32)

            def step(qj, _):
                @pl.when(number <= q_num[qj])
                def _():
                    q_rows = pl.ds(pl.multiple_of(qj * rows, rows), rows)
                    q = qg_ref[q_rows, at_k]
                    g = qg_ref[q_rows, at_v]
                    place = stat_place(qj, head, heads, k_blocks)
                    s = nt(k, q) * scale
                    s = jnp.where(jnp.logical_or(causal, number < q_num[qj]), s, masked_value)
                    p = jnp.exp(s - stat_ref[pl.ds(place, 1), :])
                    dp = nt(v, g)
                    ds = (p * (dp - stat_ref[pl.ds(place + 1, 1), :]) * scale).astype(BF16)
                    dk_acc[...] += nn(ds, q)
                    dv_acc[...] += nn(p.astype(BF16), g)

                return 0

            lax.fori_loop(0, q_blocks, step, 0)
            dk_ref[k_rows, at_k] = dk_acc[...]
            dv_ref[k_rows, at_k] = dv_acc[...]
            return 0

        lax.fori_loop(0, k_blocks, one_key_block, 0)


def stat_place(qj, head, heads, pair_blocks):
    pair, within = qj // pair_blocks, qj % pair_blocks
    return 2 * ((pair * heads + head) * pair_blocks + within)


def attention_call(kernel, name, rows, heads, matmuls, scalars, arrays, outs, scratch):
    smem = pl.BlockSpec(memory_space=pltpu.SMEM)
    vmem = pl.BlockSpec(memory_space=pltpu.VMEM)
    a, b = scalars[0].shape[0], scalars[1].shape[0]
    flops = matmuls * a * b * rows * rows * HD * heads
    return pl.pallas_call(
        functools.partial(kernel, rows, heads),
        name=name,
        out_shape=outs,
        in_specs=[smem] * len(scalars) + [vmem] * len(arrays),
        out_specs=jax.tree.map(lambda _: vmem, outs),
        scratch_shapes=scratch,
        cost_estimate=pl.CostEstimate(
            flops=flops,
            transcendentals=a * b * rows * rows * heads // 2,
            bytes_accessed=sum(x.size * x.dtype.itemsize for x in arrays),
        ),
        compiler_params=pltpu.CompilerParams(vmem_limit_bytes=56 * 1024 * 1024),
    )(*scalars, *arrays)


def shards(
    fabric,
    stream_in,
    cotangent,
    ln_gain,
    ln_bias,
    w_qkv,
    b_qkv,
    w_out,
    out_bias,
    w_up,
    b_up,
    w_down,
    block_order,
):
    rows, model = stream_in.shape
    block_rows = rows // 2
    heads = w_out.shape[0] // HD
    own_heads = heads // 2
    own_width = own_heads * HD
    hidden_half = w_up.shape[1] // 2
    line = fabric.line
    me = lax.axis_index("ctx")
    place, side = me // 2, me % 2
    block_cols = model // line

    def pair_numbers(j):
        pair = (place + j) % line
        first = lax.dynamic_slice_in_dim(block_order, pair * 4 + side * 2, 2)
        second = lax.dynamic_slice_in_dim(block_order, pair * 4 + (1 - side) * 2, 2)
        return jnp.concatenate([first, second])

    own_numbers = pair_numbers(0)
    all_numbers = jnp.concatenate([pair_numbers(j) for j in range(line)])
    cosine, sine_table = rope_tables(own_numbers, block_rows, ROT)
    cos_here, sin_here = cosine[:rows], sine_table[:rows]

    row_mean = jnp.mean(stream_in, axis=-1, keepdims=True)
    centred = stream_in - row_mean
    variance = jnp.mean(centred * centred, axis=-1, keepdims=True)
    inv_scale = lax.rsqrt(variance + norm_epsilon)
    unit = centred * inv_scale
    attn_in = (unit * ln_gain[0] + ln_bias[0]).astype(BF16)
    mlp_in = (unit * ln_gain[1] + ln_bias[1]).astype(BF16)
    cot_b = cotangent.astype(BF16)

    joined = jnp.dot(attn_in, w_qkv, preferred_element_type=F32) + b_qkv
    out_grad = lax.dot_general(
        cot_b, w_out, (((1,), (1,)), ((), ())), preferred_element_type=F32
    ).astype(BF16)

    def head_part(which, kind):
        start = which * own_heads * 3 * HD
        span = lax.dynamic_slice_in_dim(joined, start, own_heads * 3 * HD, 1)
        pieces = []
        for h in range(own_heads):
            piece = span[:, (3 * h + kind) * HD : (3 * h + kind + 1) * HD]
            if kind < 2:
                piece = rotate(piece, cos_here, sin_here)
            pieces.append(piece.astype(BF16))
        return pieces

    def qkv_of(which):
        q, k, v = (head_part(which, kind) for kind in range(3))
        return jnp.concatenate(k + v, axis=1), jnp.concatenate(q, axis=1)

    kv_mine, q_mine = qkv_of(side)
    kv_away, q_away = qkv_of(1 - side)
    g_mine = lax.dynamic_slice_in_dim(out_grad, side * own_width, own_width, 1)
    g_away = lax.dynamic_slice_in_dim(out_grad, (1 - side) * own_width, own_width, 1)
    kv_own = jnp.concatenate([kv_mine, fabric.swap(kv_away)], axis=0)
    qg_own = jnp.concatenate(
        [
            jnp.concatenate([q_mine, g_mine], axis=1),
            fabric.swap(jnp.concatenate([q_away, g_away], axis=1)),
        ],
        axis=0,
    )
    q_own, g_own = qg_own[:, :own_width], qg_own[:, own_width:]
    kv_all = jnp.concatenate(fabric.line_gather(kv_own), axis=0)
    qg_all = jnp.concatenate(fabric.line_gather(qg_own), axis=0)

    hidden = jnp.dot(mlp_in, w_up, preferred_element_type=F32) + b_up
    erf_part = 0.5 * (1.0 + lax.erf(hidden * root_half))
    act = (hidden * erf_part).astype(BF16)
    slope = erf_part + hidden * jnp.exp(-0.5 * hidden * hidden) * inverse_root_two_pi
    hidden_grad = (
        lax.dot_general(cot_b, w_down, (((1,), (1,)), ((), ())), preferred_element_type=F32)
        * slope
    )
    grad_bup = jnp.sum(hidden_grad, axis=0)
    hidden_b = hidden_grad.astype(BF16)
    mlp_back = lax.dot_general(
        hidden_b, w_up, (((1,), (1,)), ((), ())), preferred_element_type=F32
    )

    cot_pair = jnp.concatenate([cot_b, fabric.swap(cot_b)], axis=0)
    mlp_in_pair = jnp.concatenate([mlp_in, fabric.swap(mlp_in)], axis=0)
    attn_in_pair = jnp.concatenate([attn_in, fabric.swap(attn_in)], axis=0)

    def half_columns(value, which):
        return lax.dynamic_slice_in_dim(value, which * hidden_half, hidden_half, 1)

    act_pair = jnp.concatenate(
        [half_columns(act, side), fabric.swap(half_columns(act, 1 - side))], axis=0
    )
    hidden_pair = jnp.concatenate(
        [half_columns(hidden_b, side), fabric.swap(half_columns(hidden_b, 1 - side))], axis=0
    )

    def columns_of(value, j):
        return lax.dynamic_slice_in_dim(value, ((place + j) % line) * block_cols, block_cols, 1)

    def tn(a, b):
        return lax.dot_general(a, b, (((0,), (0,)), ((), ())), preferred_element_type=F32)

    def finish(total, axis):
        half = total.shape[axis] // 2
        mine = lax.dynamic_slice_in_dim(total, side * half, half, axis)
        away = lax.dynamic_slice_in_dim(total, (1 - side) * half, half, axis)
        theirs = fabric.swap(away.astype(BF16)).astype(F32)
        return both_ways(side, mine, theirs, 1 - axis)

    sum_down = fabric.line_scatter(lambda j: tn(act_pair, columns_of(cot_pair, j)))
    sum_up = fabric.line_scatter(lambda j: tn(columns_of(mlp_in_pair, j), hidden_pair))
    summed_down = finish(sum_down, 1)
    summed_up = finish(sum_up, 0)

    stat_rows = 2 * own_heads * own_numbers.shape[0]
    pair_rows = q_own.shape[0]
    attn_own, stats = attention_call(
        forward_kernel,
        "attend",
        block_rows,
        own_heads,
        4,
        (own_numbers, all_numbers),
        (q_own, g_own, kv_all),
        (
            jax.ShapeDtypeStruct((pair_rows, own_width), BF16),
            jax.ShapeDtypeStruct((stat_rows, block_rows), F32),
        ),
        [
            pltpu.VMEM((all_numbers.shape[0], block_rows, block_rows), F32),
            pltpu.VMEM((block_rows, block_rows), F32),
            pltpu.VMEM((block_rows, block_rows), F32),
            pltpu.VMEM((block_rows, HD), F32),
        ],
    )
    stats_all = jnp.concatenate(fabric.line_shift(stats), axis=0)
    attn_out = both_ways(side, attn_own[:rows], fabric.swap(attn_own[rows:]), 1)
    branch_part = jnp.dot(attn_out, w_out, preferred_element_type=F32) + jnp.dot(
        act, w_down, preferred_element_type=F32
    )
    stream_out = stream_in + out_bias + fabric.tp_sum(branch_part).astype(F32)
    mlp_total = fabric.tp_sum(mlp_back).astype(F32)

    sum_out = fabric.line_scatter(lambda j: tn(attn_own, columns_of(cot_pair, j)))
    summed_out = finish(sum_out, 1)

    (query_grad,) = attention_call(
        query_kernel,
        "attend_back_q",
        block_rows,
        own_heads,
        6,
        (own_numbers, all_numbers),
        (q_own, g_own, kv_all, stats),
        (jax.ShapeDtypeStruct((pair_rows, own_width), F32),),
        [pltpu.VMEM((block_rows, HD), F32)],
    )
    key_grad, value_grad = attention_call(
        key_kernel,
        "attend_back_k",
        block_rows,
        own_heads,
        8,
        (own_numbers, all_numbers),
        (kv_own, qg_all, stats_all),
        (
            jax.ShapeDtypeStruct((pair_rows, own_width), F32),
            jax.ShapeDtypeStruct((pair_rows, own_width), F32),
        ),
        [pltpu.VMEM((block_rows, HD), F32), pltpu.VMEM((block_rows, HD), F32)],
    )
    fused = []
    for h in range(own_heads):
        at = slice(h * HD, (h + 1) * HD)
        fused += [
            unrotate(query_grad[:, at], cosine, sine_table),
            unrotate(key_grad[:, at], cosine, sine_table),
            value_grad[:, at],
        ]
    joined_grad = jnp.concatenate(fused, axis=1)
    bias_half = jnp.sum(joined_grad, axis=0)
    grad_bqkv = both_ways(side, bias_half, jnp.zeros_like(bias_half), 0)
    joined_b = joined_grad.astype(BF16)
    joined_here = both_ways(side, joined_b[:rows], fabric.swap(joined_b[rows:]), 1)
    attn_back = lax.dot_general(
        joined_here, w_qkv, (((1,), (1,)), ((), ())), preferred_element_type=F32
    )
    sum_qkv = fabric.line_scatter(lambda j: tn(columns_of(attn_in_pair, j), joined_b))
    summed_qkv = finish(sum_qkv, 0)
    attn_total = fabric.tp_sum(attn_back).astype(F32)

    grad_in = (
        cotangent
        + normalize_back(attn_total, unit, inv_scale, ln_gain[0])
        + normalize_back(mlp_total, unit, inv_scale, ln_gain[1])
    )
    early = [grad_bup, jnp.sum(cotangent, axis=0)]
    late = [
        grad_bqkv,
        jnp.sum(attn_total * unit, axis=0),
        jnp.sum(mlp_total * unit, axis=0),
        jnp.sum(attn_total, axis=0),
        jnp.sum(mlp_total, axis=0),
    ]
    sizes = [part.shape[0] for part in early + late]
    small = fabric.ctx_sum(jnp.concatenate(early + late))
    cuts, at = [], 0
    for size in sizes:
        cuts.append(small[at : at + size])
        at += size
    return (
        stream_out,
        grad_in,
        summed_qkv,
        cuts[2],
        summed_out,
        cuts[1],
        summed_up,
        cuts[0],
        summed_down,
        jnp.stack([cuts[3], cuts[4]]),
        jnp.stack([cuts[5], cuts[6]]),
    )


def solution(mesh):
    fabric = Fabric(mesh.shape["ctx"], mesh.shape["tp"])
    placed = (
        P("ctx", None),
        P("ctx", None),
        P(),
        P(),
        P(None, "tp"),
        P("tp"),
        P("tp", None),
        P(),
        P(None, "tp"),
        P("tp"),
        P("tp", None),
        P(),
    )
    return jax.shard_map(
        functools.partial(shards, fabric),
        mesh=mesh,
        in_specs=placed,
        out_specs=(
            P("ctx", None),
            P("ctx", None),
            P("ctx", "tp"),
            P("tp"),
            P("tp", "ctx"),
            P(),
            P("ctx", "tp"),
            P("tp"),
            P("tp", "ctx"),
            P(),
            P(),
        ),
        check_vma=False,
    )
```

```python
import functools
import math

import jax
import jax.numpy as jnp
from jax import lax
from jax.experimental import pallas as pl
from jax.experimental.pallas import tpu as pltpu
from jax.sharding import PartitionSpec as P

HD = 256
ROT = 64

masked_value = -1e30
norm_epsilon = 1e-05
root_half = 0.7071067811865476
inverse_root_two_pi = 0.3989422804014327

F32 = jnp.float32
BF16 = jnp.bfloat16


def rope_tables(block_numbers, block_rows, rotary_dims):
    positions = (
        block_numbers[:, None] * block_rows + jnp.arange(block_rows, dtype=jnp.int32)[None, :]
    ).reshape(-1)
    half_rot = rotary_dims // 2
    frequency = jnp.exp(
        jnp.arange(half_rot, dtype=F32) * (-2.0 * math.log(10000.0) / rotary_dims)
    )
    angles = positions.astype(F32)[:, None] * frequency[None, :]
    angles = jnp.concatenate([angles, angles], axis=1)
    return (jnp.cos(angles), jnp.sin(angles))


def rotate(tensor, cosine, sine_table):
    half_rot = ROT // 2
    rotary_part = tensor[:, :ROT]
    turned = jnp.concatenate([-rotary_part[:, half_rot:], rotary_part[:, :half_rot]], axis=-1)
    moved = rotary_part * cosine + turned * sine_table
    return jnp.concatenate([moved, tensor[:, ROT:]], axis=-1)


def unrotate(incoming, cosine, sine_table):
    half_rot = ROT // 2
    rotary_part = incoming[:, :ROT]
    scaled = rotary_part * sine_table
    swapped = jnp.concatenate([scaled[:, half_rot:], -scaled[:, :half_rot]], axis=-1)
    moved = rotary_part * cosine + swapped
    return jnp.concatenate([moved, incoming[:, ROT:]], axis=-1)


def normalize_back(incoming, unit_field, inv_scale, gain_row):
    unit_grad = incoming * gain_row
    return inv_scale * (
        unit_grad
        - jnp.mean(unit_grad, axis=-1, keepdims=True)
        - unit_field * jnp.mean(unit_grad * unit_field, axis=-1, keepdims=True)
    )


class Fabric:
    def __init__(self, n_ctx, n_tp):
        self.n, self.tp = n_ctx, n_tp
        self.line = n_ctx // 2
        self.pair_perm = [(i, i ^ 1) for i in range(n_ctx)]

    def swap(self, value):
        return lax.ppermute(value, "ctx", self.pair_perm)

    def hop(self, value, senders, step):
        perm = [
            (2 * p + s, 2 * (p + step) + s)
            for p in senders
            for s in range(2)
        ]
        return lax.ppermute(value, "ctx", perm)

    def line_gather(self, value):
        line = self.line
        right, left = [value], [value]
        for t in range(1, line):
            right.append(self.hop(right[-1], range(t - 1, line - 1), 1))
            left.append(self.hop(left[-1], range(1, line - t + 1), -1))
        return [value] + [left[j] + right[line - j] for j in range(1, line)]

    def line_shift(self, value):
        line = self.line
        out = [value]
        for j in range(1, line):
            perm = [
                (2 * ((p + j) % line) + s, 2 * p + s) for p in range(line) for s in range(2)
            ]
            out.append(lax.ppermute(value, "ctx", perm))
        return out

    def line_scatter(self, part):
        line = self.line
        right = left = None
        for t in range(1, line):
            r, l = part(line - t), part(t)
            if t > 1:
                r, l = r + right.astype(F32), l + left.astype(F32)
            right = self.hop(r.astype(BF16), range(0, t), 1)
            left = self.hop(l.astype(BF16), range(line - t, line), -1)
            yield right, left
        yield part(0) + right.astype(F32) + left.astype(F32)

    def ctx_sum(self, value):
        step = 1
        while step < self.n:
            value = value + lax.ppermute(value, "ctx", [(i, i ^ step) for i in range(self.n)])
            step *= 2
        return value

    def tp_sum(self, value):
        core = lax.axis_index("tp") % 2
        half = value.shape[0] // 2
        sibling = [(i, i ^ 1) for i in range(self.tp)]
        away = lax.dynamic_slice_in_dim(value, (1 - core) * half, half, 0).astype(BF16)
        mine = lax.dynamic_slice_in_dim(value, core * half, half, 0)
        mine = (mine + lax.ppermute(away, "tp", sibling).astype(F32)).astype(BF16)
        step = 2
        while step < self.tp:
            other = lax.ppermute(mine, "tp", [(i, i ^ step) for i in range(self.tp)])
            mine = (mine.astype(F32) + other.astype(F32)).astype(BF16)
            step *= 2
        theirs = lax.ppermute(mine, "tp", sibling)
        return both_ways(core, mine, theirs, 0)


def both_ways(which, mine, theirs, axis):
    return jnp.where(
        which == 0,
        jnp.concatenate([mine, theirs], axis=axis),
        jnp.concatenate([theirs, mine], axis=axis),
    )


def nt(a, b):
    return lax.dot_general(a, b, (((1,), (1,)), ((), ())), preferred_element_type=F32)


def nn(a, b):
    return lax.dot_general(a, b, (((1,), (0,)), ((), ())), preferred_element_type=F32)


def forward_kernel(
    rows, heads, q_num, k_num, q_ref, g_ref, kv_ref, o_ref, stat_ref, s_ref, m_ref, l_ref, acc_ref
):
    scale = HD ** (-0.5)
    q_blocks, k_blocks = q_ref.shape[0] // rows, kv_ref.shape[0] // rows
    width = heads * HD
    row_id = lax.broadcasted_iota(jnp.int32, (rows, rows), 0)
    col_id = lax.broadcasted_iota(jnp.int32, (rows, rows), 1)
    causal = col_id <= row_id
    same = col_id == row_id

    for head in range(heads):
        at_k = slice(head * HD, (head + 1) * HD)
        at_v = slice(width + head * HD, width + (head + 1) * HD)

        def one_query_block(qi, _):
            q_rows = pl.ds(pl.multiple_of(qi * rows, rows), rows)
            q = q_ref[q_rows, at_k]
            number = q_num[qi]
            m_ref[...] = jnp.full((rows, rows), masked_value, F32)
            l_ref[...] = jnp.zeros((rows, rows), F32)
            acc_ref[...] = jnp.zeros((rows, HD), F32)

            def score(kj, _):
                @pl.when(k_num[kj] <= number)
                def _():
                    k_rows = pl.ds(pl.multiple_of(kj * rows, rows), rows)
                    s = nt(q, kv_ref[k_rows, at_k]) * scale
                    s = jnp.where(jnp.logical_or(causal, k_num[kj] < number), s, masked_value)
                    s_ref[kj] = s
                    m_ref[...] = jnp.maximum(m_ref[...], s)

                return 0

            lax.fori_loop(0, k_blocks, score, 0)
            top = jnp.max(m_ref[...], axis=1, keepdims=True)

            def weigh(kj, _):
                @pl.when(k_num[kj] <= number)
                def _():
                    k_rows = pl.ds(pl.multiple_of(kj * rows, rows), rows)
                    p = jnp.exp(s_ref[kj] - top)
                    l_ref[...] += p
                    acc_ref[...] += nn(p.astype(BF16), kv_ref[k_rows, at_v])

                return 0

            lax.fori_loop(0, k_blocks, weigh, 0)
            total = jnp.sum(l_ref[...], axis=1, keepdims=True)
            out = (acc_ref[...] / total).astype(BF16)
            o_ref[q_rows, at_k] = out
            log_total = top + jnp.log(total)
            dots = jnp.sum(
                g_ref[q_rows, at_k].astype(F32) * out.astype(F32), axis=1, keepdims=True
            )
            place = 2 * (head * q_blocks + qi)
            stat_ref[pl.ds(place, 1), :] = jnp.sum(
                jnp.where(same, log_total, 0.0), axis=0, keepdims=True
            )
            stat_ref[pl.ds(place + 1, 1), :] = jnp.sum(
                jnp.where(same, dots, 0.0), axis=0, keepdims=True
            )
            return 0

        lax.fori_loop(0, q_blocks, one_query_block, 0)


def query_kernel(rows, heads, q_num, k_num, q_ref, g_ref, kv_ref, stat_ref, dq_ref, acc_ref):
    scale = HD ** (-0.5)
    q_blocks, k_blocks = q_ref.shape[0] // rows, kv_ref.shape[0] // rows
    width = heads * HD
    row_id = lax.broadcasted_iota(jnp.int32, (rows, rows), 0)
    col_id = lax.broadcasted_iota(jnp.int32, (rows, rows), 1)
    causal = col_id <= row_id
    same = col_id == row_id
    for head in range(heads):
        at_k = slice(head * HD, (head + 1) * HD)
        at_v = slice(width + head * HD, width + (head + 1) * HD)

        def one_query_block(qi, _):
            q_rows = pl.ds(pl.multiple_of(qi * rows, rows), rows)
            q = q_ref[q_rows, at_k]
            g = g_ref[q_rows, at_k]
            number = q_num[qi]
            place = 2 * (head * q_blocks + qi)
            log_total = jnp.sum(
                jnp.where(same, stat_ref[pl.ds(place, 1), :], 0.0), axis=1, keepdims=True
            )
            dots = jnp.sum(
                jnp.where(same, stat_ref[pl.ds(place + 1, 1), :], 0.0), axis=1, keepdims=True
            )
            acc_ref[...] = jnp.zeros((rows, HD), F32)

            def step(kj, _):
                @pl.when(k_num[kj] <= number)
                def _():
                    k_rows = pl.ds(pl.multiple_of(kj * rows, rows), rows)
                    k = kv_ref[k_rows, at_k]
                    s = nt(q, k) * scale
                    s = jnp.where(jnp.logical_or(causal, k_num[kj] < number), s, masked_value)
                    p = jnp.exp(s - log_total)
                    dp = nt(g, kv_ref[k_rows, at_v])
                    ds = (p * (dp - dots) * scale).astype(BF16)
                    acc_ref[...] += nn(ds, k)

                return 0

            lax.fori_loop(0, k_blocks, step, 0)
            dq_ref[q_rows, at_k] = acc_ref[...]
            return 0

        lax.fori_loop(0, q_blocks, one_query_block, 0)


def key_kernel(
    rows, heads, k_num, q_num, kv_ref, qg_ref, stat_ref, dk_ref, dv_ref, dk_acc, dv_acc
):
    scale = HD ** (-0.5)
    k_blocks, q_blocks = kv_ref.shape[0] // rows, qg_ref.shape[0] // rows
    per_pair = stat_ref.shape[0] // (2 * heads * q_blocks)
    width = heads * HD
    row_id = lax.broadcasted_iota(jnp.int32, (rows, rows), 0)
    col_id = lax.broadcasted_iota(jnp.int32, (rows, rows), 1)
    causal = row_id <= col_id
    for head in range(heads):
        at_k = slice(head * HD, (head + 1) * HD)
        at_v = slice(width + head * HD, width + (head + 1) * HD)

        def one_key_block(ki, _):
            k_rows = pl.ds(pl.multiple_of(ki * rows, rows), rows)
            k = kv_ref[k_rows, at_k]
            v = kv_ref[k_rows, at_v]
            number = k_num[ki]
            dk_acc[...] = jnp.zeros((rows, HD), F32)
            dv_acc[...] = jnp.zeros((rows, HD), F32)

            def step(qj, _):
                @pl.when(number <= q_num[qj])
                def _():
                    q_rows = pl.ds(pl.multiple_of(qj * rows, rows), rows)
                    q = qg_ref[q_rows, at_k]
                    g = qg_ref[q_rows, at_v]
                    place = stat_place(qj, head, heads, k_blocks)
                    s = nt(k, q) * scale
                    s = jnp.where(jnp.logical_or(causal, number < q_num[qj]), s, masked_value)
                    p = jnp.exp(s - stat_ref[pl.ds(place, 1), :])
                    dp = nt(v, g)
                    ds = (p * (dp - stat_ref[pl.ds(place + 1, 1), :]) * scale).astype(BF16)
                    dk_acc[...] += nn(ds, q)
                    dv_acc[...] += nn(p.astype(BF16), g)

                return 0

            lax.fori_loop(0, q_blocks, step, 0)
            dk_ref[k_rows, at_k] = dk_acc[...]
            dv_ref[k_rows, at_k] = dv_acc[...]
            return 0

        lax.fori_loop(0, k_blocks, one_key_block, 0)


def stat_place(qj, head, heads, pair_blocks):
    pair, within = qj // pair_blocks, qj % pair_blocks
    return 2 * ((pair * heads + head) * pair_blocks + within)


def attention_call(kernel, name, rows, heads, matmuls, scalars, arrays, outs, scratch):
    smem = pl.BlockSpec(memory_space=pltpu.SMEM)
    vmem = pl.BlockSpec(memory_space=pltpu.VMEM)
    a, b = scalars[0].shape[0], scalars[1].shape[0]
    flops = matmuls * a * b * rows * rows * HD * heads
    return pl.pallas_call(
        functools.partial(kernel, rows, heads),
        name=name,
        out_shape=outs,
        in_specs=[smem] * len(scalars) + [vmem] * len(arrays),
        out_specs=jax.tree.map(lambda _: vmem, outs),
        scratch_shapes=scratch,
        cost_estimate=pl.CostEstimate(
            flops=flops,
            transcendentals=a * b * rows * rows * heads // 2,
            bytes_accessed=sum(x.size * x.dtype.itemsize for x in arrays),
        ),
        compiler_params=pltpu.CompilerParams(vmem_limit_bytes=56 * 1024 * 1024),
    )(*scalars, *arrays)


def shards(
    fabric,
    stream_in,
    cotangent,
    ln_gain,
    ln_bias,
    w_qkv,
    b_qkv,
    w_out,
    out_bias,
    w_up,
    b_up,
    w_down,
    block_order,
):
    rows, model = stream_in.shape
    block_rows = rows // 2
    heads = w_out.shape[0] // HD
    own_heads = heads // 2
    own_width = own_heads * HD
    hidden_half = w_up.shape[1] // 2
    line = fabric.line
    me = lax.axis_index("ctx")
    place, side = me // 2, me % 2
    block_cols = model // line

    def pair_numbers(j):
        pair = (place + j) % line
        first = lax.dynamic_slice_in_dim(block_order, pair * 4 + side * 2, 2)
        second = lax.dynamic_slice_in_dim(block_order, pair * 4 + (1 - side) * 2, 2)
        return jnp.concatenate([first, second])

    own_numbers = pair_numbers(0)
    all_numbers = jnp.concatenate([pair_numbers(j) for j in range(line)])
    cosine, sine_table = rope_tables(own_numbers, block_rows, ROT)
    cos_here, sin_here = cosine[:rows], sine_table[:rows]

    row_mean = jnp.mean(stream_in, axis=-1, keepdims=True)
    centred = stream_in - row_mean
    variance = jnp.mean(centred * centred, axis=-1, keepdims=True)
    inv_scale = lax.rsqrt(variance + norm_epsilon)
    unit = centred * inv_scale
    attn_in = (unit * ln_gain[0] + ln_bias[0]).astype(BF16)
    mlp_in = (unit * ln_gain[1] + ln_bias[1]).astype(BF16)
    cot_b = cotangent.astype(BF16)

    joined = jnp.dot(attn_in, w_qkv, preferred_element_type=F32) + b_qkv
    out_grad = lax.dot_general(
        cot_b, w_out, (((1,), (1,)), ((), ())), preferred_element_type=F32
    ).astype(BF16)

    def head_part(which, kind):
        start = which * own_heads * 3 * HD
        span = lax.dynamic_slice_in_dim(joined, start, own_heads * 3 * HD, 1)
        pieces = []
        for h in range(own_heads):
            piece = span[:, (3 * h + kind) * HD : (3 * h + kind + 1) * HD]
            if kind < 2:
                piece = rotate(piece, cos_here, sin_here)
            pieces.append(piece.astype(BF16))
        return pieces

    def qkv_of(which):
        q, k, v = (head_part(which, kind) for kind in range(3))
        return jnp.concatenate(k + v, axis=1), jnp.concatenate(q, axis=1)

    kv_mine, q_mine = qkv_of(side)
    kv_away, q_away = qkv_of(1 - side)
    g_mine = lax.dynamic_slice_in_dim(out_grad, side * own_width, own_width, 1)
    g_away = lax.dynamic_slice_in_dim(out_grad, (1 - side) * own_width, own_width, 1)
    kv_own = jnp.concatenate([kv_mine, fabric.swap(kv_away)], axis=0)
    qg_own = jnp.concatenate(
        [
            jnp.concatenate([q_mine, g_mine], axis=1),
            fabric.swap(jnp.concatenate([q_away, g_away], axis=1)),
        ],
        axis=0,
    )
    q_own, g_own = qg_own[:, :own_width], qg_own[:, own_width:]
    kv_all = jnp.concatenate(fabric.line_gather(kv_own), axis=0)
    qg_all = jnp.concatenate(fabric.line_gather(qg_own), axis=0)

    hidden = jnp.dot(mlp_in, w_up, preferred_element_type=F32) + b_up
    erf_part = 0.5 * (1.0 + lax.erf(hidden * root_half))
    act = (hidden * erf_part).astype(BF16)
    slope = erf_part + hidden * jnp.exp(-0.5 * hidden * hidden) * inverse_root_two_pi
    hidden_grad = (
        lax.dot_general(cot_b, w_down, (((1,), (1,)), ((), ())), preferred_element_type=F32)
        * slope
    )
    grad_bup = jnp.sum(hidden_grad, axis=0)
    hidden_b = hidden_grad.astype(BF16)
    mlp_back = lax.dot_general(
        hidden_b, w_up, (((1,), (1,)), ((), ())), preferred_element_type=F32
    )

    cot_pair = jnp.concatenate([cot_b, fabric.swap(cot_b)], axis=0)
    mlp_in_pair = jnp.concatenate([mlp_in, fabric.swap(mlp_in)], axis=0)
    attn_in_pair = jnp.concatenate([attn_in, fabric.swap(attn_in)], axis=0)

    def half_columns(value, which):
        return lax.dynamic_slice_in_dim(value, which * hidden_half, hidden_half, 1)

    act_pair = jnp.concatenate(
        [half_columns(act, side), fabric.swap(half_columns(act, 1 - side))], axis=0
    )
    hidden_pair = jnp.concatenate(
        [half_columns(hidden_b, side), fabric.swap(half_columns(hidden_b, 1 - side))], axis=0
    )

    def columns_of(value, j):
        return lax.dynamic_slice_in_dim(value, ((place + j) % line) * block_cols, block_cols, 1)

    def tn(a, b):
        return lax.dot_general(a, b, (((0,), (0,)), ((), ())), preferred_element_type=F32)

    def finish(total, axis):
        half = total.shape[axis] // 2
        mine = lax.dynamic_slice_in_dim(total, side * half, half, axis)
        away = lax.dynamic_slice_in_dim(total, (1 - side) * half, half, axis)
        theirs = fabric.swap(away.astype(BF16)).astype(F32)
        return both_ways(side, mine, theirs, 1 - axis)

    down_parts = [tn(act_pair, columns_of(cot_pair, j)) for j in range(line)]
    up_parts = [tn(columns_of(mlp_in_pair, j), hidden_pair) for j in range(line)]
    (kv_all, mlp_back, act, grad_bup, *parts) = lax.optimization_barrier(
        (kv_all, mlp_back, act, grad_bup, *down_parts, *up_parts)
    )
    down_steps = fabric.line_scatter(lambda j: parts[j])
    up_steps = fabric.line_scatter(lambda j: parts[line + j])
    *_, sum_down = down_steps
    *_, sum_up = up_steps
    summed_down = finish(sum_down, 1)
    summed_up = finish(sum_up, 0)

    stat_rows = 2 * own_heads * own_numbers.shape[0]
    pair_rows = q_own.shape[0]
    attn_own, stats = attention_call(
        forward_kernel,
        "attend",
        block_rows,
        own_heads,
        4,
        (own_numbers, all_numbers),
        (q_own, g_own, kv_all),
        (
            jax.ShapeDtypeStruct((pair_rows, own_width), BF16),
            jax.ShapeDtypeStruct((stat_rows, block_rows), F32),
        ),
        [
            pltpu.VMEM((all_numbers.shape[0], block_rows, block_rows), F32),
            pltpu.VMEM((block_rows, block_rows), F32),
            pltpu.VMEM((block_rows, block_rows), F32),
            pltpu.VMEM((block_rows, HD), F32),
        ],
    )
    stats_all = jnp.concatenate(fabric.line_shift(stats), axis=0)
    attn_out = both_ways(side, attn_own[:rows], fabric.swap(attn_own[rows:]), 1)
    branch_part = jnp.dot(attn_out, w_out, preferred_element_type=F32) + jnp.dot(
        act, w_down, preferred_element_type=F32
    )
    stream_out = stream_in + out_bias + fabric.tp_sum(branch_part).astype(F32)
    mlp_total = fabric.tp_sum(mlp_back).astype(F32)

    *_, sum_out = fabric.line_scatter(lambda j: tn(attn_own, columns_of(cot_pair, j)))
    summed_out = finish(sum_out, 1)

    (query_grad,) = attention_call(
        query_kernel,
        "attend_back_q",
        block_rows,
        own_heads,
        6,
        (own_numbers, all_numbers),
        (q_own, g_own, kv_all, stats),
        (jax.ShapeDtypeStruct((pair_rows, own_width), F32),),
        [pltpu.VMEM((block_rows, HD), F32)],
    )
    key_grad, value_grad = attention_call(
        key_kernel,
        "attend_back_k",
        block_rows,
        own_heads,
        8,
        (own_numbers, all_numbers),
        (kv_own, qg_all, stats_all),
        (
            jax.ShapeDtypeStruct((pair_rows, own_width), F32),
            jax.ShapeDtypeStruct((pair_rows, own_width), F32),
        ),
        [pltpu.VMEM((block_rows, HD), F32), pltpu.VMEM((block_rows, HD), F32)],
    )
    fused = []
    for h in range(own_heads):
        at = slice(h * HD, (h + 1) * HD)
        fused += [
            unrotate(query_grad[:, at], cosine, sine_table),
            unrotate(key_grad[:, at], cosine, sine_table),
            value_grad[:, at],
        ]
    joined_grad = jnp.concatenate(fused, axis=1)
    bias_half = jnp.sum(joined_grad, axis=0)
    grad_bqkv = both_ways(side, bias_half, jnp.zeros_like(bias_half), 0)
    joined_b = joined_grad.astype(BF16)
    joined_here = both_ways(side, joined_b[:rows], fabric.swap(joined_b[rows:]), 1)
    attn_back = lax.dot_general(
        joined_here, w_qkv, (((1,), (1,)), ((), ())), preferred_element_type=F32
    )
    *_, sum_qkv = fabric.line_scatter(lambda j: tn(columns_of(attn_in_pair, j), joined_b))
    summed_qkv = finish(sum_qkv, 0)
    attn_total = fabric.tp_sum(attn_back).astype(F32)

    grad_in = (
        cotangent
        + normalize_back(attn_total, unit, inv_scale, ln_gain[0])
        + normalize_back(mlp_total, unit, inv_scale, ln_gain[1])
    )
    early = [grad_bup, jnp.sum(cotangent, axis=0)]
    late = [
        grad_bqkv,
        jnp.sum(attn_total * unit, axis=0),
        jnp.sum(mlp_total * unit, axis=0),
        jnp.sum(attn_total, axis=0),
        jnp.sum(mlp_total, axis=0),
    ]
    sizes = [part.shape[0] for part in early + late]
    small = fabric.ctx_sum(jnp.concatenate(early + late))
    cuts, at = [], 0
    for size in sizes:
        cuts.append(small[at : at + size])
        at += size
    return (
        stream_out,
        grad_in,
        summed_qkv,
        cuts[2],
        summed_out,
        cuts[1],
        summed_up,
        cuts[0],
        summed_down,
        jnp.stack([cuts[3], cuts[4]]),
        jnp.stack([cuts[5], cuts[6]]),
    )


def solution(mesh):
    fabric = Fabric(mesh.shape["ctx"], mesh.shape["tp"])
    placed = (
        P("ctx", None),
        P("ctx", None),
        P(),
        P(),
        P(None, "tp"),
        P("tp"),
        P("tp", None),
        P(),
        P(None, "tp"),
        P("tp"),
        P("tp", None),
        P(),
    )
    return jax.shard_map(
        functools.partial(shards, fabric),
        mesh=mesh,
        in_specs=placed,
        out_specs=(
            P("ctx", None),
            P("ctx", None),
            P("ctx", "tp"),
            P("tp"),
            P("tp", "ctx"),
            P(),
            P("ctx", "tp"),
            P("tp"),
            P("tp", "ctx"),
            P(),
            P(),
        ),
        check_vma=False,
    )
```

```python
import functools
import math

import jax
import jax.numpy as jnp
from jax import lax
from jax.experimental import pallas as pl
from jax.experimental.pallas import tpu as pltpu
from jax.sharding import PartitionSpec as P

HD = 256
ROT = 64
LANES = 128
TILE = 256

masked_value = -1e30
norm_epsilon = 1e-05
root_half = 0.7071067811865476
inverse_root_two_pi = 0.3989422804014327

F32 = jnp.float32
BF16 = jnp.bfloat16
MESH = pl.DeviceIdType.MESH
ANY = pl.BlockSpec(memory_space=pl.ANY)
VMEM = pl.BlockSpec(memory_space=pltpu.VMEM)
SMEM = pl.BlockSpec(memory_space=pltpu.SMEM)


def nt(a, b):
    return lax.dot_general(a, b, (((1,), (1,)), ((), ())), preferred_element_type=F32)


def nn(a, b):
    return lax.dot_general(a, b, (((1,), (0,)), ((), ())), preferred_element_type=F32)


def tn(a, b):
    return lax.dot_general(a, b, (((0,), (0,)), ((), ())), preferred_element_type=F32)


def rope_tables(positions):
    half_rot = ROT // 2
    frequency = jnp.exp(jnp.arange(half_rot, dtype=F32) * (-2.0 * math.log(10000.0) / ROT))
    angles = positions.astype(F32)[..., None] * frequency
    cosine, sine = jnp.cos(angles), jnp.sin(angles)
    rest = angles.shape[:-1] + (LANES - ROT,)
    return (
        jnp.concatenate([cosine, cosine, jnp.ones(rest, F32)], axis=-1),
        jnp.concatenate([sine, sine, jnp.zeros(rest, F32)], axis=-1),
    )


def turn(first, cosine, sine, sign):
    half_rot = ROT // 2
    scaled = first * sine if sign < 0 else first
    lane = lax.broadcasted_iota(jnp.int32, first.shape, 1)
    down = jnp.where(lane < half_rot, pltpu.roll(scaled, LANES - half_rot, 1), 0.0)
    up = jnp.where(
        jnp.logical_and(lane >= half_rot, lane < ROT), pltpu.roll(scaled, half_rot, 1), 0.0
    )
    if sign < 0:
        return first * cosine + (down - up)
    return first * cosine + (up - down) * sine


def front_kernel(
    order,
    side_ref,
    x_ref,
    cot_ref,
    gain_ref,
    bias_ref,
    w_ref,
    b_ref,
    wo_ref,
    cos_ref,
    sin_ref,
    attn_o,
    mlp_o,
    cot_o,
    kv_o,
    qg_o,
):
    step = pl.program_id(0)
    blk = x_ref.shape[1]
    half = x_ref.shape[2] // 2
    own_heads = kv_o.shape[-1] // (2 * HD)
    width = own_heads * HD
    chunk = 64

    @pl.when(step == 0)
    def _():
        for lh in range(2):

            def norm(i, _):
                at = pl.ds(pl.multiple_of(i * chunk, chunk), chunk)
                to = pl.ds(pl.multiple_of(lh * blk + i * chunk, chunk), chunk)
                x = x_ref[order[lh], at, :]
                centred = x - jnp.mean(x, axis=-1, keepdims=True)
                variance = jnp.mean(centred * centred, axis=-1, keepdims=True)
                unit = centred * lax.rsqrt(variance + norm_epsilon)
                a = (unit * gain_ref[0:1, :] + bias_ref[0:1, :]).astype(BF16)
                m = (unit * gain_ref[1:2, :] + bias_ref[1:2, :]).astype(BF16)
                c = cot_ref[order[lh], at, :].astype(BF16)
                for out, value in ((attn_o, a), (mlp_o, m), (cot_o, c)):
                    out[0, to, :] = value[:, :half]
                    out[1, to, :] = value[:, half:]
                return 0

            lax.fori_loop(0, blk // chunk, norm, 0)

        def out_grad(h, _):
            at = pl.ds(pl.multiple_of(h * HD, HD), HD)
            g = nt(cot_o[0], wo_ref[at, :half]) + nt(cot_o[1], wo_ref[at, half:])
            g = g.astype(BF16).reshape(2, blk, HD)
            which = jnp.where(h // own_heads == side_ref[0], 0, 1)
            for k in range(own_heads):

                @pl.when(lax.rem(h, own_heads) == k)
                def _():
                    qg_o[which, :, :, width + k * HD : width + (k + 1) * HD] = g

            return 0

        lax.fori_loop(0, 2 * own_heads, out_grad, 0)

    head, kind = step // 3, lax.rem(step, 3)
    z = nn(attn_o[0], w_ref[:half, :]) + nn(attn_o[1], w_ref[half:, :]) + b_ref[0]
    which = jnp.where(head // own_heads == side_ref[0], 0, 1)
    first = z[:, :LANES]
    turned = turn(first, cos_ref[...], sin_ref[...], 1)
    first = jnp.where(kind < 2, turned, first).astype(BF16).reshape(2, blk, LANES)
    rest = z[:, LANES:].astype(BF16).reshape(2, blk, HD - LANES)
    for k in range(own_heads):
        for what, out, base in ((0, qg_o, 0), (1, kv_o, 0), (2, kv_o, width)):

            @pl.when(jnp.logical_and(kind == what, lax.rem(head, own_heads) == k))
            def _():
                at = base + k * HD
                out[which, :, :, at : at + LANES] = first
                out[which, :, :, at + LANES : at + HD] = rest


def front(order, side, stream_in, cotangent, ln_gain, ln_bias, w_qkv, b_qkv, w_out, cosine, sine):
    rows, model = stream_in.shape
    blk, half = rows // 2, model // 2
    tiles = w_qkv.shape[1] // HD
    width = w_out.shape[0] // 2
    whole = lambda a: pl.BlockSpec(a.shape, lambda i, *_: (0,) * a.ndim)
    tokens = jax.ShapeDtypeStruct((2, rows, half), BF16)
    heads = jax.ShapeDtypeStruct((2, 2, blk, 2 * width), BF16)
    outs = (tokens, tokens, tokens, heads, heads)
    x, c = stream_in.reshape(2, blk, model), cotangent.reshape(2, blk, model)
    b = b_qkv.reshape(tiles, 1, HD)
    return pl.pallas_call(
        front_kernel,
        name="front",
        out_shape=outs,
        grid_spec=pltpu.PrefetchScalarGridSpec(
            num_scalar_prefetch=2,
            grid=(tiles,),
            in_specs=[
                whole(x),
                whole(c),
                whole(ln_gain),
                whole(ln_bias),
                pl.BlockSpec((model, HD), lambda i, *_: (0, i)),
                pl.BlockSpec((1, 1, HD), lambda i, *_: (i, 0, 0)),
                whole(w_out),
                whole(cosine),
                whole(sine),
            ],
            out_specs=[whole(o) for o in outs],
        ),
        cost_estimate=pl.CostEstimate(
            flops=2 * rows * model * (w_qkv.shape[1] + w_out.shape[0]),
            transcendentals=rows,
            bytes_accessed=2 * w_qkv.size + 2 * w_out.size + 8 * x.size + 10 * x.size,
        ),
        compiler_params=pltpu.CompilerParams(vmem_limit_bytes=50 * 1024 * 1024),
    )(order, side, x, c, ln_gain, ln_bias, w_qkv, b, w_out, cosine, sine)


DOWN, UP, OUT, QKV = range(4)
(Y_KV, Y_QG, Y_COT, Y_MLP, Y_ATTN, Y_ACT, Y_HID, Y_ATT, Y_GQKV, Y_FIN) = range(10)
BRANCH, MLPB, ATTNB = range(3)


def middle_kernel(
    line,
    n_tp,
    kv_in,
    qg_in,
    attn_in,
    mlp_in,
    cot_in,
    w_up,
    w_down,
    w_out,
    w_qkv,
    b_up,
    row_pos,
    col_pos,
    cosine,
    sine,
    down_o,
    up_o,
    out_o,
    qkv_o,
    branch_o,
    mlpb_o,
    attnb_o,
    bup_o,
    bqkv_o,
    kv_all,
    qg_all,
    rs_down,
    rs_up,
    rs_out,
    rs_qkv,
    attn_far,
    cot,
    cot_far,
    norm,
    norm_far,
    act,
    hid,
    act_far,
    hid_far,
    wcol,
    wrow,
    c_down,
    c_up,
    c_out,
    c_qkv,
    stage_down,
    stage_up,
    stage_out,
    stage_qkv,
    tp_part,
    tp_recv,
    kv_own,
    qg_own,
    chunk,
    att,
    att_far,
    stats,
    stats_all,
    gqkv,
    gqkv_far,
    acc_a,
    acc_b,
    run_m,
    run_l,
    ag_s,
    ag_r,
    y_s,
    y_r,
    core_s,
    core_r,
    rs_s,
    rs_r,
    tp_s,
    tp_r,
    st_s,
    st_r,
    local,
    wsem,
    csem,
    tsem,
):
    me, tp = lax.axis_index("ctx"), lax.axis_index("tp")
    z, y = me // 2, lax.rem(me, 2)
    core = lax.rem(tp, 2)
    partner = (me + 1 - 2 * y, tp)
    sibling = (me, tp + 1 - 2 * core)
    right, left = (me + 2, tp), (me - 2, tp)
    far_steps = []
    step = 2
    while step < n_tp:
        far_steps.append((me, tp + step - 2 * step * lax.rem(tp // step, 2)))
        step *= 2

    rows = norm.shape[1]
    blk = rows // 2
    half = norm.shape[2]
    hidden_half = act.shape[2]
    own_heads = kv_own.shape[-1] // (2 * HD)
    width = own_heads * HD
    block_cols = 2 * half // line
    scale = HD ** (-0.5)

    def place_of(j):
        return lax.rem(z + j, line) * 2 + y

    barrier = pltpu.get_barrier_semaphore()
    greet = [partner, sibling] + far_steps + [(place_of(j), tp) for j in range(1, line)]
    for device in greet:
        pl.semaphore_signal(barrier, inc=1, device_id=device, device_id_type=MESH)
    pl.semaphore_wait(barrier, len(greet))

    def rcopy(src, dst, s, r, device):
        return pltpu.make_async_remote_copy(
            src_ref=src, dst_ref=dst, send_sem=s, recv_sem=r, device_id=device, device_id_type=MESH
        )

    def lcopy(src, dst, sem):
        return pltpu.make_async_copy(src, dst, sem)

    def fin_parts(t):
        c = (c_down, c_up, c_out, c_qkv)[t]
        if t == DOWN:
            dst = down_o.at[pl.ds(pl.multiple_of(y * hidden_half, hidden_half), hidden_half), :]
        elif t == UP:
            dst = up_o.at[:, pl.ds(pl.multiple_of(y * hidden_half, hidden_half), hidden_half)]
        elif t == OUT:
            dst = out_o.at[pl.ds(pl.multiple_of(y * width, width), width), :]
        else:
            dst = qkv_o.at[:, pl.ds(pl.multiple_of(y * 3 * width, 3 * width), 3 * width)]
        return c, dst

    def y_copy(item, t=0):
        if item == Y_KV:
            src, dst = kv_in.at[1], kv_all.at[:, 1]
        elif item == Y_QG:
            src, dst = qg_in.at[1], qg_all.at[:, 1]
        elif item == Y_COT:
            src, dst = cot_in.at[core], cot_far.at[core]
        elif item == Y_MLP:
            src, dst = mlp_in.at[core], norm_far.at[core]
        elif item == Y_ATTN:
            src, dst = attn_in.at[core], attn_far.at[core]
        elif item == Y_ACT:
            src, dst = act.at[1 - y], act_far
        elif item == Y_HID:
            src, dst = hid.at[1 - y], hid_far
        elif item == Y_ATT:
            src, dst = att.at[:, 1], att_far
        elif item == Y_GQKV:
            src, dst = gqkv.at[:, 1], gqkv_far
        else:
            c, dst = fin_parts(t)
            src = c.at[0, 1 - y]
            item = Y_FIN + t
        return rcopy(src, dst, y_s.at[item], y_r.at[item], partner)

    def core_copy(k):
        ref = (cot_far, norm_far, attn_far)[k]
        return rcopy(ref.at[core], ref.at[core], core_s.at[k], core_r.at[k], sibling)

    def pass_on(item, k):
        y_copy(item).wait_recv()
        core_copy(k).start()

    def ag_copy(t, h, to, hop, j_src, j_dst):
        ref = (kv_all, qg_all)[t]
        return rcopy(
            ref.at[:, 2 * j_src + h],
            ref.at[:, 2 * j_dst + h],
            ag_s.at[t, h, to, hop],
            ag_r.at[t, h, j_dst],
            (right, left)[to],
        )

    def ag_wait(t, h, hop):
        @pl.when(z >= hop)
        def _():
            ag_copy(t, h, 0, hop, line - hop, line - hop).wait_recv()

        @pl.when(z + hop <= line - 1)
        def _():
            ag_copy(t, h, 1, hop, hop, hop).wait_recv()

    def ag_send_when(hop):
        return (
            jnp.logical_and(z >= hop - 1, z <= line - 2),
            jnp.logical_and(z + hop - 1 <= line - 1, z >= 1),
        )

    def ag_hop(t, h, hop):
        if not (isinstance(hop, int) and hop == 1):
            ag_wait(t, h, hop - 1)
        to_right, to_left = ag_send_when(hop)

        @pl.when(to_right)
        def _():
            ag_copy(t, h, 0, hop, lax.rem(line - hop + 1, line), line - hop).start()

        @pl.when(to_left)
        def _():
            ag_copy(t, h, 1, hop, hop - 1, hop).start()

    def ag_rest(t, h, hop):
        def one(i, _):
            ag_hop(t, h, i)
            return 0

        if hop < line:
            lax.fori_loop(hop, line, one, 0)
        ag_wait(t, h, line - 1)

    def ag_drain(t, h):
        def one(hop, _):
            to_right, to_left = ag_send_when(hop)

            @pl.when(to_right)
            def _():
                ag_copy(t, h, 0, hop, lax.rem(line - hop + 1, line), line - hop).wait_send()

            @pl.when(to_left)
            def _():
                ag_copy(t, h, 1, hop, hop - 1, hop).wait_send()

            return 0

        lax.fori_loop(1, line, one, 0)

    rs = (
        (c_down, rs_down, stage_down),
        (c_up, rs_up, stage_up),
        (c_out, rs_out, stage_out),
        (c_qkv, rs_qkv, stage_qkv),
    )

    def rs_copy(t, j, slot, device):
        c, recv, _ = rs[t]
        return rcopy(c.at[j], recv.at[slot], rs_s.at[t, j], rs_r.at[t, slot], device)

    def rs_take(t, j, slot):
        c, recv, held = rs[t]
        rs_copy(t, j, slot, partner).wait_recv()
        copy = lcopy(recv.at[slot], held, tsem.at[t])
        copy.start()
        copy.wait()
        n = c.shape[2]
        part = min(64, n)

        def add(i, _):
            at = pl.ds(pl.multiple_of(i * part, part), part)
            for s in range(2):
                c[j, s, at, :] = (c[j, s, at, :].astype(F32) + held[s, at, :].astype(F32)).astype(
                    BF16
                )
            return 0

        lax.fori_loop(0, n // part, add, 0)

    def rs_step(t, hop):
        jr, jl = line - hop, hop

        @pl.when(hop >= z + 1)
        def _():
            @pl.when(z >= 1)
            def _():
                rs_take(t, jr, jr)

            rs_copy(t, jr, jr - 1, right).start()

        @pl.when(hop >= line - z)
        def _():
            @pl.when(z <= line - 2)
            def _():
                rs_take(t, jl, jl)

            rs_copy(t, jl, jl + 1, left).start()

    def rs_rest(t, hop):
        def one(i, _):
            rs_step(t, i)
            return 0

        if hop < line:
            lax.fori_loop(hop, line, one, 0)

    def rs_finish(t):
        @pl.when(z >= 1)
        def _():
            rs_take(t, 0, 0)

        @pl.when(z <= line - 2)
        def _():
            rs_take(t, 0, line)

        c, dst = fin_parts(t)
        y_copy(Y_FIN, t).start()
        lcopy(c.at[0, y], dst, local.at[4 + t]).start()

    def rs_drain(t):
        def one(j, _):
            @pl.when(j <= line - 1 - z)
            def _():
                rs_copy(t, j, j - 1, right).wait_send()

            @pl.when(j > line - 1 - z)
            def _():
                rs_copy(t, j, j + 1, left).wait_send()

            return 0

        lax.fori_loop(1, line, one, 0)
        c, dst = fin_parts(t)
        y_copy(Y_FIN, t).wait()
        lcopy(c.at[0, y], dst, local.at[4 + t]).wait()

    tp_out = (branch_o, mlpb_o, attnb_o)
    last = len(far_steps) + 1

    def tp_copy(i, k):
        part = tp_part.at[i]
        if k == 0:
            src, dst, device = part.at[1 - core], tp_recv.at[i, 0], sibling
        elif k < last:
            src, dst, device = part.at[core], tp_recv.at[i, k], far_steps[k - 1]
        else:
            src, dst, device = part.at[core], tp_out[i].at[core], sibling
        return rcopy(src, dst, tp_s.at[i, k], tp_r.at[i, k], device)

    def tp_add(i, k):
        part = 64

        def add(n, _):
            at = pl.ds(pl.multiple_of(n * part, part), part)
            tp_part[i, core, at, :] = (
                tp_part[i, core, at, :].astype(F32) + tp_recv[i, k, at, :].astype(F32)
            ).astype(BF16)
            return 0

        lax.fori_loop(0, blk // part, add, 0)

    def tp_next(i, k):
        if k > 1:
            tp_copy(i, k - 1).wait_send()
        tp_copy(i, k - 1).wait_recv()
        tp_add(i, k - 1)
        tp_copy(i, k).start()
        if k == last:
            lcopy(tp_part.at[i, core], tp_out[i].at[core], local.at[8 + i]).start()

    def tp_rest(i):
        for k in range(1, last + 1):
            tp_next(i, k)

    def tp_drain(i):
        tp_copy(i, 0).wait_send()
        tp_copy(i, last).wait()
        lcopy(tp_part.at[i, core], tp_out[i].at[core], local.at[8 + i]).wait()

    def stream(lo, hi, fetches, body):
        for f in fetches:
            f(lo, lax.rem(lo, 2)).start()

        def one(i, _):
            slot = lax.rem(i, 2)

            @pl.when(i + 1 < hi)
            def _():
                for f in fetches:
                    f(i + 1, 1 - slot).start()

            for f in fetches:
                f(i, slot).wait()
            body(i, slot)
            return 0

        lax.fori_loop(lo, hi, one, 0)

    def col_tile(w):
        def fetch(i, slot):
            at = pl.ds(pl.multiple_of(i * TILE, TILE), TILE)
            return lcopy(w.at[:, at], wcol.at[slot, pl.ds(0, w.shape[0]), :], wsem.at[0, slot])

        return fetch

    def row_tile(w):
        def fetch(i, slot):
            at = pl.ds(pl.multiple_of(i * TILE, TILE), TILE)
            return lcopy(w.at[at, :], wrow.at[slot, pl.ds(0, TILE), pl.ds(0, w.shape[1])], wsem.at[1, slot])

        return fetch

    kv_own_load = lcopy(kv_in.at[0], kv_own.at[:, 0], local.at[11])
    qg_own_load = lcopy(qg_in.at[0], qg_own.at[:, 0], local.at[12])
    norm_load = lcopy(mlp_in, norm, local.at[2])
    cot_load = lcopy(cot_in, cot, local.at[3])
    y_copy(Y_KV).start()
    y_copy(Y_COT).start()
    kv_own_load.start()
    qg_own_load.start()
    norm_load.start()
    cot_load.start()
    kv_own_load.wait()
    lcopy(kv_own.at[:, 0], kv_all.at[:, 0], local.at[0]).start()
    qg_own_load.wait()
    lcopy(qg_own.at[:, 0], qg_all.at[:, 0], local.at[1]).start()
    norm_load.wait()
    cot_load.wait()
    lcopy(kv_own.at[:, 0], kv_all.at[:, 0], local.at[0]).wait()
    ag_hop(0, 0, 1)

    def feed_forward(i, slot):
        h = nn(norm[0], wcol[slot, :half, :]) + nn(norm[1], wcol[slot, half : 2 * half, :]) + b_up[i]
        gate = 0.5 * (1.0 + lax.erf(h * root_half))
        slope = gate + h * jnp.exp(-0.5 * h * h) * inverse_root_two_pi
        g = nt(cot[0], wrow[slot, :TILE, :half]) + nt(cot[1], wrow[slot, :TILE, half : 2 * half])
        g = g * slope
        bup_o[i] = jnp.sum(g, axis=0, keepdims=True)
        at = pl.ds(pl.multiple_of(lax.rem(i * TILE, hidden_half), TILE), TILE)
        which = i * TILE // hidden_half
        act[which, :, at] = (h * gate).astype(BF16)
        hid[which, :, at] = g.astype(BF16)

    hidden_tiles = 2 * hidden_half // TILE
    cut = hidden_tiles // 2
    stream(0, cut, (col_tile(w_up), row_tile(w_down)), feed_forward)

    y_copy(Y_KV).wait_recv()
    ag_hop(0, 1, 1)
    pass_on(Y_COT, 0)
    ag_hop(0, 0, 2)

    stream(cut, hidden_tiles, (col_tile(w_up), row_tile(w_down)), feed_forward)
    y_copy(Y_ACT).start()
    y_copy(Y_MLP).start()
    y_copy(Y_HID).start()
    y_copy(Y_QG).start()
    ag_hop(0, 1, 2)

    def part_tile(i, slot, value):
        at = pl.ds(pl.multiple_of(i * TILE, TILE), TILE)
        return at, value.astype(BF16).reshape(2, blk, TILE)

    def mlp_back(i, slot):
        value = nt(hid[0], wrow[slot, :TILE, :hidden_half]) + nt(hid[1], wrow[slot, :TILE, hidden_half : 2 * hidden_half])
        at, value = part_tile(i, slot, value)
        tp_part[MLPB, :, :, at] = value

    model_tiles = 2 * half // TILE
    stream(0, model_tiles, (row_tile(w_up),), mlp_back)
    tp_copy(MLPB, 0).start()
    ag_rest(0, 0, 3)

    def cols_at(ref, j):
        start = lax.rem(z + j, line) * block_cols
        at = pl.ds(pl.multiple_of(lax.rem(start, half), LANES), block_cols)
        return ref[start // half, :, at]

    def split_cols(ref, j, at, value):
        n = value.shape[1] // 2
        ref[j, 0, at, :] = value[:, :n].astype(BF16)
        ref[j, 1, at, :] = value[:, n:].astype(BF16)

    def split_rows(ref, j, at, value):
        n = value.shape[0] // 2
        ref[j, 0, :, at] = value[:n].astype(BF16)
        ref[j, 1, :, at] = value[n:].astype(BF16)

    y_copy(Y_ACT).wait_recv()
    core_copy(0).wait_recv()

    def share_down(j, _):
        g0, g1 = cols_at(cot, j), cols_at(cot_far, j)

        def one(i, _):
            at = pl.ds(pl.multiple_of(i * TILE, TILE), TILE)
            split_cols(c_down, j, at, tn(act[y, :, at], g0) + tn(act_far[:, at], g1))
            return 0

        lax.fori_loop(0, hidden_half // TILE, one, 0)
        return 0

    lax.fori_loop(0, line, share_down, 0)
    rs_step(DOWN, 1)
    tp_next(MLPB, 1)
    ag_hop(0, 1, 3) if line > 3 else None
    pass_on(Y_MLP, 1)

    y_copy(Y_HID).wait_recv()
    core_copy(1).wait_recv()

    def share_up(j, _):
        m0, m1 = cols_at(norm, j), cols_at(norm_far, j)

        def one(i, _):
            at = pl.ds(pl.multiple_of(i * TILE, TILE), TILE)
            split_rows(c_up, j, at, tn(m0, hid[y, :, at]) + tn(m1, hid_far[:, at]))
            return 0

        lax.fori_loop(0, hidden_half // TILE, one, 0)
        return 0

    lax.fori_loop(0, line, share_up, 0)
    rs_step(UP, 1)
    y_copy(Y_QG).wait_recv()
    lcopy(qg_own.at[:, 0], qg_all.at[:, 0], local.at[1]).wait()
    ag_hop(1, 0, 1)
    ag_hop(1, 1, 1)
    y_copy(Y_ATTN).start()
    ag_rest(0, 1, 4 if line > 3 else 3)
    lcopy(kv_all.at[:, 1], kv_own.at[:, 1], local.at[11]).start()
    lcopy(qg_all.at[:, 1], qg_own.at[:, 1], local.at[12]).start()
    lcopy(kv_all.at[:, 1], kv_own.at[:, 1], local.at[11]).wait()
    lcopy(qg_all.at[:, 1], qg_own.at[:, 1], local.at[12]).wait()

    pair = 2 * blk
    same = lax.broadcasted_iota(jnp.int32, (pair, pair), 0) == lax.broadcasted_iota(
        jnp.int32, (pair, pair), 1
    )

    def piece(t):
        def fetch(i, slot):
            ref = (kv_all, qg_all)[t]
            return lcopy(
                ref.at[i // line, pl.ds(2 * lax.rem(i, line), 2)], chunk.at[slot], csem.at[slot]
            )

        return fetch

    def heads_of(value, at):
        return value[:, :, at : at + HD].reshape(pair, HD)

    for lh in range(2):
        for head in range(own_heads):
            at_k, at_v = head * HD, width + head * HD
            run_m[...] = jnp.full(run_m.shape, masked_value, F32)
            run_l[...] = jnp.zeros(run_l.shape, F32)
            acc_a[...] = jnp.zeros(acc_a.shape, F32)

            def attend(i, slot):
                k = chunk[slot, :, :, at_k : at_k + HD].reshape(pair, HD)
                v = chunk[slot, :, :, at_v : at_v + HD].reshape(pair, HD)
                q = qg_own[lh, :, :, at_k : at_k + HD].reshape(pair, HD)
                s = nt(q, k) * scale
                s = jnp.where(row_pos[i] <= col_pos[lh], s, masked_value)
                old = run_m[...]
                top = jnp.maximum(old, jnp.max(s, axis=1, keepdims=True))
                p = jnp.exp(s - top)
                fade = jnp.exp(old - top)
                run_m[...] = top
                run_l[...] = run_l[...] * fade + jnp.sum(p, axis=1, keepdims=True)
                acc_a[...] = acc_a[...] * fade + nn(p.astype(BF16), v)

            stream(0, line * (lh + 1), (piece(0),), attend)
            out = (acc_a[...] / run_l[...]).astype(BF16)
            att[lh, :, :, at_k : at_k + HD] = out.reshape(2, blk, HD)
            log_total = run_m[...] + jnp.log(run_l[...])
            g = qg_own[lh, :, :, at_v : at_v + HD].reshape(pair, HD)
            dots = jnp.sum(g.astype(F32) * out.astype(F32), axis=1, keepdims=True)
            stats[lh, head, 0:1, :] = jnp.sum(jnp.where(same, log_total, 0.0), 0, keepdims=True)
            stats[lh, head, 1:2, :] = jnp.sum(jnp.where(same, dots, 0.0), 0, keepdims=True)
        if lh == 0:
            rs_step(DOWN, 2)

    def stat_copy(j, k):
        return rcopy(
            stats, stats_all.at[line - j], st_s.at[j], st_r.at[line - j], (place_of(j), tp)
        )

    for j in range(1, line):
        stat_copy(j, 0).start()
    y_copy(Y_ATT).start()
    ag_hop(1, 0, 2)
    ag_hop(1, 1, 2)
    tp_next(MLPB, 2)
    rs_step(UP, 2)

    def undo(value, lh, head, kind):
        at = (3 * head + kind) * HD
        value = value[...]
        first = value[:, :LANES]
        if kind < 2:
            first = turn(first, cosine[lh], sine[lh], -1)
        for lo, hi, part in ((0, LANES, first), (LANES, HD, value[:, LANES:])):
            bqkv_o[0:1, at + lo : at + hi] += jnp.sum(part, axis=0, keepdims=True)
            gqkv[lh, :, :, at + lo : at + hi] = part.astype(BF16).reshape(2, blk, hi - lo)

    bqkv_o[...] = jnp.zeros(bqkv_o.shape, F32)
    for lh in range(2):
        for head in range(own_heads):
            at_k, at_v = head * HD, width + head * HD
            run_m[...] = jnp.sum(
                jnp.where(same, stats[lh, head, 0:1, :], 0.0), axis=1, keepdims=True
            )
            run_l[...] = jnp.sum(
                jnp.where(same, stats[lh, head, 1:2, :], 0.0), axis=1, keepdims=True
            )
            acc_a[...] = jnp.zeros(acc_a.shape, F32)

            def back_q(i, slot):
                k = chunk[slot, :, :, at_k : at_k + HD].reshape(pair, HD)
                v = chunk[slot, :, :, at_v : at_v + HD].reshape(pair, HD)
                q = qg_own[lh, :, :, at_k : at_k + HD].reshape(pair, HD)
                g = qg_own[lh, :, :, at_v : at_v + HD].reshape(pair, HD)
                s = nt(q, k) * scale
                s = jnp.where(row_pos[i] <= col_pos[lh], s, masked_value)
                p = jnp.exp(s - run_m[...])
                ds = (p * (nt(g, v) - run_l[...]) * scale).astype(BF16)
                acc_a[...] += nn(ds, k)

            stream(0, line * (lh + 1), (piece(0),), back_q)
            undo(acc_a, lh, head, 0)

    def share_out(j, _):
        g0, g1 = cols_at(cot, j), cols_at(cot_far, j)

        def one(i, _):
            at = pl.ds(pl.multiple_of(i * TILE, TILE), TILE)
            a0 = att[:, 0, :, at].reshape(rows, TILE)
            a1 = att[:, 1, :, at].reshape(rows, TILE)
            split_cols(c_out, j, at, tn(a0, g0) + tn(a1, g1))
            return 0

        lax.fori_loop(0, width // TILE, one, 0)
        return 0

    lax.fori_loop(0, line, share_out, 0)
    rs_step(OUT, 1)
    rs_step(DOWN, 3) if line > 3 else None
    ag_rest(1, 0, 3)
    ag_rest(1, 1, 3)

    y_copy(Y_ATT).wait_recv()

    def branch(i, slot):
        value = nn(act[0], wcol[slot, :hidden_half, :]) + nn(act[1], wcol[slot, hidden_half : 2 * hidden_half, :])
        at, _ = part_tile(i, slot, value)
        own = att[:, 0].reshape(rows, width)
        far = att_far[...].reshape(rows, width)
        mine = wrow[0, pl.ds(pl.multiple_of(y * width, width), width), at]
        theirs = wrow[0, pl.ds(pl.multiple_of((1 - y) * width, width), width), at]
        value += nn(own, mine) + nn(far, theirs)
        tp_part[BRANCH, :, :, at] = value.astype(BF16).reshape(2, blk, TILE)

    w_out_load = lcopy(w_out, wrow.at[0, pl.ds(0, w_out.shape[0]), :], wsem.at[1, 0])
    w_out_load.start()
    w_out_load.wait()
    stream(0, model_tiles, (col_tile(w_down),), branch)
    tp_copy(BRANCH, 0).start()
    rs_step(UP, 3) if line > 3 else None

    for j in range(1, line):
        stat_copy(line - j, 0).wait_recv()
    lcopy(stats, stats_all.at[0], local.at[0]).start()
    lcopy(stats, stats_all.at[0], local.at[0]).wait()

    for lh in range(2):
        for head in range(own_heads):
            at_k, at_v = head * HD, width + head * HD
            acc_a[...] = jnp.zeros(acc_a.shape, F32)
            acc_b[...] = jnp.zeros(acc_b.shape, F32)

            def back_k(i, slot):
                q = chunk[slot, :, :, at_k : at_k + HD].reshape(pair, HD)
                g = chunk[slot, :, :, at_v : at_v + HD].reshape(pair, HD)
                k = kv_own[lh, :, :, at_k : at_k + HD].reshape(pair, HD)
                v = kv_own[lh, :, :, at_v : at_v + HD].reshape(pair, HD)
                stat = stats_all[lax.rem(i, line), i // line, head]
                s = nt(k, q) * scale
                s = jnp.where(col_pos[lh] <= row_pos[i], s, masked_value)
                p = jnp.exp(s - stat[0:1, :])
                ds = (p * (nt(v, g) - stat[1:2, :]) * scale).astype(BF16)
                acc_a[...] += nn(ds, q)
                acc_b[...] += nn(p.astype(BF16), g)

            stream(lh * line, 2 * line, (piece(1),), back_k)
            undo(acc_a, lh, head, 1)
            undo(acc_b, lh, head, 2)
    y_copy(Y_GQKV).start()
    tp_next(BRANCH, 1)
    pass_on(Y_ATTN, 2)
    norm_again = lcopy(attn_in, norm, local.at[2])
    norm_again.start()
    core_copy(2).wait_recv()
    far_again = lcopy(attn_far, norm_far, local.at[3])
    core_copy(1).wait_send()
    far_again.start()
    norm_again.wait()
    far_again.wait()

    def share_qkv(j, _):
        m0, m1 = cols_at(norm, j), cols_at(norm_far, j)

        def one(i, _):
            at = pl.ds(pl.multiple_of(i * TILE, TILE), TILE)
            g0 = gqkv[:, 0, :, at].reshape(rows, TILE)
            g1 = gqkv[:, 1, :, at].reshape(rows, TILE)
            split_rows(c_qkv, j, at, tn(m0, g0) + tn(m1, g1))
            return 0

        lax.fori_loop(0, 3 * width // TILE, one, 0)
        return 0

    lax.fori_loop(0, line, share_qkv, 0)
    rs_step(QKV, 1)
    rs_step(OUT, 2)
    y_copy(Y_GQKV).wait_recv()

    def attn_back(i, slot):
        own = gqkv[:, 0].reshape(rows, 3 * width)
        far = gqkv_far[...].reshape(rows, 3 * width)
        mine = wrow[slot, :TILE, pl.ds(pl.multiple_of(y * 3 * width, 3 * width), 3 * width)]
        theirs = wrow[slot, :TILE, pl.ds(pl.multiple_of((1 - y) * 3 * width, 3 * width), 3 * width)]
        at, value = part_tile(i, slot, nt(own, mine) + nt(far, theirs))
        tp_part[ATTNB, :, :, at] = value

    stream(0, model_tiles, (row_tile(w_qkv),), attn_back)
    tp_copy(ATTNB, 0).start()
    tp_next(BRANCH, 2)
    tp_next(ATTNB, 1)
    rs_rest(DOWN, 4 if line > 3 else 3)
    rs_rest(UP, 4 if line > 3 else 3)
    rs_finish(DOWN)
    rs_finish(UP)
    rs_step(QKV, 2)
    tp_next(ATTNB, 2)
    rs_rest(OUT, 3)
    rs_rest(QKV, 3)
    rs_finish(OUT)
    rs_finish(QKV)

    for t in range(2):
        for h in range(2):
            ag_drain(t, h)
    for item in (Y_KV, Y_QG, Y_COT, Y_MLP, Y_ATTN, Y_ACT, Y_HID, Y_ATT, Y_GQKV):
        y_copy(item).wait_send()
    core_copy(0).wait_send()
    core_copy(2).wait_send()
    for j in range(1, line):
        stat_copy(j, 0).wait_send()
    for i in range(3):
        tp_drain(i)
    for t in range(4):
        rs_drain(t)


def middle(line, n_tp, kv, qg, attn_in, mlp_in, cot_b, w_up, w_down, w_out, w_qkv, b_up, row_pos, col_pos, cosine, sine):
    _, rows, half = mlp_in.shape
    model = 2 * half
    blk = rows // 2
    hidden = w_up.shape[1]
    hidden_half = hidden // 2
    width = kv.shape[-1] // 2
    own_heads = width // HD
    part_cols = model // line // 2
    pair = 2 * blk
    tp_steps = 0
    while (2 << tp_steps) < n_tp:
        tp_steps += 1
    shares = (
        (2, hidden_half, part_cols),
        (2, part_cols, hidden_half),
        (2, width, part_cols),
        (2, part_cols, 3 * width),
    )
    b = lambda *s: jax.ShapeDtypeStruct(s, BF16)
    f = lambda *s: jax.ShapeDtypeStruct(s, F32)
    vb = lambda *s: pltpu.VMEM(s, BF16)
    vf = lambda *s: pltpu.VMEM(s, F32)
    dma = pltpu.SemaphoreType.DMA
    outs = (
        b(hidden, part_cols),
        b(part_cols, hidden),
        b(2 * width, part_cols),
        b(part_cols, 6 * width),
        b(2, blk, model),
        b(2, blk, model),
        b(2, blk, model),
        f(hidden // TILE, 1, TILE),
        f(1, 3 * width),
        b(2, 2 * line, blk, 2 * width),
        b(2, 2 * line, blk, 2 * width),
        b(line + 1, *shares[0]),
        b(line + 1, *shares[1]),
        b(line + 1, *shares[2]),
        b(line + 1, *shares[3]),
        b(2, rows, half),
    )
    out_specs = [ANY] * 7 + [VMEM] * 2 + [ANY] * 7
    wide = max(model, hidden)
    scratch = [
        vb(2, rows, half),
        vb(2, rows, half),
        vb(2, rows, half),
        vb(2, rows, half),
        vb(2, rows, hidden_half),
        vb(2, rows, hidden_half),
        vb(rows, hidden_half),
        vb(rows, hidden_half),
        vb(2, wide, TILE),
        vb(2, max(TILE, 2 * width), wide),
        vb(line, *shares[0]),
        vb(line, *shares[1]),
        vb(line, *shares[2]),
        vb(line, *shares[3]),
        vb(*shares[0]),
        vb(*shares[1]),
        vb(*shares[2]),
        vb(*shares[3]),
        vb(3, 2, blk, model),
        vb(3, tp_steps + 1, blk, model),
        vb(2, 2, blk, 2 * width),
        vb(2, 2, blk, 2 * width),
        vb(2, 2, blk, 2 * width),
        vb(2, 2, blk, width),
        vb(2, blk, width),
        vf(2, own_heads, 2, pair),
        vf(line, 2, own_heads, 2, pair),
        vb(2, 2, blk, 3 * width),
        vb(2, blk, 3 * width),
        vf(pair, HD),
        vf(pair, HD),
        vf(pair, 1),
        vf(pair, 1),
        dma((2, 2, 2, line)),
        dma((2, 2, line)),
        dma((Y_FIN + 4,)),
        dma((Y_FIN + 4,)),
        dma((3,)),
        dma((3,)),
        dma((4, line)),
        dma((4, line + 1)),
        dma((3, tp_steps + 2)),
        dma((3, tp_steps + 2)),
        dma((line,)),
        dma((line,)),
        dma((13,)),
        dma((2, 2)),
        dma((2,)),
        dma((4,)),
    ]
    return pl.pallas_call(
        functools.partial(middle_kernel, line, n_tp),
        name="middle",
        out_shape=outs,
        in_specs=[ANY] * 9 + [VMEM] * 5,
        out_specs=out_specs,
        scratch_shapes=scratch,
        cost_estimate=pl.CostEstimate(
            flops=30 * rows * model * hidden, transcendentals=rows * hidden, bytes_accessed=8 * w_up.size
        ),
        compiler_params=pltpu.CompilerParams(
            collective_id=0, has_side_effects=True, vmem_limit_bytes=63 * 1024 * 1024
        ),
    )(kv, qg, attn_in, mlp_in, cot_b, w_up, w_down, w_out, w_qkv, b_up, row_pos, col_pos, cosine, sine)


def normalize_back(incoming, unit_field, inv_scale, gain_row):
    unit_grad = incoming * gain_row
    return inv_scale * (
        unit_grad
        - jnp.mean(unit_grad, axis=-1, keepdims=True)
        - unit_field * jnp.mean(unit_grad * unit_field, axis=-1, keepdims=True)
    )


def shards(
    n_ctx,
    n_tp,
    stream_in,
    cotangent,
    ln_gain,
    ln_bias,
    w_qkv,
    b_qkv,
    w_out,
    out_bias,
    w_up,
    b_up,
    w_down,
    block_order,
):
    rows, model = stream_in.shape
    blk = rows // 2
    line = n_ctx // 2
    me = lax.axis_index("ctx")
    place, side = me // 2, me % 2

    numbers = jnp.sort(block_order.reshape(line, 2, 2), axis=2)
    seen = (place + jnp.arange(line)) % line
    sides = jnp.stack([side, 1 - side])
    numbers = jnp.transpose(numbers[seen][:, sides], (2, 0, 1))
    positions = numbers[..., None] * blk + jnp.arange(blk, dtype=jnp.int32)
    row_pos = positions.reshape(2 * line, 1, 2 * blk)
    own_pos = positions[:, 0].reshape(2, 2 * blk)
    col_pos = own_pos[:, :, None]
    own_blocks = lax.dynamic_slice_in_dim(block_order, 2 * me, 2)
    late_first = own_blocks[0] > own_blocks[1]
    order = jnp.stack([late_first, jnp.logical_not(late_first)]).astype(jnp.int32)
    cosine, sine = rope_tables(own_pos)
    cos_here = cosine[:, :blk].reshape(rows, LANES)
    sin_here = sine[:, :blk].reshape(rows, LANES)

    attn_in, mlp_in, cot_b, kv, qg = front(
        order,
        side.reshape(1),
        stream_in,
        cotangent,
        ln_gain,
        ln_bias,
        w_qkv,
        b_qkv,
        w_out,
        cos_here,
        sin_here,
    )
    (down, up, out, qkv, branch, mlp_total, attn_total, grad_bup, grad_bqkv, *_) = middle(
        line,
        n_tp,
        kv,
        qg,
        attn_in,
        mlp_in,
        cot_b,
        w_up,
        w_down,
        w_out,
        w_qkv,
        b_up.reshape(-1, 1, TILE),
        row_pos,
        col_pos,
        cosine,
        sine,
    )

    def stored(value):
        flipped = jnp.concatenate([value[1], value[0]], axis=0)
        straight = value.reshape(rows, model)
        return jnp.where(late_first, flipped, straight).astype(F32)

    row_mean = jnp.mean(stream_in, axis=-1, keepdims=True)
    centred = stream_in - row_mean
    variance = jnp.mean(centred * centred, axis=-1, keepdims=True)
    inv_scale = lax.rsqrt(variance + norm_epsilon)
    unit = centred * inv_scale
    attn_total, mlp_total = stored(attn_total), stored(mlp_total)
    stream_out = stream_in + out_bias + stored(branch)
    grad_in = (
        cotangent
        + normalize_back(attn_total, unit, inv_scale, ln_gain[0])
        + normalize_back(mlp_total, unit, inv_scale, ln_gain[1])
    )
    bias_half = grad_bqkv.reshape(-1)
    nothing = jnp.zeros_like(bias_half)
    parts = [
        jnp.where(
            side == 0,
            jnp.concatenate([bias_half, nothing]),
            jnp.concatenate([nothing, bias_half]),
        ),
        grad_bup.reshape(-1),
        jnp.sum(cotangent, axis=0),
        jnp.sum(attn_total * unit, axis=0),
        jnp.sum(mlp_total * unit, axis=0),
        jnp.sum(attn_total, axis=0),
        jnp.sum(mlp_total, axis=0),
    ]
    small = jnp.concatenate(parts)
    step = 1
    while step < n_ctx:
        small = small + lax.ppermute(small, "ctx", [(i, i ^ step) for i in range(n_ctx)])
        step *= 2
    cuts, at = [], 0
    for part in parts:
        cuts.append(small[at : at + part.shape[0]])
        at += part.shape[0]
    return (
        stream_out,
        grad_in,
        qkv.astype(F32),
        cuts[0],
        out.astype(F32),
        cuts[2],
        up.astype(F32),
        cuts[1],
        down.astype(F32),
        jnp.stack([cuts[3], cuts[4]]),
        jnp.stack([cuts[5], cuts[6]]),
    )


def solution(mesh):
    placed = (
        P("ctx", None),
        P("ctx", None),
        P(),
        P(),
        P(None, "tp"),
        P("tp"),
        P("tp", None),
        P(),
        P(None, "tp"),
        P("tp"),
        P("tp", None),
        P(),
    )
    return jax.shard_map(
        functools.partial(shards, mesh.shape["ctx"], mesh.shape["tp"]),
        mesh=mesh,
        in_specs=placed,
        out_specs=(
            P("ctx", None),
            P("ctx", None),
            P("ctx", "tp"),
            P("tp"),
            P("tp", "ctx"),
            P(),
            P("ctx", "tp"),
            P("tp"),
            P("tp", "ctx"),
            P(),
            P(),
        ),
        check_vma=False,
    )
```

```python
import functools
import math

import jax
import jax.numpy as jnp
import numpy as np
from jax import lax
from jax.experimental import pallas as pl
from jax.experimental.pallas import tpu as pltpu
from jax.sharding import PartitionSpec as P

HD = 256
ROT = 64
LANES = 128
TILE = 256

masked_value = -1e30
norm_epsilon = 1e-05
root_half = 0.7071067811865476
inverse_root_two_pi = 0.3989422804014327

F32 = jnp.float32
BF16 = jnp.bfloat16
MESH = pl.DeviceIdType.MESH
ANY = pl.BlockSpec(memory_space=pl.ANY)
VMEM = pl.BlockSpec(memory_space=pltpu.VMEM)
SMEM = pl.BlockSpec(memory_space=pltpu.SMEM)


def nt(a, b):
    return lax.dot_general(a, b, (((1,), (1,)), ((), ())), preferred_element_type=F32)


def nn(a, b):
    return lax.dot_general(a, b, (((1,), (0,)), ((), ())), preferred_element_type=F32)


def tn(a, b):
    return lax.dot_general(a, b, (((0,), (0,)), ((), ())), preferred_element_type=F32)


def rope_tables(positions):
    half_rot = ROT // 2
    frequency = np.exp(np.arange(half_rot) * (-2.0 * math.log(10000.0) / ROT))
    angles = np.asarray(positions, np.float64)[:, None] * frequency
    table = np.zeros((2, angles.shape[0], LANES), np.float32)
    table[0] = 1.0
    for lo in (0, half_rot):
        table[0, :, lo : lo + half_rot] = np.cos(angles)
        table[1, :, lo : lo + half_rot] = np.sin(angles)
    return table


def turn(first, cosine, sine, sign):
    half_rot = ROT // 2
    scaled = first * sine if sign < 0 else first
    lane = lax.broadcasted_iota(jnp.int32, first.shape, 1)
    down = jnp.where(lane < half_rot, pltpu.roll(scaled, LANES - half_rot, 1), 0.0)
    up = jnp.where(
        jnp.logical_and(lane >= half_rot, lane < ROT), pltpu.roll(scaled, half_rot, 1), 0.0
    )
    if sign < 0:
        return first * cosine + (down - up)
    return first * cosine + (up - down) * sine


DOWN, UP, OUT, QKV = range(4)
(Y_KV, Y_QG, Y_COT, Y_MLP, Y_ATTN, Y_ACT, Y_HID, Y_ATT, Y_GQKV, Y_FIN) = range(10)
BRANCH, MLPB, ATTNB = range(3)
S_GAIN, S_SHIFT, S_OUT, S_UP, S_QKV = 0, 2, 4, 5, 6


def layer_kernel(
    line,
    n_tp,
    order,
    stream_in,
    cotangent,
    w_up,
    w_down,
    w_out,
    w_qkv,
    gain,
    shift,
    b_qkv,
    b_up,
    out_bias,
    block_table,
    row_table,
    down_o,
    up_o,
    out_o,
    qkv_o,
    stream_o,
    grad_o,
    small_o,
    kv_all,
    qg_all,
    rs_down,
    rs_up,
    rs_out,
    rs_qkv,
    attn_far,
    tp_far,
    xbuf,
    cbuf,
    cot,
    cot_far,
    norm,
    norm_far,
    attn,
    act,
    hid,
    act_far,
    hid_far,
    wcol,
    wrow,
    c_down,
    c_up,
    c_out,
    c_qkv,
    stage_down,
    stage_up,
    stage_out,
    stage_qkv,
    tp_part,
    tp_recv,
    kv_own,
    qg_own,
    kv_away,
    qg_away,
    chunk,
    att,
    att_far,
    stats,
    stats_all,
    gqkv,
    gqkv_far,
    acc_a,
    acc_b,
    run_m,
    run_l,
    cosine,
    sine,
    small,
    small_recv,
    ag_s,
    ag_r,
    y_s,
    y_r,
    core_s,
    core_r,
    rs_s,
    rs_r,
    tp_s,
    tp_r,
    st_s,
    st_r,
    sm_s,
    sm_r,
    local,
    wsem,
    csem,
    tsem,
):
    me, tp = lax.axis_index("ctx"), lax.axis_index("tp")
    z, y = me // 2, lax.rem(me, 2)
    core = lax.rem(tp, 2)
    partner = (me + 1 - 2 * y, tp)
    sibling = (me, tp + 1 - 2 * core)
    right, left = (me + 2, tp), (me - 2, tp)
    far_steps = []
    step = 2
    while step < n_tp:
        far_steps.append((me, tp + step - 2 * step * lax.rem(tp // step, 2)))
        step *= 2

    rows = norm.shape[1]
    blk = rows // 2
    half = norm.shape[2]
    hidden_half = act.shape[2]
    own_heads = kv_own.shape[-1] // (2 * HD)
    width = own_heads * HD
    block_cols = 2 * half // line
    scale = HD ** (-0.5)

    def place_of(j):
        return lax.rem(z + j, line) * 2 + y

    barrier = pltpu.get_barrier_semaphore()
    greet = [partner, sibling] + far_steps + [(place_of(j), tp) for j in range(1, line)]
    for device in greet:
        pl.semaphore_signal(barrier, inc=1, device_id=device, device_id_type=MESH)

    def rcopy(src, dst, s, r, device):
        return pltpu.make_async_remote_copy(
            src_ref=src, dst_ref=dst, send_sem=s, recv_sem=r, device_id=device, device_id_type=MESH
        )

    def lcopy(src, dst, sem):
        return pltpu.make_async_copy(src, dst, sem)

    def fin_parts(t):
        c = (c_down, c_up, c_out, c_qkv)[t]
        if t == DOWN:
            dst = down_o.at[pl.ds(pl.multiple_of(y * hidden_half, hidden_half), hidden_half), :]
        elif t == UP:
            dst = up_o.at[:, pl.ds(pl.multiple_of(y * hidden_half, hidden_half), hidden_half)]
        elif t == OUT:
            dst = out_o.at[pl.ds(pl.multiple_of(y * width, width), width), :]
        else:
            dst = qkv_o.at[:, pl.ds(pl.multiple_of(y * 3 * width, 3 * width), 3 * width)]
        return c, dst

    def y_copy(item, t=0):
        if item == Y_KV:
            src, dst = kv_away, kv_own.at[:, 1]
        elif item == Y_QG:
            src, dst = qg_away, qg_own.at[:, 1]
        elif item == Y_COT:
            src, dst = cot.at[core], cot_far.at[core]
        elif item == Y_MLP:
            src, dst = norm.at[core], norm_far.at[core]
        elif item == Y_ATTN:
            src, dst = attn.at[core], attn_far.at[core]
        elif item == Y_ACT:
            src, dst = act.at[1 - y], act_far
        elif item == Y_HID:
            src, dst = hid.at[1 - y], hid_far
        elif item == Y_ATT:
            src, dst = att.at[:, 1], att_far
        elif item == Y_GQKV:
            src, dst = gqkv.at[:, 1], gqkv_far
        else:
            c, dst = fin_parts(t)
            src = c.at[0, 1 - y]
            item = Y_FIN + t
        return rcopy(src, dst, y_s.at[item], y_r.at[item], partner)

    def core_copy(k):
        ref = (cot_far, norm_far, attn_far)[k]
        return rcopy(ref.at[core], ref.at[core], core_s.at[k], core_r.at[k], sibling)

    def pass_on(item, k):
        y_copy(item).wait_recv()
        core_copy(k).start()

    def ag_copy(t, h, to, hop, j_src, j_dst):
        ref = (kv_all, qg_all)[t]
        src = ref.at[:, 2 * j_src + h]
        if isinstance(hop, int) and hop == 1:
            src = (kv_own, qg_own)[t].at[:, h]
        return rcopy(
            src,
            ref.at[:, 2 * j_dst + h],
            ag_s.at[t, h, to, hop],
            ag_r.at[t, h, j_dst],
            (right, left)[to],
        )

    def ag_wait(t, h, hop):
        @pl.when(z >= hop)
        def _():
            ag_copy(t, h, 0, hop, line - hop, line - hop).wait_recv()

        @pl.when(z + hop <= line - 1)
        def _():
            ag_copy(t, h, 1, hop, hop, hop).wait_recv()

    def ag_send_when(hop):
        return (
            jnp.logical_and(z >= hop - 1, z <= line - 2),
            jnp.logical_and(z + hop - 1 <= line - 1, z >= 1),
        )

    def ag_hop(t, h, hop):
        if not (isinstance(hop, int) and hop == 1):
            ag_wait(t, h, hop - 1)
        to_right, to_left = ag_send_when(hop)

        @pl.when(to_right)
        def _():
            ag_copy(t, h, 0, hop, lax.rem(line - hop + 1, line), line - hop).start()

        @pl.when(to_left)
        def _():
            ag_copy(t, h, 1, hop, hop - 1, hop).start()

    def ag_rest(t, h, hop):
        def one(i, _):
            ag_hop(t, h, i)
            return 0

        if hop < line:
            lax.fori_loop(hop, line, one, 0)
        ag_wait(t, h, line - 1)

    def ag_drain(t, h):
        def one(hop, _):
            to_right, to_left = ag_send_when(hop)

            @pl.when(to_right)
            def _():
                ag_copy(t, h, 0, hop, lax.rem(line - hop + 1, line), line - hop).wait_send()

            @pl.when(to_left)
            def _():
                ag_copy(t, h, 1, hop, hop - 1, hop).wait_send()

            return 0

        lax.fori_loop(1, line, one, 0)

    rs = (
        (c_down, rs_down, stage_down),
        (c_up, rs_up, stage_up),
        (c_out, rs_out, stage_out),
        (c_qkv, rs_qkv, stage_qkv),
    )

    def rs_copy(t, j, slot, device):
        c, recv, _ = rs[t]
        return rcopy(c.at[j], recv.at[slot], rs_s.at[t, j], rs_r.at[t, slot], device)

    def rs_take(t, j, slot):
        c, recv, held = rs[t]
        rs_copy(t, j, slot, partner).wait_recv()
        copy = lcopy(recv.at[slot], held, tsem.at[t])
        copy.start()
        copy.wait()
        n = c.shape[2]
        part = min(64, n)

        def add(i, _):
            at = pl.ds(pl.multiple_of(i * part, part), part)
            for s in range(2):
                c[j, s, at, :] = (c[j, s, at, :].astype(F32) + held[s, at, :].astype(F32)).astype(
                    BF16
                )
            return 0

        lax.fori_loop(0, n // part, add, 0)

    def rs_ends(t, hops):
        def one(hop, _):
            @pl.when(z == 0)
            def _():
                rs_copy(t, line - hop, line - hop - 1, right).start()

            @pl.when(z == line - 1)
            def _():
                rs_copy(t, hop, hop + 1, left).start()

            return 0

        lax.fori_loop(*hops, one, 0)

    def rs_step(t, hop):
        jr, jl = line - hop, hop

        @pl.when(jnp.logical_and(hop >= z + 1, z >= 1))
        def _():
            rs_take(t, jr, jr)
            rs_copy(t, jr, jr - 1, right).start()

        @pl.when(jnp.logical_and(hop >= line - z, z <= line - 2))
        def _():
            rs_take(t, jl, jl)
            rs_copy(t, jl, jl + 1, left).start()

    def rs_rest(t, hop):
        def one(i, _):
            rs_step(t, i)
            return 0

        if hop < line:
            lax.fori_loop(hop, line, one, 0)

    def rs_finish(t):
        @pl.when(z >= 1)
        def _():
            rs_take(t, 0, 0)

        @pl.when(z <= line - 2)
        def _():
            rs_take(t, 0, line)

        c, dst = fin_parts(t)
        y_copy(Y_FIN, t).start()
        lcopy(c.at[0, y], dst, local.at[4 + t]).start()

    def rs_drain(t):
        def one(j, _):
            @pl.when(j <= line - 1 - z)
            def _():
                rs_copy(t, j, j - 1, right).wait_send()

            @pl.when(j > line - 1 - z)
            def _():
                rs_copy(t, j, j + 1, left).wait_send()

            return 0

        lax.fori_loop(1, line, one, 0)
        c, dst = fin_parts(t)
        y_copy(Y_FIN, t).wait()
        lcopy(c.at[0, y], dst, local.at[4 + t]).wait()

    last = len(far_steps) + 1

    def tp_copy(i, k):
        part = tp_part.at[i]
        if k == 0:
            src, dst, device = part.at[1 - core], tp_recv.at[i, 0], sibling
        elif k < last:
            src, dst, device = part.at[core], tp_recv.at[i, k], far_steps[k - 1]
        else:
            src, dst, device = part.at[core], tp_far.at[i], sibling
        return rcopy(src, dst, tp_s.at[i, k], tp_r.at[i, k], device)

    def tp_add(i, k):
        part = 64

        def add(n, _):
            at = pl.ds(pl.multiple_of(n * part, part), part)
            tp_part[i, core, at, :] = (
                tp_part[i, core, at, :].astype(F32) + tp_recv[i, k, at, :].astype(F32)
            ).astype(BF16)
            return 0

        lax.fori_loop(0, blk // part, add, 0)

    def tp_next(i, k):
        if k > 1:
            tp_copy(i, k - 1).wait_send()
        tp_copy(i, k - 1).wait_recv()
        tp_add(i, k - 1)
        tp_copy(i, k).start()

    def tp_done(i):
        tp_copy(i, last).wait_recv()
        tp_copy(i, 0).wait_send()

        other = lcopy(tp_far.at[i], tp_part.at[i, 1 - core], local.at[8])
        other.start()
        other.wait()

    def tp_drain(i):
        tp_copy(i, last).wait_send()

    def stream(lo, hi, fetches, body):
        for f in fetches:
            f(lo, lax.rem(lo, 2)).start()

        def one(i, _):
            slot = lax.rem(i, 2)

            @pl.when(i + 1 < hi)
            def _():
                for f in fetches:
                    f(i + 1, 1 - slot).start()

            for f in fetches:
                f(i, slot).wait()
            body(i, slot)
            return 0

        lax.fori_loop(lo, hi, one, 0)

    def col_tile(w):
        def fetch(i, slot):
            at = pl.ds(pl.multiple_of(i * TILE, TILE), TILE)
            return lcopy(w.at[:, at], wcol.at[slot, pl.ds(0, w.shape[0]), :], wsem.at[0, slot])

        return fetch

    def row_tile(w):
        def fetch(i, slot):
            at = pl.ds(pl.multiple_of(i * TILE, TILE), TILE)
            return lcopy(w.at[at, :], wrow.at[slot, pl.ds(0, TILE), pl.ds(0, w.shape[1])], wsem.at[1, slot])

        return fetch

    x_load = lcopy(stream_in, xbuf, local.at[0])
    c_load = lcopy(cotangent, cbuf, local.at[1])
    c_load.start()
    x_load.start()

    def number(place, side, k):
        return order[4 * place + 2 * side + k]

    late = [number(z, s, 0) > number(z, s, 1) for s in (y, 1 - y)]

    def block_number(lh, place, side):
        first, second = number(place, side, 0), number(place, side, 1)
        return jnp.minimum(first, second) if lh == 0 else jnp.maximum(first, second)

    for lh in range(2):
        for h in range(2):
            at_block = block_table[:, pl.ds(block_number(lh, z, (y, 1 - y)[h]), 1), :]
            cb, sb = at_block[0], at_block[1]
            ci, si = row_table[0], row_table[1]
            cosine[lh, h] = cb * ci - sb * si
            sine[lh, h] = sb * ci + cb * si

    def by_order(h, first, second):
        return jnp.where(late[h], second, first), jnp.where(late[h], first, second)

    small[...] = jnp.zeros(small.shape, F32)
    model = 2 * half
    chunk_rows = 64
    c_load.wait()

    def cast(i, _):
        at = pl.ds(pl.multiple_of(i * chunk_rows, chunk_rows), chunk_rows)
        c = cbuf[at, :]
        small[S_OUT : S_OUT + 1, :model] += jnp.sum(c, axis=0, keepdims=True)
        c = c.astype(BF16)
        cot[0, at, :] = c[:, :half]
        cot[1, at, :] = c[:, half:]
        return 0

    lax.fori_loop(0, rows // chunk_rows, cast, 0)
    pl.semaphore_wait(barrier, len(greet))
    y_copy(Y_COT).start()

    x_load.wait()

    def unit_of(at):
        x = xbuf[at, :]
        centred = x - jnp.mean(x, axis=-1, keepdims=True)
        variance = jnp.mean(centred * centred, axis=-1, keepdims=True)
        inv_scale = lax.rsqrt(variance + norm_epsilon)
        return centred * inv_scale, inv_scale

    def norms(i, _):
        at = pl.ds(pl.multiple_of(i * chunk_rows, chunk_rows), chunk_rows)
        unit, _ = unit_of(at)
        for n, ref in ((0, attn), (1, norm)):
            value = (unit * gain[n : n + 1, :] + shift[n : n + 1, :]).astype(BF16)
            ref[0, at, :] = value[:, :half]
            ref[1, at, :] = value[:, half:]
        return 0

    lax.fori_loop(0, rows // chunk_rows, norms, 0)


    def tile_at(i):
        return pl.ds(pl.multiple_of(i * TILE, TILE), TILE)

    def feed_forward(i, slot):
        h = nn(norm[0], wcol[slot, :half, :]) + nn(norm[1], wcol[slot, half : 2 * half, :])
        h = h + b_up[:, tile_at(i)]
        gate = 0.5 * (1.0 + lax.erf(h * root_half))
        slope = gate + h * jnp.exp(-0.5 * h * h) * inverse_root_two_pi
        g = nt(cot[0], wrow[slot, :TILE, :half]) + nt(cot[1], wrow[slot, :TILE, half : 2 * half])
        g = g * slope
        small[S_UP : S_UP + 1, tile_at(i)] = jnp.sum(g, axis=0, keepdims=True)
        at = pl.ds(pl.multiple_of(lax.rem(i * TILE, hidden_half), TILE), TILE)
        which = i * TILE // hidden_half
        act[which, :, at] = (h * gate).astype(BF16)
        hid[which, :, at] = g.astype(BF16)

    stream(0, 2 * hidden_half // TILE, (col_tile(w_up), row_tile(w_down)), feed_forward)
    y_copy(Y_ACT).start()


    def project(at, slot, place):
        value = nn(attn[0], wcol[slot, :half, :]) + nn(attn[1], wcol[slot, half : 2 * half, :])
        value = value + b_qkv[:, at]
        pieces = by_order(0, value[:blk], value[blk:])
        for lh in range(2):
            first, rest = pieces[lh][:, :LANES], pieces[lh][:, LANES:]
            place(lh, first, rest)

    def put(refs, which, lh, at, value):
        mine, away = refs

        @pl.when(which == 0)
        def _():
            mine[lh, 0, :, at] = value

        @pl.when(which == 1)
        def _():
            away[lh, :, at] = value

    def kv_index(i):
        which = 1 - i // (2 * own_heads)
        k, kind = lax.rem(i, 2 * own_heads) // 2, 1 + lax.rem(i, 2)
        head = jnp.where(which == 0, y, 1 - y) * own_heads + k
        return which, k, kind, 3 * head + kind

    def q_index(i):
        which = 1 - i // own_heads
        k = lax.rem(i, own_heads)
        head = jnp.where(which == 0, y, 1 - y) * own_heads + k
        return which, k, 3 * head, head

    def fetch_by(w, index):
        def fetch(i, slot):
            return lcopy(w.at[:, tile_at(index(i))], wcol.at[slot, pl.ds(0, w.shape[0]), :], wsem.at[0, slot])

        return fetch

    def lanes_at(start, n):
        return pl.ds(pl.multiple_of(start, LANES), n)

    def keys_values(i, slot):
        which, k, kind, tile = kv_index(i)
        base = jnp.where(kind == 1, 0, width) + k * HD

        def place(lh, first, rest):
            turned = turn(first, cosine[lh, 0], sine[lh, 0], 1)
            first = jnp.where(kind == 1, turned, first).astype(BF16)
            put((kv_own, kv_away), which, lh, lanes_at(base, LANES), first)
            put((kv_own, kv_away), which, lh, lanes_at(base + LANES, HD - LANES), rest.astype(BF16))

        project(tile_at(tile), slot, place)

    stream(0, 4 * own_heads, (fetch_by(w_qkv, lambda i: kv_index(i)[3]),), keys_values)
    y_copy(Y_KV).start()
    ag_hop(0, 0, 1)
    pass_on(Y_COT, 0)

    w_out_fetch = lcopy(w_out, wrow.at[0, pl.ds(0, w_out.shape[0]), pl.ds(0, model)], wsem.at[1, 0])
    w_out_fetch.start()
    w_out_fetch.wait()

    def queries(i, slot):
        which, k, tile, head = q_index(i)

        def place(lh, first, rest):
            turned = turn(first, cosine[lh, 0], sine[lh, 0], 1).astype(BF16)
            put((qg_own, qg_away), which, lh, lanes_at(k * HD, LANES), turned)
            put((qg_own, qg_away), which, lh, lanes_at(k * HD + LANES, HD - LANES), rest.astype(BF16))

        project(tile_at(tile), slot, place)
        at = pl.ds(pl.multiple_of(head * HD, HD), HD)
        g = nt(cot[0], wrow[0, at, :half]) + nt(cot[1], wrow[0, at, half : 2 * half])
        pieces = by_order(0, g[:blk], g[blk:])
        for lh in range(2):
            put((qg_own, qg_away), which, lh, lanes_at(width + k * HD, HD), pieces[lh].astype(BF16))

    stream(0, 2 * own_heads, (fetch_by(w_qkv, lambda i: q_index(i)[2]),), queries)
    y_copy(Y_QG).start()
    ag_hop(1, 0, 1)
    y_copy(Y_MLP).start()
    y_copy(Y_HID).start()
    y_copy(Y_ATTN).start()
    own_places = [
        lcopy(own.at[:, h], everyone.at[:, h], local.at[2 + 2 * t + h])
        for t, (own, everyone) in enumerate(((kv_own, kv_all), (qg_own, qg_all)))
        for h in range(2)
    ]
    own_places[0].start()
    own_places[2].start()

    def cols_at(ref, j):
        start = lax.rem(z + j, line) * block_cols
        at = pl.ds(pl.multiple_of(lax.rem(start, half), LANES), block_cols)
        return ref[start // half, :, at]

    def split_cols(ref, j, at, value):
        n = value.shape[1] // 2
        ref[j, 0, at, :] = value[:, :n].astype(BF16)
        ref[j, 1, at, :] = value[:, n:].astype(BF16)

    def split_rows(ref, j, at, value):
        n = value.shape[0] // 2
        ref[j, 0, :, at] = value[:n].astype(BF16)
        ref[j, 1, :, at] = value[n:].astype(BF16)

    def in_order(share, first=0, end=line):
        def one(k, _):
            j = jnp.where(lax.rem(k, 2) == 0, line - 1 - k // 2, k // 2 + 1)
            share(jnp.where(k == line - 1, 0, j))
            return 0

        lax.fori_loop(first, end, one, 0)


    def mlp_back(i, slot):
        value = nt(hid[0], wrow[slot, :TILE, :hidden_half]) + nt(
            hid[1], wrow[slot, :TILE, hidden_half : 2 * hidden_half]
        )
        tp_part[MLPB, :, :, tile_at(i)] = value.astype(BF16).reshape(2, blk, TILE)

    model_tiles = model // TILE
    stream(0, model_tiles // 2, (row_tile(w_up),), mlp_back)

    ag_hop(0, 0, 2)
    core_copy(0).wait_recv()
    y_copy(Y_ACT).wait_recv()


    def share_down(j):
        g0, g1 = cols_at(cot, j), cols_at(cot_far, j)

        def one(i, _):
            split_cols(
                c_down, j, tile_at(i), tn(act[y, :, tile_at(i)], g0) + tn(act_far[:, tile_at(i)], g1)
            )
            return 0

        lax.fori_loop(0, hidden_half // TILE, one, 0)

    in_order(share_down, 0, 2)
    rs_ends(DOWN, (1, 2))
    in_order(share_down, 2, line)
    stream(model_tiles // 2, model_tiles, (row_tile(w_up),), mlp_back)
    tp_copy(MLPB, 0).start()

    y_copy(Y_KV).wait_recv()
    ag_hop(0, 1, 1)
    own_places[1].start()
    tp_next(MLPB, 1)
    ag_hop(0, 0, 3)
    y_copy(Y_QG).wait_recv()
    own_places[3].start()
    ag_hop(1, 0, 2)
    pass_on(Y_MLP, 1)
    ag_hop(0, 1, 2)
    ag_hop(1, 1, 1)
    rs_ends(DOWN, (2, line))
    ag_hop(0, 1, 3)
    rs_step(DOWN, 1)
    rs_step(DOWN, 2)
    ag_hop(1, 0, 3)
    ag_hop(1, 1, 2)

    y_copy(Y_HID).wait_recv()
    core_copy(1).wait_recv()

    def share_up(j):
        m0, m1 = cols_at(norm, j), cols_at(norm_far, j)

        def one(i, _):
            split_rows(c_up, j, tile_at(i), tn(m0, hid[y, :, tile_at(i)]) + tn(m1, hid_far[:, tile_at(i)]))
            return 0

        lax.fori_loop(0, hidden_half // TILE, one, 0)

    in_order(share_up)
    tp_next(MLPB, 2)
    ag_rest(0, 0, 4)
    ag_rest(0, 1, 4)
    for copy in own_places:
        copy.wait()

    pair = 2 * blk
    same = lax.broadcasted_iota(jnp.int32, (pair, pair), 0) == lax.broadcasted_iota(
        jnp.int32, (pair, pair), 1
    )

    def positions(lh, place, along):
        shape = (1, pair) if along else (pair, 1)
        at = lax.broadcasted_iota(jnp.int32, shape, along)
        here, there = block_number(lh, place, y), block_number(lh, place, 1 - y)
        return at + jnp.where(at < blk, here * blk, there * blk - blk)

    def piece_positions(lh_start, i, along):
        place = lax.rem(z + i, line)
        early, late_ = positions(0, place, along), positions(1, place, along)
        return jnp.where(i < line, early, late_)

    def piece(t):
        def fetch(i, slot):
            ref = (kv_all, qg_all)[t]
            return lcopy(
                ref.at[i // line, pl.ds(2 * lax.rem(i, line), 2)], chunk.at[slot], csem.at[slot]
            )

        return fetch

    for lh in range(2):
        for head in range(own_heads):
            at_k, at_v = head * HD, width + head * HD
            run_m[...] = jnp.full(run_m.shape, masked_value, F32)
            run_l[...] = jnp.zeros(run_l.shape, F32)
            acc_a[...] = jnp.zeros(acc_a.shape, F32)

            def attend(i, slot):
                k = chunk[slot, :, :, at_k : at_k + HD].reshape(pair, HD)
                v = chunk[slot, :, :, at_v : at_v + HD].reshape(pair, HD)
                q = qg_own[lh, :, :, at_k : at_k + HD].reshape(pair, HD)
                s = nt(q, k) * scale
                seen = piece_positions(lh, i, 1) <= positions(lh, z, 0)
                s = jnp.where(seen, s, masked_value)
                old = run_m[...]
                top = jnp.maximum(old, jnp.max(s, axis=1, keepdims=True))
                p = jnp.exp(s - top)
                fade = jnp.exp(old - top)
                run_m[...] = top
                run_l[...] = run_l[...] * fade + jnp.sum(p, axis=1, keepdims=True)
                acc_a[...] = acc_a[...] * fade + nn(p.astype(BF16), v)

            stream(0, line * (lh + 1), (piece(0),), attend)
            out = (acc_a[...] / run_l[...]).astype(BF16)
            att[lh, :, :, at_k : at_k + HD] = out.reshape(2, blk, HD)
            log_total = run_m[...] + jnp.log(run_l[...])
            g = qg_own[lh, :, :, at_v : at_v + HD].reshape(pair, HD)
            dots = jnp.sum(g.astype(F32) * out.astype(F32), axis=1, keepdims=True)
            stats[lh, head, 0:1, :] = jnp.sum(jnp.where(same, log_total, 0.0), 0, keepdims=True)
            stats[lh, head, 1:2, :] = jnp.sum(jnp.where(same, dots, 0.0), 0, keepdims=True)

    def store_order(ref):
        for h in range(2):
            first, second = by_order(h, ref[0, h], ref[1, h])
            ref[0, h] = first
            ref[1, h] = second

    store_order(att)

    def stat_copy(j):
        return rcopy(
            stats, stats_all.at[line - j], st_s.at[j], st_r.at[line - j], (place_of(j), tp)
        )

    for j in range(1, line):
        stat_copy(j).start()
    y_copy(Y_ATT).start()
    rs_ends(UP, (1, line))
    ag_hop(1, 1, 3)
    rs_step(DOWN, 3) if line > 3 else None


    def undo(value, lh, head, kind):
        at = (3 * head + kind) * HD
        first = value[:, :LANES]
        if kind < 2:
            first = turn(
                first, cosine[lh].reshape(pair, LANES), sine[lh].reshape(pair, LANES), -1
            )
        for lo, hi, part in ((0, LANES, first), (LANES, HD, value[:, LANES:])):
            spot = lanes_at(y * 3 * width + at + lo, hi - lo)
            small[S_QKV : S_QKV + 1, spot] += jnp.sum(part, axis=0, keepdims=True)
            gqkv[lh, :, :, at + lo : at + hi] = part.astype(BF16).reshape(2, blk, hi - lo)

    for lh in range(2):
        for head in range(own_heads):
            at_k, at_v = head * HD, width + head * HD
            run_m[...] = jnp.sum(
                jnp.where(same, stats[lh, head, 0:1, :], 0.0), axis=1, keepdims=True
            )
            run_l[...] = jnp.sum(
                jnp.where(same, stats[lh, head, 1:2, :], 0.0), axis=1, keepdims=True
            )
            acc_a[...] = jnp.zeros(acc_a.shape, F32)

            def back_q(i, slot):
                k = chunk[slot, :, :, at_k : at_k + HD].reshape(pair, HD)
                v = chunk[slot, :, :, at_v : at_v + HD].reshape(pair, HD)
                q = qg_own[lh, :, :, at_k : at_k + HD].reshape(pair, HD)
                g = qg_own[lh, :, :, at_v : at_v + HD].reshape(pair, HD)
                s = nt(q, k) * scale
                seen = piece_positions(lh, i, 1) <= positions(lh, z, 0)
                s = jnp.where(seen, s, masked_value)
                p = jnp.exp(s - run_m[...])
                ds = (p * (nt(g, v) - run_l[...]) * scale).astype(BF16)
                acc_a[...] += nn(ds, k)

            stream(0, line * (lh + 1), (piece(0),), back_q)
            undo(acc_a[...], lh, head, 0)

    ag_rest(1, 0, 4)
    ag_rest(1, 1, 4)
    for j in range(1, line):
        stat_copy(line - j).wait_recv()
    own_stats = lcopy(stats, stats_all.at[0], local.at[0])
    own_stats.start()
    own_stats.wait()

    for lh in range(2):
        for head in range(own_heads):
            at_k, at_v = head * HD, width + head * HD
            acc_a[...] = jnp.zeros(acc_a.shape, F32)
            acc_b[...] = jnp.zeros(acc_b.shape, F32)

            def back_k(i, slot):
                q = chunk[slot, :, :, at_k : at_k + HD].reshape(pair, HD)
                g = chunk[slot, :, :, at_v : at_v + HD].reshape(pair, HD)
                k = kv_own[lh, :, :, at_k : at_k + HD].reshape(pair, HD)
                v = kv_own[lh, :, :, at_v : at_v + HD].reshape(pair, HD)
                stat = stats_all[lax.rem(i, line), i // line, head]
                s = nt(k, q) * scale
                seen = positions(lh, z, 0) <= piece_positions(lh, i, 1)
                s = jnp.where(seen, s, masked_value)
                p = jnp.exp(s - stat[0:1, :])
                ds = (p * (nt(v, g) - stat[1:2, :]) * scale).astype(BF16)
                acc_a[...] += nn(ds, q)
                acc_b[...] += nn(p.astype(BF16), g)

            stream(lh * line, 2 * line, (piece(1),), back_k)
            undo(acc_a[...], lh, head, 1)
            undo(acc_b[...], lh, head, 2)
    store_order(gqkv)
    y_copy(Y_GQKV).start()

    pass_on(Y_ATTN, 2)
    core_copy(2).wait_recv()
    core_copy(1).wait_send()
    far_again = lcopy(attn_far, norm_far, local.at[1])
    far_again.start()
    far_again.wait()


    def share_qkv(j):
        m0, m1 = cols_at(attn, j), cols_at(norm_far, j)

        def one(i, _):
            g0 = gqkv[:, 0, :, tile_at(i)].reshape(rows, TILE)
            g1 = gqkv[:, 1, :, tile_at(i)].reshape(rows, TILE)
            split_rows(c_qkv, j, tile_at(i), tn(m0, g0) + tn(m1, g1))
            return 0

        lax.fori_loop(0, 3 * width // TILE, one, 0)

    in_order(share_qkv)
    rs_step(UP, 1)
    rs_step(UP, 2)

    y_copy(Y_GQKV).wait_recv()

    def attn_back(i, slot):
        own = gqkv[:, 0].reshape(rows, 3 * width)
        far = gqkv_far[...].reshape(rows, 3 * width)
        mine = wrow[slot, :TILE, pl.ds(pl.multiple_of(y * 3 * width, LANES), 3 * width)]
        theirs = wrow[slot, :TILE, pl.ds(pl.multiple_of((1 - y) * 3 * width, LANES), 3 * width)]
        value = nt(own, mine) + nt(far, theirs)
        tp_part[ATTNB, :, :, tile_at(i)] = value.astype(BF16).reshape(2, blk, TILE)

    stream(0, model_tiles, (row_tile(w_qkv),), attn_back)
    tp_copy(ATTNB, 0).start()

    def share_out(j):
        g0, g1 = cols_at(cot, j), cols_at(cot_far, j)

        def one(i, _):
            a0 = att[:, 0, :, tile_at(i)].reshape(rows, TILE)
            a1 = att[:, 1, :, tile_at(i)].reshape(rows, TILE)
            split_cols(c_out, j, tile_at(i), tn(a0, g0) + tn(a1, g1))
            return 0

        lax.fori_loop(0, width // TILE, one, 0)

    in_order(share_out)

    tp_next(ATTNB, 1)
    rs_rest(DOWN, 4 if line > 3 else 3)
    rs_finish(DOWN)

    y_copy(Y_ATT).wait_recv()
    w_out_fetch.start()
    w_out_fetch.wait()

    def branch(i, slot):
        value = nn(act[0], wcol[slot, :hidden_half, :]) + nn(
            act[1], wcol[slot, hidden_half : 2 * hidden_half, :]
        )
        own = att[:, 0].reshape(rows, width)
        far = att_far[...].reshape(rows, width)
        mine = wrow[0, pl.ds(pl.multiple_of(y * width, width), width), tile_at(i)]
        theirs = wrow[0, pl.ds(pl.multiple_of((1 - y) * width, width), width), tile_at(i)]
        value += nn(own, mine) + nn(far, theirs)
        tp_part[BRANCH, :, :, tile_at(i)] = value.astype(BF16).reshape(2, blk, TILE)

    stream(0, model_tiles // 2, (col_tile(w_down),), branch)

    rs_step(UP, 3) if line > 3 else None
    stream(model_tiles // 2, model_tiles, (col_tile(w_down),), branch)

    tp_next(ATTNB, 2)
    tp_done(MLPB)
    tp_done(ATTNB)


    def back_norms(i, _):
        at = pl.ds(pl.multiple_of(i * chunk_rows, chunk_rows), chunk_rows)
        at_part = pl.ds(pl.multiple_of(lax.rem(i * chunk_rows, blk), chunk_rows), chunk_rows)
        which = i * chunk_rows // blk
        unit, inv_scale = unit_of(at)
        total = jnp.zeros((chunk_rows, model), F32)
        for n, part in ((0, ATTNB), (1, MLPB)):
            value = tp_part[part, which, at_part, :].astype(F32)
            small[S_GAIN + n : S_GAIN + n + 1, :model] += jnp.sum(value * unit, 0, keepdims=True)
            small[S_SHIFT + n : S_SHIFT + n + 1, :model] += jnp.sum(value, 0, keepdims=True)
            total = total + value * gain[n : n + 1, :]
        cbuf[at, :] = cbuf[at, :] + inv_scale * (
            total
            - jnp.mean(total, axis=-1, keepdims=True)
            - unit * jnp.mean(total * unit, axis=-1, keepdims=True)
        )
        return 0

    lax.fori_loop(0, rows // chunk_rows, back_norms, 0)
    grad_store = lcopy(cbuf, grad_o, local.at[1])
    grad_store.start()

    small_pair = rcopy(small, small_recv.at[0], sm_s.at[0], sm_r.at[0], partner)
    small_pair.start()
    small_pair.wait()
    small[...] += small_recv[0]

    def small_copy(j):
        return rcopy(
            small, small_recv.at[line - j], sm_s.at[j], sm_r.at[line - j], (place_of(j), tp)
        )

    for j in range(1, line):
        small_copy(j).start()
    rs_ends(QKV, (1, line))
    rs_ends(OUT, (1, line))
    tp_copy(BRANCH, 0).start()
    rs_rest(UP, 4 if line > 3 else 3)
    tp_next(BRANCH, 1)
    rs_finish(UP)
    for j in range(1, line):
        small_copy(line - j).wait_recv()
    for j in range(1, line):
        small_copy(j).wait_send()
    small_recv[0] = small[...]
    small[...] = small_recv[lax.rem(line - z, line)]
    for p in range(1, line):
        small[...] += small_recv[lax.rem(p + line - z, line)]
    small_store = lcopy(small, small_o, local.at[2])
    small_store.start()
    rs_step(QKV, 1)
    rs_step(QKV, 2)
    tp_next(BRANCH, 2)
    tp_done(BRANCH)

    def stream_rows(i, _):
        at = pl.ds(pl.multiple_of(i * chunk_rows, chunk_rows), chunk_rows)
        at_part = pl.ds(pl.multiple_of(lax.rem(i * chunk_rows, blk), chunk_rows), chunk_rows)
        which = i * chunk_rows // blk
        xbuf[at, :] = xbuf[at, :] + out_bias[...] + tp_part[BRANCH, which, at_part, :].astype(F32)
        return 0

    lax.fori_loop(0, rows // chunk_rows, stream_rows, 0)
    stream_store = lcopy(xbuf, stream_o, local.at[0])
    stream_store.start()
    rs_rest(QKV, 3)
    rs_step(OUT, 1)
    rs_step(OUT, 2)
    rs_finish(QKV)
    rs_rest(OUT, 3)
    rs_finish(OUT)

    for t in range(2):
        for h in range(2):
            ag_drain(t, h)
    for item in (Y_KV, Y_QG, Y_COT, Y_MLP, Y_ATTN, Y_ACT, Y_HID, Y_ATT, Y_GQKV):
        y_copy(item).wait_send()
    core_copy(0).wait_send()
    core_copy(2).wait_send()
    for j in range(1, line):
        stat_copy(j).wait_send()
    for i in range(3):
        tp_drain(i)
    grad_store.wait()
    small_store.wait()
    stream_store.wait()
    for t in range(4):
        rs_drain(t)


def layer(line, n_tp, order, stream_in, cotangent, ln_gain, ln_bias, w_qkv, b_qkv, w_out, out_bias, w_up, b_up, w_down):
    rows, model = stream_in.shape
    half, blk = model // 2, rows // 2
    hidden = w_up.shape[1]
    hidden_half = hidden // 2
    width = w_out.shape[0] // 2
    own_heads = width // HD
    part_cols = model // line // 2
    pair = 2 * blk
    tp_steps = 0
    while (2 << tp_steps) < n_tp:
        tp_steps += 1
    small_shape = (8, max(model, hidden, 6 * width))
    shares = (
        (2, hidden_half, part_cols),
        (2, part_cols, hidden_half),
        (2, width, part_cols),
        (2, part_cols, 3 * width),
    )
    b = lambda *s: jax.ShapeDtypeStruct(s, BF16)
    f = lambda *s: jax.ShapeDtypeStruct(s, F32)
    vb = lambda *s: pltpu.VMEM(s, BF16)
    vf = lambda *s: pltpu.VMEM(s, F32)
    dma = pltpu.SemaphoreType.DMA
    outs = (
        b(hidden, part_cols),
        b(part_cols, hidden),
        b(2 * width, part_cols),
        b(part_cols, 6 * width),
        f(rows, model),
        f(rows, model),
        f(*small_shape),
        b(2, 2 * line, blk, 2 * width),
        b(2, 2 * line, blk, 2 * width),
        b(line + 1, *shares[0]),
        b(line + 1, *shares[1]),
        b(line + 1, *shares[2]),
        b(line + 1, *shares[3]),
        b(2, rows, half),
        b(3, blk, model),
    )
    wide = max(model, hidden)
    scratch = (
        [vf(rows, model)] * 2
        + [vb(2, rows, half)] * 5
        + [vb(2, rows, hidden_half)] * 2
        + [vb(rows, hidden_half)] * 2
        + [vb(2, wide, TILE), vb(2, max(TILE, 2 * width), wide)]
        + [vb(line, *s) for s in shares]
        + [vb(*s) for s in shares]
        + [vb(3, 2, blk, model), vb(3, tp_steps + 1, blk, model)]
        + [vb(2, 2, blk, 2 * width)] * 2
        + [vb(2, blk, 2 * width)] * 2
        + [
            vb(2, 2, blk, 2 * width),
            vb(2, 2, blk, width),
            vb(2, blk, width),
            vf(2, own_heads, 2, pair),
            vf(line, 2, own_heads, 2, pair),
            vb(2, 2, blk, 3 * width),
            vb(2, blk, 3 * width),
            vf(pair, HD),
            vf(pair, HD),
            vf(pair, 1),
            vf(pair, 1),
            vf(2, 2, blk, LANES),
            vf(2, 2, blk, LANES),
            vf(*small_shape),
            vf(line, *small_shape),
            dma((2, 2, 2, line)),
            dma((2, 2, line)),
            dma((Y_FIN + 4,)),
            dma((Y_FIN + 4,)),
            dma((3,)),
            dma((3,)),
            dma((4, line)),
            dma((4, line + 1)),
            dma((3, tp_steps + 2)),
            dma((3, tp_steps + 2)),
            dma((line,)),
            dma((line,)),
            dma((line,)),
            dma((line,)),
            dma((9,)),
            dma((2, 2)),
            dma((2,)),
            dma((4,)),
        ]
    )
    blocks = order.shape[0]
    operands = (
        order,
        stream_in,
        cotangent,
        w_up,
        w_down,
        w_out,
        w_qkv,
        ln_gain,
        ln_bias,
        b_qkv.reshape(1, -1),
        b_up.reshape(1, -1),
        out_bias.reshape(1, -1),
        jnp.asarray(rope_tables(np.arange(blocks) * blk)),
        jnp.asarray(rope_tables(np.arange(blk))),
    )
    return pl.pallas_call(
        functools.partial(layer_kernel, line, n_tp),
        name="layer",
        out_shape=outs,
        in_specs=[SMEM] + [ANY] * 6 + [VMEM] * 7,
        out_specs=[ANY] * len(outs),
        scratch_shapes=scratch,
        cost_estimate=pl.CostEstimate(
            flops=40 * rows * model * hidden,
            transcendentals=rows * hidden,
            bytes_accessed=8 * w_up.size,
        ),
        compiler_params=pltpu.CompilerParams(
            collective_id=0, has_side_effects=True, vmem_limit_bytes=67043328
        ),
    )(*operands)


def shards(
    n_ctx,
    n_tp,
    stream_in,
    cotangent,
    ln_gain,
    ln_bias,
    w_qkv,
    b_qkv,
    w_out,
    out_bias,
    w_up,
    b_up,
    w_down,
    block_order,
):
    model, hidden = w_up.shape
    (down, up, out, qkv, stream_out, grad_in, small, *_) = layer(
        n_ctx // 2,
        n_tp,
        block_order,
        stream_in,
        cotangent,
        ln_gain,
        ln_bias,
        w_qkv,
        b_qkv,
        w_out,
        out_bias,
        w_up,
        b_up,
        w_down,
    )
    return (
        stream_out,
        grad_in,
        qkv.astype(F32),
        small[S_QKV, : w_qkv.shape[1]],
        out.astype(F32),
        small[S_OUT, :model],
        up.astype(F32),
        small[S_UP, :hidden],
        down.astype(F32),
        small[S_GAIN : S_GAIN + 2, :model],
        small[S_SHIFT : S_SHIFT + 2, :model],
    )


def solution(mesh):
    placed = (
        P("ctx", None),
        P("ctx", None),
        P(),
        P(),
        P(None, "tp"),
        P("tp"),
        P("tp", None),
        P(),
        P(None, "tp"),
        P("tp"),
        P("tp", None),
        P(),
    )
    return jax.shard_map(
        functools.partial(shards, mesh.shape["ctx"], mesh.shape["tp"]),
        mesh=mesh,
        in_specs=placed,
        out_specs=(
            P("ctx", None),
            P("ctx", None),
            P("ctx", "tp"),
            P("tp"),
            P("tp", "ctx"),
            P(),
            P("ctx", "tp"),
            P("tp"),
            P("tp", "ctx"),
            P(),
            P(),
        ),
        check_vma=False,
    )
```

```python
import functools
import math

import jax
import jax.numpy as jnp
import numpy as np
from jax import lax
from jax.experimental import pallas as pl
from jax.experimental.pallas import tpu as pltpu
from jax.sharding import PartitionSpec as P

HD = 256
ROT = 64
LANES = 128
TILE = 256

masked_value = -1e30
norm_epsilon = 1e-05
root_half = 0.7071067811865476
inverse_root_two_pi = 0.3989422804014327

F32 = jnp.float32
BF16 = jnp.bfloat16
MESH = pl.DeviceIdType.MESH
ANY = pl.BlockSpec(memory_space=pl.ANY)
VMEM = pl.BlockSpec(memory_space=pltpu.VMEM)
SMEM = pl.BlockSpec(memory_space=pltpu.SMEM)


def nt(a, b):
    return lax.dot_general(a, b, (((1,), (1,)), ((), ())), preferred_element_type=F32)


def nn(a, b):
    return lax.dot_general(a, b, (((1,), (0,)), ((), ())), preferred_element_type=F32)


def tn(a, b):
    return lax.dot_general(a, b, (((0,), (0,)), ((), ())), preferred_element_type=F32)


def rope_tables(positions):
    half_rot = ROT // 2
    frequency = np.exp(np.arange(half_rot) * (-2.0 * math.log(10000.0) / ROT))
    angles = np.asarray(positions, np.float64)[:, None] * frequency
    table = np.zeros((2, angles.shape[0], LANES), np.float32)
    table[0] = 1.0
    for lo in (0, half_rot):
        table[0, :, lo : lo + half_rot] = np.cos(angles)
        table[1, :, lo : lo + half_rot] = np.sin(angles)
    return table


def turn(first, cosine, sine, sign):
    half_rot = ROT // 2
    scaled = first * sine if sign < 0 else first
    lane = lax.broadcasted_iota(jnp.int32, first.shape, 1)
    down = jnp.where(lane < half_rot, pltpu.roll(scaled, LANES - half_rot, 1), 0.0)
    up = jnp.where(
        jnp.logical_and(lane >= half_rot, lane < ROT), pltpu.roll(scaled, half_rot, 1), 0.0
    )
    if sign < 0:
        return first * cosine + (down - up)
    return first * cosine + (up - down) * sine


DOWN, UP, OUT, QKV = range(4)
(Y_KV, Y_QG, Y_COT, Y_MLP, Y_ATTN, Y_ACT, Y_HID, Y_ATT, Y_GQKV, Y_FIN) = range(10)
BRANCH, MLPB, ATTNB = range(3)
S_GAIN, S_SHIFT, S_OUT, S_UP, S_QKV = 0, 2, 4, 5, 6


def layer_kernel(
    line,
    n_tp,
    order,
    stream_in,
    cotangent,
    w_up,
    w_down,
    w_out,
    w_qkv,
    gain,
    shift,
    b_qkv,
    b_up,
    out_bias,
    block_table,
    row_table,
    down_o,
    up_o,
    out_o,
    qkv_o,
    stream_o,
    grad_o,
    small_o,
    kv_all,
    qg_all,
    rs_down,
    rs_up,
    rs_out,
    rs_qkv,
    attn_far,
    tp_far,
    cot_end,
    act_end,
    xbuf,
    cbuf,
    cot,
    cot_far,
    norm,
    norm_far,
    attn,
    act,
    hid,
    act_far,
    hid_far,
    wcol,
    wrow,
    c_down,
    c_up,
    c_out,
    c_qkv,
    stage_down,
    stage_up,
    stage_out,
    stage_qkv,
    tp_part,
    tp_recv,
    kv_own,
    qg_own,
    kv_away,
    qg_away,
    chunk,
    att,
    att_far,
    stats,
    stats_all,
    gqkv,
    gqkv_far,
    acc_a,
    acc_b,
    run_m,
    run_l,
    cosine,
    sine,
    small,
    small_recv,
    ag_s,
    ag_r,
    y_s,
    y_r,
    core_s,
    core_r,
    x_s,
    x_r,
    rs_s,
    rs_r,
    tp_s,
    tp_r,
    st_s,
    st_r,
    sm_s,
    sm_r,
    end_s,
    end_r,
    ex_s,
    ex_r,
    local,
    wsem,
    csem,
    tsem,
):
    me, tp = lax.axis_index("ctx"), lax.axis_index("tp")
    z, y = me // 2, lax.rem(me, 2)
    core = lax.rem(tp, 2)
    partner = (me + 1 - 2 * y, tp)
    sibling = (me, tp + 1 - 2 * core)
    right, left = (me + 2, tp), (me - 2, tp)
    far_steps = []
    step = 2
    while step < n_tp:
        far_steps.append((me, tp + step - 2 * step * lax.rem(tp // step, 2)))
        step *= 2

    rows = norm.shape[1]
    blk = rows // 2
    across = n_tp // 2
    xpos = tp // 2
    x_others = [(me, lax.rem(tp + 2 * k, n_tp)) for k in range(1, across)]
    half = norm.shape[2]
    hidden_half = act.shape[2]
    own_heads = kv_own.shape[-1] // (2 * HD)
    width = own_heads * HD
    block_cols = 2 * half // line
    scale = HD ** (-0.5)

    def place_of(j):
        return lax.rem(z + j, line) * 2 + y

    barrier = pltpu.get_barrier_semaphore()
    greet = [partner, sibling] + x_others + [(place_of(j), tp) for j in range(1, line)]
    for device in greet:
        pl.semaphore_signal(barrier, inc=1, device_id=device, device_id_type=MESH)

    def rcopy(src, dst, s, r, device):
        return pltpu.make_async_remote_copy(
            src_ref=src, dst_ref=dst, send_sem=s, recv_sem=r, device_id=device, device_id_type=MESH
        )

    def lcopy(src, dst, sem):
        return pltpu.make_async_copy(src, dst, sem)

    def fin_parts(t):
        c = (c_down, c_up, c_out, c_qkv)[t]
        if t == DOWN:
            dst = down_o.at[pl.ds(pl.multiple_of(y * hidden_half, hidden_half), hidden_half), :]
        elif t == UP:
            dst = up_o.at[:, pl.ds(pl.multiple_of(y * hidden_half, hidden_half), hidden_half)]
        elif t == OUT:
            dst = out_o.at[pl.ds(pl.multiple_of(y * width, width), width), :]
        else:
            dst = qkv_o.at[:, pl.ds(pl.multiple_of(y * 3 * width, 3 * width), 3 * width)]
        return c, dst

    def part_rows(x):
        n = rows // across
        return pl.ds(pl.multiple_of(x * n, n), n)

    def y_copy(item, t=0):
        if item == Y_KV:
            src, dst = kv_away, kv_own.at[:, 1]
        elif item == Y_QG:
            src, dst = qg_away, qg_own.at[:, 1]
        elif item == Y_COT:
            src, dst = cot.at[core, part_rows(xpos)], cot_far.at[core, part_rows(xpos)]
        elif item == Y_MLP:
            src, dst = norm.at[core, part_rows(xpos)], norm_far.at[core, part_rows(xpos)]
        elif item == Y_ATTN:
            src, dst = attn.at[core, part_rows(xpos)], attn_far.at[core, part_rows(xpos)]
        elif item == Y_ACT:
            src, dst = act.at[1 - y], act_far
        elif item == Y_HID:
            src, dst = hid.at[1 - y], hid_far
        elif item == Y_ATT:
            src, dst = att.at[:, 1], att_far
        elif item == Y_GQKV:
            src, dst = gqkv.at[:, 1], gqkv_far
        else:
            c, dst = fin_parts(t)
            src = c.at[0, 1 - y]
            item = Y_FIN + t
        return rcopy(src, dst, y_s.at[item], y_r.at[item], partner)

    def core_copy(k):
        ref = (cot_far, norm_far, attn_far)[k]
        return rcopy(ref.at[core], ref.at[core], core_s.at[k], core_r.at[k], sibling)

    def x_copy(k, n):
        ref = (cot_far, norm_far, attn_far)[k].at[core, part_rows(xpos)]
        return rcopy(ref, ref, x_s.at[k, n], x_r.at[k, n], x_others[n])

    def x_arrival(k, n):
        ref = (cot_far, norm_far, attn_far)[k].at[core, part_rows(lax.rem(xpos + across - n - 1, across))]
        return rcopy(ref, ref, x_s.at[k, n], x_r.at[k, n], x_others[n])

    def pass_x(item, k):
        y_copy(item).wait_recv()
        for n in range(across - 1):
            x_copy(k, n).start()

    def pass_on(item, k):
        for n in range(across - 1):
            x_arrival(k, n).wait_recv()
        core_copy(k).start()

    def x_drain(k):
        for n in range(across - 1):
            x_copy(k, n).wait_send()

    E_COT, E_COT_FAR, E_ACT, E_ACT_FAR = range(4)
    next_to_end = jnp.logical_or(z == 1, z == line - 2)

    def end_part(k, x):
        n = rows // across
        return cot_end.at[
            pl.ds(pl.multiple_of(k * rows + x * n, n), n), pl.ds(pl.multiple_of(core * half, half), half)
        ]

    def end_copy(item, device):
        if item == E_COT:
            src, dst = cot.at[core, part_rows(xpos)], end_part(0, xpos)
        elif item == E_COT_FAR:
            src, dst = cot_far.at[core, part_rows(xpos)], end_part(1, xpos)
        elif item == E_ACT:
            src, dst = act.at[y], act_end.at[pl.ds(0, rows), :]
        else:
            src, dst = act_far, act_end.at[pl.ds(rows, rows), :]
        return rcopy(src, dst, end_s.at[item], end_r.at[item], device)

    def end_x(k, n, arriving):
        x = lax.rem(xpos + across - n - 1, across) if arriving else xpos
        ref = end_part(k, x)
        return rcopy(ref, ref, ex_s.at[k, n], ex_r.at[k, n], x_others[n])

    def end_share(k):
        ref = cot_end.at[pl.ds(k * rows, rows), pl.ds(pl.multiple_of(core * half, half), half)]
        return rcopy(ref, ref, end_s.at[4 + k], end_r.at[4 + k], sibling)

    def end_send(item):
        @pl.when(z == 0)
        def _():
            end_copy(item, right).start()

        @pl.when(z == line - 1)
        def _():
            end_copy(item, left).start()

    def end_pass_x(k):
        @pl.when(next_to_end)
        def _():
            end_copy(E_COT + k, partner).wait_recv()
            for n in range(across - 1):
                end_x(k, n, False).start()

    def end_pass(k):
        @pl.when(next_to_end)
        def _():
            for n in range(across - 1):
                end_x(k, n, True).wait_recv()
            end_share(k).start()

    def end_drain():
        @pl.when(jnp.logical_or(z == 0, z == line - 1))
        def _():
            for item in range(4):
                end_copy(item, partner).wait_send()

        @pl.when(next_to_end)
        def _():
            for k in range(2):
                end_share(k).wait_send()
                for n in range(across - 1):
                    end_x(k, n, False).wait_send()

    def ag_copy(t, h, to, hop, j_src, j_dst):
        ref = (kv_all, qg_all)[t]
        src = ref.at[:, 2 * j_src + h]
        if isinstance(hop, int) and hop == 1:
            src = (kv_own, qg_own)[t].at[:, h]
        return rcopy(
            src,
            ref.at[:, 2 * j_dst + h],
            ag_s.at[t, h, to, hop],
            ag_r.at[t, h, j_dst],
            (right, left)[to],
        )

    def ag_send_when(hop):
        return (
            jnp.logical_and(z >= hop - 1, z <= line - 2),
            jnp.logical_and(z + hop - 1 <= line - 1, z >= 1),
        )

    def ag_hop(t, h, hop):
        first = isinstance(hop, int) and hop == 1
        to_right, to_left = ag_send_when(hop)

        @pl.when(to_right)
        def _():
            if not first:
                ag_copy(t, h, 0, hop - 1, line - hop + 1, line - hop + 1).wait_recv()
            ag_copy(t, h, 0, hop, lax.rem(line - hop + 1, line), line - hop).start()

        @pl.when(to_left)
        def _():
            if not first:
                ag_copy(t, h, 1, hop - 1, hop - 1, hop - 1).wait_recv()
            ag_copy(t, h, 1, hop, hop - 1, hop).start()

    def ag_rest(t, h, hop):
        def one(i, _):
            ag_hop(t, h, i)
            return 0

        def come(i, _):
            ag_copy(t, h, 0, i, i, i).wait_recv()
            return 0

        if hop < line:
            lax.fori_loop(hop, line, one, 0)

        @pl.when(jnp.logical_or(z == 0, z == line - 1))
        def _():
            lax.fori_loop(1, line, come, 0)

    def ag_drain(t, h):
        def one(hop, _):
            to_right, to_left = ag_send_when(hop)

            @pl.when(to_right)
            def _():
                ag_copy(t, h, 0, hop, lax.rem(line - hop + 1, line), line - hop).wait_send()

            @pl.when(to_left)
            def _():
                ag_copy(t, h, 1, hop, hop - 1, hop).wait_send()

            return 0

        lax.fori_loop(1, line, one, 0)

    rs = (
        (c_down, rs_down, stage_down),
        (c_up, rs_up, stage_up),
        (c_out, rs_out, stage_out),
        (c_qkv, rs_qkv, stage_qkv),
    )

    def rs_copy(t, j, slot, device):
        c, recv, _ = rs[t]
        return rcopy(c.at[j], recv.at[slot], rs_s.at[t, j], rs_r.at[t, slot], device)

    def rs_take(t, j, slot):
        c, recv, held = rs[t]
        rs_copy(t, j, slot, partner).wait_recv()
        copy = lcopy(recv.at[slot], held, tsem.at[t])
        copy.start()
        copy.wait()
        n = c.shape[2]
        part = min(64, n)

        def add(i, _):
            at = pl.ds(pl.multiple_of(i * part, part), part)
            for s in range(2):
                c[j, s, at, :] = (c[j, s, at, :].astype(F32) + held[s, at, :].astype(F32)).astype(
                    BF16
                )
            return 0

        lax.fori_loop(0, n // part, add, 0)

    def first_from(t):
        return 2 if t == DOWN else 1

    def rs_ends(t, hops):
        first = first_from(t)

        def one(hop, _):
            @pl.when(jnp.logical_and(z == first - 1, hop >= first))
            def _():
                rs_copy(t, line - hop, line - hop - 1, right).start()

            @pl.when(jnp.logical_and(z == line - first, hop >= first))
            def _():
                rs_copy(t, hop, hop + 1, left).start()

            return 0

        lax.fori_loop(*hops, one, 0)

    def rs_step(t, hop):
        jr, jl = line - hop, hop
        first = first_from(t)

        @pl.when(jnp.logical_and(hop >= z + 1, z >= first))
        def _():
            rs_take(t, jr, jr)
            rs_copy(t, jr, jr - 1, right).start()

        @pl.when(jnp.logical_and(hop >= line - z, z <= line - 1 - first))
        def _():
            rs_take(t, jl, jl)
            rs_copy(t, jl, jl + 1, left).start()

    def rs_rest(t, hop):
        def one(i, _):
            rs_step(t, i)
            return 0

        if hop < line:
            lax.fori_loop(hop, line, one, 0)

    def rs_finish(t):
        first = first_from(t)

        @pl.when(z >= first)
        def _():
            rs_take(t, 0, 0)

        @pl.when(z <= line - 1 - first)
        def _():
            rs_take(t, 0, line)

        c, dst = fin_parts(t)
        y_copy(Y_FIN, t).start()
        lcopy(c.at[0, y], dst, local.at[4 + t]).start()

    def rs_drain(t):
        sends = jnp.logical_and(z >= first_from(t) - 1, z <= line - first_from(t))

        def one(j, _):
            @pl.when(jnp.logical_and(sends, j <= line - 1 - z))
            def _():
                rs_copy(t, j, j - 1, right).wait_send()

            @pl.when(jnp.logical_and(sends, j > line - 1 - z))
            def _():
                rs_copy(t, j, j + 1, left).wait_send()

            return 0

        lax.fori_loop(1, line, one, 0)
        c, dst = fin_parts(t)
        y_copy(Y_FIN, t).wait()
        lcopy(c.at[0, y], dst, local.at[4 + t]).wait()

    last = len(far_steps) + 1

    def tp_copy(i, k):
        part = tp_part.at[i]
        if k == 0:
            src, dst, device = part.at[1 - core], tp_recv.at[i, 0], sibling
        elif k < last:
            src, dst, device = part.at[core], tp_recv.at[i, k], far_steps[k - 1]
        else:
            src, dst, device = part.at[core], tp_far.at[i], sibling
        return rcopy(src, dst, tp_s.at[i, k], tp_r.at[i, k], device)

    def tp_add(i, k):
        part = 64

        def add(n, _):
            at = pl.ds(pl.multiple_of(n * part, part), part)
            tp_part[i, core, at, :] = (
                tp_part[i, core, at, :].astype(F32) + tp_recv[i, k, at, :].astype(F32)
            ).astype(BF16)
            return 0

        lax.fori_loop(0, blk // part, add, 0)

    def tp_next(i, k):
        if k > 1:
            tp_copy(i, k - 1).wait_send()
        tp_copy(i, k - 1).wait_recv()
        tp_add(i, k - 1)
        tp_copy(i, k).start()

    def tp_done(i):
        tp_copy(i, last).wait_recv()
        tp_copy(i, 0).wait_send()

        other = lcopy(tp_far.at[i], tp_part.at[i, 1 - core], local.at[8])
        other.start()
        other.wait()

    def tp_drain(i):
        tp_copy(i, last).wait_send()

    def stream(lo, hi, fetches, body):
        for f in fetches:
            f(lo, lax.rem(lo, 2)).start()

        def one(i, _):
            slot = lax.rem(i, 2)

            @pl.when(i + 1 < hi)
            def _():
                for f in fetches:
                    f(i + 1, 1 - slot).start()

            for f in fetches:
                f(i, slot).wait()
            body(i, slot)
            return 0

        lax.fori_loop(lo, hi, one, 0)

    def col_tile(w):
        def fetch(i, slot):
            at = pl.ds(pl.multiple_of(i * TILE, TILE), TILE)
            return lcopy(w.at[:, at], wcol.at[slot, pl.ds(0, w.shape[0]), :], wsem.at[0, slot])

        return fetch

    def row_tile(w):
        def fetch(i, slot):
            at = pl.ds(pl.multiple_of(i * TILE, TILE), TILE)
            return lcopy(w.at[at, :], wrow.at[slot, pl.ds(0, TILE), pl.ds(0, w.shape[1])], wsem.at[1, slot])

        return fetch

    x_load = lcopy(stream_in, xbuf, local.at[0])
    c_load = lcopy(cotangent, cbuf, local.at[1])
    c_load.start()
    x_load.start()

    def number(place, side, k):
        return order[4 * place + 2 * side + k]

    late = [number(z, s, 0) > number(z, s, 1) for s in (y, 1 - y)]

    def block_number(lh, place, side):
        first, second = number(place, side, 0), number(place, side, 1)
        return jnp.minimum(first, second) if lh == 0 else jnp.maximum(first, second)

    for lh in range(2):
        for h in range(2):
            at_block = block_table[:, pl.ds(block_number(lh, z, (y, 1 - y)[h]), 1), :]
            cb, sb = at_block[0], at_block[1]
            ci, si = row_table[0], row_table[1]
            cosine[lh, h] = cb * ci - sb * si
            sine[lh, h] = sb * ci + cb * si

    def by_order(h, first, second):
        return jnp.where(late[h], second, first), jnp.where(late[h], first, second)

    small[...] = jnp.zeros(small.shape, F32)
    model = 2 * half
    chunk_rows = 64
    c_load.wait()

    def cast(i, _):
        at = pl.ds(pl.multiple_of(i * chunk_rows, chunk_rows), chunk_rows)
        c = cbuf[at, :]
        small[S_OUT : S_OUT + 1, :model] += jnp.sum(c, axis=0, keepdims=True)
        c = c.astype(BF16)
        cot[0, at, :] = c[:, :half]
        cot[1, at, :] = c[:, half:]
        return 0

    lax.fori_loop(0, rows // chunk_rows, cast, 0)
    pl.semaphore_wait(barrier, len(greet))
    y_copy(Y_COT).start()
    end_send(E_COT)

    x_load.wait()

    def unit_of(at):
        x = xbuf[at, :]
        centred = x - jnp.mean(x, axis=-1, keepdims=True)
        variance = jnp.mean(centred * centred, axis=-1, keepdims=True)
        inv_scale = lax.rsqrt(variance + norm_epsilon)
        return centred * inv_scale, inv_scale

    def norms(i, _):
        at = pl.ds(pl.multiple_of(i * chunk_rows, chunk_rows), chunk_rows)
        unit, _ = unit_of(at)
        for n, ref in ((0, attn), (1, norm)):
            value = (unit * gain[n : n + 1, :] + shift[n : n + 1, :]).astype(BF16)
            ref[0, at, :] = value[:, :half]
            ref[1, at, :] = value[:, half:]
        return 0

    lax.fori_loop(0, rows // chunk_rows, norms, 0)


    def tile_at(i):
        return pl.ds(pl.multiple_of(i * TILE, TILE), TILE)

    def hidden_at(i):
        at = pl.ds(pl.multiple_of(lax.rem(i * TILE, hidden_half), TILE), TILE)
        return i * TILE // hidden_half, at

    def activate(i, slot):
        h = nn(norm[0], wcol[slot, :half, :]) + nn(norm[1], wcol[slot, half : 2 * half, :])
        h = h + b_up[:, tile_at(i)]
        gate = 0.5 * (1.0 + lax.erf(h * root_half))
        which, at = hidden_at(i)
        act[which, :, at] = (h * gate).astype(BF16)
        slope = gate + h * jnp.exp(-0.5 * h * h) * inverse_root_two_pi
        hid[which, :, at] = slope.astype(BF16)

    def hidden_back(i, slot):
        g = nt(cot[0], wrow[slot, :TILE, :half]) + nt(cot[1], wrow[slot, :TILE, half : 2 * half])
        which, at = hidden_at(i)
        g = g * hid[which, :, at].astype(F32)
        small[S_UP : S_UP + 1, tile_at(i)] = jnp.sum(g, axis=0, keepdims=True)
        hid[which, :, at] = g.astype(BF16)

    hidden_tiles = 2 * hidden_half // TILE
    stream(0, hidden_tiles, (col_tile(w_up),), activate)
    y_copy(Y_ACT).start()
    pass_x(Y_COT, 0)
    end_send(E_COT_FAR)


    def project(at, slot, place):
        value = nn(attn[0], wcol[slot, :half, :]) + nn(attn[1], wcol[slot, half : 2 * half, :])
        value = value + b_qkv[:, at]
        pieces = by_order(0, value[:blk], value[blk:])
        for lh in range(2):
            first, rest = pieces[lh][:, :LANES], pieces[lh][:, LANES:]
            place(lh, first, rest)

    def put(refs, which, lh, at, value):
        mine, away = refs

        @pl.when(which == 0)
        def _():
            mine[lh, 0, :, at] = value

        @pl.when(which == 1)
        def _():
            away[lh, :, at] = value

    def kv_index(i):
        which = 1 - i // (2 * own_heads)
        k, kind = lax.rem(i, 2 * own_heads) // 2, 1 + lax.rem(i, 2)
        head = jnp.where(which == 0, y, 1 - y) * own_heads + k
        return which, k, kind, 3 * head + kind

    def q_index(i):
        which = 1 - i // own_heads
        k = lax.rem(i, own_heads)
        head = jnp.where(which == 0, y, 1 - y) * own_heads + k
        return which, k, 3 * head, head

    def fetch_by(w, index):
        def fetch(i, slot):
            return lcopy(w.at[:, tile_at(index(i))], wcol.at[slot, pl.ds(0, w.shape[0]), :], wsem.at[0, slot])

        return fetch

    def lanes_at(start, n):
        return pl.ds(pl.multiple_of(start, LANES), n)

    def keys_values(i, slot):
        which, k, kind, tile = kv_index(i)
        base = jnp.where(kind == 1, 0, width) + k * HD

        def place(lh, first, rest):
            turned = turn(first, cosine[lh, 0], sine[lh, 0], 1)
            first = jnp.where(kind == 1, turned, first).astype(BF16)
            put((kv_own, kv_away), which, lh, lanes_at(base, LANES), first)
            put((kv_own, kv_away), which, lh, lanes_at(base + LANES, HD - LANES), rest.astype(BF16))

        project(tile_at(tile), slot, place)

    stream(0, 4 * own_heads, (fetch_by(w_qkv, lambda i: kv_index(i)[3]),), keys_values)
    y_copy(Y_KV).start()
    ag_hop(0, 0, 1)
    end_send(E_ACT)

    w_out_fetch = lcopy(w_out, wrow.at[0, pl.ds(0, w_out.shape[0]), pl.ds(0, model)], wsem.at[1, 0])
    w_out_fetch.start()
    w_out_fetch.wait()

    def queries(i, slot):
        which, k, tile, head = q_index(i)

        def place(lh, first, rest):
            turned = turn(first, cosine[lh, 0], sine[lh, 0], 1).astype(BF16)
            put((qg_own, qg_away), which, lh, lanes_at(k * HD, LANES), turned)
            put((qg_own, qg_away), which, lh, lanes_at(k * HD + LANES, HD - LANES), rest.astype(BF16))

        project(tile_at(tile), slot, place)
        at = pl.ds(pl.multiple_of(head * HD, HD), HD)
        g = nt(cot[0], wrow[0, at, :half]) + nt(cot[1], wrow[0, at, half : 2 * half])
        pieces = by_order(0, g[:blk], g[blk:])
        for lh in range(2):
            put((qg_own, qg_away), which, lh, lanes_at(width + k * HD, HD), pieces[lh].astype(BF16))

    stream(0, 2 * own_heads, (fetch_by(w_qkv, lambda i: q_index(i)[2]),), queries)
    y_copy(Y_QG).start()
    ag_hop(1, 0, 1)
    y_copy(Y_MLP).start()
    pass_on(Y_COT, 0)
    end_pass_x(0)
    own_places = [
        lcopy(own.at[:, h], everyone.at[:, h], local.at[2 + 2 * t + h])
        for t, (own, everyone) in enumerate(((kv_own, kv_all), (qg_own, qg_all)))
        for h in range(2)
    ]
    own_places[0].start()
    own_places[2].start()

    def cols_at(ref, j):
        start = lax.rem(z + j, line) * block_cols
        at = pl.ds(pl.multiple_of(lax.rem(start, half), LANES), block_cols)
        return ref[start // half, :, at]

    def split_cols(ref, j, at, value):
        n = value.shape[1] // 2
        ref[j, 0, at, :] = value[:, :n].astype(BF16)
        ref[j, 1, at, :] = value[:, n:].astype(BF16)

    def split_rows(ref, j, at, value):
        n = value.shape[0] // 2
        ref[j, 0, :, at] = value[:n].astype(BF16)
        ref[j, 1, :, at] = value[n:].astype(BF16)

    def in_order(share, first=0, end=line):
        def one(k, _):
            j = jnp.where(lax.rem(k, 2) == 0, line - 1 - k // 2, k // 2 + 1)
            share(jnp.where(k == line - 1, 0, j))
            return 0

        lax.fori_loop(first, end, one, 0)

    stream(0, hidden_tiles // 2, (row_tile(w_down),), hidden_back)

    def mlp_back(i, slot):
        value = nt(hid[0], wrow[slot, :TILE, :hidden_half]) + nt(
            hid[1], wrow[slot, :TILE, hidden_half : 2 * hidden_half]
        )
        tp_part[MLPB, :, :, tile_at(i)] = value.astype(BF16).reshape(2, blk, TILE)

    model_tiles = model // TILE
    end_pass_x(1)
    ag_hop(0, 0, 2)
    core_copy(0).wait_recv()
    y_copy(Y_ACT).wait_recv()


    def share_down(j):
        g0, g1 = cols_at(cot, j), cols_at(cot_far, j)

        def one(i, _):
            split_cols(
                c_down, j, tile_at(i), tn(act[y, :, tile_at(i)], g0) + tn(act_far[:, tile_at(i)], g1)
            )
            return 0

        lax.fori_loop(0, hidden_half // TILE, one, 0)

    in_order(share_down)
    end_pass(0)
    stream(hidden_tiles // 2, hidden_tiles, (row_tile(w_down),), hidden_back)
    y_copy(Y_HID).start()
    y_copy(Y_ATTN).start()

    y_copy(Y_KV).wait_recv()
    ag_hop(0, 1, 1)
    end_send(E_ACT_FAR)
    own_places[1].start()
    end_pass(1)
    ag_hop(0, 0, 3)
    y_copy(Y_QG).wait_recv()
    own_places[3].start()
    ag_hop(1, 1, 1)
    ag_hop(1, 0, 2)
    stream(0, model_tiles, (row_tile(w_up),), mlp_back)
    pass_x(Y_MLP, 1)
    tp_copy(MLPB, 0).start()
    ag_hop(0, 1, 2)
    ag_hop(0, 1, 3)
    pass_on(Y_MLP, 1)
    tp_next(MLPB, 1)
    y_copy(Y_HID).wait_recv()
    core_copy(1).wait_recv()

    def share_up(j):
        m0, m1 = cols_at(norm, j), cols_at(norm_far, j)

        def one(i, _):
            split_rows(c_up, j, tile_at(i), tn(m0, hid[y, :, tile_at(i)]) + tn(m1, hid_far[:, tile_at(i)]))
            return 0

        lax.fori_loop(0, hidden_half // TILE, one, 0)

    in_order(share_up)
    rs_ends(UP, (1, 2))
    ag_hop(1, 0, 3)
    ag_hop(1, 1, 2)


    @pl.when(next_to_end)
    def _():
        for k in range(2):
            end_share(k).wait_recv()
        blocks = [
            lcopy(
                cot_end.at[pl.ds(k * rows, rows), :],
                wrow.at[k, pl.ds(0, rows), pl.ds(0, model)],
                wsem.at[1, k],
            )
            for k in range(2)
        ]
        for copy in blocks:
            copy.start()
        for item in (E_ACT, E_ACT_FAR):
            end_copy(item, partner).wait_recv()
        for copy in blocks:
            copy.wait()

        def add_tile(i, slot):
            at = tile_at(i)

            def add_block(k, _):
                j = jnp.where(z == 1, k, lax.rem(k + 2, line))
                start = pl.multiple_of(lax.rem(z + j, line) * block_cols, LANES)
                value = tn(wcol[slot, :rows, :], wrow[0, :rows, pl.ds(start, block_cols)]) + tn(
                    wcol[slot, rows : 2 * rows, :], wrow[1, :rows, pl.ds(start, block_cols)]
                )
                n = block_cols // 2
                for side in range(2):
                    c_down[j, side, at, :] = (
                        c_down[j, side, at, :].astype(F32) + value[:, side * n : (side + 1) * n]
                    ).astype(BF16)
                return 0

            lax.fori_loop(0, line - 1, add_block, 0)

        stream(0, hidden_half // TILE, (col_tile(act_end),), add_tile)

    rs_ends(DOWN, (1, 3))
    ag_rest(0, 0, 4)
    ag_rest(0, 1, 4)
    for copy in own_places:
        copy.wait()

    pair = 2 * blk
    same = lax.broadcasted_iota(jnp.int32, (pair, pair), 0) == lax.broadcasted_iota(
        jnp.int32, (pair, pair), 1
    )

    def positions(lh, place, along):
        shape = (1, pair) if along else (pair, 1)
        at = lax.broadcasted_iota(jnp.int32, shape, along)
        here, there = block_number(lh, place, y), block_number(lh, place, 1 - y)
        return at + jnp.where(at < blk, here * blk, there * blk - blk)

    def piece_positions(lh_start, i, along):
        place = lax.rem(z + i, line)
        early, late_ = positions(0, place, along), positions(1, place, along)
        return jnp.where(i < line, early, late_)

    def piece(t):
        def fetch(i, slot):
            ref = (kv_all, qg_all)[t]
            return lcopy(
                ref.at[i // line, pl.ds(2 * lax.rem(i, line), 2)], chunk.at[slot], csem.at[slot]
            )

        return fetch

    for lh in range(2):
        for head in range(own_heads):
            at_k, at_v = head * HD, width + head * HD
            run_m[...] = jnp.full(run_m.shape, masked_value, F32)
            run_l[...] = jnp.zeros(run_l.shape, F32)
            acc_a[...] = jnp.zeros(acc_a.shape, F32)

            def attend(i, slot):
                k = chunk[slot, :, :, at_k : at_k + HD].reshape(pair, HD)
                v = chunk[slot, :, :, at_v : at_v + HD].reshape(pair, HD)
                q = qg_own[lh, :, :, at_k : at_k + HD].reshape(pair, HD)
                s = nt(q, k) * scale
                seen = piece_positions(lh, i, 1) <= positions(lh, z, 0)
                s = jnp.where(seen, s, masked_value)
                old = run_m[...]
                top = jnp.maximum(old, jnp.max(s, axis=1, keepdims=True))
                p = jnp.exp(s - top)
                fade = jnp.exp(old - top)
                run_m[...] = top
                run_l[...] = run_l[...] * fade + jnp.sum(p, axis=1, keepdims=True)
                acc_a[...] = acc_a[...] * fade + nn(p.astype(BF16), v)

            stream(0, line * (lh + 1), (piece(0),), attend)
            out = (acc_a[...] / run_l[...]).astype(BF16)
            att[lh, :, :, at_k : at_k + HD] = out.reshape(2, blk, HD)
            log_total = run_m[...] + jnp.log(run_l[...])
            g = qg_own[lh, :, :, at_v : at_v + HD].reshape(pair, HD)
            dots = jnp.sum(g.astype(F32) * out.astype(F32), axis=1, keepdims=True)
            stats[lh, head, 0:1, :] = jnp.sum(jnp.where(same, log_total, 0.0), 0, keepdims=True)
            stats[lh, head, 1:2, :] = jnp.sum(jnp.where(same, dots, 0.0), 0, keepdims=True)

    def store_order(ref):
        for h in range(2):
            first, second = by_order(h, ref[0, h], ref[1, h])
            ref[0, h] = first
            ref[1, h] = second

    store_order(att)

    def stat_copy(j):
        return rcopy(
            stats, stats_all.at[line - j], st_s.at[j], st_r.at[line - j], (place_of(j), tp)
        )

    for j in range(1, line):
        stat_copy(j).start()
    y_copy(Y_ATT).start()
    rs_ends(UP, (2, line))
    rs_ends(DOWN, (3, line))
    tp_next(MLPB, 2)
    pass_x(Y_ATTN, 2)
    ag_hop(1, 1, 3)

    def share_out(j):
        g0, g1 = cols_at(cot, j), cols_at(cot_far, j)

        def one(i, _):
            a0 = att[:, 0, :, tile_at(i)].reshape(rows, TILE)
            a1 = att[:, 1, :, tile_at(i)].reshape(rows, TILE)
            split_cols(c_out, j, tile_at(i), tn(a0, g0) + tn(a1, g1))
            return 0

        lax.fori_loop(0, width // TILE, one, 0)

    in_order(share_out)


    def undo(value, lh, head, kind):
        at = (3 * head + kind) * HD
        first = value[:, :LANES]
        if kind < 2:
            first = turn(
                first, cosine[lh].reshape(pair, LANES), sine[lh].reshape(pair, LANES), -1
            )
        for lo, hi, part in ((0, LANES, first), (LANES, HD, value[:, LANES:])):
            spot = lanes_at(y * 3 * width + at + lo, hi - lo)
            small[S_QKV : S_QKV + 1, spot] += jnp.sum(part, axis=0, keepdims=True)
            gqkv[lh, :, :, at + lo : at + hi] = part.astype(BF16).reshape(2, blk, hi - lo)

    for lh in range(2):
        for head in range(own_heads):
            at_k, at_v = head * HD, width + head * HD
            run_m[...] = jnp.sum(
                jnp.where(same, stats[lh, head, 0:1, :], 0.0), axis=1, keepdims=True
            )
            run_l[...] = jnp.sum(
                jnp.where(same, stats[lh, head, 1:2, :], 0.0), axis=1, keepdims=True
            )
            acc_a[...] = jnp.zeros(acc_a.shape, F32)

            def back_q(i, slot):
                k = chunk[slot, :, :, at_k : at_k + HD].reshape(pair, HD)
                v = chunk[slot, :, :, at_v : at_v + HD].reshape(pair, HD)
                q = qg_own[lh, :, :, at_k : at_k + HD].reshape(pair, HD)
                g = qg_own[lh, :, :, at_v : at_v + HD].reshape(pair, HD)
                s = nt(q, k) * scale
                seen = piece_positions(lh, i, 1) <= positions(lh, z, 0)
                s = jnp.where(seen, s, masked_value)
                p = jnp.exp(s - run_m[...])
                ds = (p * (nt(g, v) - run_l[...]) * scale).astype(BF16)
                acc_a[...] += nn(ds, k)

            stream(0, line * (lh + 1), (piece(0),), back_q)
            undo(acc_a[...], lh, head, 0)

    rs_step(DOWN, 1)
    rs_step(DOWN, 2)
    rs_step(DOWN, 3) if line > 3 else None
    rs_step(UP, 1)
    rs_step(UP, 2)
    y_copy(Y_ATT).wait_recv()
    w_out_fetch.start()
    w_out_fetch.wait()

    def branch(i, slot):
        value = nn(act[0], wcol[slot, :hidden_half, :]) + nn(
            act[1], wcol[slot, hidden_half : 2 * hidden_half, :]
        )
        own = att[:, 0].reshape(rows, width)
        far = att_far[...].reshape(rows, width)
        mine = wrow[0, pl.ds(pl.multiple_of(y * width, width), width), tile_at(i)]
        theirs = wrow[0, pl.ds(pl.multiple_of((1 - y) * width, width), width), tile_at(i)]
        value += nn(own, mine) + nn(far, theirs)
        tp_part[BRANCH, :, :, tile_at(i)] = value.astype(BF16).reshape(2, blk, TILE)

    stream(0, model_tiles, (col_tile(w_down),), branch)

    tp_copy(BRANCH, 0).start()
    ag_rest(1, 0, 4)
    ag_rest(1, 1, 4)
    for j in range(1, line):
        stat_copy(line - j).wait_recv()
    own_stats = lcopy(stats, stats_all.at[0], local.at[0])
    own_stats.start()
    own_stats.wait()

    for lh in range(2):
        for head in range(own_heads):
            at_k, at_v = head * HD, width + head * HD
            acc_a[...] = jnp.zeros(acc_a.shape, F32)
            acc_b[...] = jnp.zeros(acc_b.shape, F32)

            def back_k(i, slot):
                q = chunk[slot, :, :, at_k : at_k + HD].reshape(pair, HD)
                g = chunk[slot, :, :, at_v : at_v + HD].reshape(pair, HD)
                k = kv_own[lh, :, :, at_k : at_k + HD].reshape(pair, HD)
                v = kv_own[lh, :, :, at_v : at_v + HD].reshape(pair, HD)
                stat = stats_all[lax.rem(i, line), i // line, head]
                s = nt(k, q) * scale
                seen = positions(lh, z, 0) <= piece_positions(lh, i, 1)
                s = jnp.where(seen, s, masked_value)
                p = jnp.exp(s - stat[0:1, :])
                ds = (p * (nt(v, g) - stat[1:2, :]) * scale).astype(BF16)
                acc_a[...] += nn(ds, q)
                acc_b[...] += nn(p.astype(BF16), g)

            stream(lh * line, 2 * line, (piece(1),), back_k)
            undo(acc_a[...], lh, head, 1)
            undo(acc_b[...], lh, head, 2)
    tp_next(BRANCH, 1)
    store_order(gqkv)
    y_copy(Y_GQKV).start()

    pass_on(Y_ATTN, 2)
    core_copy(2).wait_recv()
    core_copy(1).wait_send()
    x_drain(1)
    far_again = lcopy(attn_far, norm_far, local.at[1])
    far_again.start()
    far_again.wait()


    def share_qkv(j):
        m0, m1 = cols_at(attn, j), cols_at(norm_far, j)

        def one(i, _):
            g0 = gqkv[:, 0, :, tile_at(i)].reshape(rows, TILE)
            g1 = gqkv[:, 1, :, tile_at(i)].reshape(rows, TILE)
            split_rows(c_qkv, j, tile_at(i), tn(m0, g0) + tn(m1, g1))
            return 0

        lax.fori_loop(0, 3 * width // TILE, one, 0)

    in_order(share_qkv)
    rs_ends(QKV, (1, line))
    rs_ends(OUT, (1, line))
    rs_step(UP, 3) if line > 3 else None

    y_copy(Y_GQKV).wait_recv()

    def attn_back(i, slot):
        own = gqkv[:, 0].reshape(rows, 3 * width)
        far = gqkv_far[...].reshape(rows, 3 * width)
        mine = wrow[slot, :TILE, pl.ds(pl.multiple_of(y * 3 * width, LANES), 3 * width)]
        theirs = wrow[slot, :TILE, pl.ds(pl.multiple_of((1 - y) * 3 * width, LANES), 3 * width)]
        value = nt(own, mine) + nt(far, theirs)
        tp_part[ATTNB, :, :, tile_at(i)] = value.astype(BF16).reshape(2, blk, TILE)

    stream(0, model_tiles, (row_tile(w_qkv),), attn_back)
    tp_copy(ATTNB, 0).start()
    tp_next(BRANCH, 2)
    tp_next(ATTNB, 1)
    rs_rest(DOWN, 4 if line > 3 else 3)
    rs_finish(DOWN)

    rs_rest(UP, 4 if line > 3 else 3)
    rs_finish(UP)
    rs_step(QKV, 1)
    rs_step(QKV, 2)
    tp_next(ATTNB, 2)
    tp_done(MLPB)
    tp_done(ATTNB)


    def back_norms(i, _):
        at = pl.ds(pl.multiple_of(i * chunk_rows, chunk_rows), chunk_rows)
        at_part = pl.ds(pl.multiple_of(lax.rem(i * chunk_rows, blk), chunk_rows), chunk_rows)
        which = i * chunk_rows // blk
        unit, inv_scale = unit_of(at)
        total = jnp.zeros((chunk_rows, model), F32)
        for n, part in ((0, ATTNB), (1, MLPB)):
            value = tp_part[part, which, at_part, :].astype(F32)
            small[S_GAIN + n : S_GAIN + n + 1, :model] += jnp.sum(value * unit, 0, keepdims=True)
            small[S_SHIFT + n : S_SHIFT + n + 1, :model] += jnp.sum(value, 0, keepdims=True)
            total = total + value * gain[n : n + 1, :]
        cbuf[at, :] = cbuf[at, :] + inv_scale * (
            total
            - jnp.mean(total, axis=-1, keepdims=True)
            - unit * jnp.mean(total * unit, axis=-1, keepdims=True)
        )
        return 0

    lax.fori_loop(0, rows // chunk_rows, back_norms, 0)
    grad_store = lcopy(cbuf, grad_o, local.at[1])
    grad_store.start()

    small_pair = rcopy(small, small_recv.at[0], sm_s.at[0], sm_r.at[0], partner)
    small_pair.start()
    small_pair.wait()
    small[...] += small_recv[0]

    def small_copy(j):
        return rcopy(
            small, small_recv.at[line - j], sm_s.at[j], sm_r.at[line - j], (place_of(j), tp)
        )

    for j in range(1, line):
        small_copy(j).start()
    rs_rest(QKV, 3)
    tp_done(BRANCH)

    def stream_rows(i, _):
        at = pl.ds(pl.multiple_of(i * chunk_rows, chunk_rows), chunk_rows)
        at_part = pl.ds(pl.multiple_of(lax.rem(i * chunk_rows, blk), chunk_rows), chunk_rows)
        which = i * chunk_rows // blk
        xbuf[at, :] = xbuf[at, :] + out_bias[...] + tp_part[BRANCH, which, at_part, :].astype(F32)
        return 0

    lax.fori_loop(0, rows // chunk_rows, stream_rows, 0)
    stream_store = lcopy(xbuf, stream_o, local.at[0])
    stream_store.start()
    rs_step(OUT, 1)
    rs_step(OUT, 2)
    rs_finish(QKV)
    rs_rest(OUT, 3)
    rs_finish(OUT)
    for j in range(1, line):
        small_copy(line - j).wait_recv()
    for j in range(1, line):
        small_copy(j).wait_send()
    small_recv[0] = small[...]
    small[...] = small_recv[lax.rem(line - z, line)]
    for p in range(1, line):
        small[...] += small_recv[lax.rem(p + line - z, line)]
    small_store = lcopy(small, small_o, local.at[2])
    small_store.start()

    for t in range(2):
        for h in range(2):
            ag_drain(t, h)
    for item in (Y_KV, Y_QG, Y_COT, Y_MLP, Y_ATTN, Y_ACT, Y_HID, Y_ATT, Y_GQKV):
        y_copy(item).wait_send()
    core_copy(0).wait_send()
    core_copy(2).wait_send()
    x_drain(0)
    x_drain(2)
    for j in range(1, line):
        stat_copy(j).wait_send()
    for i in range(3):
        tp_drain(i)
    grad_store.wait()
    small_store.wait()
    stream_store.wait()
    for t in range(4):
        rs_drain(t)
    end_drain()


def layer(line, n_tp, order, stream_in, cotangent, ln_gain, ln_bias, w_qkv, b_qkv, w_out, out_bias, w_up, b_up, w_down):
    rows, model = stream_in.shape
    half, blk = model // 2, rows // 2
    hidden = w_up.shape[1]
    hidden_half = hidden // 2
    width = w_out.shape[0] // 2
    own_heads = width // HD
    part_cols = model // line // 2
    pair = 2 * blk
    tp_steps = 0
    while (2 << tp_steps) < n_tp:
        tp_steps += 1
    small_shape = (8, max(model, hidden, 6 * width))
    shares = (
        (2, hidden_half, part_cols),
        (2, part_cols, hidden_half),
        (2, width, part_cols),
        (2, part_cols, 3 * width),
    )
    b = lambda *s: jax.ShapeDtypeStruct(s, BF16)
    f = lambda *s: jax.ShapeDtypeStruct(s, F32)
    vb = lambda *s: pltpu.VMEM(s, BF16)
    vf = lambda *s: pltpu.VMEM(s, F32)
    dma = pltpu.SemaphoreType.DMA
    outs = (
        b(hidden, part_cols),
        b(part_cols, hidden),
        b(2 * width, part_cols),
        b(part_cols, 6 * width),
        f(rows, model),
        f(rows, model),
        f(*small_shape),
        b(2, 2 * line, blk, 2 * width),
        b(2, 2 * line, blk, 2 * width),
        b(line + 1, *shares[0]),
        b(line + 1, *shares[1]),
        b(line + 1, *shares[2]),
        b(line + 1, *shares[3]),
        b(2, rows, half),
        b(3, blk, model),
        b(2 * rows, model),
        b(2 * rows, hidden_half),
    )
    wide = max(model, hidden)
    scratch = (
        [vf(rows, model)] * 2
        + [vb(2, rows, half)] * 5
        + [vb(2, rows, hidden_half)] * 2
        + [vb(rows, hidden_half)] * 2
        + [vb(2, wide, TILE), vb(2, max(TILE, 2 * width), wide)]
        + [vb(line, *s) for s in shares]
        + [vb(*s) for s in shares]
        + [vb(3, 2, blk, model), vb(3, tp_steps + 1, blk, model)]
        + [vb(2, 2, blk, 2 * width)] * 2
        + [vb(2, blk, 2 * width)] * 2
        + [
            vb(2, 2, blk, 2 * width),
            vb(2, 2, blk, width),
            vb(2, blk, width),
            vf(2, own_heads, 2, pair),
            vf(line, 2, own_heads, 2, pair),
            vb(2, 2, blk, 3 * width),
            vb(2, blk, 3 * width),
            vf(pair, HD),
            vf(pair, HD),
            vf(pair, 1),
            vf(pair, 1),
            vf(2, 2, blk, LANES),
            vf(2, 2, blk, LANES),
            vf(*small_shape),
            vf(line, *small_shape),
            dma((2, 2, 2, line)),
            dma((2, 2, line)),
            dma((Y_FIN + 4,)),
            dma((Y_FIN + 4,)),
            dma((3,)),
            dma((3,)),
            dma((3, n_tp // 2)),
            dma((3, n_tp // 2)),
            dma((4, line)),
            dma((4, line + 1)),
            dma((3, tp_steps + 2)),
            dma((3, tp_steps + 2)),
            dma((line,)),
            dma((line,)),
            dma((line,)),
            dma((line,)),
            dma((6,)),
            dma((6,)),
            dma((2, n_tp // 2)),
            dma((2, n_tp // 2)),
            dma((9,)),
            dma((2, 2)),
            dma((2,)),
            dma((4,)),
        ]
    )
    blocks = order.shape[0]
    operands = (
        order,
        stream_in,
        cotangent,
        w_up,
        w_down,
        w_out,
        w_qkv,
        ln_gain,
        ln_bias,
        b_qkv.reshape(1, -1),
        b_up.reshape(1, -1),
        out_bias.reshape(1, -1),
        jnp.asarray(rope_tables(np.arange(blocks) * blk)),
        jnp.asarray(rope_tables(np.arange(blk))),
    )
    return pl.pallas_call(
        functools.partial(layer_kernel, line, n_tp),
        name="layer",
        out_shape=outs,
        in_specs=[SMEM] + [ANY] * 6 + [VMEM] * 7,
        out_specs=[ANY] * len(outs),
        scratch_shapes=scratch,
        cost_estimate=pl.CostEstimate(
            flops=40 * rows * model * hidden,
            transcendentals=rows * hidden,
            bytes_accessed=8 * w_up.size,
        ),
        compiler_params=pltpu.CompilerParams(
            collective_id=0, has_side_effects=True, vmem_limit_bytes=67043328
        ),
    )(*operands)


def shards(
    n_ctx,
    n_tp,
    stream_in,
    cotangent,
    ln_gain,
    ln_bias,
    w_qkv,
    b_qkv,
    w_out,
    out_bias,
    w_up,
    b_up,
    w_down,
    block_order,
):
    model, hidden = w_up.shape
    (down, up, out, qkv, stream_out, grad_in, small, *_) = layer(
        n_ctx // 2,
        n_tp,
        block_order,
        stream_in,
        cotangent,
        ln_gain,
        ln_bias,
        w_qkv,
        b_qkv,
        w_out,
        out_bias,
        w_up,
        b_up,
        w_down,
    )
    return (
        stream_out,
        grad_in,
        qkv.astype(F32),
        small[S_QKV, : w_qkv.shape[1]],
        out.astype(F32),
        small[S_OUT, :model],
        up.astype(F32),
        small[S_UP, :hidden],
        down.astype(F32),
        small[S_GAIN : S_GAIN + 2, :model],
        small[S_SHIFT : S_SHIFT + 2, :model],
    )


def solution(mesh):
    placed = (
        P("ctx", None),
        P("ctx", None),
        P(),
        P(),
        P(None, "tp"),
        P("tp"),
        P("tp", None),
        P(),
        P(None, "tp"),
        P("tp"),
        P("tp", None),
        P(),
    )
    return jax.shard_map(
        functools.partial(shards, mesh.shape["ctx"], mesh.shape["tp"]),
        mesh=mesh,
        in_specs=placed,
        out_specs=(
            P("ctx", None),
            P("ctx", None),
            P("ctx", "tp"),
            P("tp"),
            P("tp", "ctx"),
            P(),
            P("ctx", "tp"),
            P("tp"),
            P("tp", "ctx"),
            P(),
            P(),
        ),
        check_vma=False,
    )
```

```python
import functools
import math

import jax
import jax.numpy as jnp
import numpy as np
from jax import lax
from jax.experimental import pallas as pl
from jax.experimental.pallas import tpu as pltpu
from jax.sharding import PartitionSpec as P

HD = 256
ROT = 64
LANES = 128
TILE = 256

masked_value = -1e30
norm_epsilon = 1e-05
root_half = 0.7071067811865476
inverse_root_two_pi = 0.3989422804014327

F32 = jnp.float32
BF16 = jnp.bfloat16
MESH = pl.DeviceIdType.MESH
ANY = pl.BlockSpec(memory_space=pl.ANY)
VMEM = pl.BlockSpec(memory_space=pltpu.VMEM)
SMEM = pl.BlockSpec(memory_space=pltpu.SMEM)


def nt(a, b):
    return lax.dot_general(a, b, (((1,), (1,)), ((), ())), preferred_element_type=F32)


def nn(a, b):
    return lax.dot_general(a, b, (((1,), (0,)), ((), ())), preferred_element_type=F32)


def tn(a, b):
    return lax.dot_general(a, b, (((0,), (0,)), ((), ())), preferred_element_type=F32)


def rope_tables(positions):
    half_rot = ROT // 2
    frequency = np.exp(np.arange(half_rot) * (-2.0 * math.log(10000.0) / ROT))
    angles = np.asarray(positions, np.float64)[:, None] * frequency
    table = np.zeros((2, angles.shape[0], LANES), np.float32)
    table[0] = 1.0
    for lo in (0, half_rot):
        table[0, :, lo : lo + half_rot] = np.cos(angles)
        table[1, :, lo : lo + half_rot] = np.sin(angles)
    return table


def turn(first, cosine, sine, sign):
    half_rot = ROT // 2
    scaled = first * sine if sign < 0 else first
    lane = lax.broadcasted_iota(jnp.int32, first.shape, 1)
    down = jnp.where(lane < half_rot, pltpu.roll(scaled, LANES - half_rot, 1), 0.0)
    up = jnp.where(
        jnp.logical_and(lane >= half_rot, lane < ROT), pltpu.roll(scaled, half_rot, 1), 0.0
    )
    if sign < 0:
        return first * cosine + (down - up)
    return first * cosine + (up - down) * sine


DOWN, UP, OUT, QKV = range(4)
(Y_KV, Y_QG, Y_COT, Y_MLP, Y_ATTN, Y_ACT, Y_HID, Y_ATT, Y_GQKV, Y_FIN) = range(10)
BRANCH, MLPB, ATTNB = range(3)
S_GAIN, S_SHIFT, S_OUT, S_UP, S_QKV = 0, 2, 4, 5, 6


def layer_kernel(
    line,
    n_tp,
    order,
    stream_in,
    cotangent,
    w_up,
    w_down,
    w_out,
    w_qkv,
    gain,
    shift,
    b_qkv,
    b_up,
    out_bias,
    block_table,
    row_table,
    down_o,
    up_o,
    out_o,
    qkv_o,
    stream_o,
    grad_o,
    small_o,
    kv_all,
    qg_all,
    rs_down,
    rs_up,
    rs_out,
    rs_qkv,
    attn_far,
    tp_far,
    cot_end,
    act_end,
    xbuf,
    cbuf,
    cot,
    cot_far,
    norm,
    norm_far,
    attn,
    act,
    hid,
    act_far,
    hid_far,
    wcol,
    wrow,
    c_down,
    c_up,
    c_out,
    c_qkv,
    stage_down,
    stage_up,
    stage_out,
    stage_qkv,
    tp_part,
    tp_recv,
    kv_own,
    qg_own,
    kv_away,
    qg_away,
    chunk,
    att,
    att_far,
    stats,
    stats_all,
    gqkv,
    gqkv_far,
    acc_a,
    acc_b,
    run_m,
    run_l,
    cosine,
    sine,
    small,
    small_pair,
    small_sent,
    small_recv,
    ag_s,
    ag_r,
    y_s,
    y_r,
    core_s,
    core_r,
    x_s,
    x_r,
    rs_s,
    rs_r,
    tp_s,
    tp_r,
    st_s,
    st_r,
    sm_s,
    sm_r,
    end_s,
    end_r,
    ex_s,
    ex_r,
    local,
    wsem,
    csem,
    tsem,
):
    me, tp = lax.axis_index("ctx"), lax.axis_index("tp")
    z, y = me // 2, lax.rem(me, 2)
    core = lax.rem(tp, 2)
    partner = (me + 1 - 2 * y, tp)
    sibling = (me, tp + 1 - 2 * core)
    right, left = (me + 2, tp), (me - 2, tp)
    far_steps = []
    step = 2
    while step < n_tp:
        far_steps.append((me, tp + step - 2 * step * lax.rem(tp // step, 2)))
        step *= 2

    rows = norm.shape[1]
    blk = rows // 2
    across = n_tp // 2
    xpos = tp // 2
    x_others = [(me, lax.rem(tp + 2 * k, n_tp)) for k in range(1, across)]
    half = norm.shape[2]
    hidden_half = act.shape[2]
    own_heads = kv_own.shape[-1] // (2 * HD)
    width = own_heads * HD
    block_cols = 2 * half // line
    scale = HD ** (-0.5)

    def place_of(j):
        return lax.rem(z + j, line) * 2 + y

    barrier = pltpu.get_barrier_semaphore()
    greet = [partner, sibling] + x_others + [(place_of(j), tp) for j in range(1, line)]
    for device in greet:
        pl.semaphore_signal(barrier, inc=1, device_id=device, device_id_type=MESH)

    def rcopy(src, dst, s, r, device):
        return pltpu.make_async_remote_copy(
            src_ref=src, dst_ref=dst, send_sem=s, recv_sem=r, device_id=device, device_id_type=MESH
        )

    def lcopy(src, dst, sem):
        return pltpu.make_async_copy(src, dst, sem)

    def fin_parts(t):
        c = (c_down, c_up, c_out, c_qkv)[t]
        if t == DOWN:
            dst = down_o.at[pl.ds(pl.multiple_of(y * hidden_half, hidden_half), hidden_half), :]
        elif t == UP:
            dst = up_o.at[:, pl.ds(pl.multiple_of(y * hidden_half, hidden_half), hidden_half)]
        elif t == OUT:
            dst = out_o.at[pl.ds(pl.multiple_of(y * width, width), width), :]
        else:
            dst = qkv_o.at[:, pl.ds(pl.multiple_of(y * 3 * width, 3 * width), 3 * width)]
        return c, dst

    def part_rows(x):
        n = rows // across
        return pl.ds(pl.multiple_of(x * n, n), n)

    def y_copy(item, t=0):
        if item == Y_KV:
            src, dst = kv_away, kv_own.at[:, 1]
        elif item == Y_QG:
            src, dst = qg_away, qg_own.at[:, 1]
        elif item == Y_COT:
            src, dst = cot.at[core, part_rows(xpos)], cot_far.at[core, part_rows(xpos)]
        elif item == Y_MLP:
            src, dst = norm.at[core, part_rows(xpos)], norm_far.at[core, part_rows(xpos)]
        elif item == Y_ATTN:
            src, dst = attn.at[core, part_rows(xpos)], attn_far.at[core, part_rows(xpos)]
        elif item == Y_ACT:
            src, dst = act.at[1 - y], act_far
        elif item == Y_HID:
            src, dst = hid.at[1 - y], hid_far
        elif item == Y_ATT:
            src, dst = att.at[:, 1], att_far
        elif item == Y_GQKV:
            src, dst = gqkv.at[:, 1], gqkv_far
        else:
            c, dst = fin_parts(t)
            src = c.at[0, 1 - y]
            item = Y_FIN + t
        return rcopy(src, dst, y_s.at[item], y_r.at[item], partner)

    def core_copy(k):
        ref = (cot_far, norm_far, attn_far)[k]
        return rcopy(ref.at[core], ref.at[core], core_s.at[k], core_r.at[k], sibling)

    def x_copy(k, n):
        ref = (cot_far, norm_far, attn_far)[k].at[core, part_rows(xpos)]
        return rcopy(ref, ref, x_s.at[k, n], x_r.at[k, n], x_others[n])

    def x_arrival(k, n):
        ref = (cot_far, norm_far, attn_far)[k].at[core, part_rows(lax.rem(xpos + across - n - 1, across))]
        return rcopy(ref, ref, x_s.at[k, n], x_r.at[k, n], x_others[n])

    def pass_x(item, k):
        y_copy(item).wait_recv()
        for n in range(across - 1):
            x_copy(k, n).start()

    def pass_on(item, k):
        for n in range(across - 1):
            x_arrival(k, n).wait_recv()
        core_copy(k).start()

    def x_drain(k):
        for n in range(across - 1):
            x_copy(k, n).wait_send()

    E_COT, E_COT_FAR, E_ACT, E_ACT_FAR = range(4)
    next_to_end = jnp.logical_or(z == 1, z == line - 2)

    def end_part(k, x):
        n = rows // across
        return cot_end.at[
            pl.ds(pl.multiple_of(k * rows + x * n, n), n), pl.ds(pl.multiple_of(core * half, half), half)
        ]

    def end_copy(item, device):
        if item == E_COT:
            src, dst = cot.at[core, part_rows(xpos)], end_part(0, xpos)
        elif item == E_COT_FAR:
            src, dst = end_part(0, xpos), end_part(1, xpos)
        elif item == E_ACT:
            src, dst = act.at[y], act_end.at[pl.ds(0, rows), :]
        else:
            src, dst = act_far, act_end.at[pl.ds(rows, rows), :]
        return rcopy(src, dst, end_s.at[item], end_r.at[item], device)

    def end_x(k, n, arriving):
        x = lax.rem(xpos + across - n - 1, across) if arriving else xpos
        ref = end_part(k, x)
        return rcopy(ref, ref, ex_s.at[k, n], ex_r.at[k, n], x_others[n])

    def end_share(k):
        ref = cot_end.at[pl.ds(k * rows, rows), pl.ds(pl.multiple_of(core * half, half), half)]
        return rcopy(ref, ref, end_s.at[4 + k], end_r.at[4 + k], sibling)

    def end_send(item):
        @pl.when(z == 0)
        def _():
            end_copy(item, right).start()

        @pl.when(z == line - 1)
        def _():
            end_copy(item, left).start()

    def end_pass_x(k):
        @pl.when(next_to_end)
        def _():
            end_copy(E_COT + k, partner).wait_recv()
            for n in range(across - 1):
                end_x(k, n, False).start()
            if k == 0:
                end_copy(E_COT_FAR, partner).start()

    def end_pass(k):
        @pl.when(next_to_end)
        def _():
            for n in range(across - 1):
                end_x(k, n, True).wait_recv()
            end_share(k).start()

    def end_drain():
        @pl.when(jnp.logical_or(z == 0, z == line - 1))
        def _():
            for item in (E_COT, E_ACT, E_ACT_FAR):
                end_copy(item, partner).wait_send()

        @pl.when(next_to_end)
        def _():
            end_copy(E_COT_FAR, partner).wait_send()
            for k in range(2):
                end_share(k).wait_send()
                for n in range(across - 1):
                    end_x(k, n, False).wait_send()

    def ag_copy(t, h, to, hop, j_src, j_dst):
        ref = (kv_all, qg_all)[t]
        src = ref.at[:, 2 * j_src + h]
        if isinstance(hop, int) and hop == 1:
            src = (kv_own, qg_own)[t].at[:, h]
        return rcopy(
            src,
            ref.at[:, 2 * j_dst + h],
            ag_s.at[t, h, to, hop],
            ag_r.at[t, h, j_dst],
            (right, left)[to],
        )

    def ag_send_when(hop):
        return (
            jnp.logical_and(z >= hop - 1, z <= line - 2),
            jnp.logical_and(z + hop - 1 <= line - 1, z >= 1),
        )

    def ag_hop(t, h, hop, only=None):
        first = isinstance(hop, int) and hop == 1
        to_right, to_left = ag_send_when(hop)
        if only is not None:
            to_right, to_left = jnp.logical_and(to_right, only), jnp.logical_and(to_left, only)

        @pl.when(to_right)
        def _():
            if not first:
                ag_copy(t, h, 0, hop - 1, line - hop + 1, line - hop + 1).wait_recv()
            ag_copy(t, h, 0, hop, lax.rem(line - hop + 1, line), line - hop).start()

        @pl.when(to_left)
        def _():
            if not first:
                ag_copy(t, h, 1, hop - 1, hop - 1, hop - 1).wait_recv()
            ag_copy(t, h, 1, hop, hop - 1, hop).start()

    def ag_rest(t, h, hop):
        def one(i, _):
            ag_hop(t, h, i)
            return 0

        def come(i, _):
            ag_copy(t, h, 0, i, i, i).wait_recv()
            return 0

        if hop < line:
            lax.fori_loop(hop, line, one, 0)

        @pl.when(jnp.logical_or(z == 0, z == line - 1))
        def _():
            lax.fori_loop(1, line, come, 0)

    def ag_drain(t, h):
        def one(hop, _):
            to_right, to_left = ag_send_when(hop)

            @pl.when(to_right)
            def _():
                ag_copy(t, h, 0, hop, lax.rem(line - hop + 1, line), line - hop).wait_send()

            @pl.when(to_left)
            def _():
                ag_copy(t, h, 1, hop, hop - 1, hop).wait_send()

            return 0

        lax.fori_loop(1, line, one, 0)

    rs = (
        (c_down, rs_down, stage_down),
        (c_up, rs_up, stage_up),
        (c_out, rs_out, stage_out),
        (c_qkv, rs_qkv, stage_qkv),
    )

    def rs_copy(t, p, j, slot, device):
        c, recv, _ = rs[t]
        return rcopy(
            c.at[j, p], recv.at[slot, p], rs_s.at[t, p, j], rs_r.at[t, p, slot], device
        )

    def rs_take(t, p, j, slot):
        c, recv, held = rs[t]
        rs_copy(t, p, j, slot, partner).wait_recv()
        copy = lcopy(recv.at[slot, p], held.at[p], tsem.at[t])
        copy.start()
        copy.wait()
        n = c.shape[2]
        part = min(64, n)

        def add(i, _):
            at = pl.ds(pl.multiple_of(i * part, part), part)
            c[j, p, at, :] = (c[j, p, at, :].astype(F32) + held[p, at, :].astype(F32)).astype(BF16)
            return 0

        lax.fori_loop(0, n // part, add, 0)

    def first_from(t):
        return 2 if t == DOWN else 1

    def rs_ends(t, hops, parts=(0, 1)):
        first = first_from(t)

        def one(hop, _):
            for p in parts:

                @pl.when(jnp.logical_and(z == first - 1, hop >= first))
                def _():
                    rs_copy(t, p, line - hop, line - hop - 1, right).start()

                @pl.when(jnp.logical_and(z == line - first, hop >= first))
                def _():
                    rs_copy(t, p, hop, hop + 1, left).start()

            return 0

        lax.fori_loop(*hops, one, 0)

    near = 2 * z < line

    def halves(step):
        def one(p, _):
            step(p)
            return 0

        lax.fori_loop(0, 2, one, 0)

    def rs_right(t, hop, only):
        jr, first = line - hop, first_from(t)

        @pl.when(jnp.logical_and(only, jnp.logical_and(hop >= z + 1, z >= first)))
        def _():
            def step(p):
                rs_take(t, p, jr, jr)
                rs_copy(t, p, jr, jr - 1, right).start()

            halves(step)

    def rs_left(t, hop, only):
        jl, first = hop, first_from(t)

        @pl.when(jnp.logical_and(only, jnp.logical_and(hop >= line - z, z <= line - 1 - first)))
        def _():
            def step(p):
                rs_take(t, p, jl, jl)
                rs_copy(t, p, jl, jl + 1, left).start()

            halves(step)

    def rs_cross(t, hop):
        rs_right(t, hop, near)
        rs_left(t, hop, jnp.logical_not(near))

    def rs_home(t, hop):
        rs_right(t, hop, jnp.logical_not(near))
        rs_left(t, hop, near)

    def rs_rest(t, hop):
        def one(i, _):
            rs_cross(t, i)
            rs_home(t, i)
            return 0

        if hop < line:
            lax.fori_loop(hop, line, one, 0)

    def rs_finish(t):
        first = first_from(t)
        c, dst = fin_parts(t)

        def take(k, _):
            p = jnp.where(k == 0, 1 - y, y)

            @pl.when(z >= first)
            def _():
                rs_take(t, p, 0, 0)

            @pl.when(z <= line - 1 - first)
            def _():
                rs_take(t, p, 0, line)

            @pl.when(k == 0)
            def _():
                y_copy(Y_FIN, t).start()

            return 0

        lax.fori_loop(0, 2, take, 0)
        lcopy(c.at[0, y], dst, local.at[4 + t]).start()

    def rs_drain(t):
        sends = jnp.logical_and(z >= first_from(t) - 1, z <= line - first_from(t))

        def one(j, _):
            for p in range(2):

                @pl.when(jnp.logical_and(sends, j <= line - 1 - z))
                def _():
                    rs_copy(t, p, j, j - 1, right).wait_send()

                @pl.when(jnp.logical_and(sends, j > line - 1 - z))
                def _():
                    rs_copy(t, p, j, j + 1, left).wait_send()

            return 0

        lax.fori_loop(1, line, one, 0)
        c, dst = fin_parts(t)
        y_copy(Y_FIN, t).wait()
        lcopy(c.at[0, y], dst, local.at[4 + t]).wait()

    last = len(far_steps) + 1

    def tp_copy(i, k):
        part = tp_part.at[i]
        if k == 0:
            src, dst, device = part.at[1 - core], tp_recv.at[i, 0], sibling
        elif k < last:
            src, dst, device = part.at[core], tp_recv.at[i, k], far_steps[k - 1]
        else:
            src, dst, device = part.at[core], tp_far.at[i], sibling
        return rcopy(src, dst, tp_s.at[i, k], tp_r.at[i, k], device)

    def tp_add(i, k):
        part = 64

        def add(n, _):
            at = pl.ds(pl.multiple_of(n * part, part), part)
            tp_part[i, core, at, :] = (
                tp_part[i, core, at, :].astype(F32) + tp_recv[i, k, at, :].astype(F32)
            ).astype(BF16)
            return 0

        lax.fori_loop(0, blk // part, add, 0)

    def tp_next(i, k):
        if k > 1:
            tp_copy(i, k - 1).wait_send()
        tp_copy(i, k - 1).wait_recv()
        tp_add(i, k - 1)
        tp_copy(i, k).start()

    def tp_done(i):
        tp_copy(i, last).wait_recv()
        tp_copy(i, 0).wait_send()

        other = lcopy(tp_far.at[i], tp_part.at[i, 1 - core], local.at[8])
        other.start()
        other.wait()

    def tp_drain(i):
        tp_copy(i, last).wait_send()

    def stream(lo, hi, fetches, body):
        for f in fetches:
            f(lo, lax.rem(lo, 2)).start()

        def one(i, _):
            slot = lax.rem(i, 2)

            @pl.when(i + 1 < hi)
            def _():
                for f in fetches:
                    f(i + 1, 1 - slot).start()

            for f in fetches:
                f(i, slot).wait()
            body(i, slot)
            return 0

        lax.fori_loop(lo, hi, one, 0)

    def col_tile(w):
        def fetch(i, slot):
            at = pl.ds(pl.multiple_of(i * TILE, TILE), TILE)
            return lcopy(w.at[:, at], wcol.at[slot, pl.ds(0, w.shape[0]), :], wsem.at[0, slot])

        return fetch

    def row_tile(w):
        def fetch(i, slot):
            at = pl.ds(pl.multiple_of(i * TILE, TILE), TILE)
            return lcopy(w.at[at, :], wrow.at[slot, pl.ds(0, TILE), pl.ds(0, w.shape[1])], wsem.at[1, slot])

        return fetch

    x_load = lcopy(stream_in, xbuf, local.at[0])
    c_load = lcopy(cotangent, cbuf, local.at[1])
    c_load.start()
    x_load.start()

    def number(place, side, k):
        return order[4 * place + 2 * side + k]

    late = [number(z, s, 0) > number(z, s, 1) for s in (y, 1 - y)]

    def block_number(lh, place, side):
        first, second = number(place, side, 0), number(place, side, 1)
        return jnp.minimum(first, second) if lh == 0 else jnp.maximum(first, second)

    for lh in range(2):
        for h in range(2):
            at_block = block_table[:, pl.ds(block_number(lh, z, (y, 1 - y)[h]), 1), :]
            cb, sb = at_block[0], at_block[1]
            ci, si = row_table[0], row_table[1]
            cosine[lh, h] = cb * ci - sb * si
            sine[lh, h] = sb * ci + cb * si

    def by_order(h, first, second):
        return jnp.where(late[h], second, first), jnp.where(late[h], first, second)

    small[...] = jnp.zeros(small.shape, F32)
    model = 2 * half
    chunk_rows = 64
    c_load.wait()

    def cast(i, _):
        at = pl.ds(pl.multiple_of(i * chunk_rows, chunk_rows), chunk_rows)
        c = cbuf[at, :]
        small[S_OUT : S_OUT + 1, :model] += jnp.sum(c, axis=0, keepdims=True)
        c = c.astype(BF16)
        cot[0, at, :] = c[:, :half]
        cot[1, at, :] = c[:, half:]
        return 0

    lax.fori_loop(0, rows // chunk_rows, cast, 0)
    pl.semaphore_wait(barrier, len(greet))
    y_copy(Y_COT).start()
    end_send(E_COT)

    x_load.wait()

    def unit_of(at):
        x = xbuf[at, :]
        centred = x - jnp.mean(x, axis=-1, keepdims=True)
        variance = jnp.mean(centred * centred, axis=-1, keepdims=True)
        inv_scale = lax.rsqrt(variance + norm_epsilon)
        return centred * inv_scale, inv_scale

    def norms(i, _):
        at = pl.ds(pl.multiple_of(i * chunk_rows, chunk_rows), chunk_rows)
        unit, _ = unit_of(at)
        for n, ref in ((0, attn), (1, norm)):
            value = (unit * gain[n : n + 1, :] + shift[n : n + 1, :]).astype(BF16)
            ref[0, at, :] = value[:, :half]
            ref[1, at, :] = value[:, half:]
        return 0

    lax.fori_loop(0, rows // chunk_rows, norms, 0)

    def tile_at(i):
        return pl.ds(pl.multiple_of(i * TILE, TILE), TILE)

    def hidden_at(i):
        at = pl.ds(pl.multiple_of(lax.rem(i * TILE, hidden_half), TILE), TILE)
        return i * TILE // hidden_half, at

    def activate(i, slot):
        h = nn(norm[0], wcol[slot, :half, :]) + nn(norm[1], wcol[slot, half : 2 * half, :])
        h = h + b_up[:, tile_at(i)]
        gate = 0.5 * (1.0 + lax.erf(h * root_half))
        which, at = hidden_at(i)
        act[which, :, at] = (h * gate).astype(BF16)
        slope = gate + h * jnp.exp(-0.5 * h * h) * inverse_root_two_pi
        hid[which, :, at] = slope.astype(BF16)

    def hidden_back(i, slot):
        g = nt(cot[0], wrow[slot, :TILE, :half]) + nt(cot[1], wrow[slot, :TILE, half : 2 * half])
        which, at = hidden_at(i)
        g = g * hid[which, :, at].astype(F32)
        small[S_UP : S_UP + 1, tile_at(i)] = jnp.sum(g, axis=0, keepdims=True)
        hid[which, :, at] = g.astype(BF16)

    hidden_tiles = 2 * hidden_half // TILE
    def project(at, slot, place):
        value = nn(attn[0], wcol[slot, :half, :]) + nn(attn[1], wcol[slot, half : 2 * half, :])
        value = value + b_qkv[at][None, :]
        pieces = by_order(0, value[:blk], value[blk:])
        for lh in range(2):
            first, rest = pieces[lh][:, :LANES], pieces[lh][:, LANES:]
            place(lh, first, rest)

    def put(refs, which, lh, at, value):
        mine, away = refs

        @pl.when(which == 0)
        def _():
            mine[lh, 0, :, at] = value

        @pl.when(which == 1)
        def _():
            away[lh, :, at] = value

    def kv_index(i):
        which = 1 - i // (2 * own_heads)
        k, kind = lax.rem(i, 2 * own_heads) // 2, 1 + lax.rem(i, 2)
        head = jnp.where(which == 0, y, 1 - y) * own_heads + k
        return which, k, kind, 3 * head + kind

    def q_index(i):
        which = 1 - i // own_heads
        k = lax.rem(i, own_heads)
        head = jnp.where(which == 0, y, 1 - y) * own_heads + k
        return which, k, 3 * head, head

    def fetch_by(w, index):
        def fetch(i, slot):
            return lcopy(w.at[:, tile_at(index(i))], wcol.at[slot, pl.ds(0, w.shape[0]), :], wsem.at[0, slot])

        return fetch

    def lanes_at(start, n):
        return pl.ds(pl.multiple_of(start, LANES), n)

    def keys_values(i, slot):
        which, k, kind, tile = kv_index(i)
        base = jnp.where(kind == 1, 0, width) + k * HD

        def place(lh, first, rest):
            turned = turn(first, cosine[lh, 0], sine[lh, 0], 1)
            first = jnp.where(kind == 1, turned, first).astype(BF16)
            put((kv_own, kv_away), which, lh, lanes_at(base, LANES), first)
            put((kv_own, kv_away), which, lh, lanes_at(base + LANES, HD - LANES), rest.astype(BF16))

        project(tile_at(tile), slot, place)

    w_out_fetch = lcopy(w_out, wrow.at[0, pl.ds(0, w_out.shape[0]), pl.ds(0, model)], wsem.at[1, 0])

    def queries(i, slot):
        which, k, tile, head = q_index(i)

        def place(lh, first, rest):
            turned = turn(first, cosine[lh, 0], sine[lh, 0], 1).astype(BF16)
            put((qg_own, qg_away), which, lh, lanes_at(k * HD, LANES), turned)
            put((qg_own, qg_away), which, lh, lanes_at(k * HD + LANES, HD - LANES), rest.astype(BF16))

        project(tile_at(tile), slot, place)
        at = pl.ds(pl.multiple_of(head * HD, HD), HD)
        g = nt(cot[0], wrow[0, at, :half]) + nt(cot[1], wrow[0, at, half : 2 * half])
        pieces = by_order(0, g[:blk], g[blk:])
        for lh in range(2):
            put((qg_own, qg_away), which, lh, lanes_at(width + k * HD, HD), pieces[lh].astype(BF16))

    own_places = [
        lcopy(own.at[:, h], everyone.at[:, h], local.at[2 + 2 * t + h])
        for t, (own, everyone) in enumerate(((kv_own, kv_all), (qg_own, qg_all)))
        for h in range(2)
    ]

    def cols_at(ref, j):
        start = lax.rem(z + j, line) * block_cols
        at = pl.ds(pl.multiple_of(lax.rem(start, half), LANES), block_cols)
        return ref[start // half, :, at]

    def split_cols(ref, j, at, value):
        n = value.shape[1] // 2
        ref[j, 0, at, :] = value[:, :n].astype(BF16)
        ref[j, 1, at, :] = value[:, n:].astype(BF16)

    def split_rows(ref, j, at, value):
        n = value.shape[0] // 2
        ref[j, 0, :, at] = value[:n].astype(BF16)
        ref[j, 1, :, at] = value[n:].astype(BF16)

    def in_order(share, first=0, end=line):
        def one(k, _):
            j = jnp.where(lax.rem(k, 2) == 0, line - 1 - k // 2, k // 2 + 1)
            share(jnp.where(k == line - 1, 0, j))
            return 0

        lax.fori_loop(first, end, one, 0)

    def mlp_back(i, slot):
        value = nt(hid[0], wrow[slot, :TILE, :hidden_half]) + nt(
            hid[1], wrow[slot, :TILE, hidden_half : 2 * hidden_half]
        )
        tp_part[MLPB, :, :, tile_at(i)] = value.astype(BF16).reshape(2, blk, TILE)

    model_tiles = model // TILE

    def share_down(j):
        g0, g1 = cols_at(cot, j), cols_at(cot_far, j)

        def one(i, _):
            split_cols(
                c_down, j, tile_at(i), tn(act[y, :, tile_at(i)], g0) + tn(act_far[:, tile_at(i)], g1)
            )
            return 0

        lax.fori_loop(0, hidden_half // TILE, one, 0)

    def share_up(j):
        m0, m1 = cols_at(norm, j), cols_at(norm_far, j)

        def one(i, _):
            split_rows(c_up, j, tile_at(i), tn(m0, hid[y, :, tile_at(i)]) + tn(m1, hid_far[:, tile_at(i)]))
            return 0

        lax.fori_loop(0, hidden_half // TILE, one, 0)

    def end_tile(k):
        def fetch(i, slot):
            return lcopy(
                act_end.at[pl.ds(k * rows, rows), tile_at(i)], wcol.at[slot, pl.ds(0, rows), :], wsem.at[0, slot]
            )

        return fetch

    def add_end_tokens(k):
        @pl.when(next_to_end)
        def _():
            end_share(k).wait_recv()
            held = lcopy(
                cot_end.at[pl.ds(k * rows, rows), :],
                wrow.at[k, pl.ds(0, rows), pl.ds(0, model)],
                wsem.at[1, k],
            )
            held.start()
            end_copy(E_ACT + k, partner).wait_recv()
            held.wait()

            def add_tile(i, slot):
                at = tile_at(i)

                def add_block(n, _):
                    j = jnp.where(z == 1, n, lax.rem(n + 2, line))
                    start = pl.multiple_of(lax.rem(z + j, line) * block_cols, LANES)
                    value = tn(wcol[slot, :rows, :], wrow[k, :rows, pl.ds(start, block_cols)])
                    n = block_cols // 2
                    for p in range(2):
                        c_down[j, p, at, :] = (
                            c_down[j, p, at, :].astype(F32) + value[:, p * n : (p + 1) * n]
                        ).astype(BF16)
                    return 0

                lax.fori_loop(0, line - 1, add_block, 0)

            stream(0, hidden_half // TILE, (end_tile(k),), add_tile)

    pair = 2 * blk
    same = lax.broadcasted_iota(jnp.int32, (pair, pair), 0) == lax.broadcasted_iota(
        jnp.int32, (pair, pair), 1
    )

    def positions(lh, place, along):
        shape = (1, pair) if along else (pair, 1)
        at = lax.broadcasted_iota(jnp.int32, shape, along)
        here, there = block_number(lh, place, y), block_number(lh, place, 1 - y)
        return at + jnp.where(at < blk, here * blk, there * blk - blk)

    def piece_positions(lh_start, i, along):
        place = lax.rem(z + i, line)
        early, late_ = positions(0, place, along), positions(1, place, along)
        return jnp.where(i < line, early, late_)

    def piece(t):
        def fetch(i, slot):
            ref = (kv_all, qg_all)[t]
            return lcopy(
                ref.at[i // line, pl.ds(2 * lax.rem(i, line), 2)], chunk.at[slot], csem.at[slot]
            )

        return fetch

    def store_order(ref):
        for h in range(2):
            first, second = by_order(h, ref[0, h], ref[1, h])
            ref[0, h] = first
            ref[1, h] = second

    def attend_forward():
        for lh in range(2):
            for head in range(own_heads):
                at_k, at_v = head * HD, width + head * HD
                run_m[...] = jnp.full(run_m.shape, masked_value, F32)
                run_l[...] = jnp.zeros(run_l.shape, F32)
                acc_a[...] = jnp.zeros(acc_a.shape, F32)

                def attend(i, slot):
                    k = chunk[slot, :, :, at_k : at_k + HD].reshape(pair, HD)
                    v = chunk[slot, :, :, at_v : at_v + HD].reshape(pair, HD)
                    q = qg_own[lh, :, :, at_k : at_k + HD].reshape(pair, HD)
                    s = nt(q, k) * scale
                    seen = piece_positions(lh, i, 1) <= positions(lh, z, 0)
                    s = jnp.where(seen, s, masked_value)
                    old = run_m[...]
                    top = jnp.maximum(old, jnp.max(s, axis=1, keepdims=True))
                    p = jnp.exp(s - top)
                    fade = jnp.exp(old - top)
                    run_m[...] = top
                    run_l[...] = run_l[...] * fade + jnp.sum(p, axis=1, keepdims=True)
                    acc_a[...] = acc_a[...] * fade + nn(p.astype(BF16), v)

                stream(0, line * (lh + 1), (piece(0),), attend)
                out = (acc_a[...] / run_l[...]).astype(BF16)
                att[lh, :, :, at_k : at_k + HD] = out.reshape(2, blk, HD)
                log_total = run_m[...] + jnp.log(run_l[...])
                g = qg_own[lh, :, :, at_v : at_v + HD].reshape(pair, HD)
                dots = jnp.sum(g.astype(F32) * out.astype(F32), axis=1, keepdims=True)
                stats[lh, head, 0:1, :] = jnp.sum(jnp.where(same, log_total, 0.0), 0, keepdims=True)
                stats[lh, head, 1:2, :] = jnp.sum(jnp.where(same, dots, 0.0), 0, keepdims=True)

    def stat_copy(j):
        return rcopy(
            stats, stats_all.at[line - j], st_s.at[j], st_r.at[line - j], (place_of(j), tp)
        )

    def share_out(j):
        g0, g1 = cols_at(cot, j), cols_at(cot_far, j)

        def one(i, _):
            a0 = att[:, 0, :, tile_at(i)].reshape(rows, TILE)
            a1 = att[:, 1, :, tile_at(i)].reshape(rows, TILE)
            split_cols(c_out, j, tile_at(i), tn(a0, g0) + tn(a1, g1))
            return 0

        lax.fori_loop(0, width // TILE, one, 0)

    def undo(value, lh, head, kind):
        at = (3 * head + kind) * HD
        first = value[:, :LANES]
        if kind < 2:
            first = turn(
                first, cosine[lh].reshape(pair, LANES), sine[lh].reshape(pair, LANES), -1
            )
        for lo, hi, part in ((0, LANES, first), (LANES, HD, value[:, LANES:])):
            spot = lanes_at(y * 3 * width + at + lo, hi - lo)
            small[S_QKV : S_QKV + 1, spot] += jnp.sum(part, axis=0, keepdims=True)
            gqkv[lh, :, :, at + lo : at + hi] = part.astype(BF16).reshape(2, blk, hi - lo)

    def attend_back_queries():
        for lh in range(2):
            for head in range(own_heads):
                at_k, at_v = head * HD, width + head * HD
                run_m[...] = jnp.sum(
                    jnp.where(same, stats[lh, head, 0:1, :], 0.0), axis=1, keepdims=True
                )
                run_l[...] = jnp.sum(
                    jnp.where(same, stats[lh, head, 1:2, :], 0.0), axis=1, keepdims=True
                )
                acc_a[...] = jnp.zeros(acc_a.shape, F32)

                def back_q(i, slot):
                    k = chunk[slot, :, :, at_k : at_k + HD].reshape(pair, HD)
                    v = chunk[slot, :, :, at_v : at_v + HD].reshape(pair, HD)
                    q = qg_own[lh, :, :, at_k : at_k + HD].reshape(pair, HD)
                    g = qg_own[lh, :, :, at_v : at_v + HD].reshape(pair, HD)
                    s = nt(q, k) * scale
                    seen = piece_positions(lh, i, 1) <= positions(lh, z, 0)
                    s = jnp.where(seen, s, masked_value)
                    p = jnp.exp(s - run_m[...])
                    ds = (p * (nt(g, v) - run_l[...]) * scale).astype(BF16)
                    acc_a[...] += nn(ds, k)

                stream(0, line * (lh + 1), (piece(0),), back_q)
                undo(acc_a[...], lh, head, 0)

    def branch(i, slot):
        value = nn(act[0], wcol[slot, :hidden_half, :]) + nn(
            act[1], wcol[slot, hidden_half : 2 * hidden_half, :]
        )
        own = att[:, 0].reshape(rows, width)
        far = att_far[...].reshape(rows, width)
        mine = wrow[0, pl.ds(pl.multiple_of(y * width, width), width), tile_at(i)]
        theirs = wrow[0, pl.ds(pl.multiple_of((1 - y) * width, width), width), tile_at(i)]
        value += nn(own, mine) + nn(far, theirs)
        tp_part[BRANCH, :, :, tile_at(i)] = value.astype(BF16).reshape(2, blk, TILE)

    def attend_back_keys():
        for lh in range(2):
            for head in range(own_heads):
                at_k, at_v = head * HD, width + head * HD
                acc_a[...] = jnp.zeros(acc_a.shape, F32)
                acc_b[...] = jnp.zeros(acc_b.shape, F32)

                def back_k(i, slot):
                    q = chunk[slot, :, :, at_k : at_k + HD].reshape(pair, HD)
                    g = chunk[slot, :, :, at_v : at_v + HD].reshape(pair, HD)
                    k = kv_own[lh, :, :, at_k : at_k + HD].reshape(pair, HD)
                    v = kv_own[lh, :, :, at_v : at_v + HD].reshape(pair, HD)
                    stat = stats_all[lax.rem(i, line), i // line, head]
                    s = nt(k, q) * scale
                    seen = positions(lh, z, 0) <= piece_positions(lh, i, 1)
                    s = jnp.where(seen, s, masked_value)
                    p = jnp.exp(s - stat[0:1, :])
                    ds = (p * (nt(v, g) - stat[1:2, :]) * scale).astype(BF16)
                    acc_a[...] += nn(ds, q)
                    acc_b[...] += nn(p.astype(BF16), g)

                stream(lh * line, 2 * line, (piece(1),), back_k)
                undo(acc_a[...], lh, head, 1)
                undo(acc_b[...], lh, head, 2)

    def share_qkv(j):
        m0, m1 = cols_at(attn, j), cols_at(norm_far, j)

        def one(i, _):
            g0 = gqkv[:, 0, :, tile_at(i)].reshape(rows, TILE)
            g1 = gqkv[:, 1, :, tile_at(i)].reshape(rows, TILE)
            split_rows(c_qkv, j, tile_at(i), tn(m0, g0) + tn(m1, g1))
            return 0

        lax.fori_loop(0, 3 * width // TILE, one, 0)

    def attn_back(i, slot):
        own = gqkv[:, 0].reshape(rows, 3 * width)
        far = gqkv_far[...].reshape(rows, 3 * width)
        mine = wrow[slot, :TILE, pl.ds(pl.multiple_of(y * 3 * width, LANES), 3 * width)]
        theirs = wrow[slot, :TILE, pl.ds(pl.multiple_of((1 - y) * 3 * width, LANES), 3 * width)]
        value = nt(own, mine) + nt(far, theirs)
        tp_part[ATTNB, :, :, tile_at(i)] = value.astype(BF16).reshape(2, blk, TILE)

    def back_norms(i, _):
        at = pl.ds(pl.multiple_of(i * chunk_rows, chunk_rows), chunk_rows)
        at_part = pl.ds(pl.multiple_of(lax.rem(i * chunk_rows, blk), chunk_rows), chunk_rows)
        which = i * chunk_rows // blk
        unit, inv_scale = unit_of(at)
        total = jnp.zeros((chunk_rows, model), F32)
        for n, part in ((0, ATTNB), (1, MLPB)):
            value = tp_part[part, which, at_part, :].astype(F32)
            small[S_GAIN + n : S_GAIN + n + 1, :model] += jnp.sum(value * unit, 0, keepdims=True)
            small[S_SHIFT + n : S_SHIFT + n + 1, :model] += jnp.sum(value, 0, keepdims=True)
            total = total + value * gain[n : n + 1, :]
        cbuf[at, :] = cbuf[at, :] + inv_scale * (
            total
            - jnp.mean(total, axis=-1, keepdims=True)
            - unit * jnp.mean(total * unit, axis=-1, keepdims=True)
        )
        return 0

    def small_copy(j):
        return rcopy(
            small_sent, small_recv.at[line - j], sm_s.at[j], sm_r.at[line - j], (place_of(j), tp)
        )

    def stream_rows(i, _):
        at = pl.ds(pl.multiple_of(i * chunk_rows, chunk_rows), chunk_rows)
        at_part = pl.ds(pl.multiple_of(lax.rem(i * chunk_rows, blk), chunk_rows), chunk_rows)
        which = i * chunk_rows // blk
        xbuf[at, :] = xbuf[at, :] + out_bias[...] + tp_part[BRANCH, which, at_part, :].astype(F32)
        return 0

    at_end = jnp.logical_or(z == 0, z == line - 1)
    stream(0, 4 * own_heads, (fetch_by(w_qkv, lambda i: kv_index(i)[3]),), keys_values)
    y_copy(Y_KV).start()
    ag_hop(0, 0, 1)
    own_places[0].start()
    w_out_fetch.start()
    w_out_fetch.wait()
    stream(0, 2 * own_heads, (fetch_by(w_qkv, lambda i: q_index(i)[2]),), queries)
    y_copy(Y_QG).start()
    ag_hop(1, 0, 1)
    own_places[2].start()
    pass_x(Y_COT, 0)

    stream(0, hidden_tiles // 2, (col_tile(w_up),), activate)
    y_copy(Y_KV).wait_recv()
    ag_hop(0, 1, 1)
    own_places[1].start()
    stream(hidden_tiles // 2, hidden_tiles, (col_tile(w_up),), activate)
    y_copy(Y_ACT).start()
    y_copy(Y_MLP).start()
    end_send(E_ACT)
    pass_on(Y_COT, 0)
    ag_hop(0, 0, 2)
    end_pass_x(0)
    stream(0, hidden_tiles // 2, (row_tile(w_down),), hidden_back)
    y_copy(Y_QG).wait_recv()
    own_places[3].start()
    ag_hop(1, 1, 1, jnp.logical_not(at_end))
    ag_hop(1, 0, 2)
    stream(hidden_tiles // 2, hidden_tiles, (row_tile(w_down),), hidden_back)
    y_copy(Y_HID).start()
    y_copy(Y_ATTN).start()
    end_pass(0)
    stream(0, model_tiles, (row_tile(w_up),), mlp_back)
    tp_copy(MLPB, 0).start()
    ag_hop(0, 0, 3)
    ag_hop(0, 1, 2)
    core_copy(0).wait_recv()
    y_copy(Y_ACT).wait_recv()
    end_send(E_ACT_FAR)
    ag_hop(1, 1, 1, at_end)
    in_order(share_down)
    pass_x(Y_MLP, 1)
    end_pass_x(1)
    ag_hop(0, 1, 3)
    add_end_tokens(0)
    pass_on(Y_MLP, 1)
    end_pass(1)
    ag_hop(1, 0, 3)
    add_end_tokens(1)
    rs_ends(DOWN, (1, 3), (0,))
    ag_hop(1, 1, 2)
    rs_ends(DOWN, (1, 3), (1,))
    tp_next(MLPB, 1)
    y_copy(Y_HID).wait_recv()
    core_copy(1).wait_recv()
    in_order(share_up)
    rs_ends(UP, (1, 2))
    ag_rest(0, 0, 4)
    ag_rest(0, 1, 4)
    for copy in own_places:
        copy.wait()

    attend_forward()
    store_order(att)
    for j in range(1, line):
        stat_copy(j).start()
    y_copy(Y_ATT).start()
    rs_ends(UP, (2, line))
    rs_ends(DOWN, (3, line))
    in_order(share_out)
    small[S_QKV : S_QKV + 1, :] = jnp.zeros((1, small.shape[1]), F32)
    attend_back_queries()
    tp_next(MLPB, 2)
    ag_hop(1, 1, 3)
    pass_x(Y_ATTN, 2)
    for hop in range(1, min(line, 4)):
        rs_cross(DOWN, hop)
    y_copy(Y_ATT).wait_recv()
    w_out_fetch.start()
    w_out_fetch.wait()
    stream(0, model_tiles, (col_tile(w_down),), branch)
    tp_copy(BRANCH, 0).start()
    rs_cross(UP, 1)
    rs_cross(UP, 2)
    ag_rest(1, 0, 4)
    ag_rest(1, 1, 4)
    for j in range(1, line):
        stat_copy(line - j).wait_recv()
    own_stats = lcopy(stats, stats_all.at[0], local.at[0])
    own_stats.start()
    own_stats.wait()
    attend_back_keys()
    store_order(gqkv)
    y_copy(Y_GQKV).start()
    tp_next(BRANCH, 1)
    pass_on(Y_ATTN, 2)
    core_copy(2).wait_recv()
    core_copy(1).wait_send()
    x_drain(1)
    far_again = lcopy(attn_far, norm_far, local.at[1])
    far_again.start()
    far_again.wait()
    in_order(share_qkv)
    rs_ends(QKV, (1, line))
    rs_ends(OUT, (1, line))
    for hop in range(1, min(line, 4)):
        rs_home(DOWN, hop)
    rs_home(UP, 1)
    rs_home(UP, 2)
    y_copy(Y_GQKV).wait_recv()
    stream(0, model_tiles, (row_tile(w_qkv),), attn_back)
    tp_copy(ATTNB, 0).start()
    tp_next(BRANCH, 2)
    rs_cross(UP, 3) if line > 3 else None
    tp_next(ATTNB, 1)

    rs_rest(DOWN, 4 if line > 3 else 3)
    rs_finish(DOWN)
    tp_done(BRANCH)
    tp_done(MLPB)
    rs_home(UP, 3) if line > 3 else None
    rs_cross(QKV, 1)
    rs_cross(QKV, 2)
    tp_next(ATTNB, 2)
    tp_done(ATTNB)
    lax.fori_loop(0, rows // chunk_rows, back_norms, 0)
    grad_store = lcopy(cbuf, grad_o, local.at[1])
    grad_store.start()
    rs_cross(QKV, 3) if line > 3 else None
    pair_copy = rcopy(small, small_pair, sm_s.at[0], sm_r.at[0], partner)
    pair_copy.start()
    pair_copy.wait()
    small_sent[...] = (small[...] + small_pair[...]).astype(BF16)
    for j in range(1, line):
        small_copy(j).start()
    lax.fori_loop(0, rows // chunk_rows, stream_rows, 0)
    stream_store = lcopy(xbuf, stream_o, local.at[0])
    stream_store.start()
    rs_rest(UP, 4 if line > 3 else 3)
    rs_finish(UP)
    rs_home(QKV, 1)
    rs_home(QKV, 2)
    rs_home(QKV, 3) if line > 3 else None
    rs_rest(QKV, 4 if line > 3 else 3)
    rs_cross(OUT, 1)
    rs_cross(OUT, 2)
    rs_cross(OUT, 3) if line > 3 else None
    rs_finish(QKV)
    for hop in range(1, min(line, 4)):
        rs_home(OUT, hop)
    rs_rest(OUT, 4 if line > 3 else 3)
    rs_finish(OUT)
    for j in range(1, line):
        small_copy(line - j).wait_recv()
    small_recv[0] = small_sent[...]
    small[...] = small_recv[lax.rem(line - z, line)].astype(F32)
    for p in range(1, line):
        small[...] += small_recv[lax.rem(p + line - z, line)].astype(F32)
    small_store = lcopy(small, small_o, local.at[2])
    small_store.start()

    for t in range(2):
        for h in range(2):
            ag_drain(t, h)
    for item in (Y_KV, Y_QG, Y_COT, Y_MLP, Y_ATTN, Y_ACT, Y_HID, Y_ATT, Y_GQKV):
        y_copy(item).wait_send()
    core_copy(0).wait_send()
    core_copy(2).wait_send()
    x_drain(0)
    x_drain(2)
    for j in range(1, line):
        stat_copy(j).wait_send()
        small_copy(j).wait_send()
    for i in range(3):
        tp_drain(i)
    grad_store.wait()
    small_store.wait()
    stream_store.wait()
    for t in range(4):
        rs_drain(t)
    end_drain()


def layer(line, n_tp, order, stream_in, cotangent, ln_gain, ln_bias, w_qkv, b_qkv, w_out, out_bias, w_up, b_up, w_down):
    rows, model = stream_in.shape
    half, blk = model // 2, rows // 2
    hidden = w_up.shape[1]
    hidden_half = hidden // 2
    width = w_out.shape[0] // 2
    own_heads = width // HD
    part_cols = model // line // 2
    pair = 2 * blk
    tp_steps = 0
    while (2 << tp_steps) < n_tp:
        tp_steps += 1
    small_shape = (16, max(model, hidden, 6 * width))
    shares = (
        (2, hidden_half, part_cols),
        (2, part_cols, hidden_half),
        (2, width, part_cols),
        (2, part_cols, 3 * width),
    )
    b = lambda *s: jax.ShapeDtypeStruct(s, BF16)
    f = lambda *s: jax.ShapeDtypeStruct(s, F32)
    vb = lambda *s: pltpu.VMEM(s, BF16)
    vf = lambda *s: pltpu.VMEM(s, F32)
    dma = pltpu.SemaphoreType.DMA
    outs = (
        b(hidden, part_cols),
        b(part_cols, hidden),
        b(2 * width, part_cols),
        b(part_cols, 6 * width),
        f(rows, model),
        f(rows, model),
        f(*small_shape),
        b(2, 2 * line, blk, 2 * width),
        b(2, 2 * line, blk, 2 * width),
        b(line + 1, *shares[0]),
        b(line + 1, *shares[1]),
        b(line + 1, *shares[2]),
        b(line + 1, *shares[3]),
        b(2, rows, half),
        b(3, blk, model),
        b(2 * rows, model),
        b(2 * rows, hidden_half),
    )
    wide = max(model, hidden)
    scratch = (
        [vf(rows, model)] * 2
        + [vb(2, rows, half)] * 5
        + [vb(2, rows, hidden_half)] * 2
        + [vb(rows, hidden_half)] * 2
        + [vb(2, wide, TILE), vb(2, max(TILE, 2 * width), wide)]
        + [vb(line, *s) for s in shares]
        + [vb(*s) for s in shares]
        + [vb(3, 2, blk, model), vb(3, tp_steps + 1, blk, model)]
        + [vb(2, 2, blk, 2 * width)] * 2
        + [vb(2, blk, 2 * width)] * 2
        + [
            vb(2, 2, blk, 2 * width),
            vb(2, 2, blk, width),
            vb(2, blk, width),
            vf(2, own_heads, 2, pair),
            vf(line, 2, own_heads, 2, pair),
            vb(2, 2, blk, 3 * width),
            vb(2, blk, 3 * width),
            vf(pair, HD),
            vf(pair, HD),
            vf(pair, 1),
            vf(pair, 1),
            vf(2, 2, blk, LANES),
            vf(2, 2, blk, LANES),
            vf(*small_shape),
            vf(*small_shape),
            vb(*small_shape),
            vb(line, *small_shape),
            dma((2, 2, 2, line)),
            dma((2, 2, line)),
            dma((Y_FIN + 4,)),
            dma((Y_FIN + 4,)),
            dma((3,)),
            dma((3,)),
            dma((3, n_tp // 2)),
            dma((3, n_tp // 2)),
            dma((4, 2, line)),
            dma((4, 2, line + 1)),
            dma((3, tp_steps + 2)),
            dma((3, tp_steps + 2)),
            dma((line,)),
            dma((line,)),
            dma((line,)),
            dma((line,)),
            dma((6,)),
            dma((6,)),
            dma((2, n_tp // 2)),
            dma((2, n_tp // 2)),
            dma((9,)),
            dma((2, 2)),
            dma((2,)),
            dma((4,)),
        ]
    )
    blocks = order.shape[0]
    operands = (
        order,
        stream_in,
        cotangent,
        w_up,
        w_down,
        w_out,
        w_qkv,
        ln_gain,
        ln_bias,
        b_qkv,
        b_up.reshape(1, -1),
        out_bias.reshape(1, -1),
        jnp.asarray(rope_tables(np.arange(blocks) * blk)),
        jnp.asarray(rope_tables(np.arange(blk))),
    )
    return pl.pallas_call(
        functools.partial(layer_kernel, line, n_tp),
        name="layer",
        out_shape=outs,
        in_specs=[SMEM] + [ANY] * 6 + [VMEM] * 7,
        out_specs=[ANY] * len(outs),
        scratch_shapes=scratch,
        cost_estimate=pl.CostEstimate(
            flops=40 * rows * model * hidden,
            transcendentals=rows * hidden,
            bytes_accessed=8 * w_up.size,
        ),
        compiler_params=pltpu.CompilerParams(
            collective_id=0, has_side_effects=True, vmem_limit_bytes=67043328
        ),
    )(*operands)


def results_kernel(
    down,
    up,
    out,
    qkv,
    stream,
    grad,
    small,
    stream_o,
    grad_o,
    qkv_o,
    bqkv_o,
    out_o,
    obias_o,
    up_o,
    bup_o,
    down_o,
    gain_o,
    shift_o,
):
    stream_o[...] = stream[...]
    grad_o[...] = grad[...]
    for src, dst in ((qkv, qkv_o), (out, out_o), (up, up_o), (down, down_o)):
        dst[...] = src[...].astype(F32)

    @pl.when(pl.program_id(0) == 0)
    def _():
        bqkv_o[...] = small[S_QKV, : bqkv_o.shape[0]]
        obias_o[...] = small[S_OUT, : obias_o.shape[0]]
        bup_o[...] = small[S_UP, : bup_o.shape[0]]
        gain_o[...] = small[S_GAIN : S_GAIN + 2, : gain_o.shape[1]]
        shift_o[...] = small[S_SHIFT : S_SHIFT + 2, : shift_o.shape[1]]


def results(down, up, out, qkv, stream_out, grad_in, small, model, fused, hidden):
    steps = 8
    f = lambda *s: jax.ShapeDtypeStruct(s, F32)
    rows_of = lambda a: pl.BlockSpec((a.shape[0] // steps,) + a.shape[1:], lambda i: (i, 0))
    whole = lambda a: pl.BlockSpec(a.shape, lambda i: (0,) * len(a.shape))
    large = (down, up, out, qkv, stream_out, grad_in)
    while any(a.shape[0] % (16 * steps) for a in large[:4]):
        steps //= 2
    outs = (
        (f(*stream_out.shape), True),
        (f(*grad_in.shape), True),
        (f(*qkv.shape), True),
        (f(fused), False),
        (f(*out.shape), True),
        (f(model), False),
        (f(*up.shape), True),
        (f(hidden), False),
        (f(*down.shape), True),
        (f(2, model), False),
        (f(2, model), False),
    )
    return pl.pallas_call(
        results_kernel,
        name="results",
        grid=(steps,),
        out_shape=[o for o, _ in outs],
        in_specs=[rows_of(a) for a in large] + [whole(small)],
        out_specs=[rows_of(o) if tall else whole(o) for o, tall in outs],
        cost_estimate=pl.CostEstimate(
            flops=down.size, transcendentals=0, bytes_accessed=8 * down.size + 16 * stream_out.size
        ),
        compiler_params=pltpu.CompilerParams(vmem_limit_bytes=67043328),
    )(*large, small)


def shards(
    n_ctx,
    n_tp,
    stream_in,
    cotangent,
    ln_gain,
    ln_bias,
    w_qkv,
    b_qkv,
    w_out,
    out_bias,
    w_up,
    b_up,
    w_down,
    block_order,
):
    (down, up, out, qkv, stream_out, grad_in, small, *_) = layer(
        n_ctx // 2,
        n_tp,
        block_order,
        stream_in,
        cotangent,
        ln_gain,
        ln_bias,
        w_qkv,
        b_qkv,
        w_out,
        out_bias,
        w_up,
        b_up,
        w_down,
    )
    return results(down, up, out, qkv, stream_out, grad_in, small, *w_qkv.shape, w_up.shape[1])


def solution(mesh):
    placed = (
        P("ctx", None),
        P("ctx", None),
        P(),
        P(),
        P(None, "tp"),
        P("tp"),
        P("tp", None),
        P(),
        P(None, "tp"),
        P("tp"),
        P("tp", None),
        P(),
    )
    return jax.shard_map(
        functools.partial(shards, mesh.shape["ctx"], mesh.shape["tp"]),
        mesh=mesh,
        in_specs=placed,
        out_specs=(
            P("ctx", None),
            P("ctx", None),
            P("ctx", "tp"),
            P("tp"),
            P("tp", "ctx"),
            P(),
            P("ctx", "tp"),
            P("tp"),
            P("tp", "ctx"),
            P(),
            P(),
        ),
        check_vma=False,
    )
```

```python
import functools
import math

import jax
import jax.numpy as jnp
import numpy as np
from jax import lax
from jax.experimental import pallas as pl
from jax.experimental.pallas import tpu as pltpu
from jax.sharding import PartitionSpec as P

HD = 256
ROT = 64
LANES = 128
TILE = 256

masked_value = -1e30
norm_epsilon = 1e-05
root_half = 0.7071067811865476
inverse_root_two_pi = 0.3989422804014327

F32 = jnp.float32
BF16 = jnp.bfloat16
MESH = pl.DeviceIdType.MESH
ANY = pl.BlockSpec(memory_space=pl.ANY)
VMEM = pl.BlockSpec(memory_space=pltpu.VMEM)
SMEM = pl.BlockSpec(memory_space=pltpu.SMEM)


def nt(a, b):
    return lax.dot_general(a, b, (((1,), (1,)), ((), ())), preferred_element_type=F32)


def nn(a, b):
    return lax.dot_general(a, b, (((1,), (0,)), ((), ())), preferred_element_type=F32)


def tn(a, b):
    return lax.dot_general(a, b, (((0,), (0,)), ((), ())), preferred_element_type=F32)


def rope_tables(positions):
    half_rot = ROT // 2
    frequency = np.exp(np.arange(half_rot) * (-2.0 * math.log(10000.0) / ROT))
    angles = np.asarray(positions, np.float64)[:, None] * frequency
    table = np.zeros((2, angles.shape[0], LANES), np.float32)
    table[0] = 1.0
    for lo in (0, half_rot):
        table[0, :, lo : lo + half_rot] = np.cos(angles)
        table[1, :, lo : lo + half_rot] = np.sin(angles)
    return table


def turn(first, cosine, sine, sign):
    half_rot = ROT // 2
    scaled = first * sine if sign < 0 else first
    lane = lax.broadcasted_iota(jnp.int32, first.shape, 1)
    down = jnp.where(lane < half_rot, pltpu.roll(scaled, LANES - half_rot, 1), 0.0)
    up = jnp.where(
        jnp.logical_and(lane >= half_rot, lane < ROT), pltpu.roll(scaled, half_rot, 1), 0.0
    )
    if sign < 0:
        return first * cosine + (down - up)
    return first * cosine + (up - down) * sine


DOWN, UP, OUT, QKV = range(4)
(Y_KV, Y_QG, Y_COT, Y_MLP, Y_ATTN, Y_ACT, Y_HID, Y_ATT, Y_GQKV, Y_FIN) = range(10)
BRANCH, MLPB, ATTNB = range(3)
S_GAIN, S_SHIFT, S_OUT, S_UP, S_QKV = 0, 2, 4, 5, 6


def layer_kernel(
    line,
    n_tp,
    order,
    stream_in,
    cotangent,
    w_up,
    w_down,
    w_out,
    w_qkv,
    gain,
    shift,
    b_qkv,
    b_up,
    out_bias,
    block_table,
    row_table,
    down_o,
    up_o,
    out_o,
    qkv_o,
    stream_o,
    grad_o,
    small_o,
    kv_all,
    qg_all,
    rs_down,
    rs_up,
    rs_out,
    rs_qkv,
    attn_far,
    tp_far,
    cot_end,
    act_end,
    xbuf,
    cbuf,
    cot,
    cot_far,
    norm,
    norm_far,
    attn,
    act,
    hid,
    act_far,
    hid_far,
    wcol,
    wrow,
    c_down,
    c_up,
    c_out,
    c_qkv,
    stage_down,
    stage_up,
    stage_out,
    stage_qkv,
    tp_part,
    tp_recv,
    kv_own,
    qg_own,
    kv_away,
    qg_away,
    chunk,
    att,
    att_far,
    stats,
    stats_all,
    gqkv,
    gqkv_far,
    acc_a,
    acc_b,
    run_m,
    run_l,
    cosine,
    sine,
    small,
    small_pair,
    small_sent,
    small_recv,
    ag_s,
    ag_r,
    y_s,
    y_r,
    core_s,
    core_r,
    x_s,
    x_r,
    rs_s,
    rs_r,
    tp_s,
    tp_r,
    st_s,
    st_r,
    sm_s,
    sm_r,
    end_s,
    end_r,
    ex_s,
    ex_r,
    local,
    wsem,
    csem,
    tsem,
):
    me, tp = lax.axis_index("ctx"), lax.axis_index("tp")
    z, y = me // 2, lax.rem(me, 2)
    core = lax.rem(tp, 2)
    partner = (me + 1 - 2 * y, tp)
    sibling = (me, tp + 1 - 2 * core)
    right, left = (me + 2, tp), (me - 2, tp)
    far_steps = []
    step = 2
    while step < n_tp:
        far_steps.append((me, tp + step - 2 * step * lax.rem(tp // step, 2)))
        step *= 2

    rows = norm.shape[1]
    blk = rows // 2
    across = n_tp // 2
    xpos = tp // 2
    x_others = [(me, lax.rem(tp + 2 * k, n_tp)) for k in range(1, across)]
    half = norm.shape[2]
    hidden_half = act.shape[2]
    own_heads = kv_own.shape[-1] // (2 * HD)
    width = own_heads * HD
    block_cols = 2 * half // line
    scale = HD ** (-0.5)

    def place_of(j):
        return lax.rem(z + j, line) * 2 + y

    barrier = pltpu.get_barrier_semaphore()
    greet = [partner, sibling] + x_others + [(place_of(j), tp) for j in range(1, line)]
    for device in greet:
        pl.semaphore_signal(barrier, inc=1, device_id=device, device_id_type=MESH)

    def rcopy(src, dst, s, r, device):
        return pltpu.make_async_remote_copy(
            src_ref=src, dst_ref=dst, send_sem=s, recv_sem=r, device_id=device, device_id_type=MESH
        )

    def lcopy(src, dst, sem):
        return pltpu.make_async_copy(src, dst, sem)

    def fin_parts(t):
        c = (c_down, c_up, c_out, c_qkv)[t]
        if t == DOWN:
            dst = down_o.at[pl.ds(pl.multiple_of(y * hidden_half, hidden_half), hidden_half), :]
        elif t == UP:
            dst = up_o.at[:, pl.ds(pl.multiple_of(y * hidden_half, hidden_half), hidden_half)]
        elif t == OUT:
            dst = out_o.at[pl.ds(pl.multiple_of(y * width, width), width), :]
        else:
            dst = qkv_o.at[:, pl.ds(pl.multiple_of(y * 3 * width, 3 * width), 3 * width)]
        return c, dst

    def part_rows(x):
        n = rows // across
        return pl.ds(pl.multiple_of(x * n, n), n)

    def y_copy(item, t=0):
        if item == Y_KV:
            src, dst = kv_away, kv_own.at[:, 1]
        elif item == Y_QG:
            src, dst = qg_away, qg_own.at[:, 1]
        elif item == Y_COT:
            src, dst = cot.at[core, part_rows(xpos)], cot_far.at[core, part_rows(xpos)]
        elif item == Y_MLP:
            src, dst = norm.at[core, part_rows(xpos)], norm_far.at[core, part_rows(xpos)]
        elif item == Y_ATTN:
            src, dst = attn.at[core, part_rows(xpos)], attn_far.at[core, part_rows(xpos)]
        elif item == Y_ACT:
            src, dst = act.at[1 - y], act_far
        elif item == Y_HID:
            src, dst = hid.at[1 - y], hid_far
        elif item == Y_ATT:
            src, dst = att.at[:, 1], att_far
        elif item == Y_GQKV:
            src, dst = gqkv.at[:, 1], gqkv_far
        else:
            c, dst = fin_parts(t)
            src = c.at[0, 1 - y]
            item = Y_FIN + t
        return rcopy(src, dst, y_s.at[item], y_r.at[item], partner)

    def core_copy(k):
        ref = (cot_far, norm_far, attn_far)[k]
        return rcopy(ref.at[core], ref.at[core], core_s.at[k], core_r.at[k], sibling)

    def x_copy(k, n):
        ref = (cot_far, norm_far, attn_far)[k].at[core, part_rows(xpos)]
        return rcopy(ref, ref, x_s.at[k, n], x_r.at[k, n], x_others[n])

    def x_arrival(k, n):
        ref = (cot_far, norm_far, attn_far)[k].at[core, part_rows(lax.rem(xpos + across - n - 1, across))]
        return rcopy(ref, ref, x_s.at[k, n], x_r.at[k, n], x_others[n])

    def pass_x(item, k):
        y_copy(item).wait_recv()
        for n in range(across - 1):
            x_copy(k, n).start()

    def pass_on(item, k):
        for n in range(across - 1):
            x_arrival(k, n).wait_recv()
        core_copy(k).start()

    def x_drain(k):
        for n in range(across - 1):
            x_copy(k, n).wait_send()

    E_COT, E_COT_FAR, E_ACT, E_ACT_FAR, E_ACT_LAST = range(5)
    next_to_end = jnp.logical_or(z == 1, z == line - 2)

    def end_part(k, x):
        n = rows // across
        return cot_end.at[
            pl.ds(pl.multiple_of(k * rows + x * n, n), n), pl.ds(pl.multiple_of(core * half, half), half)
        ]

    def end_copy(item, device):
        if item == E_COT:
            src, dst = cot.at[core, part_rows(xpos)], end_part(0, xpos)
        elif item == E_COT_FAR:
            src, dst = end_part(0, xpos), end_part(1, xpos)
        elif item == E_ACT:
            src, dst = act.at[y], act_end.at[pl.ds(0, rows), :]
        else:
            n = hidden_half // 2
            part = pl.ds(0 if item == E_ACT_FAR else n, n)
            src, dst = act_far.at[:, part], act_end.at[pl.ds(rows, rows), part]
        return rcopy(src, dst, end_s.at[item], end_r.at[item], device)

    def end_x(k, n, arriving):
        x = lax.rem(xpos + across - n - 1, across) if arriving else xpos
        ref = end_part(k, x)
        return rcopy(ref, ref, ex_s.at[k, n], ex_r.at[k, n], x_others[n])

    def end_share(k):
        ref = cot_end.at[pl.ds(k * rows, rows), pl.ds(pl.multiple_of(core * half, half), half)]
        return rcopy(ref, ref, end_s.at[5 + k], end_r.at[5 + k], sibling)

    def end_send(item):
        @pl.when(z == 0)
        def _():
            end_copy(item, right).start()

        @pl.when(z == line - 1)
        def _():
            end_copy(item, left).start()

    def end_pass_x(k):
        @pl.when(next_to_end)
        def _():
            end_copy(E_COT + k, partner).wait_recv()
            for n in range(across - 1):
                end_x(k, n, False).start()
            if k == 0:
                end_copy(E_COT_FAR, partner).start()

    def end_pass(k):
        @pl.when(next_to_end)
        def _():
            for n in range(across - 1):
                end_x(k, n, True).wait_recv()
            end_share(k).start()

    def end_drain():
        @pl.when(jnp.logical_or(z == 0, z == line - 1))
        def _():
            for item in (E_COT, E_ACT, E_ACT_FAR, E_ACT_LAST):
                end_copy(item, partner).wait_send()

        @pl.when(next_to_end)
        def _():
            end_copy(E_COT_FAR, partner).wait_send()
            for k in range(2):
                end_share(k).wait_send()
                for n in range(across - 1):
                    end_x(k, n, False).wait_send()

    def ag_copy(t, h, to, hop, j_src, j_dst):
        ref = (kv_all, qg_all)[t]
        src = ref.at[:, 2 * j_src + h]
        if isinstance(hop, int) and hop == 1:
            src = (kv_own, qg_own)[t].at[:, h]
        return rcopy(
            src,
            ref.at[:, 2 * j_dst + h],
            ag_s.at[t, h, to, hop],
            ag_r.at[t, h, j_dst],
            (right, left)[to],
        )

    def ag_send_when(hop):
        return (
            jnp.logical_and(z >= hop - 1, z <= line - 2),
            jnp.logical_and(z + hop - 1 <= line - 1, z >= 1),
        )

    def ag_hop(t, h, hop, only=None):
        first = isinstance(hop, int) and hop == 1
        to_right, to_left = ag_send_when(hop)
        if only is not None:
            to_right, to_left = jnp.logical_and(to_right, only), jnp.logical_and(to_left, only)

        @pl.when(to_right)
        def _():
            if not first:
                ag_copy(t, h, 0, hop - 1, line - hop + 1, line - hop + 1).wait_recv()
            ag_copy(t, h, 0, hop, lax.rem(line - hop + 1, line), line - hop).start()

        @pl.when(to_left)
        def _():
            if not first:
                ag_copy(t, h, 1, hop - 1, hop - 1, hop - 1).wait_recv()
            ag_copy(t, h, 1, hop, hop - 1, hop).start()

    def ag_rest(t, h, hop):
        def one(i, _):
            ag_hop(t, h, i)
            return 0

        def come(i, _):
            ag_copy(t, h, 0, i, i, i).wait_recv()
            return 0

        if hop < line:
            lax.fori_loop(hop, line, one, 0)

        @pl.when(jnp.logical_or(z == 0, z == line - 1))
        def _():
            lax.fori_loop(1, line, come, 0)

    def ag_drain(t, h):
        def one(hop, _):
            to_right, to_left = ag_send_when(hop)

            @pl.when(to_right)
            def _():
                ag_copy(t, h, 0, hop, lax.rem(line - hop + 1, line), line - hop).wait_send()

            @pl.when(to_left)
            def _():
                ag_copy(t, h, 1, hop, hop - 1, hop).wait_send()

            return 0

        lax.fori_loop(1, line, one, 0)

    rs = (
        (c_down, rs_down, stage_down),
        (c_up, rs_up, stage_up),
        (c_out, rs_out, stage_out),
        (c_qkv, rs_qkv, stage_qkv),
    )

    def piece_of(ref, t, p):
        if t != DOWN:
            return ref.at[p]
        n = hidden_half // 2
        return ref.at[:, pl.ds(pl.multiple_of(p * n, n), n), :]

    def rs_copy(t, p, j, slot, device):
        c, recv, _ = rs[t]
        return rcopy(
            piece_of(c.at[j], t, p), piece_of(recv.at[slot], t, p), rs_s.at[t, p, j], rs_r.at[t, p, slot], device
        )

    def rs_take(t, p, j, slot):
        c, recv, held = rs[t]
        rs_copy(t, p, j, slot, partner).wait_recv()
        copy = lcopy(piece_of(recv.at[slot], t, p), piece_of(held, t, p), tsem.at[t])
        copy.start()
        copy.wait()
        n = c.shape[2]
        part = min(64, n)

        def add(side, i):
            at = pl.ds(pl.multiple_of(i * part, part), part)
            c[j, side, at, :] = (
                c[j, side, at, :].astype(F32) + held[side, at, :].astype(F32)
            ).astype(BF16)

        def one(i, _):
            if t != DOWN:
                add(p, i)
            else:
                for side in range(2):
                    add(side, p * (n // part // 2) + i)
            return 0

        lax.fori_loop(0, n // part // (2 if t == DOWN else 1), one, 0)

    def first_from(t):
        return 2 if t == DOWN else 1

    def rs_ends(t, hops, parts=(0, 1)):
        first = first_from(t)

        def one(hop, _):
            for k in parts:
                p = k if t == DOWN else (1 - y if k == 0 else y)

                @pl.when(jnp.logical_and(z == first - 1, hop >= first))
                def _():
                    rs_copy(t, p, line - hop, line - hop - 1, right).start()

                @pl.when(jnp.logical_and(z == line - first, hop >= first))
                def _():
                    rs_copy(t, p, hop, hop + 1, left).start()

            return 0

        lax.fori_loop(*hops, one, 0)

    near = 2 * z < line

    def halves(t, step):
        def one(k, _):
            step(k if t == DOWN else jnp.where(k == 0, 1 - y, y))
            return 0

        lax.fori_loop(0, 2, one, 0)

    def rs_right(t, hop, only):
        jr, first = line - hop, first_from(t)

        @pl.when(jnp.logical_and(only, jnp.logical_and(hop >= z + 1, z >= first)))
        def _():
            def step(p):
                rs_take(t, p, jr, jr)
                rs_copy(t, p, jr, jr - 1, right).start()

            halves(t, step)

    def rs_left(t, hop, only):
        jl, first = hop, first_from(t)

        @pl.when(jnp.logical_and(only, jnp.logical_and(hop >= line - z, z <= line - 1 - first)))
        def _():
            def step(p):
                rs_take(t, p, jl, jl)
                rs_copy(t, p, jl, jl + 1, left).start()

            halves(t, step)

    def rs_cross(t, hop):
        rs_right(t, hop, near)
        rs_left(t, hop, jnp.logical_not(near))

    def rs_home(t, hop):
        rs_right(t, hop, jnp.logical_not(near))
        rs_left(t, hop, near)

    def rs_rest(t, hop):
        def one(i, _):
            rs_cross(t, i)
            rs_home(t, i)
            return 0

        if hop < line:
            lax.fori_loop(hop, line, one, 0)

    def rs_finish(t):
        first = first_from(t)
        c, dst = fin_parts(t)

        def take(k, _):
            p = jnp.where(k == 0, 1 - y, y)

            @pl.when(z >= first)
            def _():
                rs_take(t, p, 0, 0)

            @pl.when(z <= line - 1 - first)
            def _():
                rs_take(t, p, 0, line)

            @pl.when(k == (1 if t == DOWN else 0))
            def _():
                y_copy(Y_FIN, t).start()

            return 0

        lax.fori_loop(0, 2, take, 0)
        lcopy(c.at[0, y], dst, local.at[4 + t]).start()

    def rs_drain(t):
        sends = jnp.logical_and(z >= first_from(t) - 1, z <= line - first_from(t))

        def one(j, _):
            for p in range(2):

                @pl.when(jnp.logical_and(sends, j <= line - 1 - z))
                def _():
                    rs_copy(t, p, j, j - 1, right).wait_send()

                @pl.when(jnp.logical_and(sends, j > line - 1 - z))
                def _():
                    rs_copy(t, p, j, j + 1, left).wait_send()

            return 0

        lax.fori_loop(1, line, one, 0)
        c, dst = fin_parts(t)
        y_copy(Y_FIN, t).wait()
        lcopy(c.at[0, y], dst, local.at[4 + t]).wait()

    last = len(far_steps) + 1

    def tp_copy(i, k):
        part = tp_part.at[i]
        if k == 0:
            src, dst, device = part.at[1 - core], tp_recv.at[i, 0], sibling
        elif k < last:
            src, dst, device = part.at[core], tp_recv.at[i, k], far_steps[k - 1]
        else:
            src, dst, device = part.at[core], tp_far.at[i], sibling
        return rcopy(src, dst, tp_s.at[i, k], tp_r.at[i, k], device)

    def tp_add(i, k):
        part = 64

        def add(n, _):
            at = pl.ds(pl.multiple_of(n * part, part), part)
            tp_part[i, core, at, :] = (
                tp_part[i, core, at, :].astype(F32) + tp_recv[i, k, at, :].astype(F32)
            ).astype(BF16)
            return 0

        lax.fori_loop(0, blk // part, add, 0)

    def tp_next(i, k):
        if k > 1:
            tp_copy(i, k - 1).wait_send()
        tp_copy(i, k - 1).wait_recv()
        tp_add(i, k - 1)
        tp_copy(i, k).start()

    def tp_done(i):
        tp_copy(i, last).wait_recv()
        tp_copy(i, 0).wait_send()

        other = lcopy(tp_far.at[i], tp_part.at[i, 1 - core], local.at[8])
        other.start()
        other.wait()

    def tp_drain(i):
        tp_copy(i, last).wait_send()

    def stream(lo, hi, fetches, body):
        for f in fetches:
            f(lo, lax.rem(lo, 2)).start()

        def one(i, _):
            slot = lax.rem(i, 2)

            @pl.when(i + 1 < hi)
            def _():
                for f in fetches:
                    f(i + 1, 1 - slot).start()

            for f in fetches:
                f(i, slot).wait()
            body(i, slot)
            return 0

        lax.fori_loop(lo, hi, one, 0)

    def col_tile(w):
        def fetch(i, slot):
            at = pl.ds(pl.multiple_of(i * TILE, TILE), TILE)
            return lcopy(w.at[:, at], wcol.at[slot, pl.ds(0, w.shape[0]), :], wsem.at[0, slot])

        return fetch

    def row_tile(w):
        def fetch(i, slot):
            at = pl.ds(pl.multiple_of(i * TILE, TILE), TILE)
            return lcopy(w.at[at, :], wrow.at[slot, pl.ds(0, TILE), pl.ds(0, w.shape[1])], wsem.at[1, slot])

        return fetch

    x_load = lcopy(stream_in, xbuf, local.at[0])
    c_load = lcopy(cotangent, cbuf, local.at[1])
    c_load.start()
    x_load.start()

    def number(place, side, k):
        return order[4 * place + 2 * side + k]

    late = [number(z, s, 0) > number(z, s, 1) for s in (y, 1 - y)]

    def block_number(lh, place, side):
        first, second = number(place, side, 0), number(place, side, 1)
        return jnp.minimum(first, second) if lh == 0 else jnp.maximum(first, second)

    for lh in range(2):
        for h in range(2):
            at_block = block_table[:, pl.ds(block_number(lh, z, (y, 1 - y)[h]), 1), :]
            cb, sb = at_block[0], at_block[1]
            ci, si = row_table[0], row_table[1]
            cosine[lh, h] = cb * ci - sb * si
            sine[lh, h] = sb * ci + cb * si

    def by_order(h, first, second):
        return jnp.where(late[h], second, first), jnp.where(late[h], first, second)

    small[...] = jnp.zeros(small.shape, F32)
    model = 2 * half
    chunk_rows = 64
    c_load.wait()

    def cast(i, _):
        at = pl.ds(pl.multiple_of(i * chunk_rows, chunk_rows), chunk_rows)
        c = cbuf[at, :]
        small[S_OUT : S_OUT + 1, :model] += jnp.sum(c, axis=0, keepdims=True)
        c = c.astype(BF16)
        cot[0, at, :] = c[:, :half]
        cot[1, at, :] = c[:, half:]
        return 0

    lax.fori_loop(0, rows // chunk_rows, cast, 0)
    pl.semaphore_wait(barrier, len(greet))
    y_copy(Y_COT).start()
    end_send(E_COT)

    x_load.wait()

    def unit_of(at):
        x = xbuf[at, :]
        centred = x - jnp.mean(x, axis=-1, keepdims=True)
        variance = jnp.mean(centred * centred, axis=-1, keepdims=True)
        inv_scale = lax.rsqrt(variance + norm_epsilon)
        return centred * inv_scale, inv_scale

    def norms(i, _):
        at = pl.ds(pl.multiple_of(i * chunk_rows, chunk_rows), chunk_rows)
        unit, _ = unit_of(at)
        for n, ref in ((0, attn), (1, norm)):
            value = (unit * gain[n : n + 1, :] + shift[n : n + 1, :]).astype(BF16)
            ref[0, at, :] = value[:, :half]
            ref[1, at, :] = value[:, half:]
        return 0

    lax.fori_loop(0, rows // chunk_rows, norms, 0)

    def tile_at(i):
        return pl.ds(pl.multiple_of(i * TILE, TILE), TILE)

    def hidden_at(i):
        at = pl.ds(pl.multiple_of(lax.rem(i * TILE, hidden_half), TILE), TILE)
        return i * TILE // hidden_half, at

    def activate(i, slot):
        h = nn(norm[0], wcol[slot, :half, :]) + nn(norm[1], wcol[slot, half : 2 * half, :])
        h = h + b_up[:, tile_at(i)]
        gate = 0.5 * (1.0 + lax.erf(h * root_half))
        which, at = hidden_at(i)
        act[which, :, at] = (h * gate).astype(BF16)
        slope = gate + h * jnp.exp(-0.5 * h * h) * inverse_root_two_pi
        hid[which, :, at] = slope.astype(BF16)

    def hidden_back(i, slot):
        g = nt(cot[0], wrow[slot, :TILE, :half]) + nt(cot[1], wrow[slot, :TILE, half : 2 * half])
        which, at = hidden_at(i)
        g = g * hid[which, :, at].astype(F32)
        small[S_UP : S_UP + 1, tile_at(i)] = jnp.sum(g, axis=0, keepdims=True)
        hid[which, :, at] = g.astype(BF16)

    hidden_tiles = 2 * hidden_half // TILE
    def project(at, slot, place):
        value = nn(attn[0], wcol[slot, :half, :]) + nn(attn[1], wcol[slot, half : 2 * half, :])
        value = value + b_qkv[at][None, :]
        pieces = by_order(0, value[:blk], value[blk:])
        for lh in range(2):
            first, rest = pieces[lh][:, :LANES], pieces[lh][:, LANES:]
            place(lh, first, rest)

    def put(refs, which, lh, at, value):
        mine, away = refs

        @pl.when(which == 0)
        def _():
            mine[lh, 0, :, at] = value

        @pl.when(which == 1)
        def _():
            away[lh, :, at] = value

    def kv_index(i):
        which = 1 - i // (2 * own_heads)
        k, kind = lax.rem(i, 2 * own_heads) // 2, 1 + lax.rem(i, 2)
        head = jnp.where(which == 0, y, 1 - y) * own_heads + k
        return which, k, kind, 3 * head + kind

    def q_index(i):
        which = 1 - i // own_heads
        k = lax.rem(i, own_heads)
        head = jnp.where(which == 0, y, 1 - y) * own_heads + k
        return which, k, 3 * head, head

    def fetch_by(w, index):
        def fetch(i, slot):
            return lcopy(w.at[:, tile_at(index(i))], wcol.at[slot, pl.ds(0, w.shape[0]), :], wsem.at[0, slot])

        return fetch

    def lanes_at(start, n):
        return pl.ds(pl.multiple_of(start, LANES), n)

    def keys_values(i, slot):
        which, k, kind, tile = kv_index(i)
        base = jnp.where(kind == 1, 0, width) + k * HD

        def place(lh, first, rest):
            turned = turn(first, cosine[lh, 0], sine[lh, 0], 1)
            first = jnp.where(kind == 1, turned, first).astype(BF16)
            put((kv_own, kv_away), which, lh, lanes_at(base, LANES), first)
            put((kv_own, kv_away), which, lh, lanes_at(base + LANES, HD - LANES), rest.astype(BF16))

        project(tile_at(tile), slot, place)

    w_out_fetch = lcopy(w_out, wrow.at[0, pl.ds(0, w_out.shape[0]), pl.ds(0, model)], wsem.at[1, 0])

    def queries(i, slot):
        which, k, tile, head = q_index(i)

        def place(lh, first, rest):
            turned = turn(first, cosine[lh, 0], sine[lh, 0], 1).astype(BF16)
            put((qg_own, qg_away), which, lh, lanes_at(k * HD, LANES), turned)
            put((qg_own, qg_away), which, lh, lanes_at(k * HD + LANES, HD - LANES), rest.astype(BF16))

        project(tile_at(tile), slot, place)
        at = pl.ds(pl.multiple_of(head * HD, HD), HD)
        g = nt(cot[0], wrow[0, at, :half]) + nt(cot[1], wrow[0, at, half : 2 * half])
        pieces = by_order(0, g[:blk], g[blk:])
        for lh in range(2):
            put((qg_own, qg_away), which, lh, lanes_at(width + k * HD, HD), pieces[lh].astype(BF16))

    own_places = [
        lcopy(own.at[:, h], everyone.at[:, h], local.at[2 + 2 * t + h])
        for t, (own, everyone) in enumerate(((kv_own, kv_all), (qg_own, qg_all)))
        for h in range(2)
    ]

    def cols_at(ref, j):
        start = lax.rem(z + j, line) * block_cols
        at = pl.ds(pl.multiple_of(lax.rem(start, half), LANES), block_cols)
        return ref[start // half, :, at]

    def split_cols(ref, j, at, value):
        n = value.shape[1] // 2
        ref[j, 0, at, :] = value[:, :n].astype(BF16)
        ref[j, 1, at, :] = value[:, n:].astype(BF16)

    def split_rows(ref, j, at, value):
        n = value.shape[0] // 2
        ref[j, 0, :, at] = value[:n].astype(BF16)
        ref[j, 1, :, at] = value[n:].astype(BF16)

    def in_order(share, first=0, end=line):
        def one(k, _):
            j = jnp.where(lax.rem(k, 2) == 0, line - 1 - k // 2, k // 2 + 1)
            share(jnp.where(k == line - 1, 0, j))
            return 0

        lax.fori_loop(first, end, one, 0)

    def mlp_back(i, slot):
        value = nt(hid[0], wrow[slot, :TILE, :hidden_half]) + nt(
            hid[1], wrow[slot, :TILE, hidden_half : 2 * hidden_half]
        )
        tp_part[MLPB, :, :, tile_at(i)] = value.astype(BF16).reshape(2, blk, TILE)

    model_tiles = model // TILE

    def share_down(j):
        g0, g1 = cols_at(cot, j), cols_at(cot_far, j)

        def one(i, _):
            split_cols(
                c_down, j, tile_at(i), tn(act[y, :, tile_at(i)], g0) + tn(act_far[:, tile_at(i)], g1)
            )
            return 0

        lax.fori_loop(0, hidden_half // TILE, one, 0)

    def share_up(j):
        m0, m1 = cols_at(norm, j), cols_at(norm_far, j)

        def one(i, _):
            split_rows(c_up, j, tile_at(i), tn(m0, hid[y, :, tile_at(i)]) + tn(m1, hid_far[:, tile_at(i)]))
            return 0

        lax.fori_loop(0, hidden_half // TILE, one, 0)

    def end_tile(k):
        def fetch(i, slot):
            return lcopy(
                act_end.at[pl.ds(k * rows, rows), tile_at(i)], wcol.at[slot, pl.ds(0, rows), :], wsem.at[0, slot]
            )

        return fetch

    def add_end_tokens(k, item, tiles):
        @pl.when(next_to_end)
        def _():
            if item != E_ACT_LAST:
                end_share(k).wait_recv()
            held = lcopy(
                cot_end.at[pl.ds(k * rows, rows), :],
                wrow.at[k, pl.ds(0, rows), pl.ds(0, model)],
                wsem.at[1, k],
            )
            held.start()
            end_copy(item, partner).wait_recv()
            held.wait()

            def add_tile(i, slot):
                at = tile_at(i)

                def add_block(n, _):
                    j = jnp.where(z == 1, n, lax.rem(n + 2, line))
                    start = pl.multiple_of(lax.rem(z + j, line) * block_cols, LANES)
                    value = tn(wcol[slot, :rows, :], wrow[k, :rows, pl.ds(start, block_cols)])
                    n = block_cols // 2
                    for p in range(2):
                        c_down[j, p, at, :] = (
                            c_down[j, p, at, :].astype(F32) + value[:, p * n : (p + 1) * n]
                        ).astype(BF16)
                    return 0

                lax.fori_loop(0, line - 1, add_block, 0)

            stream(*tiles, (end_tile(k),), add_tile)

    pair = 2 * blk
    same = lax.broadcasted_iota(jnp.int32, (pair, pair), 0) == lax.broadcasted_iota(
        jnp.int32, (pair, pair), 1
    )

    def positions(lh, place, along):
        shape = (1, pair) if along else (pair, 1)
        at = lax.broadcasted_iota(jnp.int32, shape, along)
        here, there = block_number(lh, place, y), block_number(lh, place, 1 - y)
        return at + jnp.where(at < blk, here * blk, there * blk - blk)

    def piece_positions(lh_start, i, along):
        place = lax.rem(z + i, line)
        early, late_ = positions(0, place, along), positions(1, place, along)
        return jnp.where(i < line, early, late_)

    def piece(t):
        def fetch(i, slot):
            ref = (kv_all, qg_all)[t]
            return lcopy(
                ref.at[i // line, pl.ds(2 * lax.rem(i, line), 2)], chunk.at[slot], csem.at[slot]
            )

        return fetch

    def store_order(ref):
        for h in range(2):
            first, second = by_order(h, ref[0, h], ref[1, h])
            ref[0, h] = first
            ref[1, h] = second

    def attend_forward():
        for lh in range(2):
            for head in range(own_heads):
                at_k, at_v = head * HD, width + head * HD
                run_m[...] = jnp.full(run_m.shape, masked_value, F32)
                run_l[...] = jnp.zeros(run_l.shape, F32)
                acc_a[...] = jnp.zeros(acc_a.shape, F32)

                def attend(i, slot):
                    k = chunk[slot, :, :, at_k : at_k + HD].reshape(pair, HD)
                    v = chunk[slot, :, :, at_v : at_v + HD].reshape(pair, HD)
                    q = qg_own[lh, :, :, at_k : at_k + HD].reshape(pair, HD)
                    s = nt(q, k) * scale
                    seen = piece_positions(lh, i, 1) <= positions(lh, z, 0)
                    s = jnp.where(seen, s, masked_value)
                    old = run_m[...]
                    top = jnp.maximum(old, jnp.max(s, axis=1, keepdims=True))
                    p = jnp.exp(s - top)
                    fade = jnp.exp(old - top)
                    run_m[...] = top
                    run_l[...] = run_l[...] * fade + jnp.sum(p, axis=1, keepdims=True)
                    acc_a[...] = acc_a[...] * fade + nn(p.astype(BF16), v)

                stream(0, line * (lh + 1), (piece(0),), attend)
                out = (acc_a[...] / run_l[...]).astype(BF16)
                att[lh, :, :, at_k : at_k + HD] = out.reshape(2, blk, HD)
                log_total = run_m[...] + jnp.log(run_l[...])
                g = qg_own[lh, :, :, at_v : at_v + HD].reshape(pair, HD)
                dots = jnp.sum(g.astype(F32) * out.astype(F32), axis=1, keepdims=True)
                stats[lh, head, 0:1, :] = jnp.sum(jnp.where(same, log_total, 0.0), 0, keepdims=True)
                stats[lh, head, 1:2, :] = jnp.sum(jnp.where(same, dots, 0.0), 0, keepdims=True)

    def stat_copy(j):
        return rcopy(
            stats, stats_all.at[line - j], st_s.at[j], st_r.at[line - j], (place_of(j), tp)
        )

    def share_out(j):
        g0, g1 = cols_at(cot, j), cols_at(cot_far, j)

        def one(i, _):
            a0 = att[:, 0, :, tile_at(i)].reshape(rows, TILE)
            a1 = att[:, 1, :, tile_at(i)].reshape(rows, TILE)
            split_cols(c_out, j, tile_at(i), tn(a0, g0) + tn(a1, g1))
            return 0

        lax.fori_loop(0, width // TILE, one, 0)

    def undo(value, lh, head, kind):
        at = (3 * head + kind) * HD
        first = value[:, :LANES]
        if kind < 2:
            first = turn(
                first, cosine[lh].reshape(pair, LANES), sine[lh].reshape(pair, LANES), -1
            )
        for lo, hi, part in ((0, LANES, first), (LANES, HD, value[:, LANES:])):
            spot = lanes_at(y * 3 * width + at + lo, hi - lo)
            small[S_QKV : S_QKV + 1, spot] += jnp.sum(part, axis=0, keepdims=True)
            gqkv[lh, :, :, at + lo : at + hi] = part.astype(BF16).reshape(2, blk, hi - lo)

    def attend_back_queries():
        for lh in range(2):
            for head in range(own_heads):
                at_k, at_v = head * HD, width + head * HD
                run_m[...] = jnp.sum(
                    jnp.where(same, stats[lh, head, 0:1, :], 0.0), axis=1, keepdims=True
                )
                run_l[...] = jnp.sum(
                    jnp.where(same, stats[lh, head, 1:2, :], 0.0), axis=1, keepdims=True
                )
                acc_a[...] = jnp.zeros(acc_a.shape, F32)

                def back_q(i, slot):
                    k = chunk[slot, :, :, at_k : at_k + HD].reshape(pair, HD)
                    v = chunk[slot, :, :, at_v : at_v + HD].reshape(pair, HD)
                    q = qg_own[lh, :, :, at_k : at_k + HD].reshape(pair, HD)
                    g = qg_own[lh, :, :, at_v : at_v + HD].reshape(pair, HD)
                    s = nt(q, k) * scale
                    seen = piece_positions(lh, i, 1) <= positions(lh, z, 0)
                    s = jnp.where(seen, s, masked_value)
                    p = jnp.exp(s - run_m[...])
                    ds = (p * (nt(g, v) - run_l[...]) * scale).astype(BF16)
                    acc_a[...] += nn(ds, k)

                stream(0, line * (lh + 1), (piece(0),), back_q)
                undo(acc_a[...], lh, head, 0)

    def branch(i, slot):
        value = nn(act[0], wcol[slot, :hidden_half, :]) + nn(
            act[1], wcol[slot, hidden_half : 2 * hidden_half, :]
        )
        own = att[:, 0].reshape(rows, width)
        far = att_far[...].reshape(rows, width)
        mine = wrow[0, pl.ds(pl.multiple_of(y * width, width), width), tile_at(i)]
        theirs = wrow[0, pl.ds(pl.multiple_of((1 - y) * width, width), width), tile_at(i)]
        value += nn(own, mine) + nn(far, theirs)
        tp_part[BRANCH, :, :, tile_at(i)] = value.astype(BF16).reshape(2, blk, TILE)

    def attend_back_keys():
        for lh in range(2):
            for head in range(own_heads):
                at_k, at_v = head * HD, width + head * HD
                acc_a[...] = jnp.zeros(acc_a.shape, F32)
                acc_b[...] = jnp.zeros(acc_b.shape, F32)

                def back_k(i, slot):
                    q = chunk[slot, :, :, at_k : at_k + HD].reshape(pair, HD)
                    g = chunk[slot, :, :, at_v : at_v + HD].reshape(pair, HD)
                    k = kv_own[lh, :, :, at_k : at_k + HD].reshape(pair, HD)
                    v = kv_own[lh, :, :, at_v : at_v + HD].reshape(pair, HD)
                    stat = stats_all[lax.rem(i, line), i // line, head]
                    s = nt(k, q) * scale
                    seen = positions(lh, z, 0) <= piece_positions(lh, i, 1)
                    s = jnp.where(seen, s, masked_value)
                    p = jnp.exp(s - stat[0:1, :])
                    ds = (p * (nt(v, g) - stat[1:2, :]) * scale).astype(BF16)
                    acc_a[...] += nn(ds, q)
                    acc_b[...] += nn(p.astype(BF16), g)

                stream(lh * line, 2 * line, (piece(1),), back_k)
                undo(acc_a[...], lh, head, 1)
                undo(acc_b[...], lh, head, 2)

    def share_qkv(j):
        m0, m1 = cols_at(attn, j), cols_at(norm_far, j)

        def one(i, _):
            g0 = gqkv[:, 0, :, tile_at(i)].reshape(rows, TILE)
            g1 = gqkv[:, 1, :, tile_at(i)].reshape(rows, TILE)
            split_rows(c_qkv, j, tile_at(i), tn(m0, g0) + tn(m1, g1))
            return 0

        lax.fori_loop(0, 3 * width // TILE, one, 0)

    def attn_back(i, slot):
        own = gqkv[:, 0].reshape(rows, 3 * width)
        far = gqkv_far[...].reshape(rows, 3 * width)
        mine = wrow[slot, :TILE, pl.ds(pl.multiple_of(y * 3 * width, LANES), 3 * width)]
        theirs = wrow[slot, :TILE, pl.ds(pl.multiple_of((1 - y) * 3 * width, LANES), 3 * width)]
        value = nt(own, mine) + nt(far, theirs)
        tp_part[ATTNB, :, :, tile_at(i)] = value.astype(BF16).reshape(2, blk, TILE)

    def back_norms(i, _):
        at = pl.ds(pl.multiple_of(i * chunk_rows, chunk_rows), chunk_rows)
        at_part = pl.ds(pl.multiple_of(lax.rem(i * chunk_rows, blk), chunk_rows), chunk_rows)
        which = i * chunk_rows // blk
        unit, inv_scale = unit_of(at)
        total = jnp.zeros((chunk_rows, model), F32)
        for n, part in ((0, ATTNB), (1, MLPB)):
            value = tp_part[part, which, at_part, :].astype(F32)
            small[S_GAIN + n : S_GAIN + n + 1, :model] += jnp.sum(value * unit, 0, keepdims=True)
            small[S_SHIFT + n : S_SHIFT + n + 1, :model] += jnp.sum(value, 0, keepdims=True)
            total = total + value * gain[n : n + 1, :]
        cbuf[at, :] = cbuf[at, :] + inv_scale * (
            total
            - jnp.mean(total, axis=-1, keepdims=True)
            - unit * jnp.mean(total * unit, axis=-1, keepdims=True)
        )
        return 0

    def small_copy(j):
        return rcopy(
            small_sent, small_recv.at[line - j], sm_s.at[j], sm_r.at[line - j], (place_of(j), tp)
        )

    def stream_rows(i, _):
        at = pl.ds(pl.multiple_of(i * chunk_rows, chunk_rows), chunk_rows)
        at_part = pl.ds(pl.multiple_of(lax.rem(i * chunk_rows, blk), chunk_rows), chunk_rows)
        which = i * chunk_rows // blk
        xbuf[at, :] = xbuf[at, :] + out_bias[...] + tp_part[BRANCH, which, at_part, :].astype(F32)
        return 0

    stream(0, 4 * own_heads, (fetch_by(w_qkv, lambda i: kv_index(i)[3]),), keys_values)
    y_copy(Y_KV).start()
    ag_hop(0, 0, 1)
    own_places[0].start()
    w_out_fetch.start()
    w_out_fetch.wait()
    stream(0, 2 * own_heads, (fetch_by(w_qkv, lambda i: q_index(i)[2]),), queries)
    y_copy(Y_QG).start()
    ag_hop(1, 0, 1)
    own_places[2].start()
    pass_x(Y_COT, 0)

    stream(0, hidden_tiles // 2, (col_tile(w_up),), activate)
    y_copy(Y_KV).wait_recv()
    ag_hop(0, 1, 1)
    own_places[1].start()
    stream(hidden_tiles // 2, hidden_tiles, (col_tile(w_up),), activate)
    y_copy(Y_ACT).start()
    y_copy(Y_MLP).start()
    end_send(E_ACT)
    pass_on(Y_COT, 0)
    ag_hop(0, 0, 2)
    end_pass_x(0)
    stream(0, hidden_tiles // 2, (row_tile(w_down),), hidden_back)
    y_copy(Y_QG).wait_recv()
    own_places[3].start()
    ag_hop(1, 1, 1)
    ag_hop(1, 0, 2)
    stream(hidden_tiles // 2, hidden_tiles, (row_tile(w_down),), hidden_back)
    y_copy(Y_HID).start()
    y_copy(Y_ATTN).start()
    end_pass(0)
    stream(0, model_tiles, (row_tile(w_up),), mlp_back)
    tp_copy(MLPB, 0).start()
    ag_hop(0, 0, 3)
    ag_hop(0, 1, 2)
    core_copy(0).wait_recv()
    y_copy(Y_ACT).wait_recv()
    end_send(E_ACT_FAR)
    end_send(E_ACT_LAST)
    in_order(share_down)
    pass_x(Y_MLP, 1)
    end_pass_x(1)
    ag_hop(0, 1, 3)
    end_tiles = hidden_half // TILE
    add_end_tokens(0, E_ACT, (0, end_tiles))
    pass_on(Y_MLP, 1)
    end_pass(1)
    ag_hop(1, 0, 3)
    ag_hop(1, 1, 2)
    add_end_tokens(1, E_ACT_FAR, (0, end_tiles // 2))
    rs_ends(DOWN, (1, 3), (0,))
    add_end_tokens(1, E_ACT_LAST, (end_tiles // 2, end_tiles))
    rs_ends(DOWN, (1, 3), (1,))
    tp_next(MLPB, 1)
    y_copy(Y_HID).wait_recv()
    core_copy(1).wait_recv()
    in_order(share_up)
    rs_ends(UP, (1, 2))
    ag_rest(0, 0, 4)
    ag_rest(0, 1, 4)
    for copy in own_places:
        copy.wait()

    attend_forward()
    store_order(att)
    for j in range(1, line):
        stat_copy(j).start()
    y_copy(Y_ATT).start()
    rs_ends(UP, (2, line))
    rs_ends(DOWN, (3, line))
    in_order(share_out)
    small[S_QKV : S_QKV + 1, :] = jnp.zeros((1, small.shape[1]), F32)
    attend_back_queries()
    tp_next(MLPB, 2)
    ag_hop(1, 1, 3)
    pass_x(Y_ATTN, 2)
    for hop in range(1, min(line, 4)):
        rs_cross(DOWN, hop)
        rs_home(DOWN, hop)
    y_copy(Y_ATT).wait_recv()
    w_out_fetch.start()
    w_out_fetch.wait()
    stream(0, model_tiles, (col_tile(w_down),), branch)
    tp_copy(BRANCH, 0).start()
    rs_cross(UP, 1)
    rs_cross(UP, 2)
    ag_rest(1, 0, 4)
    ag_rest(1, 1, 4)
    for j in range(1, line):
        stat_copy(line - j).wait_recv()
    own_stats = lcopy(stats, stats_all.at[0], local.at[0])
    own_stats.start()
    own_stats.wait()
    attend_back_keys()
    store_order(gqkv)
    y_copy(Y_GQKV).start()
    tp_next(BRANCH, 1)
    pass_on(Y_ATTN, 2)
    core_copy(2).wait_recv()
    core_copy(1).wait_send()
    x_drain(1)
    far_again = lcopy(attn_far, norm_far, local.at[1])
    far_again.start()
    far_again.wait()
    in_order(share_qkv)
    rs_ends(QKV, (1, line))
    rs_ends(OUT, (1, line))
    rs_cross(UP, 3) if line > 3 else None
    rs_home(UP, 1)
    rs_home(UP, 2)
    rs_home(UP, 3) if line > 3 else None
    y_copy(Y_GQKV).wait_recv()
    stream(0, model_tiles, (row_tile(w_qkv),), attn_back)
    tp_copy(ATTNB, 0).start()
    tp_next(BRANCH, 2)
    tp_next(ATTNB, 1)

    rs_rest(DOWN, 4 if line > 3 else 3)
    rs_finish(DOWN)
    tp_done(BRANCH)
    tp_done(MLPB)
    rs_cross(QKV, 1)
    rs_cross(QKV, 2)
    rs_cross(QKV, 3) if line > 3 else None
    tp_next(ATTNB, 2)
    tp_done(ATTNB)
    lax.fori_loop(0, rows // chunk_rows, back_norms, 0)
    grad_store = lcopy(cbuf, grad_o, local.at[1])
    grad_store.start()
    rs_home(QKV, 1)
    rs_home(QKV, 2)
    rs_home(QKV, 3) if line > 3 else None
    rs_rest(QKV, 4 if line > 3 else 3)
    pair_copy = rcopy(small, small_pair, sm_s.at[0], sm_r.at[0], partner)
    pair_copy.start()
    pair_copy.wait()
    small_sent[...] = (small[...] + small_pair[...]).astype(BF16)
    for j in range(1, line):
        small_copy(j).start()
    lax.fori_loop(0, rows // chunk_rows, stream_rows, 0)
    stream_store = lcopy(xbuf, stream_o, local.at[0])
    stream_store.start()
    rs_rest(UP, 4 if line > 3 else 3)
    rs_finish(UP)
    rs_cross(OUT, 1)
    rs_cross(OUT, 2)
    rs_cross(OUT, 3) if line > 3 else None
    rs_finish(QKV)
    for hop in range(1, min(line, 4)):
        rs_home(OUT, hop)
    rs_rest(OUT, 4 if line > 3 else 3)
    rs_finish(OUT)
    for j in range(1, line):
        small_copy(line - j).wait_recv()
    small_recv[0] = small_sent[...]
    small[...] = small_recv[lax.rem(line - z, line)].astype(F32)
    for p in range(1, line):
        small[...] += small_recv[lax.rem(p + line - z, line)].astype(F32)
    small_store = lcopy(small, small_o, local.at[2])
    small_store.start()

    for t in range(2):
        for h in range(2):
            ag_drain(t, h)
    for item in (Y_KV, Y_QG, Y_COT, Y_MLP, Y_ATTN, Y_ACT, Y_HID, Y_ATT, Y_GQKV):
        y_copy(item).wait_send()
    core_copy(0).wait_send()
    core_copy(2).wait_send()
    x_drain(0)
    x_drain(2)
    for j in range(1, line):
        stat_copy(j).wait_send()
        small_copy(j).wait_send()
    for i in range(3):
        tp_drain(i)
    grad_store.wait()
    small_store.wait()
    stream_store.wait()
    for t in range(4):
        rs_drain(t)
    end_drain()


def layer(line, n_tp, order, stream_in, cotangent, ln_gain, ln_bias, w_qkv, b_qkv, w_out, out_bias, w_up, b_up, w_down):
    rows, model = stream_in.shape
    half, blk = model // 2, rows // 2
    hidden = w_up.shape[1]
    hidden_half = hidden // 2
    width = w_out.shape[0] // 2
    own_heads = width // HD
    part_cols = model // line // 2
    pair = 2 * blk
    tp_steps = 0
    while (2 << tp_steps) < n_tp:
        tp_steps += 1
    small_shape = (8, max(model, hidden, 6 * width))
    shares = (
        (2, hidden_half, part_cols),
        (2, part_cols, hidden_half),
        (2, width, part_cols),
        (2, part_cols, 3 * width),
    )
    b = lambda *s: jax.ShapeDtypeStruct(s, BF16)
    f = lambda *s: jax.ShapeDtypeStruct(s, F32)
    vb = lambda *s: pltpu.VMEM(s, BF16)
    vf = lambda *s: pltpu.VMEM(s, F32)
    dma = pltpu.SemaphoreType.DMA
    outs = (
        b(hidden, part_cols),
        b(part_cols, hidden),
        b(2 * width, part_cols),
        b(part_cols, 6 * width),
        f(rows, model),
        f(rows, model),
        f(*small_shape),
        b(2, 2 * line, blk, 2 * width),
        b(2, 2 * line, blk, 2 * width),
        b(line + 1, *shares[0]),
        b(line + 1, *shares[1]),
        b(line + 1, *shares[2]),
        b(line + 1, *shares[3]),
        b(2, rows, half),
        b(3, blk, model),
        b(2 * rows, model),
        b(2 * rows, hidden_half),
    )
    wide = max(model, hidden)
    scratch = (
        [vf(rows, model)] * 2
        + [vb(2, rows, half)] * 5
        + [vb(2, rows, hidden_half)] * 2
        + [vb(rows, hidden_half)] * 2
        + [vb(2, wide, TILE), vb(2, max(TILE, 2 * width), wide)]
        + [vb(line, *s) for s in shares]
        + [vb(*s) for s in shares]
        + [vb(3, 2, blk, model), vb(3, tp_steps + 1, blk, model)]
        + [vb(2, 2, blk, 2 * width)] * 2
        + [vb(2, blk, 2 * width)] * 2
        + [
            vb(2, 2, blk, 2 * width),
            vb(2, 2, blk, width),
            vb(2, blk, width),
            vf(2, own_heads, 2, pair),
            vf(line, 2, own_heads, 2, pair),
            vb(2, 2, blk, 3 * width),
            vb(2, blk, 3 * width),
            vf(pair, HD),
            vf(pair, HD),
            vf(pair, 1),
            vf(pair, 1),
            vf(2, 2, blk, LANES),
            vf(2, 2, blk, LANES),
            vf(*small_shape),
            vf(*small_shape),
            vb(*small_shape),
            vb(line, *small_shape),
            dma((2, 2, 2, line)),
            dma((2, 2, line)),
            dma((Y_FIN + 4,)),
            dma((Y_FIN + 4,)),
            dma((3,)),
            dma((3,)),
            dma((3, n_tp // 2)),
            dma((3, n_tp // 2)),
            dma((4, 2, line)),
            dma((4, 2, line + 1)),
            dma((3, tp_steps + 2)),
            dma((3, tp_steps + 2)),
            dma((line,)),
            dma((line,)),
            dma((line,)),
            dma((line,)),
            dma((7,)),
            dma((7,)),
            dma((2, n_tp // 2)),
            dma((2, n_tp // 2)),
            dma((9,)),
            dma((2, 2)),
            dma((2,)),
            dma((4,)),
        ]
    )
    blocks = order.shape[0]
    operands = (
        order,
        stream_in,
        cotangent,
        w_up,
        w_down,
        w_out,
        w_qkv,
        ln_gain,
        ln_bias,
        b_qkv,
        b_up.reshape(1, -1),
        out_bias.reshape(1, -1),
        jnp.asarray(rope_tables(np.arange(blocks) * blk)),
        jnp.asarray(rope_tables(np.arange(blk))),
    )
    return pl.pallas_call(
        functools.partial(layer_kernel, line, n_tp),
        name="layer",
        out_shape=outs,
        in_specs=[SMEM] + [ANY] * 6 + [VMEM] * 7,
        out_specs=[ANY] * len(outs),
        scratch_shapes=scratch,
        cost_estimate=pl.CostEstimate(
            flops=40 * rows * model * hidden,
            transcendentals=rows * hidden,
            bytes_accessed=8 * w_up.size,
        ),
        compiler_params=pltpu.CompilerParams(
            collective_id=0, has_side_effects=True, vmem_limit_bytes=67043328
        ),
    )(*operands)


def results_kernel(
    down,
    up,
    out,
    qkv,
    stream,
    grad,
    small,
    stream_o,
    grad_o,
    qkv_o,
    bqkv_o,
    out_o,
    obias_o,
    up_o,
    bup_o,
    down_o,
    gain_o,
    shift_o,
):
    stream_o[...] = stream[...]
    grad_o[...] = grad[...]
    for src, dst in ((qkv, qkv_o), (out, out_o), (up, up_o), (down, down_o)):
        dst[...] = src[...].astype(F32)

    @pl.when(pl.program_id(0) == 0)
    def _():
        bqkv_o[...] = small[S_QKV, : bqkv_o.shape[0]]
        obias_o[...] = small[S_OUT, : obias_o.shape[0]]
        bup_o[...] = small[S_UP, : bup_o.shape[0]]
        gain_o[...] = small[S_GAIN : S_GAIN + 2, : gain_o.shape[1]]
        shift_o[...] = small[S_SHIFT : S_SHIFT + 2, : shift_o.shape[1]]


def results(down, up, out, qkv, stream_out, grad_in, small, model, fused, hidden):
    steps = 4
    f = lambda *s: jax.ShapeDtypeStruct(s, F32)
    rows_of = lambda a: pl.BlockSpec((a.shape[0] // steps,) + a.shape[1:], lambda i: (i, 0))
    whole = lambda a: pl.BlockSpec(a.shape, lambda i: (0,) * len(a.shape))
    large = (down, up, out, qkv, stream_out, grad_in)
    while any(a.shape[0] % (16 * steps) for a in large[:4]):
        steps //= 2
    outs = (
        (f(*stream_out.shape), True),
        (f(*grad_in.shape), True),
        (f(*qkv.shape), True),
        (f(fused), False),
        (f(*out.shape), True),
        (f(model), False),
        (f(*up.shape), True),
        (f(hidden), False),
        (f(*down.shape), True),
        (f(2, model), False),
        (f(2, model), False),
    )
    return pl.pallas_call(
        results_kernel,
        name="results",
        grid=(steps,),
        out_shape=[o for o, _ in outs],
        in_specs=[rows_of(a) for a in large] + [whole(small)],
        out_specs=[rows_of(o) if tall else whole(o) for o, tall in outs],
        cost_estimate=pl.CostEstimate(
            flops=down.size, transcendentals=0, bytes_accessed=8 * down.size + 16 * stream_out.size
        ),
        compiler_params=pltpu.CompilerParams(vmem_limit_bytes=67043328),
    )(*large, small)


def shards(
    n_ctx,
    n_tp,
    stream_in,
    cotangent,
    ln_gain,
    ln_bias,
    w_qkv,
    b_qkv,
    w_out,
    out_bias,
    w_up,
    b_up,
    w_down,
    block_order,
):
    (down, up, out, qkv, stream_out, grad_in, small, *_) = layer(
        n_ctx // 2,
        n_tp,
        block_order,
        stream_in,
        cotangent,
        ln_gain,
        ln_bias,
        w_qkv,
        b_qkv,
        w_out,
        out_bias,
        w_up,
        b_up,
        w_down,
    )
    return results(down, up, out, qkv, stream_out, grad_in, small, *w_qkv.shape, w_up.shape[1])


def solution(mesh):
    placed = (
        P("ctx", None),
        P("ctx", None),
        P(),
        P(),
        P(None, "tp"),
        P("tp"),
        P("tp", None),
        P(),
        P(None, "tp"),
        P("tp"),
        P("tp", None),
        P(),
    )
    return jax.shard_map(
        functools.partial(shards, mesh.shape["ctx"], mesh.shape["tp"]),
        mesh=mesh,
        in_specs=placed,
        out_specs=(
            P("ctx", None),
            P("ctx", None),
            P("ctx", "tp"),
            P("tp"),
            P("tp", "ctx"),
            P(),
            P("ctx", "tp"),
            P("tp"),
            P("tp", "ctx"),
            P(),
            P(),
        ),
        check_vma=False,
    )
```

```python
import functools
import math

import jax
import jax.numpy as jnp
import numpy as np
from jax import lax
from jax.experimental import pallas as pl
from jax.experimental.pallas import tpu as pltpu
from jax.sharding import PartitionSpec as P

HD = 256
ROT = 64
LANES = 128
TILE = 256

masked_value = -1e30
norm_epsilon = 1e-05
root_half = 0.7071067811865476
inverse_root_two_pi = 0.3989422804014327

F32 = jnp.float32
BF16 = jnp.bfloat16
MESH = pl.DeviceIdType.MESH
ANY = pl.BlockSpec(memory_space=pl.ANY)
VMEM = pl.BlockSpec(memory_space=pltpu.VMEM)
SMEM = pl.BlockSpec(memory_space=pltpu.SMEM)


def nt(a, b):
    return lax.dot_general(a, b, (((1,), (1,)), ((), ())), preferred_element_type=F32)


def nn(a, b):
    return lax.dot_general(a, b, (((1,), (0,)), ((), ())), preferred_element_type=F32)


def tn(a, b):
    return lax.dot_general(a, b, (((0,), (0,)), ((), ())), preferred_element_type=F32)


def rope_tables(positions):
    half_rot = ROT // 2
    frequency = np.exp(np.arange(half_rot) * (-2.0 * math.log(10000.0) / ROT))
    angles = np.asarray(positions, np.float64)[:, None] * frequency
    table = np.zeros((2, angles.shape[0], LANES), np.float32)
    table[0] = 1.0
    for lo in (0, half_rot):
        table[0, :, lo : lo + half_rot] = np.cos(angles)
        table[1, :, lo : lo + half_rot] = np.sin(angles)
    return table


def turn(first, cosine, sine, sign):
    half_rot = ROT // 2
    scaled = first * sine if sign < 0 else first
    lane = lax.broadcasted_iota(jnp.int32, first.shape, 1)
    down = jnp.where(lane < half_rot, pltpu.roll(scaled, LANES - half_rot, 1), 0.0)
    up = jnp.where(
        jnp.logical_and(lane >= half_rot, lane < ROT), pltpu.roll(scaled, half_rot, 1), 0.0
    )
    if sign < 0:
        return first * cosine + (down - up)
    return first * cosine + (up - down) * sine


DOWN, UP, OUT, QKV = range(4)
(Y_KV, Y_QG, Y_COT, Y_MLP, Y_ATTN, Y_ACT, Y_HID, Y_ATT, Y_GQKV, Y_FIN) = range(10)
BRANCH, MLPB, ATTNB = range(3)
S_GAIN, S_SHIFT, S_OUT, S_UP, S_QKV = 0, 2, 4, 5, 6


def layer_kernel(
    line,
    n_tp,
    order,
    stream_in,
    cotangent,
    w_up,
    w_down,
    w_out,
    w_qkv,
    gain,
    shift,
    b_qkv,
    b_up,
    out_bias,
    block_table,
    row_table,
    down_o,
    up_o,
    out_o,
    qkv_o,
    stream_o,
    grad_o,
    small_o,
    kv_all,
    qg_all,
    rs_down,
    rs_up,
    rs_out,
    rs_qkv,
    attn_far,
    tp_far,
    cot_end,
    act_end,
    xbuf,
    cbuf,
    cot,
    cot_far,
    norm,
    norm_far,
    attn,
    act,
    hid,
    act_far,
    hid_far,
    wcol,
    wrow,
    c_down,
    c_up,
    c_out,
    c_qkv,
    stage_down,
    stage_up,
    stage_out,
    stage_qkv,
    tp_part,
    tp_recv,
    kv_own,
    qg_own,
    kv_away,
    qg_away,
    chunk,
    att,
    att_far,
    stats,
    stats_all,
    gqkv,
    gqkv_far,
    acc_a,
    acc_b,
    run_m,
    run_l,
    cosine,
    sine,
    small,
    small_pair,
    small_sent,
    small_recv,
    ag_s,
    ag_r,
    y_s,
    y_r,
    core_s,
    core_r,
    x_s,
    x_r,
    rs_s,
    rs_r,
    tp_s,
    tp_r,
    st_s,
    st_r,
    sm_s,
    sm_r,
    end_s,
    end_r,
    ex_s,
    ex_r,
    local,
    wsem,
    csem,
    tsem,
):
    me, tp = lax.axis_index("ctx"), lax.axis_index("tp")
    z, y = me // 2, lax.rem(me, 2)
    core = lax.rem(tp, 2)
    partner = (me + 1 - 2 * y, tp)
    sibling = (me, tp + 1 - 2 * core)
    right, left = (me + 2, tp), (me - 2, tp)
    far_steps = []
    step = 2
    while step < n_tp:
        far_steps.append((me, tp + step - 2 * step * lax.rem(tp // step, 2)))
        step *= 2

    rows = norm.shape[1]
    blk = rows // 2
    across = n_tp // 2
    xpos = tp // 2
    x_others = [(me, lax.rem(tp + 2 * k, n_tp)) for k in range(1, across)]
    half = norm.shape[2]
    hidden_half = act.shape[2]
    own_heads = kv_own.shape[-1] // (2 * HD)
    width = own_heads * HD
    block_cols = 2 * half // line
    scale = HD ** (-0.5)

    def place_of(j):
        return lax.rem(z + j, line) * 2 + y

    barrier = pltpu.get_barrier_semaphore()
    greet = [partner, sibling] + x_others + [(place_of(j), tp) for j in range(1, line)]
    for device in greet:
        pl.semaphore_signal(barrier, inc=1, device_id=device, device_id_type=MESH)

    def rcopy(src, dst, s, r, device):
        return pltpu.make_async_remote_copy(
            src_ref=src, dst_ref=dst, send_sem=s, recv_sem=r, device_id=device, device_id_type=MESH
        )

    def lcopy(src, dst, sem):
        return pltpu.make_async_copy(src, dst, sem)

    def fin_parts(t):
        c = (c_down, c_up, c_out, c_qkv)[t]
        if t == DOWN:
            dst = down_o.at[pl.ds(pl.multiple_of(y * hidden_half, hidden_half), hidden_half), :]
        elif t == UP:
            dst = up_o.at[:, pl.ds(pl.multiple_of(y * hidden_half, hidden_half), hidden_half)]
        elif t == OUT:
            dst = out_o.at[pl.ds(pl.multiple_of(y * width, width), width), :]
        else:
            dst = qkv_o.at[:, pl.ds(pl.multiple_of(y * 3 * width, 3 * width), 3 * width)]
        return c, dst

    def part_rows(x):
        n = rows // across
        return pl.ds(pl.multiple_of(x * n, n), n)

    def y_copy(item, t=0):
        if item == Y_KV:
            src, dst = kv_away, kv_own.at[:, 1]
        elif item == Y_QG:
            src, dst = qg_away, qg_own.at[:, 1]
        elif item == Y_COT:
            src, dst = cot.at[core, part_rows(xpos)], cot_far.at[core, part_rows(xpos)]
        elif item == Y_MLP:
            src, dst = norm.at[core, part_rows(xpos)], norm_far.at[core, part_rows(xpos)]
        elif item == Y_ATTN:
            src, dst = attn.at[core, part_rows(xpos)], attn_far.at[core, part_rows(xpos)]
        elif item == Y_ACT:
            src, dst = act.at[1 - y], act_far
        elif item == Y_HID:
            src, dst = hid.at[1 - y], hid_far
        elif item == Y_ATT:
            src, dst = att.at[:, 1], att_far
        elif item == Y_GQKV:
            src, dst = gqkv.at[:, 1], gqkv_far
        else:
            c, dst = fin_parts(t)
            src = c.at[0, 1 - y]
            item = Y_FIN + t
        return rcopy(src, dst, y_s.at[item], y_r.at[item], partner)

    def core_copy(k):
        ref = (cot_far, norm_far, attn_far)[k]
        return rcopy(ref.at[core], ref.at[core], core_s.at[k], core_r.at[k], sibling)

    def x_copy(k, n):
        ref = (cot_far, norm_far, attn_far)[k].at[core, part_rows(xpos)]
        return rcopy(ref, ref, x_s.at[k, n], x_r.at[k, n], x_others[n])

    def x_arrival(k, n):
        ref = (cot_far, norm_far, attn_far)[k].at[core, part_rows(lax.rem(xpos + across - n - 1, across))]
        return rcopy(ref, ref, x_s.at[k, n], x_r.at[k, n], x_others[n])

    def pass_x(item, k):
        y_copy(item).wait_recv()
        for n in range(across - 1):
            x_copy(k, n).start()

    def pass_on(item, k):
        for n in range(across - 1):
            x_arrival(k, n).wait_recv()
        core_copy(k).start()

    def x_drain(k):
        for n in range(across - 1):
            x_copy(k, n).wait_send()

    E_COT, E_COT_FAR, E_ACT, E_ACT_FAR, E_ACT_LAST = range(5)
    next_to_end = jnp.logical_or(z == 1, z == line - 2)

    def end_part(k, x):
        n = rows // across
        return cot_end.at[
            pl.ds(pl.multiple_of(k * rows + x * n, n), n), pl.ds(pl.multiple_of(core * half, half), half)
        ]

    def end_copy(item, device):
        if item == E_COT:
            src, dst = cot.at[core, part_rows(xpos)], end_part(0, xpos)
        elif item == E_COT_FAR:
            src, dst = end_part(0, xpos), end_part(1, xpos)
        elif item == E_ACT:
            src, dst = act.at[y], act_end.at[pl.ds(0, rows), :]
        else:
            n = hidden_half // 2
            part = pl.ds(0 if item == E_ACT_FAR else n, n)
            src, dst = act_far.at[:, part], act_end.at[pl.ds(rows, rows), part]
        return rcopy(src, dst, end_s.at[item], end_r.at[item], device)

    def end_x(k, n, arriving):
        x = lax.rem(xpos + across - n - 1, across) if arriving else xpos
        ref = end_part(k, x)
        return rcopy(ref, ref, ex_s.at[k, n], ex_r.at[k, n], x_others[n])

    def end_share(k):
        ref = cot_end.at[pl.ds(k * rows, rows), pl.ds(pl.multiple_of(core * half, half), half)]
        return rcopy(ref, ref, end_s.at[5 + k], end_r.at[5 + k], sibling)

    def end_send(item):
        @pl.when(z == 0)
        def _():
            end_copy(item, right).start()

        @pl.when(z == line - 1)
        def _():
            end_copy(item, left).start()

    def end_pass_x(k):
        @pl.when(next_to_end)
        def _():
            end_copy(E_COT + k, partner).wait_recv()
            for n in range(across - 1):
                end_x(k, n, False).start()
            if k == 0:
                end_copy(E_COT_FAR, partner).start()

    def end_pass(k):
        @pl.when(next_to_end)
        def _():
            for n in range(across - 1):
                end_x(k, n, True).wait_recv()
            end_share(k).start()

    def end_drain():
        @pl.when(jnp.logical_or(z == 0, z == line - 1))
        def _():
            for item in (E_COT, E_ACT, E_ACT_FAR, E_ACT_LAST):
                end_copy(item, partner).wait_send()

        @pl.when(next_to_end)
        def _():
            end_copy(E_COT_FAR, partner).wait_send()
            for k in range(2):
                end_share(k).wait_send()
                for n in range(across - 1):
                    end_x(k, n, False).wait_send()

    def ag_copy(t, h, to, hop, j_src, j_dst):
        ref = (kv_all, qg_all)[t]
        src = ref.at[:, 2 * j_src + h]
        if isinstance(hop, int) and hop == 1:
            src = (kv_own, qg_own)[t].at[:, h]
        return rcopy(
            src,
            ref.at[:, 2 * j_dst + h],
            ag_s.at[t, h, to, hop],
            ag_r.at[t, h, j_dst],
            (right, left)[to],
        )

    def ag_send_when(hop):
        return (
            jnp.logical_and(z >= hop - 1, z <= line - 2),
            jnp.logical_and(z + hop - 1 <= line - 1, z >= 1),
        )

    def ag_hop(t, h, hop, only=None):
        first = isinstance(hop, int) and hop == 1
        to_right, to_left = ag_send_when(hop)
        if only is not None:
            to_right, to_left = jnp.logical_and(to_right, only), jnp.logical_and(to_left, only)

        @pl.when(to_right)
        def _():
            if not first:
                ag_copy(t, h, 0, hop - 1, line - hop + 1, line - hop + 1).wait_recv()
            ag_copy(t, h, 0, hop, lax.rem(line - hop + 1, line), line - hop).start()

        @pl.when(to_left)
        def _():
            if not first:
                ag_copy(t, h, 1, hop - 1, hop - 1, hop - 1).wait_recv()
            ag_copy(t, h, 1, hop, hop - 1, hop).start()

    def ag_rest(t, h, hop):
        def one(i, _):
            ag_hop(t, h, i)
            return 0

        def come(i, _):
            ag_copy(t, h, 0, i, i, i).wait_recv()
            return 0

        if hop < line:
            lax.fori_loop(hop, line, one, 0)

        @pl.when(jnp.logical_or(z == 0, z == line - 1))
        def _():
            lax.fori_loop(1, line, come, 0)

    def ag_drain(t, h):
        def one(hop, _):
            to_right, to_left = ag_send_when(hop)

            @pl.when(to_right)
            def _():
                ag_copy(t, h, 0, hop, lax.rem(line - hop + 1, line), line - hop).wait_send()

            @pl.when(to_left)
            def _():
                ag_copy(t, h, 1, hop, hop - 1, hop).wait_send()

            return 0

        lax.fori_loop(1, line, one, 0)

    rs = (
        (c_down, rs_down, stage_down),
        (c_up, rs_up, stage_up),
        (c_out, rs_out, stage_out),
        (c_qkv, rs_qkv, stage_qkv),
    )

    def piece_of(ref, t, p):
        if t != DOWN:
            return ref.at[p]
        n = hidden_half // 2
        return ref.at[:, pl.ds(pl.multiple_of(p * n, n), n), :]

    def rs_copy(t, p, j, slot, device):
        c, recv, _ = rs[t]
        return rcopy(
            piece_of(c.at[j], t, p), piece_of(recv.at[slot], t, p), rs_s.at[t, p, j], rs_r.at[t, p, slot], device
        )

    def rs_take(t, p, j, slot):
        c, recv, held = rs[t]
        rs_copy(t, p, j, slot, partner).wait_recv()
        copy = lcopy(piece_of(recv.at[slot], t, p), piece_of(held, t, p), tsem.at[t])
        copy.start()
        copy.wait()
        n = c.shape[2]
        part = min(64, n)

        def add(side, i):
            at = pl.ds(pl.multiple_of(i * part, part), part)
            c[j, side, at, :] = (
                c[j, side, at, :].astype(F32) + held[side, at, :].astype(F32)
            ).astype(BF16)

        def one(i, _):
            if t != DOWN:
                add(p, i)
            else:
                for side in range(2):
                    add(side, p * (n // part // 2) + i)
            return 0

        lax.fori_loop(0, n // part // (2 if t == DOWN else 1), one, 0)

    def first_from(t):
        return 2 if t == DOWN else 1

    def rs_ends(t, hops, parts=(0, 1)):
        first = first_from(t)

        def one(hop, _):
            for k in parts:
                p = k if t == DOWN else (1 - y if k == 0 else y)

                @pl.when(jnp.logical_and(z == first - 1, hop >= first))
                def _():
                    rs_copy(t, p, line - hop, line - hop - 1, right).start()

                @pl.when(jnp.logical_and(z == line - first, hop >= first))
                def _():
                    rs_copy(t, p, hop, hop + 1, left).start()

            return 0

        lax.fori_loop(*hops, one, 0)

    near = 2 * z < line

    def halves(t, step):
        def one(k, _):
            step(k if t == DOWN else jnp.where(k == 0, 1 - y, y))
            return 0

        lax.fori_loop(0, 2, one, 0)

    def rs_right(t, hop, only):
        jr, first = line - hop, first_from(t)

        @pl.when(jnp.logical_and(only, jnp.logical_and(hop >= z + 1, z >= first)))
        def _():
            def step(p):
                rs_take(t, p, jr, jr)
                rs_copy(t, p, jr, jr - 1, right).start()

            halves(t, step)

    def rs_left(t, hop, only):
        jl, first = hop, first_from(t)

        @pl.when(jnp.logical_and(only, jnp.logical_and(hop >= line - z, z <= line - 1 - first)))
        def _():
            def step(p):
                rs_take(t, p, jl, jl)
                rs_copy(t, p, jl, jl + 1, left).start()

            halves(t, step)

    def rs_cross(t, hop):
        rs_right(t, hop, near)
        rs_left(t, hop, jnp.logical_not(near))

    def rs_home(t, hop):
        rs_right(t, hop, jnp.logical_not(near))
        rs_left(t, hop, near)

    def rs_rest(t, hop):
        def one(i, _):
            rs_cross(t, i)
            rs_home(t, i)
            return 0

        if hop < line:
            lax.fori_loop(hop, line, one, 0)

    def rs_finish_half(t, k):
        first = first_from(t)
        c, dst = fin_parts(t)
        p = k if t == DOWN else (1 - y if k == 0 else y)

        @pl.when(z >= first)
        def _():
            rs_take(t, p, 0, 0)

        @pl.when(z <= line - 1 - first)
        def _():
            rs_take(t, p, 0, line)

        if k == (1 if t == DOWN else 0):
            y_copy(Y_FIN, t).start()
        if k == 1:
            lcopy(c.at[0, y], dst, local.at[4 + t]).start()

    def rs_finish(t):
        rs_finish_half(t, 0)
        rs_finish_half(t, 1)

    def rs_drain(t):
        sends = jnp.logical_and(z >= first_from(t) - 1, z <= line - first_from(t))

        def one(j, _):
            for p in range(2):

                @pl.when(jnp.logical_and(sends, j <= line - 1 - z))
                def _():
                    rs_copy(t, p, j, j - 1, right).wait_send()

                @pl.when(jnp.logical_and(sends, j > line - 1 - z))
                def _():
                    rs_copy(t, p, j, j + 1, left).wait_send()

            return 0

        lax.fori_loop(1, line, one, 0)
        c, dst = fin_parts(t)
        y_copy(Y_FIN, t).wait()
        lcopy(c.at[0, y], dst, local.at[4 + t]).wait()

    last = len(far_steps) + 1

    def tp_copy(i, k):
        part = tp_part.at[i]
        if k == 0:
            src, dst, device = part.at[1 - core], tp_recv.at[i, 0], sibling
        elif k < last:
            src, dst, device = part.at[core], tp_recv.at[i, k], far_steps[k - 1]
        else:
            src, dst, device = part.at[core], tp_far.at[i], sibling
        return rcopy(src, dst, tp_s.at[i, k], tp_r.at[i, k], device)

    def tp_add(i, k):
        part = 64

        def add(n, _):
            at = pl.ds(pl.multiple_of(n * part, part), part)
            tp_part[i, core, at, :] = (
                tp_part[i, core, at, :].astype(F32) + tp_recv[i, k, at, :].astype(F32)
            ).astype(BF16)
            return 0

        lax.fori_loop(0, blk // part, add, 0)

    def tp_next(i, k):
        if k > 1:
            tp_copy(i, k - 1).wait_send()
        tp_copy(i, k - 1).wait_recv()
        tp_add(i, k - 1)
        tp_copy(i, k).start()

    def tp_done(i):
        tp_copy(i, last).wait_recv()
        tp_copy(i, 0).wait_send()

        other = lcopy(tp_far.at[i], tp_part.at[i, 1 - core], local.at[8])
        other.start()
        other.wait()

    def tp_drain(i):
        tp_copy(i, last).wait_send()

    def stream(lo, hi, fetches, body):
        for f in fetches:
            f(lo, lax.rem(lo, 2)).start()

        def one(i, _):
            slot = lax.rem(i, 2)

            @pl.when(i + 1 < hi)
            def _():
                for f in fetches:
                    f(i + 1, 1 - slot).start()

            for f in fetches:
                f(i, slot).wait()
            body(i, slot)
            return 0

        lax.fori_loop(lo, hi, one, 0)

    def col_tile(w):
        def fetch(i, slot):
            at = pl.ds(pl.multiple_of(i * TILE, TILE), TILE)
            return lcopy(w.at[:, at], wcol.at[slot, pl.ds(0, w.shape[0]), :], wsem.at[0, slot])

        return fetch

    def row_tile(w):
        def fetch(i, slot):
            at = pl.ds(pl.multiple_of(i * TILE, TILE), TILE)
            return lcopy(w.at[at, :], wrow.at[slot, pl.ds(0, TILE), pl.ds(0, w.shape[1])], wsem.at[1, slot])

        return fetch

    x_load = lcopy(stream_in, xbuf, local.at[0])
    c_load = lcopy(cotangent, cbuf, local.at[1])
    c_load.start()
    x_load.start()

    def number(place, side, k):
        return order[4 * place + 2 * side + k]

    late = [number(z, s, 0) > number(z, s, 1) for s in (y, 1 - y)]

    def block_number(lh, place, side):
        first, second = number(place, side, 0), number(place, side, 1)
        return jnp.minimum(first, second) if lh == 0 else jnp.maximum(first, second)

    for lh in range(2):
        for h in range(2):
            at_block = block_table[:, pl.ds(block_number(lh, z, (y, 1 - y)[h]), 1), :]
            cb, sb = at_block[0], at_block[1]
            ci, si = row_table[0], row_table[1]
            cosine[lh, h] = cb * ci - sb * si
            sine[lh, h] = sb * ci + cb * si

    def by_order(h, first, second):
        return jnp.where(late[h], second, first), jnp.where(late[h], first, second)

    small[...] = jnp.zeros(small.shape, F32)
    model = 2 * half
    chunk_rows = 64
    c_load.wait()

    def cast(i, _):
        at = pl.ds(pl.multiple_of(i * chunk_rows, chunk_rows), chunk_rows)
        c = cbuf[at, :]
        small[S_OUT : S_OUT + 1, :model] += jnp.sum(c, axis=0, keepdims=True)
        c = c.astype(BF16)
        cot[0, at, :] = c[:, :half]
        cot[1, at, :] = c[:, half:]
        return 0

    lax.fori_loop(0, rows // chunk_rows, cast, 0)
    pl.semaphore_wait(barrier, len(greet))
    y_copy(Y_COT).start()
    end_send(E_COT)

    x_load.wait()

    def unit_of(at):
        x = xbuf[at, :]
        centred = x - jnp.mean(x, axis=-1, keepdims=True)
        variance = jnp.mean(centred * centred, axis=-1, keepdims=True)
        inv_scale = lax.rsqrt(variance + norm_epsilon)
        return centred * inv_scale, inv_scale

    def norms(i, _):
        at = pl.ds(pl.multiple_of(i * chunk_rows, chunk_rows), chunk_rows)
        unit, _ = unit_of(at)
        for n, ref in ((0, attn), (1, norm)):
            value = (unit * gain[n : n + 1, :] + shift[n : n + 1, :]).astype(BF16)
            ref[0, at, :] = value[:, :half]
            ref[1, at, :] = value[:, half:]
        return 0

    lax.fori_loop(0, rows // chunk_rows, norms, 0)

    def tile_at(i):
        return pl.ds(pl.multiple_of(i * TILE, TILE), TILE)

    def hidden_at(i):
        at = pl.ds(pl.multiple_of(lax.rem(i * TILE, hidden_half), TILE), TILE)
        return i * TILE // hidden_half, at

    def activate(i, slot):
        h = nn(norm[0], wcol[slot, :half, :]) + nn(norm[1], wcol[slot, half : 2 * half, :])
        h = h + b_up[:, tile_at(i)]
        gate = 0.5 * (1.0 + lax.erf(h * root_half))
        which, at = hidden_at(i)
        act[which, :, at] = (h * gate).astype(BF16)
        slope = gate + h * jnp.exp(-0.5 * h * h) * inverse_root_two_pi
        hid[which, :, at] = slope.astype(BF16)

    def hidden_back(i, slot):
        g = nt(cot[0], wrow[slot, :TILE, :half]) + nt(cot[1], wrow[slot, :TILE, half : 2 * half])
        which, at = hidden_at(i)
        g = g * hid[which, :, at].astype(F32)
        small[S_UP : S_UP + 1, tile_at(i)] = jnp.sum(g, axis=0, keepdims=True)
        hid[which, :, at] = g.astype(BF16)

    hidden_tiles = 2 * hidden_half // TILE
    def project(at, slot, place):
        value = nn(attn[0], wcol[slot, :half, :]) + nn(attn[1], wcol[slot, half : 2 * half, :])
        value = value + b_qkv[at][None, :]
        pieces = by_order(0, value[:blk], value[blk:])
        for lh in range(2):
            first, rest = pieces[lh][:, :LANES], pieces[lh][:, LANES:]
            place(lh, first, rest)

    def put(refs, which, lh, at, value):
        mine, away = refs

        @pl.when(which == 0)
        def _():
            mine[lh, 0, :, at] = value

        @pl.when(which == 1)
        def _():
            away[lh, :, at] = value

    def kv_index(i):
        which = 1 - i // (2 * own_heads)
        k, kind = lax.rem(i, 2 * own_heads) // 2, 1 + lax.rem(i, 2)
        head = jnp.where(which == 0, y, 1 - y) * own_heads + k
        return which, k, kind, 3 * head + kind

    def q_index(i):
        which = 1 - i // own_heads
        k = lax.rem(i, own_heads)
        head = jnp.where(which == 0, y, 1 - y) * own_heads + k
        return which, k, 3 * head, head

    def fetch_by(w, index):
        def fetch(i, slot):
            return lcopy(w.at[:, tile_at(index(i))], wcol.at[slot, pl.ds(0, w.shape[0]), :], wsem.at[0, slot])

        return fetch

    def lanes_at(start, n):
        return pl.ds(pl.multiple_of(start, LANES), n)

    def keys_values(i, slot):
        which, k, kind, tile = kv_index(i)
        base = jnp.where(kind == 1, 0, width) + k * HD

        def place(lh, first, rest):
            turned = turn(first, cosine[lh, 0], sine[lh, 0], 1)
            first = jnp.where(kind == 1, turned, first).astype(BF16)
            put((kv_own, kv_away), which, lh, lanes_at(base, LANES), first)
            put((kv_own, kv_away), which, lh, lanes_at(base + LANES, HD - LANES), rest.astype(BF16))

        project(tile_at(tile), slot, place)

    w_out_fetch = lcopy(w_out, wrow.at[0, pl.ds(0, w_out.shape[0]), pl.ds(0, model)], wsem.at[1, 0])

    def queries(i, slot):
        which, k, tile, head = q_index(i)

        def place(lh, first, rest):
            turned = turn(first, cosine[lh, 0], sine[lh, 0], 1).astype(BF16)
            put((qg_own, qg_away), which, lh, lanes_at(k * HD, LANES), turned)
            put((qg_own, qg_away), which, lh, lanes_at(k * HD + LANES, HD - LANES), rest.astype(BF16))

        project(tile_at(tile), slot, place)
        at = pl.ds(pl.multiple_of(head * HD, HD), HD)
        g = nt(cot[0], wrow[0, at, :half]) + nt(cot[1], wrow[0, at, half : 2 * half])
        pieces = by_order(0, g[:blk], g[blk:])
        for lh in range(2):
            put((qg_own, qg_away), which, lh, lanes_at(width + k * HD, HD), pieces[lh].astype(BF16))

    own_places = [
        lcopy(own.at[:, h], everyone.at[:, h], local.at[2 + 2 * t + h])
        for t, (own, everyone) in enumerate(((kv_own, kv_all), (qg_own, qg_all)))
        for h in range(2)
    ]

    def cols_at(ref, j):
        start = lax.rem(z + j, line) * block_cols
        at = pl.ds(pl.multiple_of(lax.rem(start, half), LANES), block_cols)
        return ref[start // half, :, at]

    def split_cols(ref, j, at, value):
        n = value.shape[1] // 2
        ref[j, 0, at, :] = value[:, :n].astype(BF16)
        ref[j, 1, at, :] = value[:, n:].astype(BF16)

    def split_rows(ref, j, at, value):
        n = value.shape[0] // 2
        ref[j, 0, :, at] = value[:n].astype(BF16)
        ref[j, 1, :, at] = value[n:].astype(BF16)

    def in_order(share, first=0, end=line):
        def one(k, _):
            j = jnp.where(lax.rem(k, 2) == 0, line - 1 - k // 2, k // 2 + 1)
            share(jnp.where(k == line - 1, 0, j))
            return 0

        lax.fori_loop(first, end, one, 0)

    def mlp_back(i, slot):
        value = nt(hid[0], wrow[slot, :TILE, :hidden_half]) + nt(
            hid[1], wrow[slot, :TILE, hidden_half : 2 * hidden_half]
        )
        tp_part[MLPB, :, :, tile_at(i)] = value.astype(BF16).reshape(2, blk, TILE)

    model_tiles = model // TILE

    def share_down(j):
        g0, g1 = cols_at(cot, j), cols_at(cot_far, j)

        def one(i, _):
            split_cols(
                c_down, j, tile_at(i), tn(act[y, :, tile_at(i)], g0) + tn(act_far[:, tile_at(i)], g1)
            )
            return 0

        lax.fori_loop(0, hidden_half // TILE, one, 0)

    def share_up(j):
        m0, m1 = cols_at(norm, j), cols_at(norm_far, j)

        def one(i, _):
            split_rows(c_up, j, tile_at(i), tn(m0, hid[y, :, tile_at(i)]) + tn(m1, hid_far[:, tile_at(i)]))
            return 0

        lax.fori_loop(0, hidden_half // TILE, one, 0)

    def end_tile(k):
        def fetch(i, slot):
            return lcopy(
                act_end.at[pl.ds(k * rows, rows), tile_at(i)], wcol.at[slot, pl.ds(0, rows), :], wsem.at[0, slot]
            )

        return fetch

    def add_end_tokens(k, item, tiles):
        @pl.when(next_to_end)
        def _():
            if item != E_ACT_LAST:
                end_share(k).wait_recv()
            held = lcopy(
                cot_end.at[pl.ds(k * rows, rows), :],
                wrow.at[k, pl.ds(0, rows), pl.ds(0, model)],
                wsem.at[1, k],
            )
            held.start()
            end_copy(item, partner).wait_recv()
            held.wait()

            def add_tile(i, slot):
                at = tile_at(i)

                def add_block(n, _):
                    j = jnp.where(z == 1, n, lax.rem(n + 2, line))
                    start = pl.multiple_of(lax.rem(z + j, line) * block_cols, LANES)
                    value = tn(wcol[slot, :rows, :], wrow[k, :rows, pl.ds(start, block_cols)])
                    n = block_cols // 2
                    for p in range(2):
                        c_down[j, p, at, :] = (
                            c_down[j, p, at, :].astype(F32) + value[:, p * n : (p + 1) * n]
                        ).astype(BF16)
                    return 0

                lax.fori_loop(0, line - 1, add_block, 0)

            stream(*tiles, (end_tile(k),), add_tile)

    pair = 2 * blk
    same = lax.broadcasted_iota(jnp.int32, (pair, pair), 0) == lax.broadcasted_iota(
        jnp.int32, (pair, pair), 1
    )

    def positions(lh, place, along):
        shape = (1, pair) if along else (pair, 1)
        at = lax.broadcasted_iota(jnp.int32, shape, along)
        here, there = block_number(lh, place, y), block_number(lh, place, 1 - y)
        return at + jnp.where(at < blk, here * blk, there * blk - blk)

    def piece_positions(lh_start, i, along):
        place = lax.rem(z + i, line)
        early, late_ = positions(0, place, along), positions(1, place, along)
        return jnp.where(i < line, early, late_)

    def piece(t):
        def fetch(i, slot):
            ref = (kv_all, qg_all)[t]
            return lcopy(
                ref.at[i // line, pl.ds(2 * lax.rem(i, line), 2)], chunk.at[slot], csem.at[slot]
            )

        return fetch

    def store_order(ref):
        for h in range(2):
            first, second = by_order(h, ref[0, h], ref[1, h])
            ref[0, h] = first
            ref[1, h] = second

    def attend_forward():
        for lh in range(2):
            for head in range(own_heads):
                at_k, at_v = head * HD, width + head * HD
                run_m[...] = jnp.full(run_m.shape, masked_value, F32)
                run_l[...] = jnp.zeros(run_l.shape, F32)
                acc_a[...] = jnp.zeros(acc_a.shape, F32)

                def attend(i, slot):
                    k = chunk[slot, :, :, at_k : at_k + HD].reshape(pair, HD)
                    v = chunk[slot, :, :, at_v : at_v + HD].reshape(pair, HD)
                    q = qg_own[lh, :, :, at_k : at_k + HD].reshape(pair, HD)
                    s = nt(q, k) * scale
                    seen = piece_positions(lh, i, 1) <= positions(lh, z, 0)
                    s = jnp.where(seen, s, masked_value)
                    old = run_m[...]
                    top = jnp.maximum(old, jnp.max(s, axis=1, keepdims=True))
                    p = jnp.exp(s - top)
                    fade = jnp.exp(old - top)
                    run_m[...] = top
                    run_l[...] = run_l[...] * fade + jnp.sum(p, axis=1, keepdims=True)
                    acc_a[...] = acc_a[...] * fade + nn(p.astype(BF16), v)

                stream(0, line * (lh + 1), (piece(0),), attend)
                out = (acc_a[...] / run_l[...]).astype(BF16)
                att[lh, :, :, at_k : at_k + HD] = out.reshape(2, blk, HD)
                log_total = run_m[...] + jnp.log(run_l[...])
                g = qg_own[lh, :, :, at_v : at_v + HD].reshape(pair, HD)
                dots = jnp.sum(g.astype(F32) * out.astype(F32), axis=1, keepdims=True)
                stats[lh, head, 0:1, :] = jnp.sum(jnp.where(same, log_total, 0.0), 0, keepdims=True)
                stats[lh, head, 1:2, :] = jnp.sum(jnp.where(same, dots, 0.0), 0, keepdims=True)

    def stat_copy(j):
        return rcopy(
            stats, stats_all.at[line - j], st_s.at[j], st_r.at[line - j], (place_of(j), tp)
        )

    def share_out(j):
        g0, g1 = cols_at(cot, j), cols_at(cot_far, j)

        def one(i, _):
            a0 = att[:, 0, :, tile_at(i)].reshape(rows, TILE)
            a1 = att[:, 1, :, tile_at(i)].reshape(rows, TILE)
            split_cols(c_out, j, tile_at(i), tn(a0, g0) + tn(a1, g1))
            return 0

        lax.fori_loop(0, width // TILE, one, 0)

    def undo(value, lh, head, kind):
        at = (3 * head + kind) * HD
        first = value[:, :LANES]
        if kind < 2:
            first = turn(
                first, cosine[lh].reshape(pair, LANES), sine[lh].reshape(pair, LANES), -1
            )
        for lo, hi, part in ((0, LANES, first), (LANES, HD, value[:, LANES:])):
            spot = lanes_at(y * 3 * width + at + lo, hi - lo)
            small[S_QKV : S_QKV + 1, spot] += jnp.sum(part, axis=0, keepdims=True)
            gqkv[lh, :, :, at + lo : at + hi] = part.astype(BF16).reshape(2, blk, hi - lo)

    def attend_back_queries():
        for lh in range(2):
            for head in range(own_heads):
                at_k, at_v = head * HD, width + head * HD
                run_m[...] = jnp.sum(
                    jnp.where(same, stats[lh, head, 0:1, :], 0.0), axis=1, keepdims=True
                )
                run_l[...] = jnp.sum(
                    jnp.where(same, stats[lh, head, 1:2, :], 0.0), axis=1, keepdims=True
                )
                acc_a[...] = jnp.zeros(acc_a.shape, F32)

                def back_q(i, slot):
                    k = chunk[slot, :, :, at_k : at_k + HD].reshape(pair, HD)
                    v = chunk[slot, :, :, at_v : at_v + HD].reshape(pair, HD)
                    q = qg_own[lh, :, :, at_k : at_k + HD].reshape(pair, HD)
                    g = qg_own[lh, :, :, at_v : at_v + HD].reshape(pair, HD)
                    s = nt(q, k) * scale
                    seen = piece_positions(lh, i, 1) <= positions(lh, z, 0)
                    s = jnp.where(seen, s, masked_value)
                    p = jnp.exp(s - run_m[...])
                    ds = (p * (nt(g, v) - run_l[...]) * scale).astype(BF16)
                    acc_a[...] += nn(ds, k)

                stream(0, line * (lh + 1), (piece(0),), back_q)
                undo(acc_a[...], lh, head, 0)

    def branch(i, slot):
        value = nn(act[0], wcol[slot, :hidden_half, :]) + nn(
            act[1], wcol[slot, hidden_half : 2 * hidden_half, :]
        )
        own = att[:, 0].reshape(rows, width)
        far = att_far[...].reshape(rows, width)
        mine = wrow[0, pl.ds(pl.multiple_of(y * width, width), width), tile_at(i)]
        theirs = wrow[0, pl.ds(pl.multiple_of((1 - y) * width, width), width), tile_at(i)]
        value += nn(own, mine) + nn(far, theirs)
        tp_part[BRANCH, :, :, tile_at(i)] = value.astype(BF16).reshape(2, blk, TILE)

    def attend_back_keys():
        for lh in range(2):
            for head in range(own_heads):
                at_k, at_v = head * HD, width + head * HD
                acc_a[...] = jnp.zeros(acc_a.shape, F32)
                acc_b[...] = jnp.zeros(acc_b.shape, F32)

                def back_k(i, slot):
                    q = chunk[slot, :, :, at_k : at_k + HD].reshape(pair, HD)
                    g = chunk[slot, :, :, at_v : at_v + HD].reshape(pair, HD)
                    k = kv_own[lh, :, :, at_k : at_k + HD].reshape(pair, HD)
                    v = kv_own[lh, :, :, at_v : at_v + HD].reshape(pair, HD)
                    stat = stats_all[lax.rem(i, line), i // line, head]
                    s = nt(k, q) * scale
                    seen = positions(lh, z, 0) <= piece_positions(lh, i, 1)
                    s = jnp.where(seen, s, masked_value)
                    p = jnp.exp(s - stat[0:1, :])
                    ds = (p * (nt(v, g) - stat[1:2, :]) * scale).astype(BF16)
                    acc_a[...] += nn(ds, q)
                    acc_b[...] += nn(p.astype(BF16), g)

                stream(lh * line, 2 * line, (piece(1),), back_k)
                undo(acc_a[...], lh, head, 1)
                undo(acc_b[...], lh, head, 2)

    def share_qkv(j):
        m0, m1 = cols_at(attn, j), cols_at(norm_far, j)

        def one(i, _):
            g0 = gqkv[:, 0, :, tile_at(i)].reshape(rows, TILE)
            g1 = gqkv[:, 1, :, tile_at(i)].reshape(rows, TILE)
            split_rows(c_qkv, j, tile_at(i), tn(m0, g0) + tn(m1, g1))
            return 0

        lax.fori_loop(0, 3 * width // TILE, one, 0)

    def attn_back(i, slot):
        own = gqkv[:, 0].reshape(rows, 3 * width)
        far = gqkv_far[...].reshape(rows, 3 * width)
        mine = wrow[slot, :TILE, pl.ds(pl.multiple_of(y * 3 * width, LANES), 3 * width)]
        theirs = wrow[slot, :TILE, pl.ds(pl.multiple_of((1 - y) * 3 * width, LANES), 3 * width)]
        value = nt(own, mine) + nt(far, theirs)
        tp_part[ATTNB, :, :, tile_at(i)] = value.astype(BF16).reshape(2, blk, TILE)

    def back_norms(i, _):
        at = pl.ds(pl.multiple_of(i * chunk_rows, chunk_rows), chunk_rows)
        at_part = pl.ds(pl.multiple_of(lax.rem(i * chunk_rows, blk), chunk_rows), chunk_rows)
        which = i * chunk_rows // blk
        unit, inv_scale = unit_of(at)
        total = jnp.zeros((chunk_rows, model), F32)
        for n, part in ((0, ATTNB), (1, MLPB)):
            value = tp_part[part, which, at_part, :].astype(F32)
            small[S_GAIN + n : S_GAIN + n + 1, :model] += jnp.sum(value * unit, 0, keepdims=True)
            small[S_SHIFT + n : S_SHIFT + n + 1, :model] += jnp.sum(value, 0, keepdims=True)
            total = total + value * gain[n : n + 1, :]
        cbuf[at, :] = cbuf[at, :] + inv_scale * (
            total
            - jnp.mean(total, axis=-1, keepdims=True)
            - unit * jnp.mean(total * unit, axis=-1, keepdims=True)
        )
        return 0

    def small_copy(j):
        return rcopy(
            small_sent, small_recv.at[line - j], sm_s.at[j], sm_r.at[line - j], (place_of(j), tp)
        )

    def stream_rows(i, _):
        at = pl.ds(pl.multiple_of(i * chunk_rows, chunk_rows), chunk_rows)
        at_part = pl.ds(pl.multiple_of(lax.rem(i * chunk_rows, blk), chunk_rows), chunk_rows)
        which = i * chunk_rows // blk
        xbuf[at, :] = xbuf[at, :] + out_bias[...] + tp_part[BRANCH, which, at_part, :].astype(F32)
        return 0

    stream(0, 4 * own_heads, (fetch_by(w_qkv, lambda i: kv_index(i)[3]),), keys_values)
    y_copy(Y_KV).start()
    ag_hop(0, 0, 1)
    own_places[0].start()
    w_out_fetch.start()
    w_out_fetch.wait()
    stream(0, 2 * own_heads, (fetch_by(w_qkv, lambda i: q_index(i)[2]),), queries)
    y_copy(Y_QG).start()
    ag_hop(1, 0, 1)
    own_places[2].start()
    pass_x(Y_COT, 0)

    stream(0, hidden_tiles // 2, (col_tile(w_up),), activate)
    y_copy(Y_KV).wait_recv()
    ag_hop(0, 1, 1)
    own_places[1].start()
    stream(hidden_tiles // 2, hidden_tiles, (col_tile(w_up),), activate)
    y_copy(Y_ACT).start()
    y_copy(Y_MLP).start()
    end_send(E_ACT)
    pass_on(Y_COT, 0)
    ag_hop(0, 0, 2)
    end_pass_x(0)
    stream(0, hidden_tiles // 2, (row_tile(w_down),), hidden_back)
    y_copy(Y_QG).wait_recv()
    own_places[3].start()
    ag_hop(1, 1, 1)
    ag_hop(1, 0, 2)
    stream(hidden_tiles // 2, hidden_tiles, (row_tile(w_down),), hidden_back)
    y_copy(Y_HID).start()
    y_copy(Y_ATTN).start()
    end_pass(0)
    stream(0, model_tiles, (row_tile(w_up),), mlp_back)
    tp_copy(MLPB, 0).start()
    ag_hop(0, 0, 3)
    ag_hop(0, 1, 2)
    core_copy(0).wait_recv()
    y_copy(Y_ACT).wait_recv()
    end_send(E_ACT_FAR)
    end_send(E_ACT_LAST)
    in_order(share_down)
    pass_x(Y_MLP, 1)
    end_pass_x(1)
    ag_hop(0, 1, 3)
    end_tiles = hidden_half // TILE
    add_end_tokens(0, E_ACT, (0, end_tiles))
    pass_on(Y_MLP, 1)
    end_pass(1)
    ag_hop(1, 0, 3)
    ag_hop(1, 1, 2)
    add_end_tokens(1, E_ACT_FAR, (0, end_tiles // 2))
    rs_ends(DOWN, (1, 3), (0,))
    add_end_tokens(1, E_ACT_LAST, (end_tiles // 2, end_tiles))
    rs_ends(DOWN, (1, 3), (1,))
    tp_next(MLPB, 1)
    y_copy(Y_HID).wait_recv()
    core_copy(1).wait_recv()
    in_order(share_up)
    rs_ends(UP, (1, 2))
    ag_hop(1, 1, 3)
    ag_rest(0, 0, 4)
    ag_rest(0, 1, 4)
    for copy in own_places:
        copy.wait()

    attend_forward()
    store_order(att)
    for j in range(1, line):
        stat_copy(j).start()
    y_copy(Y_ATT).start()
    rs_ends(UP, (2, line))
    rs_ends(DOWN, (3, line))
    in_order(share_out)
    small[S_QKV : S_QKV + 1, :] = jnp.zeros((1, small.shape[1]), F32)
    attend_back_queries()
    tp_next(MLPB, 2)
    pass_x(Y_ATTN, 2)
    for hop in range(1, min(line, 4)):
        rs_cross(DOWN, hop)
        rs_home(DOWN, hop)
    rs_cross(UP, 1)
    rs_cross(UP, 2)
    y_copy(Y_ATT).wait_recv()
    w_out_fetch.start()
    w_out_fetch.wait()
    stream(0, model_tiles, (col_tile(w_down),), branch)
    tp_copy(BRANCH, 0).start()
    ag_rest(1, 0, 4)
    ag_rest(1, 1, 4)
    for j in range(1, line):
        stat_copy(line - j).wait_recv()
    own_stats = lcopy(stats, stats_all.at[0], local.at[0])
    own_stats.start()
    own_stats.wait()
    rs_cross(UP, 3) if line > 3 else None
    attend_back_keys()
    store_order(gqkv)
    y_copy(Y_GQKV).start()
    tp_next(BRANCH, 1)
    pass_on(Y_ATTN, 2)
    core_copy(2).wait_recv()
    core_copy(1).wait_send()
    x_drain(1)
    far_again = lcopy(attn_far, norm_far, local.at[1])
    far_again.start()
    far_again.wait()
    in_order(share_qkv)
    rs_ends(QKV, (1, line))
    rs_ends(OUT, (1, line))
    rs_home(UP, 1)
    rs_home(UP, 2)
    rs_home(UP, 3) if line > 3 else None
    y_copy(Y_GQKV).wait_recv()
    stream(0, model_tiles, (row_tile(w_qkv),), attn_back)
    tp_copy(ATTNB, 0).start()
    tp_next(BRANCH, 2)
    tp_next(ATTNB, 1)

    rs_cross(QKV, 1)
    rs_cross(QKV, 2)
    rs_rest(DOWN, 4 if line > 3 else 3)
    rs_finish(DOWN)
    tp_done(BRANCH)
    tp_done(MLPB)
    rs_cross(QKV, 3) if line > 3 else None
    rs_rest(UP, 4 if line > 3 else 3)
    rs_finish(UP)
    rs_home(QKV, 1)
    rs_home(QKV, 2)
    rs_home(QKV, 3) if line > 3 else None
    rs_rest(QKV, 4 if line > 3 else 3)
    tp_next(ATTNB, 2)
    tp_done(ATTNB)
    lax.fori_loop(0, rows // chunk_rows, back_norms, 0)
    grad_store = lcopy(cbuf, grad_o, local.at[1])
    grad_store.start()
    pair_copy = rcopy(small, small_pair, sm_s.at[0], sm_r.at[0], partner)
    pair_copy.start()
    pair_copy.wait()
    small_sent[...] = (small[...] + small_pair[...]).astype(BF16)
    for j in range(1, line):
        small_copy(j).start()
    lax.fori_loop(0, rows // chunk_rows, stream_rows, 0)
    stream_store = lcopy(xbuf, stream_o, local.at[0])
    stream_store.start()
    rs_cross(OUT, 1)
    rs_cross(OUT, 2)
    rs_cross(OUT, 3) if line > 3 else None
    rs_finish_half(QKV, 0)
    for hop in range(1, min(line, 4)):
        rs_home(OUT, hop)
    rs_rest(OUT, 4 if line > 3 else 3)
    rs_finish_half(QKV, 1)
    rs_finish(OUT)
    for j in range(1, line):
        small_copy(line - j).wait_recv()
    small_recv[0] = small_sent[...]
    small[...] = small_recv[lax.rem(line - z, line)].astype(F32)
    for p in range(1, line):
        small[...] += small_recv[lax.rem(p + line - z, line)].astype(F32)
    small_store = lcopy(small, small_o, local.at[2])
    small_store.start()

    for t in range(2):
        for h in range(2):
            ag_drain(t, h)
    for item in (Y_KV, Y_QG, Y_COT, Y_MLP, Y_ATTN, Y_ACT, Y_HID, Y_ATT, Y_GQKV):
        y_copy(item).wait_send()
    core_copy(0).wait_send()
    core_copy(2).wait_send()
    x_drain(0)
    x_drain(2)
    for j in range(1, line):
        stat_copy(j).wait_send()
        small_copy(j).wait_send()
    for i in range(3):
        tp_drain(i)
    grad_store.wait()
    small_store.wait()
    stream_store.wait()
    for t in range(4):
        rs_drain(t)
    end_drain()


def layer(line, n_tp, order, stream_in, cotangent, ln_gain, ln_bias, w_qkv, b_qkv, w_out, out_bias, w_up, b_up, w_down):
    rows, model = stream_in.shape
    half, blk = model // 2, rows // 2
    hidden = w_up.shape[1]
    hidden_half = hidden // 2
    width = w_out.shape[0] // 2
    own_heads = width // HD
    part_cols = model // line // 2
    pair = 2 * blk
    tp_steps = 0
    while (2 << tp_steps) < n_tp:
        tp_steps += 1
    small_shape = (8, max(model, hidden, 6 * width))
    shares = (
        (2, hidden_half, part_cols),
        (2, part_cols, hidden_half),
        (2, width, part_cols),
        (2, part_cols, 3 * width),
    )
    b = lambda *s: jax.ShapeDtypeStruct(s, BF16)
    f = lambda *s: jax.ShapeDtypeStruct(s, F32)
    vb = lambda *s: pltpu.VMEM(s, BF16)
    vf = lambda *s: pltpu.VMEM(s, F32)
    dma = pltpu.SemaphoreType.DMA
    outs = (
        b(hidden, part_cols),
        b(part_cols, hidden),
        b(2 * width, part_cols),
        b(part_cols, 6 * width),
        f(rows, model),
        f(rows, model),
        f(*small_shape),
        b(2, 2 * line, blk, 2 * width),
        b(2, 2 * line, blk, 2 * width),
        b(line + 1, *shares[0]),
        b(line + 1, *shares[1]),
        b(line + 1, *shares[2]),
        b(line + 1, *shares[3]),
        b(2, rows, half),
        b(3, blk, model),
        b(2 * rows, model),
        b(2 * rows, hidden_half),
    )
    wide = max(model, hidden)
    scratch = (
        [vf(rows, model)] * 2
        + [vb(2, rows, half)] * 5
        + [vb(2, rows, hidden_half)] * 2
        + [vb(rows, hidden_half)] * 2
        + [vb(2, wide, TILE), vb(2, max(TILE, 2 * width), wide)]
        + [vb(line, *s) for s in shares]
        + [vb(*s) for s in shares]
        + [vb(3, 2, blk, model), vb(3, tp_steps + 1, blk, model)]
        + [vb(2, 2, blk, 2 * width)] * 2
        + [vb(2, blk, 2 * width)] * 2
        + [
            vb(2, 2, blk, 2 * width),
            vb(2, 2, blk, width),
            vb(2, blk, width),
            vf(2, own_heads, 2, pair),
            vf(line, 2, own_heads, 2, pair),
            vb(2, 2, blk, 3 * width),
            vb(2, blk, 3 * width),
            vf(pair, HD),
            vf(pair, HD),
            vf(pair, 1),
            vf(pair, 1),
            vf(2, 2, blk, LANES),
            vf(2, 2, blk, LANES),
            vf(*small_shape),
            vf(*small_shape),
            vb(*small_shape),
            vb(line, *small_shape),
            dma((2, 2, 2, line)),
            dma((2, 2, line)),
            dma((Y_FIN + 4,)),
            dma((Y_FIN + 4,)),
            dma((3,)),
            dma((3,)),
            dma((3, n_tp // 2)),
            dma((3, n_tp // 2)),
            dma((4, 2, line)),
            dma((4, 2, line + 1)),
            dma((3, tp_steps + 2)),
            dma((3, tp_steps + 2)),
            dma((line,)),
            dma((line,)),
            dma((line,)),
            dma((line,)),
            dma((7,)),
            dma((7,)),
            dma((2, n_tp // 2)),
            dma((2, n_tp // 2)),
            dma((9,)),
            dma((2, 2)),
            dma((2,)),
            dma((4,)),
        ]
    )
    blocks = order.shape[0]
    operands = (
        order,
        stream_in,
        cotangent,
        w_up,
        w_down,
        w_out,
        w_qkv,
        ln_gain,
        ln_bias,
        b_qkv,
        b_up.reshape(1, -1),
        out_bias.reshape(1, -1),
        jnp.asarray(rope_tables(np.arange(blocks) * blk)),
        jnp.asarray(rope_tables(np.arange(blk))),
    )
    return pl.pallas_call(
        functools.partial(layer_kernel, line, n_tp),
        name="layer",
        out_shape=outs,
        in_specs=[SMEM] + [ANY] * 6 + [VMEM] * 7,
        out_specs=[ANY] * len(outs),
        scratch_shapes=scratch,
        cost_estimate=pl.CostEstimate(
            flops=40 * rows * model * hidden,
            transcendentals=rows * hidden,
            bytes_accessed=8 * w_up.size,
        ),
        compiler_params=pltpu.CompilerParams(
            collective_id=0, has_side_effects=True, vmem_limit_bytes=67043328
        ),
    )(*operands)


def results_kernel(
    down,
    up,
    out,
    qkv,
    stream,
    grad,
    small,
    stream_o,
    grad_o,
    qkv_o,
    bqkv_o,
    out_o,
    obias_o,
    up_o,
    bup_o,
    down_o,
    gain_o,
    shift_o,
):
    stream_o[...] = stream[...]
    grad_o[...] = grad[...]
    for src, dst in ((qkv, qkv_o), (out, out_o), (up, up_o), (down, down_o)):
        dst[...] = src[...].astype(F32)

    @pl.when(pl.program_id(0) == 0)
    def _():
        bqkv_o[...] = small[S_QKV, : bqkv_o.shape[0]]
        obias_o[...] = small[S_OUT, : obias_o.shape[0]]
        bup_o[...] = small[S_UP, : bup_o.shape[0]]
        gain_o[...] = small[S_GAIN : S_GAIN + 2, : gain_o.shape[1]]
        shift_o[...] = small[S_SHIFT : S_SHIFT + 2, : shift_o.shape[1]]


def results(down, up, out, qkv, stream_out, grad_in, small, model, fused, hidden):
    steps = 2
    f = lambda *s: jax.ShapeDtypeStruct(s, F32)
    rows_of = lambda a: pl.BlockSpec((a.shape[0] // steps,) + a.shape[1:], lambda i: (i, 0))
    whole = lambda a: pl.BlockSpec(a.shape, lambda i: (0,) * len(a.shape))
    large = (down, up, out, qkv, stream_out, grad_in)
    while any(a.shape[0] % (16 * steps) for a in large[:4]):
        steps //= 2
    outs = (
        (f(*stream_out.shape), True),
        (f(*grad_in.shape), True),
        (f(*qkv.shape), True),
        (f(fused), False),
        (f(*out.shape), True),
        (f(model), False),
        (f(*up.shape), True),
        (f(hidden), False),
        (f(*down.shape), True),
        (f(2, model), False),
        (f(2, model), False),
    )
    return pl.pallas_call(
        results_kernel,
        name="results",
        grid=(steps,),
        out_shape=[o for o, _ in outs],
        in_specs=[rows_of(a) for a in large] + [whole(small)],
        out_specs=[rows_of(o) if tall else whole(o) for o, tall in outs],
        cost_estimate=pl.CostEstimate(
            flops=down.size, transcendentals=0, bytes_accessed=8 * down.size + 16 * stream_out.size
        ),
        compiler_params=pltpu.CompilerParams(vmem_limit_bytes=67043328),
    )(*large, small)


def shards(
    n_ctx,
    n_tp,
    stream_in,
    cotangent,
    ln_gain,
    ln_bias,
    w_qkv,
    b_qkv,
    w_out,
    out_bias,
    w_up,
    b_up,
    w_down,
    block_order,
):
    (down, up, out, qkv, stream_out, grad_in, small, *_) = layer(
        n_ctx // 2,
        n_tp,
        block_order,
        stream_in,
        cotangent,
        ln_gain,
        ln_bias,
        w_qkv,
        b_qkv,
        w_out,
        out_bias,
        w_up,
        b_up,
        w_down,
    )
    return results(down, up, out, qkv, stream_out, grad_in, small, *w_qkv.shape, w_up.shape[1])


def solution(mesh):
    placed = (
        P("ctx", None),
        P("ctx", None),
        P(),
        P(),
        P(None, "tp"),
        P("tp"),
        P("tp", None),
        P(),
        P(None, "tp"),
        P("tp"),
        P("tp", None),
        P(),
    )
    return jax.shard_map(
        functools.partial(shards, mesh.shape["ctx"], mesh.shape["tp"]),
        mesh=mesh,
        in_specs=placed,
        out_specs=(
            P("ctx", None),
            P("ctx", None),
            P("ctx", "tp"),
            P("tp"),
            P("tp", "ctx"),
            P(),
            P("ctx", "tp"),
            P("tp"),
            P("tp", "ctx"),
            P(),
            P(),
        ),
        check_vma=False,
    )
```

```python
import functools
import math

import jax
import jax.numpy as jnp
import numpy as np
from jax import lax
from jax.experimental import pallas as pl
from jax.experimental.pallas import tpu as pltpu
from jax.sharding import PartitionSpec as P

HD = 256
ROT = 64
LANES = 128
TILE = 256

masked_value = -1e30
norm_epsilon = 1e-05
root_half = 0.7071067811865476
inverse_root_two_pi = 0.3989422804014327

F32 = jnp.float32
BF16 = jnp.bfloat16
MESH = pl.DeviceIdType.MESH
ANY = pl.BlockSpec(memory_space=pl.ANY)
VMEM = pl.BlockSpec(memory_space=pltpu.VMEM)
SMEM = pl.BlockSpec(memory_space=pltpu.SMEM)


def nt(a, b):
    return lax.dot_general(a, b, (((1,), (1,)), ((), ())), preferred_element_type=F32)


def nn(a, b):
    return lax.dot_general(a, b, (((1,), (0,)), ((), ())), preferred_element_type=F32)


def tn(a, b):
    return lax.dot_general(a, b, (((0,), (0,)), ((), ())), preferred_element_type=F32)


def rope_tables(positions):
    half_rot = ROT // 2
    frequency = np.exp(np.arange(half_rot) * (-2.0 * math.log(10000.0) / ROT))
    angles = np.asarray(positions, np.float64)[:, None] * frequency
    table = np.zeros((2, angles.shape[0], LANES), np.float32)
    table[0] = 1.0
    for lo in (0, half_rot):
        table[0, :, lo : lo + half_rot] = np.cos(angles)
        table[1, :, lo : lo + half_rot] = np.sin(angles)
    return table


def turn(first, cosine, sine, sign):
    half_rot = ROT // 2
    scaled = first * sine if sign < 0 else first
    lane = lax.broadcasted_iota(jnp.int32, first.shape, 1)
    down = jnp.where(lane < half_rot, pltpu.roll(scaled, LANES - half_rot, 1), 0.0)
    up = jnp.where(
        jnp.logical_and(lane >= half_rot, lane < ROT), pltpu.roll(scaled, half_rot, 1), 0.0
    )
    if sign < 0:
        return first * cosine + (down - up)
    return first * cosine + (up - down) * sine


DOWN, UP, OUT, QKV = range(4)
(Y_KV, Y_QG, Y_COT, Y_MLP, Y_ATTN, Y_ACT, Y_HID, Y_ATT, Y_GQKV, Y_FIN) = range(10)
BRANCH, MLPB, ATTNB = range(3)
S_GAIN, S_SHIFT, S_OUT, S_UP, S_QKV = 0, 2, 4, 5, 6


def layer_kernel(
    line,
    n_tp,
    order,
    stream_in,
    cotangent,
    w_up,
    w_down,
    w_out,
    w_qkv,
    gain,
    shift,
    b_qkv,
    b_up,
    out_bias,
    block_table,
    row_table,
    down_o,
    up_o,
    out_o,
    qkv_o,
    stream_o,
    grad_o,
    small_o,
    kv_all,
    qg_all,
    rs_down,
    rs_up,
    rs_out,
    rs_qkv,
    attn_far,
    tp_far,
    cot_end,
    act_end,
    xbuf,
    cbuf,
    cot,
    cot_far,
    norm,
    norm_far,
    attn,
    act,
    hid,
    act_far,
    hid_far,
    wcol,
    wrow,
    c_down,
    c_up,
    c_out,
    c_qkv,
    stage_down,
    stage_up,
    stage_out,
    stage_qkv,
    tp_part,
    tp_recv,
    kv_own,
    qg_own,
    kv_away,
    qg_away,
    chunk,
    att,
    att_far,
    stats,
    stats_all,
    gqkv,
    gqkv_far,
    acc_a,
    acc_b,
    run_m,
    run_l,
    cosine,
    sine,
    small,
    small_pair,
    small_sent,
    small_recv,
    ag_s,
    ag_r,
    y_s,
    y_r,
    core_s,
    core_r,
    x_s,
    x_r,
    rs_s,
    rs_r,
    tp_s,
    tp_r,
    st_s,
    st_r,
    sm_s,
    sm_r,
    end_s,
    end_r,
    ex_s,
    ex_r,
    local,
    wsem,
    csem,
    tsem,
):
    me, tp = lax.axis_index("ctx"), lax.axis_index("tp")
    z, y = me // 2, lax.rem(me, 2)
    core = lax.rem(tp, 2)
    partner = (me + 1 - 2 * y, tp)
    sibling = (me, tp + 1 - 2 * core)
    right, left = (me + 2, tp), (me - 2, tp)
    far_steps = []
    step = 2
    while step < n_tp:
        far_steps.append((me, tp + step - 2 * step * lax.rem(tp // step, 2)))
        step *= 2

    rows = norm.shape[1]
    blk = rows // 2
    across = n_tp // 2
    xpos = tp // 2
    x_others = [(me, lax.rem(tp + 2 * k, n_tp)) for k in range(1, across)]
    half = norm.shape[2]
    hidden_half = act.shape[2]
    own_heads = kv_own.shape[-1] // (2 * HD)
    width = own_heads * HD
    block_cols = 2 * half // line
    scale = HD ** (-0.5)

    def place_of(j):
        return lax.rem(z + j, line) * 2 + y

    barrier = pltpu.get_barrier_semaphore()
    greet = [partner, sibling] + x_others + [(place_of(j), tp) for j in range(1, line)]
    for device in greet:
        pl.semaphore_signal(barrier, inc=1, device_id=device, device_id_type=MESH)

    def rcopy(src, dst, s, r, device):
        return pltpu.make_async_remote_copy(
            src_ref=src, dst_ref=dst, send_sem=s, recv_sem=r, device_id=device, device_id_type=MESH
        )

    def lcopy(src, dst, sem):
        return pltpu.make_async_copy(src, dst, sem)

    def fin_parts(t):
        c = (c_down, c_up, c_out, c_qkv)[t]
        if t == DOWN:
            dst = down_o.at[pl.ds(pl.multiple_of(y * hidden_half, hidden_half), hidden_half), :]
        elif t == UP:
            dst = up_o.at[:, pl.ds(pl.multiple_of(y * hidden_half, hidden_half), hidden_half)]
        elif t == OUT:
            dst = out_o.at[pl.ds(pl.multiple_of(y * width, width), width), :]
        else:
            dst = qkv_o.at[:, pl.ds(pl.multiple_of(y * 3 * width, 3 * width), 3 * width)]
        return c, dst

    def part_rows(x):
        n = rows // across
        return pl.ds(pl.multiple_of(x * n, n), n)

    def y_copy(item, t=0):
        if item == Y_KV:
            src, dst = kv_away, kv_own.at[:, 1]
        elif item == Y_QG:
            src, dst = qg_away, qg_own.at[:, 1]
        elif item == Y_COT:
            src, dst = cot.at[core, part_rows(xpos)], cot_far.at[core, part_rows(xpos)]
        elif item == Y_MLP:
            src, dst = norm.at[core, part_rows(xpos)], norm_far.at[core, part_rows(xpos)]
        elif item == Y_ATTN:
            src, dst = attn.at[core, part_rows(xpos)], attn_far.at[core, part_rows(xpos)]
        elif item == Y_ACT:
            src, dst = act.at[1 - y], act_far
        elif item == Y_HID:
            src, dst = hid.at[1 - y], hid_far
        elif item == Y_ATT:
            src, dst = att.at[:, 1], att_far
        elif item == Y_GQKV:
            src, dst = gqkv.at[:, 1], gqkv_far
        else:
            c, dst = fin_parts(t)
            src = c.at[0, 1 - y]
            item = Y_FIN + t
        return rcopy(src, dst, y_s.at[item], y_r.at[item], partner)

    def core_copy(k):
        ref = (cot_far, norm_far, attn_far)[k]
        return rcopy(ref.at[core], ref.at[core], core_s.at[k], core_r.at[k], sibling)

    def x_copy(k, n):
        ref = (cot_far, norm_far, attn_far)[k].at[core, part_rows(xpos)]
        return rcopy(ref, ref, x_s.at[k, n], x_r.at[k, n], x_others[n])

    def x_arrival(k, n):
        ref = (cot_far, norm_far, attn_far)[k].at[core, part_rows(lax.rem(xpos + across - n - 1, across))]
        return rcopy(ref, ref, x_s.at[k, n], x_r.at[k, n], x_others[n])

    def pass_x(item, k):
        y_copy(item).wait_recv()
        for n in range(across - 1):
            x_copy(k, n).start()

    def pass_on(item, k):
        for n in range(across - 1):
            x_arrival(k, n).wait_recv()
        core_copy(k).start()

    def x_drain(k):
        for n in range(across - 1):
            x_copy(k, n).wait_send()

    E_COT, E_COT_FAR, E_ACT, E_ACT_FAR, E_ACT_LAST = range(5)
    next_to_end = jnp.logical_or(z == 1, z == line - 2)

    def end_part(k, x):
        n = rows // across
        return cot_end.at[
            pl.ds(pl.multiple_of(k * rows + x * n, n), n), pl.ds(pl.multiple_of(core * half, half), half)
        ]

    def end_copy(item, device):
        if item == E_COT:
            src, dst = cot.at[core, part_rows(xpos)], end_part(0, xpos)
        elif item == E_COT_FAR:
            src, dst = end_part(0, xpos), end_part(1, xpos)
        elif item == E_ACT:
            src, dst = act.at[y], act_end.at[pl.ds(0, rows), :]
        else:
            n = hidden_half // 2
            part = pl.ds(0 if item == E_ACT_FAR else n, n)
            src, dst = act_far.at[:, part], act_end.at[pl.ds(rows, rows), part]
        return rcopy(src, dst, end_s.at[item], end_r.at[item], device)

    def end_x(k, n, arriving):
        x = lax.rem(xpos + across - n - 1, across) if arriving else xpos
        ref = end_part(k, x)
        return rcopy(ref, ref, ex_s.at[k, n], ex_r.at[k, n], x_others[n])

    def end_share(k):
        ref = cot_end.at[pl.ds(k * rows, rows), pl.ds(pl.multiple_of(core * half, half), half)]
        return rcopy(ref, ref, end_s.at[5 + k], end_r.at[5 + k], sibling)

    def end_send(item):
        @pl.when(z == 0)
        def _():
            end_copy(item, right).start()

        @pl.when(z == line - 1)
        def _():
            end_copy(item, left).start()

    def end_pass_x(k):
        @pl.when(next_to_end)
        def _():
            end_copy(E_COT + k, partner).wait_recv()
            for n in range(across - 1):
                end_x(k, n, False).start()
            if k == 0:
                end_copy(E_COT_FAR, partner).start()

    def end_pass(k):
        @pl.when(next_to_end)
        def _():
            for n in range(across - 1):
                end_x(k, n, True).wait_recv()
            end_share(k).start()

    def end_drain():
        @pl.when(jnp.logical_or(z == 0, z == line - 1))
        def _():
            for item in (E_COT, E_ACT, E_ACT_FAR, E_ACT_LAST):
                end_copy(item, partner).wait_send()

        @pl.when(next_to_end)
        def _():
            end_copy(E_COT_FAR, partner).wait_send()
            for k in range(2):
                end_share(k).wait_send()
                for n in range(across - 1):
                    end_x(k, n, False).wait_send()

    def ag_copy(t, h, to, hop, j_src, j_dst):
        ref = (kv_all, qg_all)[t]
        src = ref.at[:, 2 * j_src + h]
        if isinstance(hop, int) and hop == 1:
            src = (kv_own, qg_own)[t].at[:, h]
        return rcopy(
            src,
            ref.at[:, 2 * j_dst + h],
            ag_s.at[t, h, to, hop],
            ag_r.at[t, h, j_dst],
            (right, left)[to],
        )

    def ag_send_when(hop):
        return (
            jnp.logical_and(z >= hop - 1, z <= line - 2),
            jnp.logical_and(z + hop - 1 <= line - 1, z >= 1),
        )

    def ag_hop(t, h, hop, only=None):
        first = isinstance(hop, int) and hop == 1
        to_right, to_left = ag_send_when(hop)
        if only is not None:
            to_right, to_left = jnp.logical_and(to_right, only), jnp.logical_and(to_left, only)

        @pl.when(to_right)
        def _():
            if not first:
                ag_copy(t, h, 0, hop - 1, line - hop + 1, line - hop + 1).wait_recv()
            ag_copy(t, h, 0, hop, lax.rem(line - hop + 1, line), line - hop).start()

        @pl.when(to_left)
        def _():
            if not first:
                ag_copy(t, h, 1, hop - 1, hop - 1, hop - 1).wait_recv()
            ag_copy(t, h, 1, hop, hop - 1, hop).start()

    def ag_rest(t, h, hop):
        def one(i, _):
            ag_hop(t, h, i)
            return 0

        def come(i, _):
            ag_copy(t, h, 0, i, i, i).wait_recv()
            return 0

        if hop < line:
            lax.fori_loop(hop, line, one, 0)

        @pl.when(jnp.logical_or(z == 0, z == line - 1))
        def _():
            lax.fori_loop(1, line, come, 0)

    def ag_drain(t, h):
        def one(hop, _):
            to_right, to_left = ag_send_when(hop)

            @pl.when(to_right)
            def _():
                ag_copy(t, h, 0, hop, lax.rem(line - hop + 1, line), line - hop).wait_send()

            @pl.when(to_left)
            def _():
                ag_copy(t, h, 1, hop, hop - 1, hop).wait_send()

            return 0

        lax.fori_loop(1, line, one, 0)

    rs = (
        (c_down, rs_down, stage_down),
        (c_up, rs_up, stage_up),
        (c_out, rs_out, stage_out),
        (c_qkv, rs_qkv, stage_qkv),
    )

    def piece_of(ref, t, p):
        if t != DOWN:
            return ref.at[p]
        n = hidden_half // 2
        return ref.at[:, pl.ds(pl.multiple_of(p * n, n), n), :]

    def rs_copy(t, p, j, slot, device):
        c, recv, _ = rs[t]
        return rcopy(
            piece_of(c.at[j], t, p), piece_of(recv.at[slot], t, p), rs_s.at[t, p, j], rs_r.at[t, p, slot], device
        )

    def rs_take(t, p, j, slot):
        c, recv, held = rs[t]
        rs_copy(t, p, j, slot, partner).wait_recv()
        copy = lcopy(piece_of(recv.at[slot], t, p), piece_of(held, t, p), tsem.at[t])
        copy.start()
        copy.wait()
        n = c.shape[2]
        part = min(64, n)

        def add(side, i):
            at = pl.ds(pl.multiple_of(i * part, part), part)
            c[j, side, at, :] = (
                c[j, side, at, :].astype(F32) + held[side, at, :].astype(F32)
            ).astype(BF16)

        def one(i, _):
            if t != DOWN:
                add(p, i)
            else:
                for side in range(2):
                    add(side, p * (n // part // 2) + i)
            return 0

        lax.fori_loop(0, n // part // (2 if t == DOWN else 1), one, 0)

    def first_from(t):
        return 2 if t == DOWN else 1

    def rs_ends(t, hops, parts=(0, 1)):
        first = first_from(t)

        def one(hop, _):
            for k in parts:
                p = k if t == DOWN else (1 - y if k == 0 else y)

                @pl.when(jnp.logical_and(z == first - 1, hop >= first))
                def _():
                    rs_copy(t, p, line - hop, line - hop - 1, right).start()

                @pl.when(jnp.logical_and(z == line - first, hop >= first))
                def _():
                    rs_copy(t, p, hop, hop + 1, left).start()

            return 0

        lax.fori_loop(*hops, one, 0)

    near = 2 * z < line

    def halves(t, step):
        def one(k, _):
            step(k if t == DOWN else jnp.where(k == 0, 1 - y, y))
            return 0

        lax.fori_loop(0, 2, one, 0)

    def rs_right(t, hop, only):
        jr, first = line - hop, first_from(t)

        @pl.when(jnp.logical_and(only, jnp.logical_and(hop >= z + 1, z >= first)))
        def _():
            def step(p):
                rs_take(t, p, jr, jr)
                rs_copy(t, p, jr, jr - 1, right).start()

            halves(t, step)

    def rs_left(t, hop, only):
        jl, first = hop, first_from(t)

        @pl.when(jnp.logical_and(only, jnp.logical_and(hop >= line - z, z <= line - 1 - first)))
        def _():
            def step(p):
                rs_take(t, p, jl, jl)
                rs_copy(t, p, jl, jl + 1, left).start()

            halves(t, step)

    def rs_cross(t, hop):
        rs_right(t, hop, near)
        rs_left(t, hop, jnp.logical_not(near))

    def rs_home(t, hop):
        rs_right(t, hop, jnp.logical_not(near))
        rs_left(t, hop, near)

    def rs_rest(t, hop):
        def one(i, _):
            rs_cross(t, i)
            rs_home(t, i)
            return 0

        if hop < line:
            lax.fori_loop(hop, line, one, 0)

    def rs_finish_half(t, k):
        first = first_from(t)
        c, dst = fin_parts(t)
        p = k if t == DOWN else (1 - y if k == 0 else y)

        @pl.when(z >= first)
        def _():
            rs_take(t, p, 0, 0)

        @pl.when(z <= line - 1 - first)
        def _():
            rs_take(t, p, 0, line)

        if k == (1 if t == DOWN else 0):
            y_copy(Y_FIN, t).start()
        if k == 1:
            lcopy(c.at[0, y], dst, local.at[4 + t]).start()

    def rs_finish(t):
        rs_finish_half(t, 0)
        rs_finish_half(t, 1)

    def rs_drain(t):
        sends = jnp.logical_and(z >= first_from(t) - 1, z <= line - first_from(t))

        def one(j, _):
            for p in range(2):

                @pl.when(jnp.logical_and(sends, j <= line - 1 - z))
                def _():
                    rs_copy(t, p, j, j - 1, right).wait_send()

                @pl.when(jnp.logical_and(sends, j > line - 1 - z))
                def _():
                    rs_copy(t, p, j, j + 1, left).wait_send()

            return 0

        lax.fori_loop(1, line, one, 0)
        c, dst = fin_parts(t)
        y_copy(Y_FIN, t).wait()
        lcopy(c.at[0, y], dst, local.at[4 + t]).wait()

    last = len(far_steps) + 1

    def tp_copy(i, k):
        part = tp_part.at[i]
        if k == 0:
            src, dst, device = part.at[1 - core], tp_recv.at[i, 0], sibling
        elif k < last:
            src, dst, device = part.at[core], tp_recv.at[i, k], far_steps[k - 1]
        else:
            src, dst, device = part.at[core], tp_far.at[i], sibling
        return rcopy(src, dst, tp_s.at[i, k], tp_r.at[i, k], device)

    def tp_add(i, k):
        part = 64

        def add(n, _):
            at = pl.ds(pl.multiple_of(n * part, part), part)
            tp_part[i, core, at, :] = (
                tp_part[i, core, at, :].astype(F32) + tp_recv[i, k, at, :].astype(F32)
            ).astype(BF16)
            return 0

        lax.fori_loop(0, blk // part, add, 0)

    def tp_next(i, k):
        if k > 1:
            tp_copy(i, k - 1).wait_send()
        tp_copy(i, k - 1).wait_recv()
        tp_add(i, k - 1)
        tp_copy(i, k).start()

    def tp_done(i):
        tp_copy(i, last).wait_recv()
        tp_copy(i, 0).wait_send()

        other = lcopy(tp_far.at[i], tp_part.at[i, 1 - core], local.at[8])
        other.start()
        other.wait()

    def tp_drain(i):
        tp_copy(i, last).wait_send()

    def stream(lo, hi, fetches, body):
        for f in fetches:
            f(lo, lax.rem(lo, 2)).start()

        def one(i, _):
            slot = lax.rem(i, 2)

            @pl.when(i + 1 < hi)
            def _():
                for f in fetches:
                    f(i + 1, 1 - slot).start()

            for f in fetches:
                f(i, slot).wait()
            body(i, slot)
            return 0

        lax.fori_loop(lo, hi, one, 0)

    def col_tile(w):
        def fetch(i, slot):
            at = pl.ds(pl.multiple_of(i * TILE, TILE), TILE)
            return lcopy(w.at[:, at], wcol.at[slot, pl.ds(0, w.shape[0]), :], wsem.at[0, slot])

        return fetch

    def row_tile(w):
        def fetch(i, slot):
            at = pl.ds(pl.multiple_of(i * TILE, TILE), TILE)
            return lcopy(w.at[at, :], wrow.at[slot, pl.ds(0, TILE), pl.ds(0, w.shape[1])], wsem.at[1, slot])

        return fetch

    x_load = lcopy(stream_in, xbuf, local.at[0])
    c_load = lcopy(cotangent, cbuf, local.at[1])
    c_load.start()
    x_load.start()

    def number(place, side, k):
        return order[4 * place + 2 * side + k]

    late = [number(z, s, 0) > number(z, s, 1) for s in (y, 1 - y)]

    def block_number(lh, place, side):
        first, second = number(place, side, 0), number(place, side, 1)
        return jnp.minimum(first, second) if lh == 0 else jnp.maximum(first, second)

    for lh in range(2):
        for h in range(2):
            at_block = block_table[:, pl.ds(block_number(lh, z, (y, 1 - y)[h]), 1), :]
            cb, sb = at_block[0], at_block[1]
            ci, si = row_table[0], row_table[1]
            cosine[lh, h] = cb * ci - sb * si
            sine[lh, h] = sb * ci + cb * si

    def by_order(h, first, second):
        return jnp.where(late[h], second, first), jnp.where(late[h], first, second)

    small[...] = jnp.zeros(small.shape, F32)
    model = 2 * half
    chunk_rows = 64
    c_load.wait()

    def cast(i, _):
        at = pl.ds(pl.multiple_of(i * chunk_rows, chunk_rows), chunk_rows)
        c = cbuf[at, :]
        small[S_OUT : S_OUT + 1, :model] += jnp.sum(c, axis=0, keepdims=True)
        c = c.astype(BF16)
        cot[0, at, :] = c[:, :half]
        cot[1, at, :] = c[:, half:]
        return 0

    lax.fori_loop(0, rows // chunk_rows, cast, 0)
    pl.semaphore_wait(barrier, len(greet))
    y_copy(Y_COT).start()
    end_send(E_COT)

    x_load.wait()

    def unit_of(at):
        x = xbuf[at, :]
        centred = x - jnp.mean(x, axis=-1, keepdims=True)
        variance = jnp.mean(centred * centred, axis=-1, keepdims=True)
        inv_scale = lax.rsqrt(variance + norm_epsilon)
        return centred * inv_scale, inv_scale

    def norms(i, _):
        at = pl.ds(pl.multiple_of(i * chunk_rows, chunk_rows), chunk_rows)
        unit, _ = unit_of(at)
        for n, ref in ((0, attn), (1, norm)):
            value = (unit * gain[n : n + 1, :] + shift[n : n + 1, :]).astype(BF16)
            ref[0, at, :] = value[:, :half]
            ref[1, at, :] = value[:, half:]
        return 0

    lax.fori_loop(0, rows // chunk_rows, norms, 0)

    def tile_at(i):
        return pl.ds(pl.multiple_of(i * TILE, TILE), TILE)

    def hidden_at(i):
        at = pl.ds(pl.multiple_of(lax.rem(i * TILE, hidden_half), TILE), TILE)
        return i * TILE // hidden_half, at

    def activate(i, slot):
        h = nn(norm[0], wcol[slot, :half, :]) + nn(norm[1], wcol[slot, half : 2 * half, :])
        h = h + b_up[:, tile_at(i)]
        gate = 0.5 * (1.0 + lax.erf(h * root_half))
        which, at = hidden_at(i)
        act[which, :, at] = (h * gate).astype(BF16)
        slope = gate + h * jnp.exp(-0.5 * h * h) * inverse_root_two_pi
        hid[which, :, at] = slope.astype(BF16)

    def hidden_back(i, slot):
        g = nt(cot[0], wrow[slot, :TILE, :half]) + nt(cot[1], wrow[slot, :TILE, half : 2 * half])
        which, at = hidden_at(i)
        g = g * hid[which, :, at].astype(F32)
        small[S_UP : S_UP + 1, tile_at(i)] = jnp.sum(g, axis=0, keepdims=True)
        hid[which, :, at] = g.astype(BF16)

    hidden_tiles = 2 * hidden_half // TILE
    def project(at, slot, place):
        value = nn(attn[0], wcol[slot, :half, :]) + nn(attn[1], wcol[slot, half : 2 * half, :])
        value = value + b_qkv[at][None, :]
        pieces = by_order(0, value[:blk], value[blk:])
        for lh in range(2):
            first, rest = pieces[lh][:, :LANES], pieces[lh][:, LANES:]
            place(lh, first, rest)

    def put(refs, which, lh, at, value):
        mine, away = refs

        @pl.when(which == 0)
        def _():
            mine[lh, 0, :, at] = value

        @pl.when(which == 1)
        def _():
            away[lh, :, at] = value

    def kv_index(i):
        which = 1 - i // (2 * own_heads)
        k, kind = lax.rem(i, 2 * own_heads) // 2, 1 + lax.rem(i, 2)
        head = jnp.where(which == 0, y, 1 - y) * own_heads + k
        return which, k, kind, 3 * head + kind

    def q_index(i):
        which = 1 - i // own_heads
        k = lax.rem(i, own_heads)
        head = jnp.where(which == 0, y, 1 - y) * own_heads + k
        return which, k, 3 * head, head

    def fetch_by(w, index):
        def fetch(i, slot):
            return lcopy(w.at[:, tile_at(index(i))], wcol.at[slot, pl.ds(0, w.shape[0]), :], wsem.at[0, slot])

        return fetch

    def lanes_at(start, n):
        return pl.ds(pl.multiple_of(start, LANES), n)

    def keys_values(i, slot):
        which, k, kind, tile = kv_index(i)
        base = jnp.where(kind == 1, 0, width) + k * HD

        def place(lh, first, rest):
            turned = turn(first, cosine[lh, 0], sine[lh, 0], 1)
            first = jnp.where(kind == 1, turned, first).astype(BF16)
            put((kv_own, kv_away), which, lh, lanes_at(base, LANES), first)
            put((kv_own, kv_away), which, lh, lanes_at(base + LANES, HD - LANES), rest.astype(BF16))

        project(tile_at(tile), slot, place)

    w_out_fetch = lcopy(w_out, wrow.at[0, pl.ds(0, w_out.shape[0]), pl.ds(0, model)], wsem.at[1, 0])

    def queries(i, slot):
        which, k, tile, head = q_index(i)

        def place(lh, first, rest):
            turned = turn(first, cosine[lh, 0], sine[lh, 0], 1).astype(BF16)
            put((qg_own, qg_away), which, lh, lanes_at(k * HD, LANES), turned)
            put((qg_own, qg_away), which, lh, lanes_at(k * HD + LANES, HD - LANES), rest.astype(BF16))

        project(tile_at(tile), slot, place)
        at = pl.ds(pl.multiple_of(head * HD, HD), HD)
        g = nt(cot[0], wrow[0, at, :half]) + nt(cot[1], wrow[0, at, half : 2 * half])
        pieces = by_order(0, g[:blk], g[blk:])
        for lh in range(2):
            put((qg_own, qg_away), which, lh, lanes_at(width + k * HD, HD), pieces[lh].astype(BF16))

    own_places = [
        lcopy(own.at[:, h], everyone.at[:, h], local.at[2 + 2 * t + h])
        for t, (own, everyone) in enumerate(((kv_own, kv_all), (qg_own, qg_all)))
        for h in range(2)
    ]

    def cols_at(ref, j):
        start = lax.rem(z + j, line) * block_cols
        at = pl.ds(pl.multiple_of(lax.rem(start, half), LANES), block_cols)
        return ref[start // half, :, at]

    def split_cols(ref, j, at, value):
        n = value.shape[1] // 2
        ref[j, 0, at, :] = value[:, :n].astype(BF16)
        ref[j, 1, at, :] = value[:, n:].astype(BF16)

    def split_rows(ref, j, at, value):
        n = value.shape[0] // 2
        ref[j, 0, :, at] = value[:n].astype(BF16)
        ref[j, 1, :, at] = value[n:].astype(BF16)

    def in_order(share, first=0, end=line):
        def one(k, _):
            j = jnp.where(lax.rem(k, 2) == 0, line - 1 - k // 2, k // 2 + 1)
            share(jnp.where(k == line - 1, 0, j))
            return 0

        lax.fori_loop(first, end, one, 0)

    def mlp_back(i, slot):
        value = nt(hid[0], wrow[slot, :TILE, :hidden_half]) + nt(
            hid[1], wrow[slot, :TILE, hidden_half : 2 * hidden_half]
        )
        tp_part[MLPB, :, :, tile_at(i)] = value.astype(BF16).reshape(2, blk, TILE)

    model_tiles = model // TILE

    def share_down(j):
        g0, g1 = cols_at(cot, j), cols_at(cot_far, j)

        def one(i, _):
            split_cols(
                c_down, j, tile_at(i), tn(act[y, :, tile_at(i)], g0) + tn(act_far[:, tile_at(i)], g1)
            )
            return 0

        lax.fori_loop(0, hidden_half // TILE, one, 0)

    def share_up(j):
        m0, m1 = cols_at(norm, j), cols_at(norm_far, j)

        def one(i, _):
            split_rows(c_up, j, tile_at(i), tn(m0, hid[y, :, tile_at(i)]) + tn(m1, hid_far[:, tile_at(i)]))
            return 0

        lax.fori_loop(0, hidden_half // TILE, one, 0)

    def end_tile(k):
        def fetch(i, slot):
            return lcopy(
                act_end.at[pl.ds(k * rows, rows), tile_at(i)], wcol.at[slot, pl.ds(0, rows), :], wsem.at[0, slot]
            )

        return fetch

    def add_end_tokens(k, item, tiles):
        @pl.when(next_to_end)
        def _():
            if item != E_ACT_LAST:
                end_share(k).wait_recv()
            held = lcopy(
                cot_end.at[pl.ds(k * rows, rows), :],
                wrow.at[k, pl.ds(0, rows), pl.ds(0, model)],
                wsem.at[1, k],
            )
            held.start()
            end_copy(item, partner).wait_recv()
            held.wait()

            def add_tile(i, slot):
                at = tile_at(i)

                def add_block(n, _):
                    j = jnp.where(z == 1, n, lax.rem(n + 2, line))
                    start = pl.multiple_of(lax.rem(z + j, line) * block_cols, LANES)
                    value = tn(wcol[slot, :rows, :], wrow[k, :rows, pl.ds(start, block_cols)])
                    n = block_cols // 2
                    for p in range(2):
                        c_down[j, p, at, :] = (
                            c_down[j, p, at, :].astype(F32) + value[:, p * n : (p + 1) * n]
                        ).astype(BF16)
                    return 0

                lax.fori_loop(0, line - 1, add_block, 0)

            stream(*tiles, (end_tile(k),), add_tile)

    pair = 2 * blk
    same = lax.broadcasted_iota(jnp.int32, (pair, pair), 0) == lax.broadcasted_iota(
        jnp.int32, (pair, pair), 1
    )

    def positions(lh, place, along):
        shape = (1, pair) if along else (pair, 1)
        at = lax.broadcasted_iota(jnp.int32, shape, along)
        here, there = block_number(lh, place, y), block_number(lh, place, 1 - y)
        return at + jnp.where(at < blk, here * blk, there * blk - blk)

    def piece_positions(lh_start, i, along):
        place = lax.rem(z + i, line)
        early, late_ = positions(0, place, along), positions(1, place, along)
        return jnp.where(i < line, early, late_)

    def piece(t):
        def fetch(i, slot):
            ref = (kv_all, qg_all)[t]
            return lcopy(
                ref.at[i // line, pl.ds(2 * lax.rem(i, line), 2)], chunk.at[slot], csem.at[slot]
            )

        return fetch

    def store_order(ref):
        for h in range(2):
            first, second = by_order(h, ref[0, h], ref[1, h])
            ref[0, h] = first
            ref[1, h] = second

    def attend_forward():
        for lh in range(2):
            for head in range(own_heads):
                at_k, at_v = head * HD, width + head * HD
                run_m[...] = jnp.full(run_m.shape, masked_value, F32)
                run_l[...] = jnp.zeros(run_l.shape, F32)
                acc_a[...] = jnp.zeros(acc_a.shape, F32)

                def attend(i, slot):
                    k = chunk[slot, :, :, at_k : at_k + HD].reshape(pair, HD)
                    v = chunk[slot, :, :, at_v : at_v + HD].reshape(pair, HD)
                    q = qg_own[lh, :, :, at_k : at_k + HD].reshape(pair, HD)
                    s = nt(q, k) * scale
                    seen = piece_positions(lh, i, 1) <= positions(lh, z, 0)
                    s = jnp.where(seen, s, masked_value)
                    old = run_m[...]
                    top = jnp.maximum(old, jnp.max(s, axis=1, keepdims=True))
                    p = jnp.exp(s - top)
                    fade = jnp.exp(old - top)
                    run_m[...] = top
                    run_l[...] = run_l[...] * fade + jnp.sum(p, axis=1, keepdims=True)
                    acc_a[...] = acc_a[...] * fade + nn(p.astype(BF16), v)

                stream(0, line * (lh + 1), (piece(0),), attend)
                out = (acc_a[...] / run_l[...]).astype(BF16)
                att[lh, :, :, at_k : at_k + HD] = out.reshape(2, blk, HD)
                log_total = run_m[...] + jnp.log(run_l[...])
                g = qg_own[lh, :, :, at_v : at_v + HD].reshape(pair, HD)
                dots = jnp.sum(g.astype(F32) * out.astype(F32), axis=1, keepdims=True)
                stats[lh, head, 0:1, :] = jnp.sum(jnp.where(same, log_total, 0.0), 0, keepdims=True)
                stats[lh, head, 1:2, :] = jnp.sum(jnp.where(same, dots, 0.0), 0, keepdims=True)

    def stat_copy(j):
        return rcopy(
            stats, stats_all.at[line - j], st_s.at[j], st_r.at[line - j], (place_of(j), tp)
        )

    def share_out(j):
        g0, g1 = cols_at(cot, j), cols_at(cot_far, j)

        def one(i, _):
            a0 = att[:, 0, :, tile_at(i)].reshape(rows, TILE)
            a1 = att[:, 1, :, tile_at(i)].reshape(rows, TILE)
            split_cols(c_out, j, tile_at(i), tn(a0, g0) + tn(a1, g1))
            return 0

        lax.fori_loop(0, width // TILE, one, 0)

    def undo(value, lh, head, kind):
        at = (3 * head + kind) * HD
        first = value[:, :LANES]
        if kind < 2:
            first = turn(
                first, cosine[lh].reshape(pair, LANES), sine[lh].reshape(pair, LANES), -1
            )
        for lo, hi, part in ((0, LANES, first), (LANES, HD, value[:, LANES:])):
            spot = lanes_at(y * 3 * width + at + lo, hi - lo)
            small[S_QKV : S_QKV + 1, spot] += jnp.sum(part, axis=0, keepdims=True)
            gqkv[lh, :, :, at + lo : at + hi] = part.astype(BF16).reshape(2, blk, hi - lo)

    def attend_back_queries():
        for lh in range(2):
            for head in range(own_heads):
                at_k, at_v = head * HD, width + head * HD
                run_m[...] = jnp.sum(
                    jnp.where(same, stats[lh, head, 0:1, :], 0.0), axis=1, keepdims=True
                )
                run_l[...] = jnp.sum(
                    jnp.where(same, stats[lh, head, 1:2, :], 0.0), axis=1, keepdims=True
                )
                acc_a[...] = jnp.zeros(acc_a.shape, F32)

                def back_q(i, slot):
                    k = chunk[slot, :, :, at_k : at_k + HD].reshape(pair, HD)
                    v = chunk[slot, :, :, at_v : at_v + HD].reshape(pair, HD)
                    q = qg_own[lh, :, :, at_k : at_k + HD].reshape(pair, HD)
                    g = qg_own[lh, :, :, at_v : at_v + HD].reshape(pair, HD)
                    s = nt(q, k) * scale
                    seen = piece_positions(lh, i, 1) <= positions(lh, z, 0)
                    s = jnp.where(seen, s, masked_value)
                    p = jnp.exp(s - run_m[...])
                    ds = (p * (nt(g, v) - run_l[...]) * scale).astype(BF16)
                    acc_a[...] += nn(ds, k)

                stream(0, line * (lh + 1), (piece(0),), back_q)
                undo(acc_a[...], lh, head, 0)

    def branch(i, slot):
        value = nn(act[0], wcol[slot, :hidden_half, :]) + nn(
            act[1], wcol[slot, hidden_half : 2 * hidden_half, :]
        )
        own = att[:, 0].reshape(rows, width)
        far = att_far[...].reshape(rows, width)
        mine = wrow[0, pl.ds(pl.multiple_of(y * width, width), width), tile_at(i)]
        theirs = wrow[0, pl.ds(pl.multiple_of((1 - y) * width, width), width), tile_at(i)]
        value += nn(own, mine) + nn(far, theirs)
        tp_part[BRANCH, :, :, tile_at(i)] = value.astype(BF16).reshape(2, blk, TILE)

    def attend_back_keys():
        for lh in range(2):
            for head in range(own_heads):
                at_k, at_v = head * HD, width + head * HD
                acc_a[...] = jnp.zeros(acc_a.shape, F32)
                acc_b[...] = jnp.zeros(acc_b.shape, F32)

                def back_k(i, slot):
                    q = chunk[slot, :, :, at_k : at_k + HD].reshape(pair, HD)
                    g = chunk[slot, :, :, at_v : at_v + HD].reshape(pair, HD)
                    k = kv_own[lh, :, :, at_k : at_k + HD].reshape(pair, HD)
                    v = kv_own[lh, :, :, at_v : at_v + HD].reshape(pair, HD)
                    stat = stats_all[lax.rem(i, line), i // line, head]
                    s = nt(k, q) * scale
                    seen = positions(lh, z, 0) <= piece_positions(lh, i, 1)
                    s = jnp.where(seen, s, masked_value)
                    p = jnp.exp(s - stat[0:1, :])
                    ds = (p * (nt(v, g) - stat[1:2, :]) * scale).astype(BF16)
                    acc_a[...] += nn(ds, q)
                    acc_b[...] += nn(p.astype(BF16), g)

                stream(lh * line, 2 * line, (piece(1),), back_k)
                undo(acc_a[...], lh, head, 1)
                undo(acc_b[...], lh, head, 2)

    def share_qkv(j):
        m0, m1 = cols_at(attn, j), cols_at(norm_far, j)

        def one(i, _):
            g0 = gqkv[:, 0, :, tile_at(i)].reshape(rows, TILE)
            g1 = gqkv[:, 1, :, tile_at(i)].reshape(rows, TILE)
            split_rows(c_qkv, j, tile_at(i), tn(m0, g0) + tn(m1, g1))
            return 0

        lax.fori_loop(0, 3 * width // TILE, one, 0)

    def attn_back(i, slot):
        own = gqkv[:, 0].reshape(rows, 3 * width)
        far = gqkv_far[...].reshape(rows, 3 * width)
        mine = wrow[slot, :TILE, pl.ds(pl.multiple_of(y * 3 * width, LANES), 3 * width)]
        theirs = wrow[slot, :TILE, pl.ds(pl.multiple_of((1 - y) * 3 * width, LANES), 3 * width)]
        value = nt(own, mine) + nt(far, theirs)
        tp_part[ATTNB, :, :, tile_at(i)] = value.astype(BF16).reshape(2, blk, TILE)

    def back_norms(i, _):
        at = pl.ds(pl.multiple_of(i * chunk_rows, chunk_rows), chunk_rows)
        at_part = pl.ds(pl.multiple_of(lax.rem(i * chunk_rows, blk), chunk_rows), chunk_rows)
        which = i * chunk_rows // blk
        unit, inv_scale = unit_of(at)
        total = jnp.zeros((chunk_rows, model), F32)
        for n, part in ((0, ATTNB), (1, MLPB)):
            value = tp_part[part, which, at_part, :].astype(F32)
            small[S_GAIN + n : S_GAIN + n + 1, :model] += jnp.sum(value * unit, 0, keepdims=True)
            small[S_SHIFT + n : S_SHIFT + n + 1, :model] += jnp.sum(value, 0, keepdims=True)
            total = total + value * gain[n : n + 1, :]
        cbuf[at, :] = cbuf[at, :] + inv_scale * (
            total
            - jnp.mean(total, axis=-1, keepdims=True)
            - unit * jnp.mean(total * unit, axis=-1, keepdims=True)
        )
        return 0

    def small_copy(j):
        return rcopy(
            small_sent, small_recv.at[line - j], sm_s.at[j], sm_r.at[line - j], (place_of(j), tp)
        )

    def stream_rows(i, _):
        at = pl.ds(pl.multiple_of(i * chunk_rows, chunk_rows), chunk_rows)
        at_part = pl.ds(pl.multiple_of(lax.rem(i * chunk_rows, blk), chunk_rows), chunk_rows)
        which = i * chunk_rows // blk
        xbuf[at, :] = xbuf[at, :] + out_bias[...] + tp_part[BRANCH, which, at_part, :].astype(F32)
        return 0

    stream(0, 4 * own_heads, (fetch_by(w_qkv, lambda i: kv_index(i)[3]),), keys_values)
    y_copy(Y_KV).start()
    ag_hop(0, 0, 1)
    own_places[0].start()
    w_out_fetch.start()
    w_out_fetch.wait()
    stream(0, 2 * own_heads, (fetch_by(w_qkv, lambda i: q_index(i)[2]),), queries)
    y_copy(Y_QG).start()
    ag_hop(1, 0, 1)
    own_places[2].start()
    pass_x(Y_COT, 0)

    stream(0, hidden_tiles // 2, (col_tile(w_up),), activate)
    y_copy(Y_KV).wait_recv()
    ag_hop(0, 1, 1)
    own_places[1].start()
    stream(hidden_tiles // 2, hidden_tiles, (col_tile(w_up),), activate)
    y_copy(Y_ACT).start()
    y_copy(Y_MLP).start()
    end_send(E_ACT)
    pass_on(Y_COT, 0)
    ag_hop(0, 0, 2)
    end_pass_x(0)
    stream(0, hidden_tiles // 2, (row_tile(w_down),), hidden_back)
    y_copy(Y_QG).wait_recv()
    own_places[3].start()
    ag_hop(1, 1, 1)
    ag_hop(1, 0, 2)
    stream(hidden_tiles // 2, hidden_tiles, (row_tile(w_down),), hidden_back)
    y_copy(Y_HID).start()
    y_copy(Y_ATTN).start()
    end_pass(0)
    stream(0, model_tiles, (row_tile(w_up),), mlp_back)
    tp_copy(MLPB, 0).start()
    ag_hop(0, 0, 3)
    ag_hop(0, 1, 2)
    core_copy(0).wait_recv()
    y_copy(Y_ACT).wait_recv()
    end_send(E_ACT_FAR)
    end_send(E_ACT_LAST)
    in_order(share_down)
    pass_x(Y_MLP, 1)
    end_pass_x(1)
    ag_hop(0, 1, 3)
    ag_hop(1, 1, 2)
    end_tiles = hidden_half // TILE
    add_end_tokens(0, E_ACT, (0, end_tiles))
    pass_on(Y_MLP, 1)
    end_pass(1)
    ag_hop(1, 0, 3)
    add_end_tokens(1, E_ACT_FAR, (0, end_tiles // 2))
    rs_ends(DOWN, (1, 3), (0,))
    add_end_tokens(1, E_ACT_LAST, (end_tiles // 2, end_tiles))
    rs_ends(DOWN, (1, 3), (1,))
    tp_next(MLPB, 1)
    y_copy(Y_HID).wait_recv()
    core_copy(1).wait_recv()
    in_order(share_up)
    rs_ends(UP, (1, 2))
    ag_hop(1, 1, 3)
    ag_rest(0, 0, 4)
    ag_rest(0, 1, 4)
    for copy in own_places:
        copy.wait()

    attend_forward()
    store_order(att)
    for j in range(1, line):
        stat_copy(j).start()
    y_copy(Y_ATT).start()
    rs_ends(UP, (2, line))
    rs_ends(DOWN, (3, line))
    in_order(share_out)
    small[S_QKV : S_QKV + 1, :] = jnp.zeros((1, small.shape[1]), F32)
    attend_back_queries()
    tp_next(MLPB, 2)
    pass_x(Y_ATTN, 2)
    for hop in range(1, min(line, 4)):
        rs_cross(DOWN, hop)
        rs_home(DOWN, hop)
    rs_cross(UP, 1)
    rs_cross(UP, 2)
    y_copy(Y_ATT).wait_recv()
    w_out_fetch.start()
    w_out_fetch.wait()
    stream(0, model_tiles, (col_tile(w_down),), branch)
    tp_copy(BRANCH, 0).start()
    ag_rest(1, 0, 4)
    ag_rest(1, 1, 4)
    for j in range(1, line):
        stat_copy(line - j).wait_recv()
    own_stats = lcopy(stats, stats_all.at[0], local.at[0])
    own_stats.start()
    own_stats.wait()
    rs_cross(UP, 3) if line > 3 else None
    attend_back_keys()
    store_order(gqkv)
    y_copy(Y_GQKV).start()
    tp_next(BRANCH, 1)
    pass_on(Y_ATTN, 2)
    core_copy(2).wait_recv()
    core_copy(1).wait_send()
    x_drain(1)
    far_again = lcopy(attn_far, norm_far, local.at[1])
    far_again.start()
    far_again.wait()
    in_order(share_qkv)
    rs_ends(QKV, (1, line))
    rs_ends(OUT, (1, line))
    rs_home(UP, 1)
    rs_home(UP, 2)
    rs_home(UP, 3) if line > 3 else None
    y_copy(Y_GQKV).wait_recv()
    stream(0, model_tiles, (row_tile(w_qkv),), attn_back)
    tp_copy(ATTNB, 0).start()
    tp_next(BRANCH, 2)
    tp_next(ATTNB, 1)

    rs_cross(QKV, 1)
    rs_cross(QKV, 2)
    rs_rest(DOWN, 4 if line > 3 else 3)
    rs_finish(DOWN)
    tp_done(BRANCH)
    tp_done(MLPB)
    rs_cross(QKV, 3) if line > 3 else None
    rs_rest(UP, 4 if line > 3 else 3)
    rs_finish(UP)
    rs_home(QKV, 1)
    rs_home(QKV, 2)
    rs_home(QKV, 3) if line > 3 else None
    rs_rest(QKV, 4 if line > 3 else 3)
    tp_next(ATTNB, 2)
    tp_done(ATTNB)
    lax.fori_loop(0, rows // chunk_rows, back_norms, 0)
    grad_store = lcopy(cbuf, grad_o, local.at[1])
    grad_store.start()
    pair_copy = rcopy(small, small_pair, sm_s.at[0], sm_r.at[0], partner)
    pair_copy.start()
    pair_copy.wait()
    small_sent[...] = (small[...] + small_pair[...]).astype(BF16)
    for j in range(1, line):
        small_copy(j).start()
    lax.fori_loop(0, rows // chunk_rows, stream_rows, 0)
    stream_store = lcopy(xbuf, stream_o, local.at[0])
    stream_store.start()
    rs_cross(OUT, 1)
    rs_cross(OUT, 2)
    rs_cross(OUT, 3) if line > 3 else None
    rs_finish_half(QKV, 0)
    for hop in range(1, min(line, 4)):
        rs_home(OUT, hop)
    rs_rest(OUT, 4 if line > 3 else 3)
    rs_finish_half(QKV, 1)
    rs_finish(OUT)
    for j in range(1, line):
        small_copy(line - j).wait_recv()
    small_recv[0] = small_sent[...]
    small[...] = small_recv[lax.rem(line - z, line)].astype(F32)
    for p in range(1, line):
        small[...] += small_recv[lax.rem(p + line - z, line)].astype(F32)
    small_store = lcopy(small, small_o, local.at[2])
    small_store.start()

    for t in range(2):
        for h in range(2):
            ag_drain(t, h)
    for item in (Y_KV, Y_QG, Y_COT, Y_MLP, Y_ATTN, Y_ACT, Y_HID, Y_ATT, Y_GQKV):
        y_copy(item).wait_send()
    core_copy(0).wait_send()
    core_copy(2).wait_send()
    x_drain(0)
    x_drain(2)
    for j in range(1, line):
        stat_copy(j).wait_send()
        small_copy(j).wait_send()
    for i in range(3):
        tp_drain(i)
    grad_store.wait()
    small_store.wait()
    stream_store.wait()
    for t in range(4):
        rs_drain(t)
    end_drain()


def layer(line, n_tp, order, stream_in, cotangent, ln_gain, ln_bias, w_qkv, b_qkv, w_out, out_bias, w_up, b_up, w_down):
    rows, model = stream_in.shape
    half, blk = model // 2, rows // 2
    hidden = w_up.shape[1]
    hidden_half = hidden // 2
    width = w_out.shape[0] // 2
    own_heads = width // HD
    part_cols = model // line // 2
    pair = 2 * blk
    tp_steps = 0
    while (2 << tp_steps) < n_tp:
        tp_steps += 1
    small_shape = (8, max(model, hidden, 6 * width))
    shares = (
        (2, hidden_half, part_cols),
        (2, part_cols, hidden_half),
        (2, width, part_cols),
        (2, part_cols, 3 * width),
    )
    b = lambda *s: jax.ShapeDtypeStruct(s, BF16)
    f = lambda *s: jax.ShapeDtypeStruct(s, F32)
    vb = lambda *s: pltpu.VMEM(s, BF16)
    vf = lambda *s: pltpu.VMEM(s, F32)
    dma = pltpu.SemaphoreType.DMA
    outs = (
        b(hidden, part_cols),
        b(part_cols, hidden),
        b(2 * width, part_cols),
        b(part_cols, 6 * width),
        f(rows, model),
        f(rows, model),
        f(*small_shape),
        b(2, 2 * line, blk, 2 * width),
        b(2, 2 * line, blk, 2 * width),
        b(line + 1, *shares[0]),
        b(line + 1, *shares[1]),
        b(line + 1, *shares[2]),
        b(line + 1, *shares[3]),
        b(2, rows, half),
        b(3, blk, model),
        b(2 * rows, model),
        b(2 * rows, hidden_half),
    )
    wide = max(model, hidden)
    scratch = (
        [vf(rows, model)] * 2
        + [vb(2, rows, half)] * 5
        + [vb(2, rows, hidden_half)] * 2
        + [vb(rows, hidden_half)] * 2
        + [vb(2, wide, TILE), vb(2, max(TILE, 2 * width), wide)]
        + [vb(line, *s) for s in shares]
        + [vb(*s) for s in shares]
        + [vb(3, 2, blk, model), vb(3, tp_steps + 1, blk, model)]
        + [vb(2, 2, blk, 2 * width)] * 2
        + [vb(2, blk, 2 * width)] * 2
        + [
            vb(2, 2, blk, 2 * width),
            vb(2, 2, blk, width),
            vb(2, blk, width),
            vf(2, own_heads, 2, pair),
            vf(line, 2, own_heads, 2, pair),
            vb(2, 2, blk, 3 * width),
            vb(2, blk, 3 * width),
            vf(pair, HD),
            vf(pair, HD),
            vf(pair, 1),
            vf(pair, 1),
            vf(2, 2, blk, LANES),
            vf(2, 2, blk, LANES),
            vf(*small_shape),
            vf(*small_shape),
            vb(*small_shape),
            vb(line, *small_shape),
            dma((2, 2, 2, line)),
            dma((2, 2, line)),
            dma((Y_FIN + 4,)),
            dma((Y_FIN + 4,)),
            dma((3,)),
            dma((3,)),
            dma((3, n_tp // 2)),
            dma((3, n_tp // 2)),
            dma((4, 2, line)),
            dma((4, 2, line + 1)),
            dma((3, tp_steps + 2)),
            dma((3, tp_steps + 2)),
            dma((line,)),
            dma((line,)),
            dma((line,)),
            dma((line,)),
            dma((7,)),
            dma((7,)),
            dma((2, n_tp // 2)),
            dma((2, n_tp // 2)),
            dma((9,)),
            dma((2, 2)),
            dma((2,)),
            dma((4,)),
        ]
    )
    blocks = order.shape[0]
    operands = (
        order,
        stream_in,
        cotangent,
        w_up,
        w_down,
        w_out,
        w_qkv,
        ln_gain,
        ln_bias,
        b_qkv,
        b_up.reshape(1, -1),
        out_bias.reshape(1, -1),
        jnp.asarray(rope_tables(np.arange(blocks) * blk)),
        jnp.asarray(rope_tables(np.arange(blk))),
    )
    return pl.pallas_call(
        functools.partial(layer_kernel, line, n_tp),
        name="layer",
        out_shape=outs,
        in_specs=[SMEM] + [ANY] * 6 + [VMEM] * 7,
        out_specs=[ANY] * len(outs),
        scratch_shapes=scratch,
        cost_estimate=pl.CostEstimate(
            flops=40 * rows * model * hidden,
            transcendentals=rows * hidden,
            bytes_accessed=8 * w_up.size,
        ),
        compiler_params=pltpu.CompilerParams(
            collective_id=0, has_side_effects=True, vmem_limit_bytes=67043328
        ),
    )(*operands)


def results_kernel(
    down,
    up,
    out,
    qkv,
    stream,
    grad,
    small,
    stream_o,
    grad_o,
    qkv_o,
    bqkv_o,
    out_o,
    obias_o,
    up_o,
    bup_o,
    down_o,
    gain_o,
    shift_o,
):
    stream_o[...] = stream[...]
    grad_o[...] = grad[...]
    for src, dst in ((qkv, qkv_o), (out, out_o), (up, up_o), (down, down_o)):
        dst[...] = src[...].astype(F32)

    @pl.when(pl.program_id(0) == 0)
    def _():
        bqkv_o[...] = small[S_QKV, : bqkv_o.shape[0]]
        obias_o[...] = small[S_OUT, : obias_o.shape[0]]
        bup_o[...] = small[S_UP, : bup_o.shape[0]]
        gain_o[...] = small[S_GAIN : S_GAIN + 2, : gain_o.shape[1]]
        shift_o[...] = small[S_SHIFT : S_SHIFT + 2, : shift_o.shape[1]]


def results(down, up, out, qkv, stream_out, grad_in, small, model, fused, hidden):
    steps = 2
    f = lambda *s: jax.ShapeDtypeStruct(s, F32)
    rows_of = lambda a: pl.BlockSpec((a.shape[0] // steps,) + a.shape[1:], lambda i: (i, 0))
    whole = lambda a: pl.BlockSpec(a.shape, lambda i: (0,) * len(a.shape))
    large = (down, up, out, qkv, stream_out, grad_in)
    while any(a.shape[0] % (16 * steps) for a in large[:4]):
        steps //= 2
    outs = (
        (f(*stream_out.shape), True),
        (f(*grad_in.shape), True),
        (f(*qkv.shape), True),
        (f(fused), False),
        (f(*out.shape), True),
        (f(model), False),
        (f(*up.shape), True),
        (f(hidden), False),
        (f(*down.shape), True),
        (f(2, model), False),
        (f(2, model), False),
    )
    return pl.pallas_call(
        results_kernel,
        name="results",
        grid=(steps,),
        out_shape=[o for o, _ in outs],
        in_specs=[rows_of(a) for a in large] + [whole(small)],
        out_specs=[rows_of(o) if tall else whole(o) for o, tall in outs],
        cost_estimate=pl.CostEstimate(
            flops=down.size, transcendentals=0, bytes_accessed=8 * down.size + 16 * stream_out.size
        ),
        compiler_params=pltpu.CompilerParams(vmem_limit_bytes=67043328),
    )(*large, small)


def shards(
    n_ctx,
    n_tp,
    stream_in,
    cotangent,
    ln_gain,
    ln_bias,
    w_qkv,
    b_qkv,
    w_out,
    out_bias,
    w_up,
    b_up,
    w_down,
    block_order,
):
    (down, up, out, qkv, stream_out, grad_in, small, *_) = layer(
        n_ctx // 2,
        n_tp,
        block_order,
        stream_in,
        cotangent,
        ln_gain,
        ln_bias,
        w_qkv,
        b_qkv,
        w_out,
        out_bias,
        w_up,
        b_up,
        w_down,
    )
    return results(down, up, out, qkv, stream_out, grad_in, small, *w_qkv.shape, w_up.shape[1])


def solution(mesh):
    placed = (
        P("ctx", None),
        P("ctx", None),
        P(),
        P(),
        P(None, "tp"),
        P("tp"),
        P("tp", None),
        P(),
        P(None, "tp"),
        P("tp"),
        P("tp", None),
        P(),
    )
    return jax.shard_map(
        functools.partial(shards, mesh.shape["ctx"], mesh.shape["tp"]),
        mesh=mesh,
        in_specs=placed,
        out_specs=(
            P("ctx", None),
            P("ctx", None),
            P("ctx", "tp"),
            P("tp"),
            P("tp", "ctx"),
            P(),
            P("ctx", "tp"),
            P("tp"),
            P("tp", "ctx"),
            P(),
            P(),
        ),
        check_vma=False,
    )
```
